16 devices in a mesh: model: 2 (over z), data: 2 (over y), stage: 4 (over x, core).
Axes of the slice: x: 2, y: 2, z: 2, core: 2. Of those that a mesh axis runs over, the one named last changes fastest.
Arguments:
- w_up: float32 [4, 768, 3072], P('stage', None, 'model')
- w_down: float32 [4, 3072, 768], P('stage', 'model')
- m_up: float32 [4, 768, 3072], P('stage', None, 'model')
- m_down: float32 [4, 3072, 768], P('stage', 'model')
- v_up: float32 [4, 768, 3072], P('stage', None, 'model')
- v_down: float32 [4, 3072, 768], P('stage', 'model')
- g_up: float32 [2, 4, 768, 3072], P('data', 'stage', None, 'model')
- g_down: float32 [2, 4, 3072, 768], P('data', 'stage', 'model')
- acts_last: bfloat16 [4, 1024, 768], P('stage', 'data')
- grad_out: bfloat16 [1024, 768], P('data')
- x_next: bfloat16 [3, 1024, 768], P(None, 'data')
- learn_rate: float32 [1], replicated
- max_norm: float32 [1], replicated
Outputs:
- output 1: float32 [4, 768, 3072], P('stage', None, 'model')
- output 2: float32 [4, 3072, 768], P('stage', 'model')
- output 3: float32 [4, 768, 3072], P('stage', None, 'model')
- output 4: float32 [4, 3072, 768], P('stage', 'model')
- output 5: float32 [4, 768, 3072], P('stage', None, 'model')
- output 6: float32 [4, 3072, 768], P('stage', 'model')
- output 7: bfloat16 [3, 1024, 768], P(None, 'data')
All inputs are finite; a program needn't handle non-finite values.
Results may differ from the reference program's by a relative error of at most 0.00893322.
Values are sent between devices in bfloat16 or wider.
A program may use at most 1 GiB of HBM per device.

```python
import jax
import jax.numpy as jnp
from jax import lax

STAGES = 4
REPLICAS = 2
D_MODEL = 768
FF_WIDTH = 3072
MICRO_ROWS = 512
NEXT_MICRO = 3
ADAM_STEP = 10
BETA_ONE = 0.9
BETA_TWO = 0.95
ADAM_EPS = 1e-8
WEIGHT_DECAY = 0.1
NORM_EPS = 1e-6
ALL_ROWS = REPLICAS * MICRO_ROWS


def gelu_vjp(pre_act, upstream):
    pull_back = jax.vjp(jax.nn.gelu, pre_act)[1]
    return pull_back(upstream)[0]


def stage_apply(acts_in, up_bf, down_bf):
    pre_act = jnp.dot(acts_in, up_bf, preferred_element_type=jnp.float32)
    hidden = jax.nn.gelu(pre_act).astype(jnp.bfloat16)
    branch = jnp.dot(hidden, down_bf, preferred_element_type=jnp.float32)
    return (acts_in.astype(jnp.float32) + branch).astype(jnp.bfloat16)


def averaged_grads(w_up, w_down, g_up, g_down, acts_last, grad_out):
    def back_step(upstream, layer_in):
        up_bf, down_bf, acts_in = layer_in
        pre_act = jnp.dot(acts_in, up_bf, preferred_element_type=jnp.float32)
        hidden = jax.nn.gelu(pre_act).astype(jnp.bfloat16)
        grad_down = jnp.dot(hidden.T, upstream, preferred_element_type=jnp.float32)
        grad_hid = jnp.dot(upstream, down_bf.T, preferred_element_type=jnp.float32)
        grad_pre = gelu_vjp(pre_act, grad_hid).astype(jnp.bfloat16)
        grad_up = jnp.dot(acts_in.T, grad_pre, preferred_element_type=jnp.float32)
        back_in = jnp.dot(grad_pre, up_bf.T, preferred_element_type=jnp.float32)
        grad_in = (upstream.astype(jnp.float32) + back_in).astype(jnp.bfloat16)
        return grad_in, (grad_up, grad_down)
    layer_all = (w_up.astype(jnp.bfloat16), w_down.astype(jnp.bfloat16), acts_last)
    grad_pair = lax.scan(back_step, grad_out, layer_all, reverse=True)[1]
    mean_up = (jnp.sum(g_up, axis=0) + grad_pair[0]) / REPLICAS
    mean_down = (jnp.sum(g_down, axis=0) + grad_pair[1]) / REPLICAS
    return mean_up, mean_down


def adamw_update(weight, moment_one, moment_two, grad_step, step_rate):
    mom_new = BETA_ONE * moment_one + (1.0 - BETA_ONE) * grad_step
    sec_new = BETA_TWO * moment_two + (1.0 - BETA_TWO) * grad_step * grad_step
    one_corr = 1.0 - BETA_ONE ** ADAM_STEP
    two_corr = 1.0 - BETA_TWO ** ADAM_STEP
    direction = (mom_new / one_corr) / (jnp.sqrt(sec_new / two_corr) + ADAM_EPS)
    weight_new = weight - step_rate * (direction + WEIGHT_DECAY * weight)
    return weight_new, mom_new, sec_new


def forward_all(up_bf, down_bf, x_next):
    def one_micro(acts_in):
        def fwd_step(acts_carry, layer_in):
            return stage_apply(acts_carry, layer_in[0], layer_in[1]), None
        return lax.scan(fwd_step, acts_in, (up_bf, down_bf))[0]
    return lax.map(one_micro, x_next)


def setup_inputs(seed: int = 0) -> dict:
    key_list = jax.random.split(jax.random.key(seed), 13)
    up_scale = D_MODEL ** -0.5
    down_scale = FF_WIDTH ** -0.5
    grad_scale = MICRO_ROWS ** 0.5
    w_up = jax.random.normal(key_list[0], (STAGES, D_MODEL, FF_WIDTH), jnp.float32) * up_scale
    w_down = jax.random.normal(key_list[1], (STAGES, FF_WIDTH, D_MODEL), jnp.float32) * down_scale
    g_up = jax.random.normal(key_list[2], (REPLICAS, STAGES, D_MODEL, FF_WIDTH), jnp.float32) * (0.3 * grad_scale)
    g_down = jax.random.normal(key_list[3], (REPLICAS, STAGES, FF_WIDTH, D_MODEL), jnp.float32) * (0.5 * grad_scale)
    acts_last = jax.random.normal(key_list[4], (STAGES, ALL_ROWS, D_MODEL), jnp.float32).astype(jnp.bfloat16)
    grad_out = jax.random.normal(key_list[5], (ALL_ROWS, D_MODEL), jnp.float32).astype(jnp.bfloat16)
    x_next = jax.random.normal(key_list[6], (NEXT_MICRO, ALL_ROWS, D_MODEL), jnp.float32).astype(jnp.bfloat16)
    learn_rate = jax.random.uniform(key_list[7], (1,), jnp.float32, 0.1, 0.25) * up_scale
    mean_up, mean_down = averaged_grads(w_up, w_down, g_up, g_down, acts_last, grad_out)
    grad_norm = jnp.sqrt(jnp.sum(mean_up * mean_up) + jnp.sum(mean_down * mean_down))
    clip_frac = jax.random.uniform(key_list[8], (1,), jnp.float32, 0.35, 0.65)
    max_norm = clip_frac * grad_norm
    up_rms = clip_frac[0] * jnp.sqrt(jnp.mean(mean_up * mean_up))
    down_rms = clip_frac[0] * jnp.sqrt(jnp.mean(mean_down * mean_down))
    m_up = jax.random.normal(key_list[9], w_up.shape, jnp.float32) * (0.1 * up_rms)
    m_down = jax.random.normal(key_list[10], w_down.shape, jnp.float32) * (0.1 * down_rms)
    v_up = (0.5 + jax.random.uniform(key_list[11], w_up.shape, jnp.float32)) * (0.02 * up_rms * up_rms)
    v_down = (0.5 + jax.random.uniform(key_list[12], w_down.shape, jnp.float32)) * (0.02 * down_rms * down_rms)
    return {'w_up': w_up, 'w_down': w_down, 'm_up': m_up, 'm_down': m_down, 'v_up': v_up, 'v_down': v_down, 'g_up': g_up, 'g_down': g_down, 'acts_last': acts_last, 'grad_out': grad_out, 'x_next': x_next, 'learn_rate': learn_rate, 'max_norm': max_norm}


def reference(w_up, w_down, m_up, m_down, v_up, v_down, g_up, g_down, acts_last, grad_out, x_next, learn_rate, max_norm):
    mean_up, mean_down = averaged_grads(w_up, w_down, g_up, g_down, acts_last, grad_out)
    norm_sq = jnp.sum(mean_up * mean_up) + jnp.sum(mean_down * mean_down)
    clip_scale = jnp.minimum(1.0, max_norm[0] / (jnp.sqrt(norm_sq) + NORM_EPS))
    up_new, up_mom, up_sec = adamw_update(w_up, m_up, v_up, clip_scale * mean_up, learn_rate[0])
    down_new, down_mom, down_sec = adamw_update(w_down, m_down, v_down, clip_scale * mean_down, learn_rate[0])
    y_next = forward_all(up_new.astype(jnp.bfloat16), down_new.astype(jnp.bfloat16), x_next)
    return (up_new, down_new, up_mom, down_mom, up_sec, down_sec, y_next)
```

```python
import functools

import jax
import jax.numpy as jnp
from jax import lax
from jax.experimental import pallas as pl
from jax.experimental.pallas import tpu as pltpu
from jax.sharding import PartitionSpec as P

ADAM_STEP = 10
BETA_ONE = 0.9
BETA_TWO = 0.95
ADAM_EPS = 1e-8
WEIGHT_DECAY = 0.1
NORM_EPS = 1e-6
ONE_CORR = 1.0 - BETA_ONE ** ADAM_STEP
TWO_CORR = 1.0 - BETA_TWO ** ADAM_STEP
GELU_SCALE = (2.0 / 3.141592653589793) ** 0.5
GELU_CUBE = 0.044715
NN = (((1,), (0,)), ((), ()))
NT = (((1,), (1,)), ((), ()))
TN = (((0,), (0,)), ((), ()))
F32 = jnp.float32
BF16 = jnp.bfloat16
MESH = pl.DeviceIdType.MESH
BACK_ROWS = 128
FWD_ROWS = 128
VMEM_LIMIT = 66_000_000


def mm(lhs, rhs, dims):
    return lax.dot_general(lhs, rhs, dims, preferred_element_type=F32)


def gelu_val(pre):
    return pre * (0.5 * (1.0 + jnp.tanh(GELU_SCALE * (pre + GELU_CUBE * (pre * pre * pre)))))


def gelu_both(pre):
    sq = pre * pre
    tan = jnp.tanh(GELU_SCALE * (pre + GELU_CUBE * (sq * pre)))
    cdf = 0.5 * (1.0 + tan)
    slope = cdf + 0.5 * pre * (1.0 - tan * tan) * (GELU_SCALE * (1.0 + (3.0 * GELU_CUBE) * sq))
    return pre * cdf, slope


def adamw_update(weight, moment_one, moment_two, grad_step, step_rate):
    mom_new = BETA_ONE * moment_one + (1.0 - BETA_ONE) * grad_step
    sec_new = BETA_TWO * moment_two + (1.0 - BETA_TWO) * grad_step * grad_step
    direction = (mom_new / ONE_CORR) / (jnp.sqrt(sec_new / TWO_CORR) + ADAM_EPS)
    weight_new = weight - step_rate * (direction + WEIGHT_DECAY * weight)
    return weight_new, mom_new, sec_new


def clip_of(norm_tile, max_norm):
    total = jnp.sum(jnp.sum(norm_tile, axis=0, keepdims=True), axis=1, keepdims=True)
    return jnp.minimum(1.0, max_norm / (jnp.sqrt(total) + NORM_EPS))


def whole_barrier(n_model, n_data, n_stage):
    barrier = pltpu.get_barrier_semaphore()
    me = (lax.axis_index('model'), lax.axis_index('data'), lax.axis_index('stage'))
    for dm in range(n_model):
        for dd in range(n_data):
            for ds in range(n_stage):
                if dm or dd or ds:
                    peer = (lax.rem(me[0] + dm, n_model), lax.rem(me[1] + dd, n_data), lax.rem(me[2] + ds, n_stage))
                    pl.semaphore_signal(barrier, inc=1, device_id=peer, device_id_type=MESH)
    pl.semaphore_wait(barrier, n_model * n_data * n_stage - 1)


def remote(src, dst, send_sem, recv_sem, device):
    return pltpu.make_async_remote_copy(src_ref=src, dst_ref=dst, send_sem=send_sem, recv_sem=recv_sem, device_id=device, device_id_type=MESH)


def bwd_kernel(dims, wu_hbm, wd_hbm, acts_hbm, dy_hbm, gu_hbm, gd_hbm,
               gbu_hbm, gbd_hbm, norm_out,
               wu32, wd32, wu_bf, wd_bf, aa, gg, hh, dzz, slope, slope_o, dz_own, h_own,
               gu_own, gd_own, gu_rcv, gd_rcv, part, part_rcv, fin, norm_buf,
               ld_sem, ysend, yrecv, psend, precv, fsend, frecv, nsend, nrecv, st_sem):
    n_model, n_data, n_stage = dims
    z, d, p = lax.axis_index('model'), lax.axis_index('data'), lax.axis_index('stage')
    zo, do = 1 - z, 1 - d
    ypeer, zpeer = (z, do, p), (zo, d, p)
    last = n_stage - 1
    rows = aa.shape[0] // 2
    width = aa.shape[1]
    half = hh.shape[1]
    rb = BACK_ROWS
    hb = rb // 2
    nb = rows // rb
    own_ff = pl.ds(pl.multiple_of(d * half, 128), half)
    oth_ff = pl.ds(pl.multiple_of(do * half, 128), half)
    mine, theirs = pl.ds(0, rows), pl.ds(rows, rows)

    loads = [
        pltpu.make_async_copy(wu_hbm, wu32, ld_sem.at[0]),
        pltpu.make_async_copy(acts_hbm, aa.at[mine], ld_sem.at[2]),
        pltpu.make_async_copy(wd_hbm, wd32, ld_sem.at[1]),
        pltpu.make_async_copy(gu_hbm.at[:, own_ff], gu_own, ld_sem.at[4]),
        pltpu.make_async_copy(gd_hbm.at[own_ff, :], gd_own, ld_sem.at[5]),
    ]
    for copy in loads:
        copy.start()
    dy_load = pltpu.make_async_copy(dy_hbm, gg.at[mine], ld_sem.at[3])

    @pl.when(p == last)
    def _():
        dy_load.start()

    whole_barrier(n_model, n_data, n_stage)
    send_acts = remote(acts_hbm, aa.at[theirs], ysend.at[0], yrecv.at[0], ypeer)
    send_gu = remote(gu_hbm.at[:, oth_ff], gu_rcv, ysend.at[1], yrecv.at[1], ypeer)
    send_gd = remote(gd_hbm.at[oth_ff, :], gd_rcv, ysend.at[2], yrecv.at[2], ypeer)
    send_g = remote(gg.at[mine], gg.at[theirs], ysend.at[3], yrecv.at[3], ypeer)
    send_acts.start()
    send_gu.start()

    loads[0].wait()
    loads[1].wait()

    def cast_up(i, carry):
        at = pl.ds(pl.multiple_of(i * 128, 128), 128)
        wu_bf[at, :] = wu32[at, :].astype(BF16)
        return carry
    lax.fori_loop(0, width // 128, cast_up, 0)

    def own_pre(i, carry):
        at = pl.ds(pl.multiple_of(i * rb, rb), rb)
        val, slp = gelu_both(mm(aa[at, :], wu_bf[...], NN))
        h_own[at, :] = val.astype(BF16)
        slope[at, :] = slp
        return carry
    lax.fori_loop(0, nb, own_pre, 0)
    loads[2].wait()

    def cast_down(i, carry):
        at = pl.ds(pl.multiple_of(i * 128, 128), 128)
        wd_bf[at, :] = wd32[at, :].astype(BF16)
        return carry
    lax.fori_loop(0, 2 * half // 128, cast_down, 0)

    @pl.when(p == last)
    def _():
        dy_load.wait()

    def g_at(c, zi):
        return gg.at[pl.ds(pl.multiple_of(c * rb + zi * hb, hb), hb)]

    def part_copy(c):
        return remote(part.at[c, pl.ds(pl.multiple_of(zo * hb, hb), hb)], part_rcv.at[c], psend.at[c], precv.at[c], zpeer)

    def fin_copy(c, zi):
        return remote(fin.at[c], g_at(c, z), fsend.at[c, zi], frecv.at[c, z], (zi, d, lax.max(p - 1, 0)))

    def compute(c):
        @pl.when(p < last)
        def _():
            for zi in range(n_model):
                pltpu.make_async_copy(fin.at[c], g_at(c, zi), frecv.at[c, zi]).wait()
        at = pl.ds(pl.multiple_of(c * rb, rb), rb)
        grad_hid = mm(gg[at, :], wd_bf[...], NT)
        dz_own[at, :] = (slope[at, :] * grad_hid).astype(BF16)

        @pl.when(p > 0)
        def _():
            part[c] = mm(dz_own[at, :], wu_bf[...], NT)
            part_copy(c).start()

    def finalize(c):
        part_copy(c).wait_recv()
        at = pl.ds(pl.multiple_of(c * rb + z * hb, hb), hb)
        total = part[c, pl.ds(pl.multiple_of(z * hb, hb), hb), :] + part_rcv[c]
        fin[c] = (gg[at, :].astype(F32) + total).astype(BF16)
        for zi in range(n_model):
            fin_copy(c, zi).start()

    lag = jnp.where(p == last, 1, 0)

    def chain(i, carry):
        @pl.when(i < nb)
        def _():
            compute(i)
        f = i - lag

        @pl.when((f >= 0) & (f < nb) & (p > 0))
        def _():
            finalize(f)
        return carry
    lax.fori_loop(0, nb + 1, chain, 0)

    send_g.start()
    send_gd.start()

    hh[mine, :] = h_own[:, own_ff]
    dzz[mine, :] = dz_own[:, own_ff]
    send_acts.wait_recv()

    def oth_pre(i, carry):
        at = pl.ds(pl.multiple_of(rows + i * rb, rb), rb)
        val, slp = gelu_both(mm(aa[at, :], wu_bf[:, own_ff], NN))
        hh[at, :] = val.astype(BF16)
        slope_o[pl.ds(pl.multiple_of(i * rb, rb), rb), :] = slp
        return carry
    lax.fori_loop(0, nb, oth_pre, 0)
    send_g.wait_recv()

    def oth_dz(i, carry):
        at = pl.ds(pl.multiple_of(rows + i * rb, rb), rb)
        grad_hid = mm(gg[at, :], wd_bf[own_ff, :], NT)
        dzz[at, :] = (slope_o[pl.ds(pl.multiple_of(i * rb, rb), rb), :] * grad_hid).astype(BF16)
        return carry
    lax.fori_loop(0, nb, oth_dz, 0)
    loads[3].wait()
    loads[4].wait()

    def weight_grads(j, carry):
        at = pl.ds(pl.multiple_of(j * 128, 128), 128)
        gd_own[at, :] += mm(hh[:, at], gg[...], TN)
        gu_own[at, :] += mm(aa[:, at], dzz[...], TN)
        return carry
    lax.fori_loop(0, half // 128, weight_grads, 0)

    def combine(own, rcv):
        def body(i, acc):
            at = pl.ds(pl.multiple_of(i * 32, 32), 32)
            mean = (own[at, :] + rcv[at, :]) * 0.5
            own[at, :] = mean
            return acc + jnp.sum((mean * mean).reshape(4, 8, mean.shape[1]), axis=0)
        return body
    acc = jnp.zeros((8, half), F32)
    send_gu.wait_recv()
    acc = lax.fori_loop(0, gu_own.shape[0] // 32, combine(gu_own, gu_rcv), acc)
    store_u = pltpu.make_async_copy(gu_own, gbu_hbm, st_sem.at[0])
    store_u.start()
    send_gd.wait_recv()
    acc = lax.fori_loop(0, gd_own.shape[0] // 32, combine(gd_own, gd_rcv), acc)
    store_d = pltpu.make_async_copy(gd_own, gbd_hbm, st_sem.at[1])
    store_d.start()
    tile = acc[:, 0:128]
    for k in range(1, half // 128):
        tile = tile + acc[:, k * 128:(k + 1) * 128]
    n_all = n_model * n_data * n_stage
    my_id = (z * n_data + d) * n_stage + p
    norm_buf[my_id] = tile

    def norm_copy(k):
        peer = lax.rem(my_id + k, n_all)
        device = (peer // (n_data * n_stage), lax.rem(peer // n_stage, n_data), lax.rem(peer, n_stage))
        return remote(norm_buf.at[my_id], norm_buf.at[my_id], nsend.at[k], nrecv.at[my_id], device)
    for k in range(1, n_all):
        norm_copy(k).start()
    for k in range(1, n_all):
        peer = lax.rem(my_id + k, n_all)
        pltpu.make_async_copy(norm_buf.at[peer], norm_buf.at[peer], nrecv.at[peer]).wait()
    total = norm_buf[0]
    for k in range(1, n_all):
        total = total + norm_buf[k]
    norm_out[...] = total

    for k in range(1, n_all):
        norm_copy(k).wait_send()
    for copy in (send_acts, send_gu, send_gd, send_g):
        copy.wait_send()

    @pl.when(p > 0)
    def _():
        for c in range(nb):
            part_copy(c).wait_send()
            for zi in range(n_model):
                fin_copy(c, zi).wait_send()
    store_u.wait()
    store_d.wait()


def fwd_kernel(dims, norm_ref, lr_ref, mn_ref, wu_hbm, wd_hbm, mu_hbm, md_hbm, vu_hbm, vd_hbm, gbu_hbm, gbd_hbm, x_hbm,
               gu_full, gd_full, y_hbm,
               wu32, wd32, mu32, md32, vu32, vd32, gu32, gd32, wu_bf, wd_bf, a_buf, y_buf, part, part_rcv, fin,
               ld_sem, ysend, yrecv, psend, precv, fsend, frecv, agsend, agrecv, outsend, outrecv, st_sem):
    n_model, n_data, n_stage = dims
    z, d, p = lax.axis_index('model'), lax.axis_index('data'), lax.axis_index('stage')
    zo, do = 1 - z, 1 - d
    ypeer, zpeer = (z, do, p), (zo, d, p)
    last = n_stage - 1
    half = wu32.shape[1]
    nc, rb, width = a_buf.shape
    hb = rb // 2
    own_ff = pl.ds(pl.multiple_of(d * half, 128), half)

    loads = [
        pltpu.make_async_copy(gbu_hbm, gu32, ld_sem.at[0]),
        pltpu.make_async_copy(wu_hbm.at[:, own_ff], wu32, ld_sem.at[1]),
        pltpu.make_async_copy(mu_hbm.at[:, own_ff], mu32, ld_sem.at[2]),
        pltpu.make_async_copy(vu_hbm.at[:, own_ff], vu32, ld_sem.at[3]),
        pltpu.make_async_copy(gbd_hbm, gd32, ld_sem.at[4]),
        pltpu.make_async_copy(wd_hbm.at[own_ff, :], wd32, ld_sem.at[5]),
        pltpu.make_async_copy(md_hbm.at[own_ff, :], md32, ld_sem.at[6]),
        pltpu.make_async_copy(vd_hbm.at[own_ff, :], vd32, ld_sem.at[7]),
    ]
    for copy in loads:
        copy.start()
    x_load = pltpu.make_async_copy(x_hbm, a_buf, ld_sem.at[8])

    @pl.when(p == 0)
    def _():
        x_load.start()
    whole_barrier(n_model, n_data, n_stage)

    clip = clip_of(norm_ref[...], mn_ref[0])
    rate = lr_ref[0]
    for copy in loads[:4]:
        copy.wait()

    def update_up(i, carry):
        at = pl.ds(pl.multiple_of(i * 32, 32), 32)
        new = adamw_update(wu32[at, :], mu32[at, :], vu32[at, :], clip * gu32[at, :], rate)[0]
        wu_bf[at, own_ff] = new.astype(BF16)
        return carry
    lax.fori_loop(0, width // 32, update_up, 0)
    send_wu = remote(wu_bf.at[:, own_ff], wu_bf.at[:, own_ff], ysend.at[0], yrecv.at[0], ypeer)
    send_wd = remote(wd_bf.at[own_ff, :], wd_bf.at[own_ff, :], ysend.at[1], yrecv.at[1], ypeer)
    send_gu = remote(gu32, gu_full.at[:, own_ff], ysend.at[2], yrecv.at[2], ypeer)
    send_gd = remote(gd32, gd_full.at[own_ff, :], ysend.at[3], yrecv.at[3], ypeer)
    for copy in loads[4:]:
        copy.wait()
    send_wu.start()

    def update_down(i, carry):
        at = pl.ds(pl.multiple_of(i * 32, 32), 32)
        new = adamw_update(wd32[at, :], md32[at, :], vd32[at, :], clip * gd32[at, :], rate)[0]
        wd_bf[pl.ds(pl.multiple_of(d * half + i * 32, 32), 32), :] = new.astype(BF16)
        return carry
    lax.fori_loop(0, half // 32, update_down, 0)
    store_u = pltpu.make_async_copy(gu32, gu_full.at[:, own_ff], st_sem.at[0])
    store_d = pltpu.make_async_copy(gd32, gd_full.at[own_ff, :], st_sem.at[1])
    store_u.start()
    store_d.start()
    send_wd.start()
    send_gu.start()
    send_gd.start()

    @pl.when(p == 0)
    def _():
        x_load.wait()
    send_wu.wait_recv()
    send_wd.wait_recv()

    def half_rows(zi):
        return pl.ds(pl.multiple_of(zi * hb, hb), hb)

    def part_copy(c):
        return remote(part.at[c, half_rows(zo)], part_rcv.at[c], psend.at[c], precv.at[c], zpeer)

    def fin_copy(c, zi):
        return remote(fin.at[c], a_buf.at[c, half_rows(z)], fsend.at[c, zi], frecv.at[c, z], (zi, d, lax.min(p + 1, last)))

    def gather_copy(c):
        return remote(fin.at[c], y_buf.at[c, half_rows(z)], agsend.at[c], agrecv.at[c], zpeer)

    def out_copy(c, q):
        return remote(y_buf.at[c], y_hbm.at[c], outsend.at[c, q], outrecv.at[c], (z, d, q))

    def out_local(c):
        return pltpu.make_async_copy(y_buf.at[c], y_hbm.at[c], outsend.at[c, last])

    def compute(c):
        @pl.when(p > 0)
        def _():
            for zi in range(n_model):
                pltpu.make_async_copy(fin.at[c], a_buf.at[c, half_rows(zi)], frecv.at[c, zi]).wait()
        hid = gelu_val(mm(a_buf[c], wu_bf[...], NN)).astype(BF16)
        part[c] = mm(hid, wd_bf[...], NN)
        part_copy(c).start()

    def finalize(c):
        part_copy(c).wait_recv()
        total = part[c, half_rows(z), :] + part_rcv[c]
        new = (a_buf[c, half_rows(z), :].astype(F32) + total).astype(BF16)
        fin[c] = new

        @pl.when(p < last)
        def _():
            for zi in range(n_model):
                fin_copy(c, zi).start()

        @pl.when(p == last)
        def _():
            y_buf[c, half_rows(z), :] = new
            gather_copy(c).start()

    def publish(c):
        gather_copy(c).wait_recv()
        out_local(c).start()
        for q in range(last):
            out_copy(c, q).start()

    lag = jnp.where(p == 0, 1, 0)

    def chain(i, carry):
        @pl.when(i < nc)
        def _():
            compute(i)
        f = i - lag

        @pl.when((f >= 0) & (f < nc))
        def _():
            finalize(f)

        @pl.when((i >= 1) & (p == last))
        def _():
            publish(i - 1)
        return carry
    lax.fori_loop(0, nc + 1, chain, 0)

    def drain(c, carry):
        part_copy(c).wait_send()

        @pl.when(p < last)
        def _():
            for zi in range(n_model):
                fin_copy(c, zi).wait_send()
            pltpu.make_async_copy(y_buf.at[c], y_hbm.at[c], outrecv.at[c]).wait()

        @pl.when(p == last)
        def _():
            gather_copy(c).wait_send()
            out_local(c).wait()
            for q in range(last):
                out_copy(c, q).wait_send()
        return carry
    lax.fori_loop(0, nc, drain, 0)
    send_wu.wait_send()
    send_wd.wait_send()
    store_u.wait()
    store_d.wait()
    send_gu.wait()
    send_gd.wait()


def solution(mesh):
    n_model, n_data, n_stage = (mesh.shape[k] for k in ('model', 'data', 'stage'))
    dims = (n_model, n_data, n_stage)
    n_all = n_model * n_data * n_stage
    up_spec = P('stage', None, 'model')
    down_spec = P('stage', 'model', None)
    row_spec = P(None, 'data', None)
    in_specs = (up_spec, down_spec, up_spec, down_spec, up_spec, down_spec, P('data', 'stage', None, 'model'), P('data', 'stage', 'model', None), P('stage', 'data', None), P('data', None), row_spec, P(None), P(None))
    out_specs = (up_spec, down_spec, up_spec, down_spec, up_spec, down_spec, row_spec)
    any_spec = pl.BlockSpec(memory_space=pl.ANY)
    vmem_spec = pl.BlockSpec(memory_space=pltpu.VMEM)
    smem_spec = pl.BlockSpec(memory_space=pltpu.SMEM)
    dma = pltpu.SemaphoreType.DMA

    def device_step(w_up, w_down, m_up, m_down, v_up, v_down, g_up, g_down, acts_last, grad_out, x_next, learn_rate, max_norm):
        rows, width = grad_out.shape
        ff = w_up.shape[2]
        half = ff // 2
        nb = rows // BACK_ROWS
        hb = BACK_ROWS // 2
        sds = jax.ShapeDtypeStruct
        gbar_u, gbar_d, norm_tile = pl.pallas_call(
            functools.partial(bwd_kernel, dims),
            out_shape=(sds((width, half), F32), sds((half, width), F32), sds((8, 128), F32)),
            in_specs=[any_spec] * 6,
            out_specs=(any_spec, any_spec, vmem_spec),
            scratch_shapes=[
                pltpu.VMEM((width, ff), F32), pltpu.VMEM((ff, width), F32),
                pltpu.VMEM((width, ff), BF16), pltpu.VMEM((ff, width), BF16),
                pltpu.VMEM((2 * rows, width), BF16), pltpu.VMEM((2 * rows, width), BF16),
                pltpu.VMEM((2 * rows, half), BF16), pltpu.VMEM((2 * rows, half), BF16),
                pltpu.VMEM((rows, ff), F32), pltpu.VMEM((rows, half), F32),
                pltpu.VMEM((rows, ff), BF16), pltpu.VMEM((rows, ff), BF16),
                pltpu.VMEM((width, half), F32), pltpu.VMEM((half, width), F32),
                pltpu.VMEM((width, half), F32), pltpu.VMEM((half, width), F32),
                pltpu.VMEM((nb, BACK_ROWS, width), F32), pltpu.VMEM((nb, hb, width), F32),
                pltpu.VMEM((nb, hb, width), BF16), pltpu.VMEM((n_all, 8, 128), F32),
                dma((6,)), dma((4,)), dma((4,)), dma((nb,)), dma((nb,)), dma((nb, 2)), dma((nb, 2)),
                dma((n_all,)), dma((n_all,)), dma((2,)),
            ],
            compiler_params=pltpu.CompilerParams(collective_id=0, has_side_effects=True, vmem_limit_bytes=VMEM_LIMIT),
            name='backward',
        )(w_up[0], w_down[0], acts_last[0], grad_out, g_up[0, 0], g_down[0, 0])

        n_micro = x_next.shape[0]
        nc = n_micro * rows // FWD_ROWS
        fb = FWD_ROWS // 2
        gu_full, gd_full, y_next = pl.pallas_call(
            functools.partial(fwd_kernel, dims),
            out_shape=(sds((width, ff), F32), sds((ff, width), F32), sds((nc, FWD_ROWS, width), BF16)),
            in_specs=[vmem_spec, smem_spec, smem_spec] + [any_spec] * 9,
            out_specs=(any_spec, any_spec, any_spec),
            scratch_shapes=[pltpu.VMEM((width, half), F32), pltpu.VMEM((half, width), F32)] * 4 + [
                pltpu.VMEM((width, ff), BF16), pltpu.VMEM((ff, width), BF16),
                pltpu.VMEM((nc, FWD_ROWS, width), BF16), pltpu.VMEM((nc, FWD_ROWS, width), BF16),
                pltpu.VMEM((nc, FWD_ROWS, width), F32), pltpu.VMEM((nc, fb, width), F32),
                pltpu.VMEM((nc, fb, width), BF16),
                dma((9,)), dma((4,)), dma((4,)), dma((nc,)), dma((nc,)), dma((nc, 2)), dma((nc, 2)),
                dma((nc,)), dma((nc,)), dma((nc, n_stage)), dma((nc,)), dma((2,)),
            ],
            compiler_params=pltpu.CompilerParams(collective_id=1, has_side_effects=True, vmem_limit_bytes=VMEM_LIMIT),
            name='forward',
        )(norm_tile, learn_rate, max_norm, w_up[0], w_down[0], m_up[0], m_down[0], v_up[0], v_down[0], gbar_u, gbar_d, x_next.reshape(nc, FWD_ROWS, width))

        clip = clip_of(norm_tile, max_norm[0])
        rate = learn_rate[0]
        up_w, up_m, up_v = adamw_update(w_up[0], m_up[0], v_up[0], clip * gu_full, rate)
        down_w, down_m, down_v = adamw_update(w_down[0], m_down[0], v_down[0], clip * gd_full, rate)
        return (up_w[None], down_w[None], up_m[None], down_m[None], up_v[None], down_v[None], y_next.reshape(n_micro, rows, width))

    return jax.shard_map(device_step, mesh=mesh, in_specs=in_specs, out_specs=out_specs, check_vma=False)
```

```python
import functools

import jax
import jax.numpy as jnp
from jax import lax
from jax.experimental import pallas as pl
from jax.experimental.pallas import tpu as pltpu
from jax.sharding import PartitionSpec as P

ADAM_STEP = 10
BETA_ONE = 0.9
BETA_TWO = 0.95
ADAM_EPS = 1e-8
WEIGHT_DECAY = 0.1
NORM_EPS = 1e-6
ONE_CORR = 1.0 - BETA_ONE ** ADAM_STEP
TWO_CORR = 1.0 - BETA_TWO ** ADAM_STEP
GELU_SCALE = (2.0 / 3.141592653589793) ** 0.5
GELU_CUBE = 0.044715
NN = (((1,), (0,)), ((), ()))
NT = (((1,), (1,)), ((), ()))
TN = (((0,), (0,)), ((), ()))
F32 = jnp.float32
BF16 = jnp.bfloat16
MESH = pl.DeviceIdType.MESH
BACK_ROWS = 128
FWD_ROWS = 64
UPD_ROWS = 128
TURN_STEP = 8
VMEM_LIMIT = 66_000_000


def mm(lhs, rhs, dims):
    return lax.dot_general(lhs, rhs, dims, preferred_element_type=F32)


def gelu_val(pre):
    return pre * (0.5 * (1.0 + jnp.tanh(GELU_SCALE * (pre + GELU_CUBE * (pre * pre * pre)))))


def gelu_both(pre):
    sq = pre * pre
    tan = jnp.tanh(GELU_SCALE * (pre + GELU_CUBE * (sq * pre)))
    cdf = 0.5 * (1.0 + tan)
    slope = cdf + 0.5 * pre * (1.0 - tan * tan) * (GELU_SCALE * (1.0 + (3.0 * GELU_CUBE) * sq))
    return pre * cdf, slope


def adamw_update(weight, moment_one, moment_two, grad_step, step_rate):
    mom_new = BETA_ONE * moment_one + (1.0 - BETA_ONE) * grad_step
    sec_new = BETA_TWO * moment_two + (1.0 - BETA_TWO) * grad_step * grad_step
    direction = (mom_new / ONE_CORR) / (jnp.sqrt(sec_new / TWO_CORR) + ADAM_EPS)
    weight_new = weight - step_rate * (direction + WEIGHT_DECAY * weight)
    return weight_new, mom_new, sec_new


def clip_of(norm_tile, max_norm):
    total = jnp.sum(jnp.sum(norm_tile, axis=0, keepdims=True), axis=1, keepdims=True)
    return jnp.minimum(1.0, max_norm / (jnp.sqrt(total) + NORM_EPS))


def whole_barrier(n_model, n_data, n_stage):
    barrier = pltpu.get_barrier_semaphore()
    me = (lax.axis_index('model'), lax.axis_index('data'), lax.axis_index('stage'))
    for dm in range(n_model):
        for dd in range(n_data):
            for ds in range(n_stage):
                if dm or dd or ds:
                    peer = (lax.rem(me[0] + dm, n_model), lax.rem(me[1] + dd, n_data), lax.rem(me[2] + ds, n_stage))
                    pl.semaphore_signal(barrier, inc=1, device_id=peer, device_id_type=MESH)
    pl.semaphore_wait(barrier, n_model * n_data * n_stage - 1)


def remote(src, dst, send_sem, recv_sem, device):
    return pltpu.make_async_remote_copy(src_ref=src, dst_ref=dst, send_sem=send_sem, recv_sem=recv_sem, device_id=device, device_id_type=MESH)


def bwd_kernel(dims, wu_hbm, wd_hbm, acts_hbm, dy_hbm, gu_hbm, gd_hbm,
               gbu_hbm, gbd_hbm, norm_out,
               wu32, wd32, wu_bf, wd_bf, aa, gg, hid_o, dz_o, slope, slope_o, dz_own, h_own,
               gu_own, gd_own, gu_oth, gd_oth, gu_rcv, gd_rcv, part, part_rcv, fin, norm_buf,
               ld_sem, ysend, yrecv, psend, precv, fsend, frecv, nsend, nrecv, st_sem):
    n_model, n_data, n_stage = dims
    z, d, p = lax.axis_index('model'), lax.axis_index('data'), lax.axis_index('stage')
    zo, do = 1 - z, 1 - d
    ypeer, zpeer = (z, do, p), (zo, d, p)
    last = n_stage - 1
    rows = aa.shape[0] // 2
    width = aa.shape[1]
    half = hid_o.shape[1]
    rb = BACK_ROWS
    hb = rb // 2
    nb = rows // rb
    own_ff = pl.ds(pl.multiple_of(d * half, 128), half)
    oth_ff = pl.ds(pl.multiple_of(do * half, 128), half)
    mine, theirs = pl.ds(0, rows), pl.ds(rows, rows)

    loads = [
        pltpu.make_async_copy(wu_hbm, wu32, ld_sem.at[0]),
        pltpu.make_async_copy(acts_hbm, aa.at[mine], ld_sem.at[2]),
        pltpu.make_async_copy(wd_hbm, wd32, ld_sem.at[1]),
        pltpu.make_async_copy(gu_hbm.at[:, own_ff], gu_own, ld_sem.at[4]),
        pltpu.make_async_copy(gd_hbm.at[own_ff, :], gd_own, ld_sem.at[5]),
    ]
    dy_load = pltpu.make_async_copy(dy_hbm, gg.at[mine], ld_sem.at[3])
    gu_load = pltpu.make_async_copy(gu_hbm.at[:, oth_ff], gu_oth, ld_sem.at[6])
    gd_load = pltpu.make_async_copy(gd_hbm.at[oth_ff, :], gd_oth, ld_sem.at[7])
    for copy in loads[:3]:
        copy.start()

    @pl.when(p == last)
    def _():
        dy_load.start()
    for copy in loads[3:]:
        copy.start()

    @pl.when(p > 0)
    def _():
        gd_load.start()
        gu_load.start()

    whole_barrier(n_model, n_data, n_stage)
    send_acts = remote(acts_hbm, aa.at[theirs], ysend.at[0], yrecv.at[0], ypeer)
    raw_gu = remote(gu_hbm.at[:, oth_ff], gu_rcv, ysend.at[1], yrecv.at[1], ypeer)
    raw_gd = remote(gd_hbm.at[oth_ff, :], gd_rcv, ysend.at[2], yrecv.at[2], ypeer)
    sum_gu = remote(gu_oth, gu_rcv, ysend.at[1], yrecv.at[1], ypeer)
    sum_gd = remote(gd_oth, gd_rcv, ysend.at[2], yrecv.at[2], ypeer)
    send_g = remote(gg.at[mine], gg.at[theirs], ysend.at[3], yrecv.at[3], ypeer)

    @pl.when(p == 0)
    def _():
        send_acts.start()
        raw_gu.start()

    loads[0].wait()
    loads[1].wait()

    def cast_up(i, carry):
        at = pl.ds(pl.multiple_of(i * 128, 128), 128)
        wu_bf[at, :] = wu32[at, :].astype(BF16)
        return carry
    lax.fori_loop(0, width // 128, cast_up, 0)

    def own_pre(i, carry):
        at = pl.ds(pl.multiple_of(i * rb, rb), rb)
        val, slp = gelu_both(mm(aa[at, :], wu_bf[...], NN))
        h_own[at, :] = val.astype(BF16)
        slope[at, :] = slp
        return carry
    lax.fori_loop(0, nb, own_pre, 0)
    loads[2].wait()

    def cast_down(i, carry):
        at = pl.ds(pl.multiple_of(i * 128, 128), 128)
        wd_bf[at, :] = wd32[at, :].astype(BF16)
        return carry
    lax.fori_loop(0, 2 * half // 128, cast_down, 0)

    @pl.when(p == last)
    def _():
        dy_load.wait()

    def g_at(c, zi):
        return gg.at[pl.ds(pl.multiple_of(c * rb + zi * hb, hb), hb)]

    def part_copy(c):
        return remote(part.at[c, pl.ds(pl.multiple_of(zo * hb, hb), hb)], part_rcv.at[c], psend.at[c], precv.at[c], zpeer)

    def fin_copy(c, zi):
        return remote(fin.at[c], g_at(c, z), fsend.at[c, zi], frecv.at[c, z], (zi, d, lax.max(p - 1, 0)))

    def compute(c):
        @pl.when(p < last)
        def _():
            for zi in range(n_model):
                pltpu.make_async_copy(fin.at[c], g_at(c, zi), frecv.at[c, zi]).wait()
        at = pl.ds(pl.multiple_of(c * rb, rb), rb)
        grad_hid = mm(gg[at, :], wd_bf[...], NT)
        dz_own[at, :] = (slope[at, :] * grad_hid).astype(BF16)

        @pl.when(p > 0)
        def _():
            part[c] = mm(dz_own[at, :], wu_bf[...], NT)
            part_copy(c).start()

    def finalize(c):
        part_copy(c).wait_recv()
        at = pl.ds(pl.multiple_of(c * rb + z * hb, hb), hb)
        total = part[c, pl.ds(pl.multiple_of(z * hb, hb), hb), :] + part_rcv[c]
        fin[c] = (gg[at, :].astype(F32) + total).astype(BF16)
        for zi in range(n_model):
            fin_copy(c, zi).start()

    def chain(i, carry):
        @pl.when(i < nb)
        def _():
            compute(i)

        @pl.when((i >= 1) & (p > 0))
        def _():
            finalize(i - 1)
        return carry
    lax.fori_loop(0, nb + 1, chain, 0)

    def down_block(j, base):
        at = pl.ds(pl.multiple_of(base * half + j * 128, 128), 128)
        return mm(h_own[:, at], gg[mine, :], TN)

    def up_block(j, ff_at):
        at = pl.ds(pl.multiple_of(j * 128, 128), 128)
        return mm(aa[mine, at], dz_own[:, ff_at], TN)

    @pl.when(p > 0)
    def _():
        gd_load.wait()

        def down_oth(j, carry):
            gd_oth[pl.ds(pl.multiple_of(j * 128, 128), 128), :] += down_block(j, do)
            return carry
        lax.fori_loop(0, half // 128, down_oth, 0)
        gu_load.wait()
        sum_gd.start()

        def up_oth(j, carry):
            gu_oth[pl.ds(pl.multiple_of(j * 128, 128), 128), :] += up_block(j, oth_ff)
            return carry
        lax.fori_loop(0, width // 128, up_oth, 0)

    @pl.when(p == 0)
    def _():
        send_g.start()
        raw_gd.start()
    loads[3].wait()
    loads[4].wait()

    def down_own(j, carry):
        gd_own[pl.ds(pl.multiple_of(j * 128, 128), 128), :] += down_block(j, d)
        return carry
    lax.fori_loop(0, half // 128, down_own, 0)

    @pl.when(p > 0)
    def _():
        sum_gu.start()

    def up_own(j, carry):
        gu_own[pl.ds(pl.multiple_of(j * 128, 128), 128), :] += up_block(j, own_ff)
        return carry
    lax.fori_loop(0, width // 128, up_own, 0)

    @pl.when(p == 0)
    def _():
        send_acts.wait_recv()

        def oth_pre(i, carry):
            at = pl.ds(pl.multiple_of(i * rb, rb), rb)
            val, slp = gelu_both(mm(aa[pl.ds(pl.multiple_of(rows + i * rb, rb), rb), :], wu_bf[:, own_ff], NN))
            hid_o[at, :] = val.astype(BF16)
            slope_o[at, :] = slp
            return carry
        lax.fori_loop(0, nb, oth_pre, 0)
        send_g.wait_recv()

        def oth_dz(i, carry):
            at = pl.ds(pl.multiple_of(i * rb, rb), rb)
            grad_hid = mm(gg[pl.ds(pl.multiple_of(rows + i * rb, rb), rb), :], wd_bf[own_ff, :], NT)
            dz_o[at, :] = (slope_o[at, :] * grad_hid).astype(BF16)
            return carry
        lax.fori_loop(0, nb, oth_dz, 0)

        def oth_grads(j, carry):
            at = pl.ds(pl.multiple_of(j * 128, 128), 128)
            gd_own[at, :] += mm(hid_o[:, at], gg[theirs, :], TN)
            gu_own[at, :] += mm(aa[theirs, at], dz_o[...], TN)
            return carry
        lax.fori_loop(0, half // 128, oth_grads, 0)

    def combine(own, rcv):
        def body(i, acc):
            at = pl.ds(pl.multiple_of(i * 32, 32), 32)
            mean = (own[at, :] + rcv[at, :]) * 0.5
            own[at, :] = mean
            return acc + jnp.sum((mean * mean).reshape(4, 8, mean.shape[1]), axis=0)
        return body

    def combine_up(acc):
        raw_gu.wait_recv()
        return lax.fori_loop(0, gu_own.shape[0] // 32, combine(gu_own, gu_rcv), acc)

    def combine_down(acc):
        raw_gd.wait_recv()
        return lax.fori_loop(0, gd_own.shape[0] // 32, combine(gd_own, gd_rcv), acc)
    acc = jnp.zeros((8, half), F32)
    acc = combine_down(acc)
    store_d = pltpu.make_async_copy(gd_own, gbd_hbm, st_sem.at[1])
    store_d.start()
    acc = combine_up(acc)
    store_u = pltpu.make_async_copy(gu_own, gbu_hbm, st_sem.at[0])
    store_u.start()
    tile = acc[:, 0:128]
    for k in range(1, half // 128):
        tile = tile + acc[:, k * 128:(k + 1) * 128]
    n_all = n_model * n_data * n_stage
    my_id = (z * n_data + d) * n_stage + p
    norm_buf[my_id] = tile

    def norm_copy(k):
        peer = lax.rem(my_id + k, n_all)
        device = (peer // (n_data * n_stage), lax.rem(peer // n_stage, n_data), lax.rem(peer, n_stage))
        return remote(norm_buf.at[my_id], norm_buf.at[my_id], nsend.at[k], nrecv.at[my_id], device)
    for k in range(1, n_all):
        norm_copy(k).start()
    for k in range(1, n_all):
        peer = lax.rem(my_id + k, n_all)
        pltpu.make_async_copy(norm_buf.at[peer], norm_buf.at[peer], nrecv.at[peer]).wait()
    total = norm_buf[0]
    for k in range(1, n_all):
        total = total + norm_buf[k]
    norm_out[...] = total

    for k in range(1, n_all):
        norm_copy(k).wait_send()

    @pl.when(p == 0)
    def _():
        for copy in (send_acts, raw_gu, raw_gd, send_g):
            copy.wait_send()

    @pl.when(p > 0)
    def _():
        sum_gu.wait_send()
        sum_gd.wait_send()
        for c in range(nb):
            part_copy(c).wait_send()
            for zi in range(n_model):
                fin_copy(c, zi).wait_send()
    store_u.wait()
    store_d.wait()


def update_kernel(d_ref, lr_ref, mn_ref, norm_ref, gu, gd, wu, wd, mu, md, vu, vd, *rest):
    owu, owd, omu, omd, ovu, ovd = rest[:6]
    clip = clip_of(norm_ref[...], mn_ref[0])
    rate = lr_ref[0]
    owu[...], omu[...], ovu[...] = adamw_update(wu[...], mu[...], vu[...], clip * gu[...], rate)
    owd[...], omd[...], ovd[...] = adamw_update(wd[...], md[...], vd[...], clip * gd[...], rate)
    if len(rest) == 8:
        rest[6][...] = owu[...].astype(BF16)
        rest[7][...] = owd[...].astype(BF16)


def fill_kernel(d_ref, lr_ref, mn_ref, norm_ref, gu, gd, wu, wd, mu, md, vu, vd, *rest):
    update_kernel(d_ref, lr_ref, mn_ref, norm_ref, gu, gd, wu, wd, mu, md, vu, vd, *rest[6:])


def fwd_kernel(dims, bu_hbm, bd_hbm, gbu_hbm, gbd_hbm, x_hbm,
               gu_oth, gd_oth, y_hbm,
               wu_bf, wd_bf, a_buf, y_buf, part, part_rcv, fin,
               ld_sem, ysend, yrecv, psend, precv, fsend, frecv, agsend, agrecv, outsend, outrecv, turn):
    n_model, n_data, n_stage = dims
    z, d, p = lax.axis_index('model'), lax.axis_index('data'), lax.axis_index('stage')
    zo, do = 1 - z, 1 - d
    ypeer, zpeer = (z, do, p), (zo, d, p)
    last = n_stage - 1
    nc, rb, width = a_buf.shape
    half = wu_bf.shape[1] // 2
    hb = rb // 2
    own_ff = pl.ds(pl.multiple_of(d * half, 128), half)
    even = lax.rem(p, 2) == 0

    load_u = pltpu.make_async_copy(bu_hbm, wu_bf.at[:, own_ff], ld_sem.at[0])
    load_d = pltpu.make_async_copy(bd_hbm, wd_bf.at[own_ff, :], ld_sem.at[1])
    load_u.start()
    load_d.start()
    x_load = pltpu.make_async_copy(x_hbm, a_buf, ld_sem.at[2])

    @pl.when(p == 0)
    def _():
        x_load.start()
    whole_barrier(n_model, n_data, n_stage)

    send_wu = remote(wu_bf.at[:, own_ff], wu_bf.at[:, own_ff], ysend.at[0], yrecv.at[0], ypeer)
    send_wd = remote(wd_bf.at[own_ff, :], wd_bf.at[own_ff, :], ysend.at[1], yrecv.at[1], ypeer)
    send_gu = remote(gbu_hbm, gu_oth, ysend.at[2], yrecv.at[2], ypeer)
    send_gd = remote(gbd_hbm, gd_oth, ysend.at[3], yrecv.at[3], ypeer)
    load_u.wait()
    load_d.wait()

    @pl.when(even)
    def _():
        send_wu.start()
        send_wd.start()
        send_wu.wait_send()
        send_wd.wait_send()
        pl.semaphore_signal(turn, inc=1, device_id=(z, d, p + 1), device_id_type=MESH)

    @pl.when(jnp.logical_not(even))
    def _():
        pl.semaphore_wait(turn, 1)
        send_wu.start()
        send_wd.start()
        send_gu.start()
        send_gd.start()

    @pl.when(p == 0)
    def _():
        x_load.wait()
    send_wu.wait_recv()
    send_wd.wait_recv()

    def half_rows(zi):
        return pl.ds(pl.multiple_of(zi * hb, hb), hb)

    def part_copy(c):
        return remote(part.at[c, half_rows(zo)], part_rcv.at[c], psend.at[c], precv.at[c], zpeer)

    def fin_copy(c, zi):
        return remote(fin.at[c], a_buf.at[c, half_rows(z)], fsend.at[c, zi], frecv.at[c, z], (zi, d, lax.min(p + 1, last)))

    def gather_copy(c):
        return remote(fin.at[c], y_buf.at[c, half_rows(z)], agsend.at[c], agrecv.at[c], zpeer)

    def out_copy(c, q):
        return remote(y_buf.at[c], y_hbm.at[c], outsend.at[c, q], outrecv.at[c], (z, d, q))

    def out_local(c):
        return pltpu.make_async_copy(y_buf.at[c], y_hbm.at[c], outsend.at[c, last])

    def compute(c):
        @pl.when(p > 0)
        def _():
            for zi in range(n_model):
                pltpu.make_async_copy(fin.at[c], a_buf.at[c, half_rows(zi)], frecv.at[c, zi]).wait()
        hid = gelu_val(mm(a_buf[c], wu_bf[...], NN)).astype(BF16)
        part[c] = mm(hid, wd_bf[...], NN)
        part_copy(c).start()

    def finalize(c):
        part_copy(c).wait_recv()
        total = part[c, half_rows(z), :] + part_rcv[c]
        new = (a_buf[c, half_rows(z), :].astype(F32) + total).astype(BF16)
        fin[c] = new

        @pl.when(p < last)
        def _():
            for zi in range(n_model):
                fin_copy(c, zi).start()

        @pl.when(p == last)
        def _():
            y_buf[c, half_rows(z), :] = new
            gather_copy(c).start()

    def publish(c):
        gather_copy(c).wait_recv()
        out_local(c).start()
        for q in range(last):
            out_copy(c, q).start()

    def chain(i, carry):
        @pl.when(i < nc)
        def _():
            compute(i)

        @pl.when((i >= 1) & (i <= nc))
        def _():
            finalize(i - 1)

        @pl.when((i >= 2) & (p == last))
        def _():
            publish(i - 2)

        @pl.when((i == TURN_STEP) & even)
        def _():
            pl.semaphore_wait(turn, 1)
            send_gu.start()
            send_gd.start()

        @pl.when((i == TURN_STEP - 1) & jnp.logical_not(even))
        def _():
            send_wu.wait_send()
            send_wd.wait_send()
            pl.semaphore_signal(turn, inc=1, device_id=(z, d, p - 1), device_id_type=MESH)
        return carry
    lax.fori_loop(0, nc + 2, chain, 0)

    def drain(c, carry):
        part_copy(c).wait_send()

        @pl.when(p < last)
        def _():
            for zi in range(n_model):
                fin_copy(c, zi).wait_send()
            pltpu.make_async_copy(y_buf.at[c], y_hbm.at[c], outrecv.at[c]).wait()

        @pl.when(p == last)
        def _():
            gather_copy(c).wait_send()
            out_local(c).wait()
            for q in range(last):
                out_copy(c, q).wait_send()
        return carry
    lax.fori_loop(0, nc, drain, 0)
    send_gu.wait()
    send_gd.wait()


def solution(mesh):
    n_model, n_data, n_stage = (mesh.shape[k] for k in ('model', 'data', 'stage'))
    dims = (n_model, n_data, n_stage)
    n_all = n_model * n_data * n_stage
    up_spec = P('stage', None, 'model')
    down_spec = P('stage', 'model', None)
    row_spec = P(None, 'data', None)
    in_specs = (up_spec, down_spec, up_spec, down_spec, up_spec, down_spec, P('data', 'stage', None, 'model'), P('data', 'stage', 'model', None), P('stage', 'data', None), P('data', None), row_spec, P(None), P(None))
    out_specs = (up_spec, down_spec, up_spec, down_spec, up_spec, down_spec, row_spec)
    any_spec = pl.BlockSpec(memory_space=pl.ANY)
    vmem_spec = pl.BlockSpec(memory_space=pltpu.VMEM)
    smem_spec = pl.BlockSpec(memory_space=pltpu.SMEM)
    dma = pltpu.SemaphoreType.DMA

    def device_step(w_up, w_down, m_up, m_down, v_up, v_down, g_up, g_down, acts_last, grad_out, x_next, learn_rate, max_norm):
        rows, width = grad_out.shape
        ff = w_up.shape[2]
        half = ff // 2
        nb = rows // BACK_ROWS
        hb = BACK_ROWS // 2
        sds = jax.ShapeDtypeStruct
        gbar_u, gbar_d, norm_tile = pl.pallas_call(
            functools.partial(bwd_kernel, dims),
            out_shape=(sds((width, half), F32), sds((half, width), F32), sds((8, 128), F32)),
            in_specs=[any_spec] * 6,
            out_specs=(any_spec, any_spec, vmem_spec),
            scratch_shapes=[
                pltpu.VMEM((width, ff), F32), pltpu.VMEM((ff, width), F32),
                pltpu.VMEM((width, ff), BF16), pltpu.VMEM((ff, width), BF16),
                pltpu.VMEM((2 * rows, width), BF16), pltpu.VMEM((2 * rows, width), BF16),
                pltpu.VMEM((rows, half), BF16), pltpu.VMEM((rows, half), BF16),
                pltpu.VMEM((rows, ff), F32), pltpu.VMEM((rows, half), F32),
                pltpu.VMEM((rows, ff), BF16), pltpu.VMEM((rows, ff), BF16),
            ] + [pltpu.VMEM((width, half), F32), pltpu.VMEM((half, width), F32)] * 3 + [
                pltpu.VMEM((nb, BACK_ROWS, width), F32), pltpu.VMEM((nb, hb, width), F32),
                pltpu.VMEM((nb, hb, width), BF16), pltpu.VMEM((n_all, 8, 128), F32),
                dma((8,)), dma((4,)), dma((4,)), dma((nb,)), dma((nb,)), dma((nb, 2)), dma((nb, 2)),
                dma((n_all,)), dma((n_all,)), dma((2,)),
            ],
            compiler_params=pltpu.CompilerParams(collective_id=0, has_side_effects=True, vmem_limit_bytes=VMEM_LIMIT),
            name='backward',
        )(w_up[0], w_down[0], acts_last[0], grad_out, g_up[0, 0], g_down[0, 0])

        blocks = half // UPD_ROWS
        state = (w_up[0], w_down[0], m_up[0], m_down[0], v_up[0], v_down[0])
        state_shapes = tuple(sds(s.shape, F32) for s in state)
        which = lax.axis_index('data').astype(jnp.int32).reshape(1)

        def update_specs(pick):
            up = pl.BlockSpec((UPD_ROWS, half), lambda i, w: (i, pick(w[0])))
            down = pl.BlockSpec((UPD_ROWS, width), lambda i, w: (pick(w[0]) * blocks + i, 0))
            return [up, down]
        plain_up = pl.BlockSpec((UPD_ROWS, half), lambda i, w: (i, 0))
        plain_down = pl.BlockSpec((UPD_ROWS, width), lambda i, w: (i, 0))
        small = [smem_spec, smem_spec, pl.BlockSpec((8, 128), lambda i, w: (0, 0))]
        own = update_specs(lambda w: w)
        *fresh, b_up, b_down = pl.pallas_call(
            update_kernel,
            out_shape=state_shapes + (sds((width, half), BF16), sds((half, width), BF16)),
            grid_spec=pltpu.PrefetchScalarGridSpec(
                num_scalar_prefetch=1, grid=(width // UPD_ROWS,),
                in_specs=small + [plain_up, plain_down] + own * 3,
                out_specs=own * 3 + [plain_up, plain_down]),
            compiler_params=pltpu.CompilerParams(dimension_semantics=('arbitrary',), vmem_limit_bytes=VMEM_LIMIT),
            name='update_own',
        )(which, learn_rate, max_norm, norm_tile, gbar_u, gbar_d, *state)

        n_micro = x_next.shape[0]
        nc = n_micro * rows // FWD_ROWS
        fb = FWD_ROWS // 2
        gu_oth, gd_oth, y_next = pl.pallas_call(
            functools.partial(fwd_kernel, dims),
            out_shape=(sds((width, half), F32), sds((half, width), F32), sds((nc, FWD_ROWS, width), BF16)),
            in_specs=[any_spec] * 5,
            out_specs=(any_spec, any_spec, any_spec),
            scratch_shapes=[
                pltpu.VMEM((width, ff), BF16), pltpu.VMEM((ff, width), BF16),
                pltpu.VMEM((nc, FWD_ROWS, width), BF16), pltpu.VMEM((nc, FWD_ROWS, width), BF16),
                pltpu.VMEM((nc, FWD_ROWS, width), F32), pltpu.VMEM((nc, fb, width), F32),
                pltpu.VMEM((nc, fb, width), BF16),
                dma((3,)), dma((4,)), dma((4,)), dma((nc,)), dma((nc,)), dma((nc, 2)), dma((nc, 2)),
                dma((nc,)), dma((nc,)), dma((nc, n_stage)), dma((nc,)), pltpu.SemaphoreType.REGULAR,
            ],
            compiler_params=pltpu.CompilerParams(collective_id=1, has_side_effects=True, vmem_limit_bytes=VMEM_LIMIT),
            name='forward',
        )(b_up, b_down, gbar_u, gbar_d, x_next.reshape(nc, FWD_ROWS, width))

        other = update_specs(lambda w: 1 - w)
        filled = pl.pallas_call(
            fill_kernel,
            out_shape=state_shapes,
            grid_spec=pltpu.PrefetchScalarGridSpec(
                num_scalar_prefetch=1, grid=(width // UPD_ROWS,),
                in_specs=small + [plain_up, plain_down] + other * 3 + [any_spec] * 6,
                out_specs=other * 3),
            input_output_aliases={12 + k: k for k in range(6)},
            compiler_params=pltpu.CompilerParams(dimension_semantics=('arbitrary',), vmem_limit_bytes=VMEM_LIMIT),
            name='update_other',
        )(which, learn_rate, max_norm, norm_tile, gu_oth, gd_oth, *state, *fresh)
        return tuple(s[None] for s in filled) + (y_next.reshape(n_micro, rows, width),)

    return jax.shard_map(device_step, mesh=mesh, in_specs=in_specs, out_specs=out_specs, check_vma=False)
```

```python
import functools

import jax
import jax.numpy as jnp
from jax import lax
from jax.experimental import pallas as pl
from jax.experimental.pallas import tpu as pltpu
from jax.sharding import PartitionSpec as P

ADAM_STEP = 10
BETA_ONE = 0.9
BETA_TWO = 0.95
ADAM_EPS = 1e-8
WEIGHT_DECAY = 0.1
NORM_EPS = 1e-6
ONE_CORR = 1.0 - BETA_ONE ** ADAM_STEP
TWO_CORR = 1.0 - BETA_TWO ** ADAM_STEP
GELU_SCALE = (2.0 / 3.141592653589793) ** 0.5
GELU_CUBE = 0.044715
NN = (((1,), (0,)), ((), ()))
NT = (((1,), (1,)), ((), ()))
TN = (((0,), (0,)), ((), ()))
F32 = jnp.float32
BF16 = jnp.bfloat16
MESH = pl.DeviceIdType.MESH
BACK_ROWS = 128
FWD_ROWS = 64
UPD_ROWS = 64
EARLY_ROWS = 256
TURN_STEP = 8
VMEM_LIMIT = 66_000_000


def mm(lhs, rhs, dims):
    return lax.dot_general(lhs, rhs, dims, preferred_element_type=F32)


def gelu_val(pre):
    return pre * (0.5 * (1.0 + jnp.tanh(GELU_SCALE * (pre + GELU_CUBE * (pre * pre * pre)))))


def gelu_both(pre):
    sq = pre * pre
    tan = jnp.tanh(GELU_SCALE * (pre + GELU_CUBE * (sq * pre)))
    cdf = 0.5 * (1.0 + tan)
    slope = cdf + 0.5 * pre * (1.0 - tan * tan) * (GELU_SCALE * (1.0 + (3.0 * GELU_CUBE) * sq))
    return pre * cdf, slope


def adamw_update(weight, moment_one, moment_two, grad_step, step_rate):
    mom_new = BETA_ONE * moment_one + (1.0 - BETA_ONE) * grad_step
    sec_new = BETA_TWO * moment_two + (1.0 - BETA_TWO) * grad_step * grad_step
    direction = (mom_new / ONE_CORR) / (jnp.sqrt(sec_new / TWO_CORR) + ADAM_EPS)
    weight_new = weight - step_rate * (direction + WEIGHT_DECAY * weight)
    return weight_new, mom_new, sec_new


def clip_of(norm_tile, max_norm):
    total = jnp.sum(jnp.sum(norm_tile, axis=0, keepdims=True), axis=1, keepdims=True)
    return jnp.minimum(1.0, max_norm / (jnp.sqrt(total) + NORM_EPS))


def whole_barrier(n_model, n_data, n_stage):
    barrier = pltpu.get_barrier_semaphore()
    me = (lax.axis_index('model'), lax.axis_index('data'), lax.axis_index('stage'))
    for dm in range(n_model):
        for dd in range(n_data):
            for ds in range(n_stage):
                if dm or dd or ds:
                    peer = (lax.rem(me[0] + dm, n_model), lax.rem(me[1] + dd, n_data), lax.rem(me[2] + ds, n_stage))
                    pl.semaphore_signal(barrier, inc=1, device_id=peer, device_id_type=MESH)
    pl.semaphore_wait(barrier, n_model * n_data * n_stage - 1)


def remote(src, dst, send_sem, recv_sem, device):
    return pltpu.make_async_remote_copy(src_ref=src, dst_ref=dst, send_sem=send_sem, recv_sem=recv_sem, device_id=device, device_id_type=MESH)


def bwd_kernel(dims, wu_hbm, wd_hbm, acts_hbm, dy_hbm, gu_hbm, gd_hbm,
               gbu_hbm, gbd_hbm, early_hbm, norm_out,
               wu32, wd32, wu_bf, wd_bf, aa, gg, hid_o, dz_o, slope, slope_o, dz_own, h_own,
               gu_own, gd_own, gu_oth, gd_oth, gu_rcv, gd_rcv, part, part_rcv, fin, norm_buf,
               ld_sem, ysend, yrecv, psend, precv, fsend, frecv, nsend, nrecv, st_sem):
    n_model, n_data, n_stage = dims
    z, d, p = lax.axis_index('model'), lax.axis_index('data'), lax.axis_index('stage')
    zo, do = 1 - z, 1 - d
    ypeer, zpeer = (z, do, p), (zo, d, p)
    last = n_stage - 1
    by_rows = lax.rem(p, 2) == 0
    by_sums = lax.rem(p, 2) == 1
    rows = aa.shape[0] // 2
    width = aa.shape[1]
    half = hid_o.shape[1]
    rb = BACK_ROWS
    hb = rb // 2
    nb = rows // rb
    own_ff = pl.ds(pl.multiple_of(d * half, 128), half)
    oth_ff = pl.ds(pl.multiple_of(do * half, 128), half)
    mine, theirs = pl.ds(0, rows), pl.ds(rows, rows)

    loads = [
        pltpu.make_async_copy(wu_hbm, wu32, ld_sem.at[0]),
        pltpu.make_async_copy(acts_hbm, aa.at[mine], ld_sem.at[2]),
        pltpu.make_async_copy(wd_hbm, wd32, ld_sem.at[1]),
        pltpu.make_async_copy(gu_hbm.at[:, own_ff], gu_own, ld_sem.at[4]),
        pltpu.make_async_copy(gd_hbm.at[own_ff, :], gd_own, ld_sem.at[5]),
    ]
    dy_load = pltpu.make_async_copy(dy_hbm, gg.at[mine], ld_sem.at[3])
    gu_load = pltpu.make_async_copy(gu_hbm.at[:, oth_ff], gu_oth, ld_sem.at[6])
    gd_load = pltpu.make_async_copy(gd_hbm.at[oth_ff, :], gd_oth, ld_sem.at[7])
    for copy in loads[:3]:
        copy.start()

    @pl.when(p == last)
    def _():
        dy_load.start()
    for copy in loads[3:]:
        copy.start()

    @pl.when(by_sums)
    def _():
        gd_load.start()
        gu_load.start()

    whole_barrier(n_model, n_data, n_stage)
    send_acts = remote(acts_hbm, aa.at[theirs], ysend.at[0], yrecv.at[0], ypeer)
    raw_gu = remote(gu_hbm.at[:, oth_ff], gu_rcv, ysend.at[1], yrecv.at[1], ypeer)
    raw_gd = remote(gd_hbm.at[oth_ff, :], gd_rcv, ysend.at[2], yrecv.at[2], ypeer)
    sum_gu = remote(gu_oth, gu_rcv, ysend.at[1], yrecv.at[1], ypeer)
    sum_gd = remote(gd_oth, gd_rcv, ysend.at[2], yrecv.at[2], ypeer)
    send_g = remote(gg.at[mine], gg.at[theirs], ysend.at[3], yrecv.at[3], ypeer)

    @pl.when(by_rows)
    def _():
        send_acts.start()
        raw_gd.start()
        raw_gu.start()

    loads[0].wait()
    loads[1].wait()

    def cast_up(i, carry):
        at = pl.ds(pl.multiple_of(i * 128, 128), 128)
        wu_bf[at, :] = wu32[at, :].astype(BF16)
        return carry
    lax.fori_loop(0, width // 128, cast_up, 0)

    def own_pre(i, carry):
        at = pl.ds(pl.multiple_of(i * rb, rb), rb)
        val, slp = gelu_both(mm(aa[at, :], wu_bf[...], NN))
        h_own[at, :] = val.astype(BF16)
        slope[at, :] = slp
        return carry
    lax.fori_loop(0, nb, own_pre, 0)
    loads[2].wait()

    def cast_down(i, carry):
        at = pl.ds(pl.multiple_of(i * 128, 128), 128)
        wd_bf[at, :] = wd32[at, :].astype(BF16)
        return carry
    lax.fori_loop(0, 2 * half // 128, cast_down, 0)

    @pl.when(p == last)
    def _():
        dy_load.wait()

    def g_at(c, zi):
        return gg.at[pl.ds(pl.multiple_of(c * rb + zi * hb, hb), hb)]

    def part_copy(c):
        return remote(part.at[c, pl.ds(pl.multiple_of(zo * hb, hb), hb)], part_rcv.at[c], psend.at[c], precv.at[c], zpeer)

    def fin_copy(c, zi):
        return remote(fin.at[c], g_at(c, z), fsend.at[c, zi], frecv.at[c, z], (zi, d, lax.max(p - 1, 0)))

    def compute(c):
        @pl.when(p < last)
        def _():
            for zi in range(n_model):
                pltpu.make_async_copy(fin.at[c], g_at(c, zi), frecv.at[c, zi]).wait()
        at = pl.ds(pl.multiple_of(c * rb, rb), rb)
        grad_hid = mm(gg[at, :], wd_bf[...], NT)
        dz_own[at, :] = (slope[at, :] * grad_hid).astype(BF16)

        @pl.when(p > 0)
        def _():
            part[c] = mm(dz_own[at, :], wu_bf[...], NT)
            part_copy(c).start()

    def finalize(c):
        part_copy(c).wait_recv()
        at = pl.ds(pl.multiple_of(c * rb + z * hb, hb), hb)
        total = part[c, pl.ds(pl.multiple_of(z * hb, hb), hb), :] + part_rcv[c]
        fin[c] = (gg[at, :].astype(F32) + total).astype(BF16)
        for zi in range(n_model):
            fin_copy(c, zi).start()

    def chain(i, carry):
        @pl.when(i < nb)
        def _():
            compute(i)

        @pl.when((i >= 1) & (p > 0))
        def _():
            finalize(i - 1)
        return carry
    lax.fori_loop(0, nb + 1, chain, 0)

    def down_block(j, base):
        at = pl.ds(pl.multiple_of(base * half + j * 128, 128), 128)
        return mm(h_own[:, at], gg[mine, :], TN)

    def up_block(j, ff_at):
        at = pl.ds(pl.multiple_of(j * 128, 128), 128)
        return mm(aa[mine, at], dz_own[:, ff_at], TN)

    @pl.when(by_sums)
    def _():
        gd_load.wait()

        def down_oth(j, carry):
            gd_oth[pl.ds(pl.multiple_of(j * 128, 128), 128), :] += down_block(j, do)
            return carry
        lax.fori_loop(0, half // 128, down_oth, 0)
        gu_load.wait()
        sum_gd.start()

        def up_oth(j, carry):
            gu_oth[pl.ds(pl.multiple_of(j * 128, 128), 128), :] += up_block(j, oth_ff)
            return carry
        lax.fori_loop(0, width // 128, up_oth, 0)

    @pl.when(by_rows)
    def _():
        send_g.start()
    loads[3].wait()
    loads[4].wait()

    def down_own(j, carry):
        gd_own[pl.ds(pl.multiple_of(j * 128, 128), 128), :] += down_block(j, d)
        return carry
    lax.fori_loop(0, half // 128, down_own, 0)

    @pl.when(by_sums)
    def _():
        sum_gu.start()

    def up_own(j, carry):
        gu_own[pl.ds(pl.multiple_of(j * 128, 128), 128), :] += up_block(j, own_ff)
        return carry
    lax.fori_loop(0, width // 128, up_own, 0)

    @pl.when(by_rows)
    def _():
        send_acts.wait_recv()

        def oth_pre(i, carry):
            at = pl.ds(pl.multiple_of(i * rb, rb), rb)
            val, slp = gelu_both(mm(aa[pl.ds(pl.multiple_of(rows + i * rb, rb), rb), :], wu_bf[:, own_ff], NN))
            hid_o[at, :] = val.astype(BF16)
            slope_o[at, :] = slp
            return carry
        lax.fori_loop(0, nb, oth_pre, 0)
        send_g.wait_recv()

        def oth_dz(i, carry):
            at = pl.ds(pl.multiple_of(i * rb, rb), rb)
            grad_hid = mm(gg[pl.ds(pl.multiple_of(rows + i * rb, rb), rb), :], wd_bf[own_ff, :], NT)
            dz_o[at, :] = (slope_o[at, :] * grad_hid).astype(BF16)
            return carry
        lax.fori_loop(0, nb, oth_dz, 0)

        def oth_grads(j, carry):
            at = pl.ds(pl.multiple_of(j * 128, 128), 128)
            gd_own[at, :] += mm(hid_o[:, at], gg[theirs, :], TN)
            gu_own[at, :] += mm(aa[theirs, at], dz_o[...], TN)
            return carry
        lax.fori_loop(0, half // 128, oth_grads, 0)

    def combine(own, rcv):
        def body(i, acc):
            at = pl.ds(pl.multiple_of(i * 32, 32), 32)
            mean = (own[at, :] + rcv[at, :]) * 0.5
            own[at, :] = mean
            return acc + jnp.sum((mean * mean).reshape(4, 8, mean.shape[1]), axis=0)
        return body

    def combine_up(acc):
        raw_gu.wait_recv()
        return lax.fori_loop(0, gu_own.shape[0] // 32, combine(gu_own, gu_rcv), acc)

    def combine_down(acc):
        raw_gd.wait_recv()
        return lax.fori_loop(0, gd_own.shape[0] // 32, combine(gd_own, gd_rcv), acc)
    acc = jnp.zeros((8, half), F32)
    acc = combine_down(acc)
    store_d = pltpu.make_async_copy(gd_own, gbd_hbm, st_sem.at[1])
    store_d.start()
    store_early = pltpu.make_async_copy(gd_own.at[pl.ds(0, early_hbm.shape[0])], early_hbm, st_sem.at[2])
    store_early.start()
    acc = combine_up(acc)
    store_u = pltpu.make_async_copy(gu_own, gbu_hbm, st_sem.at[0])
    store_u.start()
    tile = acc[:, 0:128]
    for k in range(1, half // 128):
        tile = tile + acc[:, k * 128:(k + 1) * 128]
    n_all = n_model * n_data * n_stage
    my_id = (z * n_data + d) * n_stage + p
    norm_buf[my_id] = tile

    def norm_copy(k):
        peer = lax.rem(my_id + k, n_all)
        device = (peer // (n_data * n_stage), lax.rem(peer // n_stage, n_data), lax.rem(peer, n_stage))
        return remote(norm_buf.at[my_id], norm_buf.at[my_id], nsend.at[k], nrecv.at[my_id], device)
    for k in range(1, n_all):
        norm_copy(k).start()
    for k in range(1, n_all):
        peer = lax.rem(my_id + k, n_all)
        pltpu.make_async_copy(norm_buf.at[peer], norm_buf.at[peer], nrecv.at[peer]).wait()
    total = norm_buf[0]
    for k in range(1, n_all):
        total = total + norm_buf[k]
    norm_out[...] = total

    for k in range(1, n_all):
        norm_copy(k).wait_send()

    @pl.when(by_rows)
    def _():
        for copy in (send_acts, raw_gu, raw_gd, send_g):
            copy.wait_send()

    @pl.when(by_sums)
    def _():
        sum_gu.wait_send()
        sum_gd.wait_send()

    @pl.when(p > 0)
    def _():
        for c in range(nb):
            part_copy(c).wait_send()
            for zi in range(n_model):
                fin_copy(c, zi).wait_send()
    store_u.wait()
    store_d.wait()
    store_early.wait()


def update_kernel(d_ref, lr_ref, mn_ref, norm_ref, gu, gd, wu, wd, mu, md, vu, vd, *rest):
    owu, owd, omu, omd, ovu, ovd = rest[:6]
    clip = clip_of(norm_ref[...], mn_ref[0])
    rate = lr_ref[0]
    owu[...], omu[...], ovu[...] = adamw_update(wu[...], mu[...], vu[...], clip * gu[...], rate)
    owd[...], omd[...], ovd[...] = adamw_update(wd[...], md[...], vd[...], clip * gd[...], rate)
    if len(rest) == 8:
        rest[6][...] = owu[...].astype(BF16)
        rest[7][...] = owd[...].astype(BF16)


def fill_kernel(d_ref, lr_ref, mn_ref, norm_ref, gu, gd_early, gd_late, y_in, wu, wd, mu, md, vu, vd, *rest):
    owu, owd, omu, omd, ovu, ovd, y_out = rest[6:]
    clip = clip_of(norm_ref[...], mn_ref[0])
    rate = lr_ref[0]
    gd = jnp.where(pl.program_id(0) < EARLY_ROWS // UPD_ROWS, gd_early[...], gd_late[...])
    owu[...], omu[...], ovu[...] = adamw_update(wu[...], mu[...], vu[...], clip * gu[...], rate)
    owd[...], omd[...], ovd[...] = adamw_update(wd[...], md[...], vd[...], clip * gd, rate)
    y_out[...] = y_in[...]


def fwd_kernel(dims, bu_hbm, bd_hbm, gbu_hbm, gbd_hbm, x_hbm,
               gu_oth, gd_oth, y_hbm,
               wu_bf, wd_bf, a_buf, y_buf, part, part_rcv, fin,
               ld_sem, ysend, yrecv, psend, precv, fsend, frecv, agsend, agrecv, outsend, outrecv, turn):
    n_model, n_data, n_stage = dims
    z, d, p = lax.axis_index('model'), lax.axis_index('data'), lax.axis_index('stage')
    zo, do = 1 - z, 1 - d
    ypeer, zpeer = (z, do, p), (zo, d, p)
    last = n_stage - 1
    nc, rb, width = a_buf.shape
    half = wu_bf.shape[1] // 2
    hb = rb // 2
    own_ff = pl.ds(pl.multiple_of(d * half, 128), half)
    even = lax.rem(p, 2) == 0

    load_u = pltpu.make_async_copy(bu_hbm, wu_bf.at[:, own_ff], ld_sem.at[0])
    load_d = pltpu.make_async_copy(bd_hbm, wd_bf.at[own_ff, :], ld_sem.at[1])
    load_u.start()
    load_d.start()
    x_load = pltpu.make_async_copy(x_hbm, a_buf, ld_sem.at[2])

    @pl.when(p == 0)
    def _():
        x_load.start()
    whole_barrier(n_model, n_data, n_stage)

    send_wu = remote(wu_bf.at[:, own_ff], wu_bf.at[:, own_ff], ysend.at[0], yrecv.at[0], ypeer)
    send_wd = remote(wd_bf.at[own_ff, :], wd_bf.at[own_ff, :], ysend.at[1], yrecv.at[1], ypeer)
    send_gu = remote(gbu_hbm, gu_oth, ysend.at[2], yrecv.at[2], ypeer)
    send_gd = remote(gbd_hbm.at[pl.ds(half - gd_oth.shape[0], gd_oth.shape[0])], gd_oth, ysend.at[3], yrecv.at[3], ypeer)
    load_u.wait()
    load_d.wait()

    @pl.when(even)
    def _():
        send_wu.start()
        send_wd.start()
        send_wu.wait_send()
        send_wd.wait_send()
        pl.semaphore_signal(turn, inc=1, device_id=(z, d, p + 1), device_id_type=MESH)

    @pl.when(jnp.logical_not(even))
    def _():
        pl.semaphore_wait(turn, 1)
        send_wu.start()
        send_wd.start()
        send_gu.start()
        send_gd.start()

    @pl.when(p == 0)
    def _():
        x_load.wait()
    send_wu.wait_recv()
    send_wd.wait_recv()

    def half_rows(zi):
        return pl.ds(pl.multiple_of(zi * hb, hb), hb)

    def part_copy(c):
        return remote(part.at[c, half_rows(zo)], part_rcv.at[c], psend.at[c], precv.at[c], zpeer)

    def fin_copy(c, zi):
        return remote(fin.at[c], a_buf.at[c, half_rows(z)], fsend.at[c, zi], frecv.at[c, z], (zi, d, lax.min(p + 1, last)))

    def gather_copy(c):
        return remote(fin.at[c], y_buf.at[c, half_rows(z)], agsend.at[c], agrecv.at[c], zpeer)

    def out_copy(c, q):
        return remote(y_buf.at[c], y_hbm.at[c], outsend.at[c, q], outrecv.at[c], (z, d, q))

    def out_local(c):
        return pltpu.make_async_copy(y_buf.at[c], y_hbm.at[c], outsend.at[c, last])

    def compute(c):
        @pl.when(p > 0)
        def _():
            for zi in range(n_model):
                pltpu.make_async_copy(fin.at[c], a_buf.at[c, half_rows(zi)], frecv.at[c, zi]).wait()
        hid = gelu_val(mm(a_buf[c], wu_bf[...], NN)).astype(BF16)
        part[c] = mm(hid, wd_bf[...], NN)
        part_copy(c).start()

    def finalize(c):
        part_copy(c).wait_recv()
        total = part[c, half_rows(z), :] + part_rcv[c]
        new = (a_buf[c, half_rows(z), :].astype(F32) + total).astype(BF16)
        fin[c] = new

        @pl.when(p < last)
        def _():
            for zi in range(n_model):
                fin_copy(c, zi).start()

        @pl.when(p == last)
        def _():
            y_buf[c, half_rows(z), :] = new
            gather_copy(c).start()

    def publish(c):
        gather_copy(c).wait_recv()
        out_local(c).start()
        for q in range(last):
            out_copy(c, q).start()

    def chain(i, carry):
        @pl.when(i < nc)
        def _():
            compute(i)

        @pl.when((i >= 1) & (i <= nc))
        def _():
            finalize(i - 1)

        @pl.when((i >= 2) & (p == last))
        def _():
            publish(i - 2)

        @pl.when((i == TURN_STEP) & even)
        def _():
            pl.semaphore_wait(turn, 1)
            send_gu.start()
            send_gd.start()

        @pl.when((i == TURN_STEP - 1) & jnp.logical_not(even))
        def _():
            send_wu.wait_send()
            send_wd.wait_send()
            pl.semaphore_signal(turn, inc=1, device_id=(z, d, p - 1), device_id_type=MESH)
        return carry
    lax.fori_loop(0, nc + 2, chain, 0)

    def drain(c, carry):
        part_copy(c).wait_send()

        @pl.when(p < last)
        def _():
            for zi in range(n_model):
                fin_copy(c, zi).wait_send()
            pltpu.make_async_copy(y_buf.at[c], y_hbm.at[c], outrecv.at[c]).wait()

        @pl.when(p == last)
        def _():
            gather_copy(c).wait_send()
            out_local(c).wait()
            for q in range(last):
                out_copy(c, q).wait_send()
        return carry
    lax.fori_loop(0, nc, drain, 0)
    send_gu.wait()
    send_gd.wait()


def solution(mesh):
    n_model, n_data, n_stage = (mesh.shape[k] for k in ('model', 'data', 'stage'))
    dims = (n_model, n_data, n_stage)
    n_all = n_model * n_data * n_stage
    up_spec = P('stage', None, 'model')
    down_spec = P('stage', 'model', None)
    row_spec = P(None, 'data', None)
    in_specs = (up_spec, down_spec, up_spec, down_spec, up_spec, down_spec, P('data', 'stage', None, 'model'), P('data', 'stage', 'model', None), P('stage', 'data', None), P('data', None), row_spec, P(None), P(None))
    out_specs = (up_spec, down_spec, up_spec, down_spec, up_spec, down_spec, row_spec)
    any_spec = pl.BlockSpec(memory_space=pl.ANY)
    vmem_spec = pl.BlockSpec(memory_space=pltpu.VMEM)
    smem_spec = pl.BlockSpec(memory_space=pltpu.SMEM)
    dma = pltpu.SemaphoreType.DMA

    def device_step(w_up, w_down, m_up, m_down, v_up, v_down, g_up, g_down, acts_last, grad_out, x_next, learn_rate, max_norm):
        rows, width = grad_out.shape
        ff = w_up.shape[2]
        half = ff // 2
        nb = rows // BACK_ROWS
        hb = BACK_ROWS // 2
        sds = jax.ShapeDtypeStruct
        gbar_u, gbar_d, early, norm_tile = pl.pallas_call(
            functools.partial(bwd_kernel, dims),
            out_shape=(sds((width, half), F32), sds((half, width), F32), sds((EARLY_ROWS, width), F32), sds((8, 128), F32)),
            in_specs=[any_spec] * 6,
            out_specs=(any_spec, any_spec, any_spec, vmem_spec),
            scratch_shapes=[
                pltpu.VMEM((width, ff), F32), pltpu.VMEM((ff, width), F32),
                pltpu.VMEM((width, ff), BF16), pltpu.VMEM((ff, width), BF16),
                pltpu.VMEM((2 * rows, width), BF16), pltpu.VMEM((2 * rows, width), BF16),
                pltpu.VMEM((rows, half), BF16), pltpu.VMEM((rows, half), BF16),
                pltpu.VMEM((rows, ff), F32), pltpu.VMEM((rows, half), F32),
                pltpu.VMEM((rows, ff), BF16), pltpu.VMEM((rows, ff), BF16),
            ] + [pltpu.VMEM((width, half), F32), pltpu.VMEM((half, width), F32)] * 3 + [
                pltpu.VMEM((nb, BACK_ROWS, width), F32), pltpu.VMEM((nb, hb, width), F32),
                pltpu.VMEM((nb, hb, width), BF16), pltpu.VMEM((n_all, 8, 128), F32),
                dma((8,)), dma((4,)), dma((4,)), dma((nb,)), dma((nb,)), dma((nb, 2)), dma((nb, 2)),
                dma((n_all,)), dma((n_all,)), dma((3,)),
            ],
            compiler_params=pltpu.CompilerParams(collective_id=0, has_side_effects=True, vmem_limit_bytes=VMEM_LIMIT),
            name='backward',
        )(w_up[0], w_down[0], acts_last[0], grad_out, g_up[0, 0], g_down[0, 0])

        early_oth = lax.ppermute(early, 'data', [(k, 1 - k) for k in range(n_data)])
        blocks = half // UPD_ROWS
        state = (w_up[0], w_down[0], m_up[0], m_down[0], v_up[0], v_down[0])
        state_shapes = tuple(sds(s.shape, F32) for s in state)
        which = lax.axis_index('data').astype(jnp.int32).reshape(1)

        def update_specs(pick):
            up = pl.BlockSpec((UPD_ROWS, half), lambda i, w: (i, pick(w[0])))
            down = pl.BlockSpec((UPD_ROWS, width), lambda i, w: (pick(w[0]) * blocks + i, 0))
            return [up, down]
        plain_up = pl.BlockSpec((UPD_ROWS, half), lambda i, w: (i, 0))
        plain_down = pl.BlockSpec((UPD_ROWS, width), lambda i, w: (i, 0))
        small = [smem_spec, smem_spec, pl.BlockSpec((8, 128), lambda i, w: (0, 0))]
        own = update_specs(lambda w: w)
        *fresh, b_up, b_down = pl.pallas_call(
            update_kernel,
            out_shape=state_shapes + (sds((width, half), BF16), sds((half, width), BF16)),
            grid_spec=pltpu.PrefetchScalarGridSpec(
                num_scalar_prefetch=1, grid=(width // UPD_ROWS,),
                in_specs=small + [plain_up, plain_down] + own * 3,
                out_specs=own * 3 + [plain_up, plain_down]),
            compiler_params=pltpu.CompilerParams(dimension_semantics=('arbitrary',), vmem_limit_bytes=VMEM_LIMIT),
            name='update_own',
        )(which, learn_rate, max_norm, norm_tile, gbar_u, gbar_d, *state)

        n_micro = x_next.shape[0]
        nc = n_micro * rows // FWD_ROWS
        fb = FWD_ROWS // 2
        gu_oth, gd_oth, y_next = pl.pallas_call(
            functools.partial(fwd_kernel, dims),
            out_shape=(sds((width, half), F32), sds((half - EARLY_ROWS, width), F32), sds((nc, FWD_ROWS, width), BF16)),
            in_specs=[any_spec] * 5,
            out_specs=(any_spec, any_spec, any_spec),
            scratch_shapes=[
                pltpu.VMEM((width, ff), BF16), pltpu.VMEM((ff, width), BF16),
                pltpu.VMEM((nc, FWD_ROWS, width), BF16), pltpu.VMEM((nc, FWD_ROWS, width), BF16),
                pltpu.VMEM((nc, FWD_ROWS, width), F32), pltpu.VMEM((nc, fb, width), F32),
                pltpu.VMEM((nc, fb, width), BF16),
                dma((3,)), dma((4,)), dma((4,)), dma((nc,)), dma((nc,)), dma((nc, 2)), dma((nc, 2)),
                dma((nc,)), dma((nc,)), dma((nc, n_stage)), dma((nc,)), pltpu.SemaphoreType.REGULAR,
            ],
            compiler_params=pltpu.CompilerParams(collective_id=1, has_side_effects=True, vmem_limit_bytes=VMEM_LIMIT),
            name='forward',
        )(b_up, b_down, gbar_u, gbar_d, x_next.reshape(nc, FWD_ROWS, width))

        other = update_specs(lambda w: 1 - w)
        ne = EARLY_ROWS // UPD_ROWS
        steps = width // UPD_ROWS
        early_spec = pl.BlockSpec((UPD_ROWS, width), lambda i, w: (jnp.minimum(i, ne - 1), 0))
        late_spec = pl.BlockSpec((UPD_ROWS, width), lambda i, w: (jnp.maximum(i - ne, 0), 0))
        y_spec = pl.BlockSpec((nc // steps, FWD_ROWS, width), lambda i, w: (i, 0, 0))
        *filled, y_next = pl.pallas_call(
            fill_kernel,
            out_shape=state_shapes + (sds(y_next.shape, BF16),),
            grid_spec=pltpu.PrefetchScalarGridSpec(
                num_scalar_prefetch=1, grid=(steps,),
                in_specs=small + [plain_up, early_spec, late_spec, y_spec] + other * 3 + [any_spec] * 6,
                out_specs=other * 3 + [y_spec]),
            input_output_aliases={14 + k: k for k in range(6)},
            compiler_params=pltpu.CompilerParams(dimension_semantics=('arbitrary',), vmem_limit_bytes=VMEM_LIMIT),
            name='update_other',
        )(which, learn_rate, max_norm, norm_tile, gu_oth, early_oth, gd_oth, y_next, *state, *fresh)
        return tuple(s[None] for s in filled) + (y_next.reshape(n_micro, rows, width),)

    return jax.shard_map(device_step, mesh=mesh, in_specs=in_specs, out_specs=out_specs, check_vma=False)
```

```python
import functools

import jax
import jax.numpy as jnp
from jax import lax
from jax.experimental import pallas as pl
from jax.experimental.pallas import tpu as pltpu
from jax.sharding import PartitionSpec as P

ADAM_STEP = 10
BETA_ONE = 0.9
BETA_TWO = 0.95
ADAM_EPS = 1e-8
WEIGHT_DECAY = 0.1
NORM_EPS = 1e-6
ONE_CORR = 1.0 - BETA_ONE ** ADAM_STEP
TWO_CORR = 1.0 - BETA_TWO ** ADAM_STEP
GELU_SCALE = (2.0 / 3.141592653589793) ** 0.5
GELU_CUBE = 0.044715
NN = (((1,), (0,)), ((), ()))
NT = (((1,), (1,)), ((), ()))
TN = (((0,), (0,)), ((), ()))
F32 = jnp.float32
BF16 = jnp.bfloat16
MESH = pl.DeviceIdType.MESH
BACK_ROWS = 128
FWD_ROWS = 128
UPD_ROWS = 128
EARLY_ROWS = 256
TURN_STEP = 4
VMEM_LIMIT = 66_000_000


def mm(lhs, rhs, dims):
    return lax.dot_general(lhs, rhs, dims, preferred_element_type=F32)


def gelu_val(pre):
    return pre * (0.5 * (1.0 + jnp.tanh(GELU_SCALE * (pre + GELU_CUBE * (pre * pre * pre)))))


def gelu_both(pre):
    sq = pre * pre
    tan = jnp.tanh(GELU_SCALE * (pre + GELU_CUBE * (sq * pre)))
    cdf = 0.5 * (1.0 + tan)
    slope = cdf + 0.5 * pre * (1.0 - tan * tan) * (GELU_SCALE * (1.0 + (3.0 * GELU_CUBE) * sq))
    return pre * cdf, slope


def adamw_update(weight, moment_one, moment_two, grad_step, step_rate):
    mom_new = BETA_ONE * moment_one + (1.0 - BETA_ONE) * grad_step
    sec_new = BETA_TWO * moment_two + (1.0 - BETA_TWO) * grad_step * grad_step
    direction = (mom_new / ONE_CORR) / (jnp.sqrt(sec_new / TWO_CORR) + ADAM_EPS)
    weight_new = weight - step_rate * (direction + WEIGHT_DECAY * weight)
    return weight_new, mom_new, sec_new


def clip_of(norm_tile, max_norm):
    total = jnp.sum(jnp.sum(norm_tile, axis=0, keepdims=True), axis=1, keepdims=True)
    return jnp.minimum(1.0, max_norm / (jnp.sqrt(total) + NORM_EPS))


def whole_barrier(n_model, n_data, n_stage):
    barrier = pltpu.get_barrier_semaphore()
    me = (lax.axis_index('model'), lax.axis_index('data'), lax.axis_index('stage'))
    for dm in range(n_model):
        for dd in range(n_data):
            for ds in range(n_stage):
                if dm or dd or ds:
                    peer = (lax.rem(me[0] + dm, n_model), lax.rem(me[1] + dd, n_data), lax.rem(me[2] + ds, n_stage))
                    pl.semaphore_signal(barrier, inc=1, device_id=peer, device_id_type=MESH)
    pl.semaphore_wait(barrier, n_model * n_data * n_stage - 1)


def remote(src, dst, send_sem, recv_sem, device):
    return pltpu.make_async_remote_copy(src_ref=src, dst_ref=dst, send_sem=send_sem, recv_sem=recv_sem, device_id=device, device_id_type=MESH)


def bwd_kernel(dims, wu_hbm, wd_hbm, acts_hbm, dy_hbm, gu_hbm, gd_hbm,
               gbu_hbm, gbd_hbm, early_hbm, norm_out,
               wu32, wd32, wu_bf, wd_bf, aa, gg, hid_o, dz_o, slope, slope_o, dz_own, h_own,
               gu_own, gd_own, gu_oth, gd_oth, gu_rcv, gd_rcv, part, part_rcv, fin, norm_buf,
               ld_sem, ysend, yrecv, psend, precv, fsend, frecv, nsend, nrecv, st_sem):
    n_model, n_data, n_stage = dims
    z, d, p = lax.axis_index('model'), lax.axis_index('data'), lax.axis_index('stage')
    zo, do = 1 - z, 1 - d
    ypeer, zpeer = (z, do, p), (zo, d, p)
    last = n_stage - 1
    by_rows = lax.rem(p, 2) == 0
    by_sums = lax.rem(p, 2) == 1
    rows = aa.shape[0] // 2
    width = aa.shape[1]
    half = hid_o.shape[1]
    rb = BACK_ROWS
    hb = rb // 2
    nb = rows // rb
    own_ff = pl.ds(pl.multiple_of(d * half, 128), half)
    oth_ff = pl.ds(pl.multiple_of(do * half, 128), half)
    mine, theirs = pl.ds(0, rows), pl.ds(rows, rows)

    loads = [
        pltpu.make_async_copy(wu_hbm, wu32, ld_sem.at[0]),
        pltpu.make_async_copy(acts_hbm, aa.at[mine], ld_sem.at[2]),
        pltpu.make_async_copy(wd_hbm, wd32, ld_sem.at[1]),
        pltpu.make_async_copy(gu_hbm.at[:, own_ff], gu_own, ld_sem.at[4]),
        pltpu.make_async_copy(gd_hbm.at[own_ff, :], gd_own, ld_sem.at[5]),
    ]
    dy_load = pltpu.make_async_copy(dy_hbm, gg.at[mine], ld_sem.at[3])
    gu_load = pltpu.make_async_copy(gu_hbm.at[:, oth_ff], gu_oth, ld_sem.at[6])
    gd_load = pltpu.make_async_copy(gd_hbm.at[oth_ff, :], gd_oth, ld_sem.at[7])
    for copy in loads[:3]:
        copy.start()

    @pl.when(p == last)
    def _():
        dy_load.start()
    for copy in loads[3:]:
        copy.start()

    @pl.when(by_sums)
    def _():
        gd_load.start()
        gu_load.start()

    whole_barrier(n_model, n_data, n_stage)
    send_acts = remote(acts_hbm, aa.at[theirs], ysend.at[0], yrecv.at[0], ypeer)
    raw_gu = remote(gu_hbm.at[:, oth_ff], gu_rcv, ysend.at[1], yrecv.at[1], ypeer)
    raw_gd = remote(gd_hbm.at[oth_ff, :], gd_rcv, ysend.at[2], yrecv.at[2], ypeer)
    sum_gu = remote(gu_oth, gu_rcv, ysend.at[1], yrecv.at[1], ypeer)
    sum_gd = remote(gd_oth, gd_rcv, ysend.at[2], yrecv.at[2], ypeer)
    send_g = remote(gg.at[mine], gg.at[theirs], ysend.at[3], yrecv.at[3], ypeer)

    @pl.when(by_rows)
    def _():
        send_acts.start()
        raw_gd.start()
        raw_gu.start()

    loads[0].wait()
    loads[1].wait()

    def cast_up(i, carry):
        at = pl.ds(pl.multiple_of(i * 128, 128), 128)
        wu_bf[at, :] = wu32[at, :].astype(BF16)
        return carry
    lax.fori_loop(0, width // 128, cast_up, 0)

    def own_pre(i, carry):
        at = pl.ds(pl.multiple_of(i * rb, rb), rb)
        val, slp = gelu_both(mm(aa[at, :], wu_bf[...], NN))
        h_own[at, :] = val.astype(BF16)
        slope[at, :] = slp
        return carry
    lax.fori_loop(0, nb, own_pre, 0)
    loads[2].wait()

    def cast_down(i, carry):
        at = pl.ds(pl.multiple_of(i * 128, 128), 128)
        wd_bf[at, :] = wd32[at, :].astype(BF16)
        return carry
    lax.fori_loop(0, 2 * half // 128, cast_down, 0)

    @pl.when(p == last)
    def _():
        dy_load.wait()

    def g_at(c, zi):
        return gg.at[pl.ds(pl.multiple_of(c * rb + zi * hb, hb), hb)]

    def part_copy(c):
        return remote(part.at[c, pl.ds(pl.multiple_of(zo * hb, hb), hb)], part_rcv.at[c], psend.at[c], precv.at[c], zpeer)

    def fin_copy(c, zi):
        return remote(fin.at[c], g_at(c, z), fsend.at[c, zi], frecv.at[c, z], (zi, d, lax.max(p - 1, 0)))

    def compute(c):
        @pl.when(p < last)
        def _():
            for zi in range(n_model):
                pltpu.make_async_copy(fin.at[c], g_at(c, zi), frecv.at[c, zi]).wait()
        at = pl.ds(pl.multiple_of(c * rb, rb), rb)
        grad_hid = mm(gg[at, :], wd_bf[...], NT)
        dz_own[at, :] = (slope[at, :] * grad_hid).astype(BF16)

        @pl.when(p > 0)
        def _():
            part[c] = mm(dz_own[at, :], wu_bf[...], NT)
            part_copy(c).start()

    def finalize(c):
        part_copy(c).wait_recv()
        at = pl.ds(pl.multiple_of(c * rb + z * hb, hb), hb)
        total = part[c, pl.ds(pl.multiple_of(z * hb, hb), hb), :] + part_rcv[c]
        fin[c] = (gg[at, :].astype(F32) + total).astype(BF16)
        for zi in range(n_model):
            fin_copy(c, zi).start()

    def chain(i, carry):
        @pl.when(i < nb)
        def _():
            compute(i)

        @pl.when((i >= 1) & (p > 0))
        def _():
            finalize(i - 1)
        return carry
    lax.fori_loop(0, nb + 1, chain, 0)

    def down_block(j, base):
        at = pl.ds(pl.multiple_of(base * half + j * 128, 128), 128)
        return mm(h_own[:, at], gg[mine, :], TN)

    def up_block(j, ff_at):
        at = pl.ds(pl.multiple_of(j * 128, 128), 128)
        return mm(aa[mine, at], dz_own[:, ff_at], TN)

    @pl.when(by_sums)
    def _():
        gd_load.wait()

        def down_oth(j, carry):
            gd_oth[pl.ds(pl.multiple_of(j * 128, 128), 128), :] += down_block(j, do)
            return carry
        lax.fori_loop(0, half // 128, down_oth, 0)
        gu_load.wait()
        sum_gd.start()

        def up_oth(j, carry):
            gu_oth[pl.ds(pl.multiple_of(j * 128, 128), 128), :] += up_block(j, oth_ff)
            return carry
        lax.fori_loop(0, width // 128, up_oth, 0)

    @pl.when(by_rows)
    def _():
        send_g.start()
    loads[3].wait()
    loads[4].wait()

    def down_own(j, carry):
        gd_own[pl.ds(pl.multiple_of(j * 128, 128), 128), :] += down_block(j, d)
        return carry
    lax.fori_loop(0, half // 128, down_own, 0)

    @pl.when(by_sums)
    def _():
        sum_gu.start()

    def up_own(j, carry):
        gu_own[pl.ds(pl.multiple_of(j * 128, 128), 128), :] += up_block(j, own_ff)
        return carry
    lax.fori_loop(0, width // 128, up_own, 0)

    @pl.when(by_rows)
    def _():
        send_acts.wait_recv()

        def oth_pre(i, carry):
            at = pl.ds(pl.multiple_of(i * rb, rb), rb)
            val, slp = gelu_both(mm(aa[pl.ds(pl.multiple_of(rows + i * rb, rb), rb), :], wu_bf[:, own_ff], NN))
            hid_o[at, :] = val.astype(BF16)
            slope_o[at, :] = slp
            return carry
        lax.fori_loop(0, nb, oth_pre, 0)
        send_g.wait_recv()

        def oth_dz(i, carry):
            at = pl.ds(pl.multiple_of(i * rb, rb), rb)
            grad_hid = mm(gg[pl.ds(pl.multiple_of(rows + i * rb, rb), rb), :], wd_bf[own_ff, :], NT)
            dz_o[at, :] = (slope_o[at, :] * grad_hid).astype(BF16)
            return carry
        lax.fori_loop(0, nb, oth_dz, 0)

        def oth_grads(j, carry):
            at = pl.ds(pl.multiple_of(j * 128, 128), 128)
            gd_own[at, :] += mm(hid_o[:, at], gg[theirs, :], TN)
            gu_own[at, :] += mm(aa[theirs, at], dz_o[...], TN)
            return carry
        lax.fori_loop(0, half // 128, oth_grads, 0)

    def combine(own, rcv):
        def body(i, acc):
            at = pl.ds(pl.multiple_of(i * 32, 32), 32)
            mean = (own[at, :] + rcv[at, :]) * 0.5
            own[at, :] = mean
            return acc + jnp.sum((mean * mean).reshape(4, 8, mean.shape[1]), axis=0)
        return body

    def combine_up(acc):
        raw_gu.wait_recv()
        return lax.fori_loop(0, gu_own.shape[0] // 32, combine(gu_own, gu_rcv), acc)

    def combine_down(acc):
        raw_gd.wait_recv()
        return lax.fori_loop(0, gd_own.shape[0] // 32, combine(gd_own, gd_rcv), acc)
    acc = jnp.zeros((8, half), F32)
    acc = combine_down(acc)
    store_d = pltpu.make_async_copy(gd_own, gbd_hbm, st_sem.at[1])
    store_d.start()
    store_early = pltpu.make_async_copy(gd_own.at[pl.ds(0, early_hbm.shape[0])], early_hbm, st_sem.at[2])
    store_early.start()
    acc = combine_up(acc)
    store_u = pltpu.make_async_copy(gu_own, gbu_hbm, st_sem.at[0])
    store_u.start()
    tile = acc[:, 0:128]
    for k in range(1, half // 128):
        tile = tile + acc[:, k * 128:(k + 1) * 128]
    n_all = n_model * n_data * n_stage
    my_id = (z * n_data + d) * n_stage + p
    norm_buf[my_id] = tile

    def norm_copy(k):
        peer = lax.rem(my_id + k, n_all)
        device = (peer // (n_data * n_stage), lax.rem(peer // n_stage, n_data), lax.rem(peer, n_stage))
        return remote(norm_buf.at[my_id], norm_buf.at[my_id], nsend.at[k], nrecv.at[my_id], device)
    for k in range(1, n_all):
        norm_copy(k).start()
    for k in range(1, n_all):
        peer = lax.rem(my_id + k, n_all)
        pltpu.make_async_copy(norm_buf.at[peer], norm_buf.at[peer], nrecv.at[peer]).wait()
    total = norm_buf[0]
    for k in range(1, n_all):
        total = total + norm_buf[k]
    norm_out[...] = total

    for k in range(1, n_all):
        norm_copy(k).wait_send()

    @pl.when(by_rows)
    def _():
        for copy in (send_acts, raw_gu, raw_gd, send_g):
            copy.wait_send()

    @pl.when(by_sums)
    def _():
        sum_gu.wait_send()
        sum_gd.wait_send()

    @pl.when(p > 0)
    def _():
        for c in range(nb):
            part_copy(c).wait_send()
            for zi in range(n_model):
                fin_copy(c, zi).wait_send()
    store_u.wait()
    store_d.wait()
    store_early.wait()


def update_kernel(d_ref, lr_ref, mn_ref, norm_ref, gu, gd, wu, wd, mu, md, vu, vd, *rest):
    owu, owd, omu, omd, ovu, ovd = rest[:6]
    clip = clip_of(norm_ref[...], mn_ref[0])
    rate = lr_ref[0]
    owu[...], omu[...], ovu[...] = adamw_update(wu[...], mu[...], vu[...], clip * gu[...], rate)
    owd[...], omd[...], ovd[...] = adamw_update(wd[...], md[...], vd[...], clip * gd[...], rate)
    if len(rest) == 8:
        rest[6][...] = owu[...].astype(BF16)
        rest[7][...] = owd[...].astype(BF16)


def fill_kernel(d_ref, lr_ref, mn_ref, norm_ref, gu, gd_early, gd_late, y_in, wu, wd, mu, md, vu, vd, *rest):
    owu, owd, omu, omd, ovu, ovd, y_out = rest[6:]
    clip = clip_of(norm_ref[...], mn_ref[0])
    rate = lr_ref[0]
    gd = jnp.where(pl.program_id(0) < EARLY_ROWS // UPD_ROWS, gd_early[...], gd_late[...])
    owu[...], omu[...], ovu[...] = adamw_update(wu[...], mu[...], vu[...], clip * gu[...], rate)
    owd[...], omd[...], ovd[...] = adamw_update(wd[...], md[...], vd[...], clip * gd, rate)
    y_out[...] = y_in[...]


def fwd_kernel(dims, bu_hbm, bd_hbm, gbu_hbm, gbd_hbm, x_hbm,
               gu_oth, gd_oth, y_hbm,
               wu_bf, wd_bf, a_buf, y_buf, part, part_rcv, fin,
               ld_sem, ysend, yrecv, psend, precv, fsend, frecv, agsend, agrecv, outsend, outrecv, turn):
    n_model, n_data, n_stage = dims
    z, d, p = lax.axis_index('model'), lax.axis_index('data'), lax.axis_index('stage')
    zo, do = 1 - z, 1 - d
    ypeer, zpeer = (z, do, p), (zo, d, p)
    last = n_stage - 1
    nc, rb, width = a_buf.shape
    half = wu_bf.shape[1] // 2
    hb = rb // 2
    own_ff = pl.ds(pl.multiple_of(d * half, 128), half)
    even = lax.rem(p, 2) == 0

    load_u = pltpu.make_async_copy(bu_hbm, wu_bf.at[:, own_ff], ld_sem.at[0])
    load_d = pltpu.make_async_copy(bd_hbm, wd_bf.at[own_ff, :], ld_sem.at[1])
    load_u.start()
    load_d.start()
    x_load = pltpu.make_async_copy(x_hbm, a_buf, ld_sem.at[2])

    @pl.when(p == 0)
    def _():
        x_load.start()
    whole_barrier(n_model, n_data, n_stage)

    send_wu = remote(wu_bf.at[:, own_ff], wu_bf.at[:, own_ff], ysend.at[0], yrecv.at[0], ypeer)
    send_wd = remote(wd_bf.at[own_ff, :], wd_bf.at[own_ff, :], ysend.at[1], yrecv.at[1], ypeer)
    send_gu = remote(gbu_hbm, gu_oth, ysend.at[2], yrecv.at[2], ypeer)
    send_gd = remote(gbd_hbm.at[pl.ds(half - gd_oth.shape[0], gd_oth.shape[0])], gd_oth, ysend.at[3], yrecv.at[3], ypeer)
    load_u.wait()
    load_d.wait()

    @pl.when(even)
    def _():
        send_wu.start()
        send_wd.start()
        send_wu.wait_send()
        send_wd.wait_send()
        pl.semaphore_signal(turn, inc=1, device_id=(z, d, p + 1), device_id_type=MESH)

    @pl.when(jnp.logical_not(even))
    def _():
        pl.semaphore_wait(turn, 1)
        send_wu.start()
        send_wd.start()
        send_gu.start()
        send_gd.start()

    @pl.when(p == 0)
    def _():
        x_load.wait()
    send_wu.wait_recv()
    send_wd.wait_recv()

    def half_rows(zi):
        return pl.ds(pl.multiple_of(zi * hb, hb), hb)

    def part_copy(c):
        return remote(part.at[c, half_rows(zo)], part_rcv.at[c], psend.at[c], precv.at[c], zpeer)

    def fin_copy(c, zi):
        return remote(fin.at[c], a_buf.at[c, half_rows(z)], fsend.at[c, zi], frecv.at[c, z], (zi, d, lax.min(p + 1, last)))

    def gather_copy(c):
        return remote(fin.at[c], y_buf.at[c, half_rows(z)], agsend.at[c], agrecv.at[c], zpeer)

    def out_copy(c, q):
        return remote(y_buf.at[c], y_hbm.at[c], outsend.at[c, q], outrecv.at[c], (z, d, q))

    def out_local(c):
        return pltpu.make_async_copy(y_buf.at[c], y_hbm.at[c], outsend.at[c, last])

    def compute(c):
        @pl.when(p > 0)
        def _():
            for zi in range(n_model):
                pltpu.make_async_copy(fin.at[c], a_buf.at[c, half_rows(zi)], frecv.at[c, zi]).wait()
        hid = gelu_val(mm(a_buf[c], wu_bf[...], NN)).astype(BF16)
        part[c] = mm(hid, wd_bf[...], NN)
        part_copy(c).start()

    def finalize(c):
        part_copy(c).wait_recv()
        total = part[c, half_rows(z), :] + part_rcv[c]
        new = (a_buf[c, half_rows(z), :].astype(F32) + total).astype(BF16)
        fin[c] = new

        @pl.when(p < last)
        def _():
            for zi in range(n_model):
                fin_copy(c, zi).start()

        @pl.when(p == last)
        def _():
            y_buf[c, half_rows(z), :] = new
            gather_copy(c).start()

    def publish(c):
        gather_copy(c).wait_recv()
        out_local(c).start()
        for q in range(last):
            out_copy(c, q).start()

    def chain(i, carry):
        @pl.when(i < nc)
        def _():
            compute(i)

        @pl.when((i >= 1) & (i <= nc))
        def _():
            finalize(i - 1)

        @pl.when((i >= 2) & (p == last))
        def _():
            publish(i - 2)

        @pl.when((i == TURN_STEP) & even)
        def _():
            pl.semaphore_wait(turn, 1)
            send_gu.start()
            send_gd.start()

        @pl.when((i == TURN_STEP - 1) & jnp.logical_not(even))
        def _():
            send_wu.wait_send()
            send_wd.wait_send()
            pl.semaphore_signal(turn, inc=1, device_id=(z, d, p - 1), device_id_type=MESH)
        return carry
    lax.fori_loop(0, nc + 2, chain, 0)

    def drain(c, carry):
        part_copy(c).wait_send()

        @pl.when(p < last)
        def _():
            for zi in range(n_model):
                fin_copy(c, zi).wait_send()
            pltpu.make_async_copy(y_buf.at[c], y_hbm.at[c], outrecv.at[c]).wait()

        @pl.when(p == last)
        def _():
            gather_copy(c).wait_send()
            out_local(c).wait()
            for q in range(last):
                out_copy(c, q).wait_send()
        return carry
    lax.fori_loop(0, nc, drain, 0)
    send_gu.wait()
    send_gd.wait()


def solution(mesh):
    n_model, n_data, n_stage = (mesh.shape[k] for k in ('model', 'data', 'stage'))
    dims = (n_model, n_data, n_stage)
    n_all = n_model * n_data * n_stage
    up_spec = P('stage', None, 'model')
    down_spec = P('stage', 'model', None)
    row_spec = P(None, 'data', None)
    in_specs = (up_spec, down_spec, up_spec, down_spec, up_spec, down_spec, P('data', 'stage', None, 'model'), P('data', 'stage', 'model', None), P('stage', 'data', None), P('data', None), row_spec, P(None), P(None))
    out_specs = (up_spec, down_spec, up_spec, down_spec, up_spec, down_spec, row_spec)
    any_spec = pl.BlockSpec(memory_space=pl.ANY)
    vmem_spec = pl.BlockSpec(memory_space=pltpu.VMEM)
    smem_spec = pl.BlockSpec(memory_space=pltpu.SMEM)
    dma = pltpu.SemaphoreType.DMA

    def device_step(w_up, w_down, m_up, m_down, v_up, v_down, g_up, g_down, acts_last, grad_out, x_next, learn_rate, max_norm):
        rows, width = grad_out.shape
        ff = w_up.shape[2]
        half = ff // 2
        nb = rows // BACK_ROWS
        hb = BACK_ROWS // 2
        sds = jax.ShapeDtypeStruct
        gbar_u, gbar_d, early, norm_tile = pl.pallas_call(
            functools.partial(bwd_kernel, dims),
            out_shape=(sds((width, half), F32), sds((half, width), F32), sds((EARLY_ROWS, width), F32), sds((8, 128), F32)),
            in_specs=[any_spec] * 6,
            out_specs=(any_spec, any_spec, any_spec, vmem_spec),
            scratch_shapes=[
                pltpu.VMEM((width, ff), F32), pltpu.VMEM((ff, width), F32),
                pltpu.VMEM((width, ff), BF16), pltpu.VMEM((ff, width), BF16),
                pltpu.VMEM((2 * rows, width), BF16), pltpu.VMEM((2 * rows, width), BF16),
                pltpu.VMEM((rows, half), BF16), pltpu.VMEM((rows, half), BF16),
                pltpu.VMEM((rows, ff), F32), pltpu.VMEM((rows, half), F32),
                pltpu.VMEM((rows, ff), BF16), pltpu.VMEM((rows, ff), BF16),
            ] + [pltpu.VMEM((width, half), F32), pltpu.VMEM((half, width), F32)] * 3 + [
                pltpu.VMEM((nb, BACK_ROWS, width), F32), pltpu.VMEM((nb, hb, width), F32),
                pltpu.VMEM((nb, hb, width), BF16), pltpu.VMEM((n_all, 8, 128), F32),
                dma((8,)), dma((4,)), dma((4,)), dma((nb,)), dma((nb,)), dma((nb, 2)), dma((nb, 2)),
                dma((n_all,)), dma((n_all,)), dma((3,)),
            ],
            compiler_params=pltpu.CompilerParams(collective_id=0, has_side_effects=True, vmem_limit_bytes=VMEM_LIMIT),
            name='backward',
        )(w_up[0], w_down[0], acts_last[0], grad_out, g_up[0, 0], g_down[0, 0])

        early_oth = lax.ppermute(early, 'data', [(k, 1 - k) for k in range(n_data)])
        blocks = half // UPD_ROWS
        state = (w_up[0], w_down[0], m_up[0], m_down[0], v_up[0], v_down[0])
        state_shapes = tuple(sds(s.shape, F32) for s in state)
        which = lax.axis_index('data').astype(jnp.int32).reshape(1)

        def update_specs(pick):
            up = pl.BlockSpec((UPD_ROWS, half), lambda i, w: (i, pick(w[0])))
            down = pl.BlockSpec((UPD_ROWS, width), lambda i, w: (pick(w[0]) * blocks + i, 0))
            return [up, down]
        plain_up = pl.BlockSpec((UPD_ROWS, half), lambda i, w: (i, 0))
        plain_down = pl.BlockSpec((UPD_ROWS, width), lambda i, w: (i, 0))
        small = [smem_spec, smem_spec, pl.BlockSpec((8, 128), lambda i, w: (0, 0))]
        own = update_specs(lambda w: w)
        *fresh, b_up, b_down = pl.pallas_call(
            update_kernel,
            out_shape=state_shapes + (sds((width, half), BF16), sds((half, width), BF16)),
            grid_spec=pltpu.PrefetchScalarGridSpec(
                num_scalar_prefetch=1, grid=(width // UPD_ROWS,),
                in_specs=small + [plain_up, plain_down] + own * 3,
                out_specs=own * 3 + [plain_up, plain_down]),
            compiler_params=pltpu.CompilerParams(dimension_semantics=('arbitrary',), vmem_limit_bytes=VMEM_LIMIT),
            name='update_own',
        )(which, learn_rate, max_norm, norm_tile, gbar_u, gbar_d, *state)

        n_micro = x_next.shape[0]
        nc = n_micro * rows // FWD_ROWS
        fb = FWD_ROWS // 2
        gu_oth, gd_oth, y_next = pl.pallas_call(
            functools.partial(fwd_kernel, dims),
            out_shape=(sds((width, half), F32), sds((half - EARLY_ROWS, width), F32), sds((nc, FWD_ROWS, width), BF16)),
            in_specs=[any_spec] * 5,
            out_specs=(any_spec, any_spec, any_spec),
            scratch_shapes=[
                pltpu.VMEM((width, ff), BF16), pltpu.VMEM((ff, width), BF16),
                pltpu.VMEM((nc, FWD_ROWS, width), BF16), pltpu.VMEM((nc, FWD_ROWS, width), BF16),
                pltpu.VMEM((nc, FWD_ROWS, width), F32), pltpu.VMEM((nc, fb, width), F32),
                pltpu.VMEM((nc, fb, width), BF16),
                dma((3,)), dma((4,)), dma((4,)), dma((nc,)), dma((nc,)), dma((nc, 2)), dma((nc, 2)),
                dma((nc,)), dma((nc,)), dma((nc, n_stage)), dma((nc,)), pltpu.SemaphoreType.REGULAR,
            ],
            compiler_params=pltpu.CompilerParams(collective_id=1, has_side_effects=True, vmem_limit_bytes=VMEM_LIMIT),
            name='forward',
        )(b_up, b_down, gbar_u, gbar_d, x_next.reshape(nc, FWD_ROWS, width))

        other = update_specs(lambda w: 1 - w)
        ne = EARLY_ROWS // UPD_ROWS
        steps = width // UPD_ROWS
        early_spec = pl.BlockSpec((UPD_ROWS, width), lambda i, w: (jnp.minimum(i, ne - 1), 0))
        late_spec = pl.BlockSpec((UPD_ROWS, width), lambda i, w: (jnp.maximum(i - ne, 0), 0))
        y_spec = pl.BlockSpec((nc // steps, FWD_ROWS, width), lambda i, w: (i, 0, 0))
        *filled, y_next = pl.pallas_call(
            fill_kernel,
            out_shape=state_shapes + (sds(y_next.shape, BF16),),
            grid_spec=pltpu.PrefetchScalarGridSpec(
                num_scalar_prefetch=1, grid=(steps,),
                in_specs=small + [plain_up, early_spec, late_spec, y_spec] + other * 3 + [any_spec] * 6,
                out_specs=other * 3 + [y_spec]),
            input_output_aliases={14 + k: k for k in range(6)},
            compiler_params=pltpu.CompilerParams(dimension_semantics=('arbitrary',), vmem_limit_bytes=VMEM_LIMIT),
            name='update_other',
        )(which, learn_rate, max_norm, norm_tile, gu_oth, early_oth, gd_oth, y_next, *state, *fresh)
        return tuple(s[None] for s in filled) + (y_next.reshape(n_micro, rows, width),)

    return jax.shard_map(device_step, mesh=mesh, in_specs=in_specs, out_specs=out_specs, check_vma=False)
```

```python
import functools

import jax
import jax.numpy as jnp
from jax import lax
from jax.experimental import pallas as pl
from jax.experimental.pallas import tpu as pltpu
from jax.sharding import PartitionSpec as P

ADAM_STEP = 10
BETA_ONE = 0.9
BETA_TWO = 0.95
ADAM_EPS = 1e-8
WEIGHT_DECAY = 0.1
NORM_EPS = 1e-6
ONE_CORR = 1.0 - BETA_ONE ** ADAM_STEP
TWO_CORR = 1.0 - BETA_TWO ** ADAM_STEP
GELU_SCALE = (2.0 / 3.141592653589793) ** 0.5
GELU_CUBE = 0.044715
NN = (((1,), (0,)), ((), ()))
NT = (((1,), (1,)), ((), ()))
TN = (((0,), (0,)), ((), ()))
F32 = jnp.float32
BF16 = jnp.bfloat16
MESH = pl.DeviceIdType.MESH
BACK_ROWS = 128
FWD_ROWS = 64
UPD_ROWS = 128
EARLY_ROWS = 256
TURN_STEP = 8
VMEM_LIMIT = 66_000_000


def mm(lhs, rhs, dims):
    return lax.dot_general(lhs, rhs, dims, preferred_element_type=F32)


def gelu_val(pre):
    return pre * (0.5 * (1.0 + jnp.tanh(GELU_SCALE * (pre + GELU_CUBE * (pre * pre * pre)))))


def gelu_both(pre):
    sq = pre * pre
    tan = jnp.tanh(GELU_SCALE * (pre + GELU_CUBE * (sq * pre)))
    cdf = 0.5 * (1.0 + tan)
    slope = cdf + 0.5 * pre * (1.0 - tan * tan) * (GELU_SCALE * (1.0 + (3.0 * GELU_CUBE) * sq))
    return pre * cdf, slope


def adamw_update(weight, moment_one, moment_two, grad_step, step_rate):
    mom_new = BETA_ONE * moment_one + (1.0 - BETA_ONE) * grad_step
    sec_new = BETA_TWO * moment_two + (1.0 - BETA_TWO) * grad_step * grad_step
    direction = (mom_new / ONE_CORR) / (jnp.sqrt(sec_new / TWO_CORR) + ADAM_EPS)
    weight_new = weight - step_rate * (direction + WEIGHT_DECAY * weight)
    return weight_new, mom_new, sec_new


def clip_of(norm_tile, max_norm):
    total = jnp.sum(jnp.sum(norm_tile, axis=0, keepdims=True), axis=1, keepdims=True)
    return jnp.minimum(1.0, max_norm / (jnp.sqrt(total) + NORM_EPS))


def whole_barrier(n_model, n_data, n_stage):
    barrier = pltpu.get_barrier_semaphore()
    me = (lax.axis_index('model'), lax.axis_index('data'), lax.axis_index('stage'))
    for dm in range(n_model):
        for dd in range(n_data):
            for ds in range(n_stage):
                if dm or dd or ds:
                    peer = (lax.rem(me[0] + dm, n_model), lax.rem(me[1] + dd, n_data), lax.rem(me[2] + ds, n_stage))
                    pl.semaphore_signal(barrier, inc=1, device_id=peer, device_id_type=MESH)
    pl.semaphore_wait(barrier, n_model * n_data * n_stage - 1)


def remote(src, dst, send_sem, recv_sem, device):
    return pltpu.make_async_remote_copy(src_ref=src, dst_ref=dst, send_sem=send_sem, recv_sem=recv_sem, device_id=device, device_id_type=MESH)


def bwd_kernel(dims, wu_hbm, wd_hbm, acts_hbm, dy_hbm, gu_hbm, gd_hbm,
               gbu_hbm, gbd_hbm, early_hbm, norm_out,
               wu32, wd32, wu_bf, wd_bf, aa, gg, hid_o, dz_o, slope, slope_o, dz_own, h_own,
               gu_own, gd_own, gu_oth, gd_oth, gu_rcv, gd_rcv, part, part_rcv, fin, norm_buf,
               ld_sem, ysend, yrecv, psend, precv, fsend, frecv, nsend, nrecv, st_sem):
    n_model, n_data, n_stage = dims
    z, d, p = lax.axis_index('model'), lax.axis_index('data'), lax.axis_index('stage')
    zo, do = 1 - z, 1 - d
    ypeer, zpeer = (z, do, p), (zo, d, p)
    last = n_stage - 1
    by_rows = lax.rem(p, 2) == 0
    by_sums = lax.rem(p, 2) == 1
    rows = aa.shape[0] // 2
    width = aa.shape[1]
    half = hid_o.shape[1]
    rb = BACK_ROWS
    hb = rb // 2
    nb = rows // rb
    own_ff = pl.ds(pl.multiple_of(d * half, 128), half)
    oth_ff = pl.ds(pl.multiple_of(do * half, 128), half)
    mine, theirs = pl.ds(0, rows), pl.ds(rows, rows)

    loads = [
        pltpu.make_async_copy(wu_hbm, wu32, ld_sem.at[0]),
        pltpu.make_async_copy(acts_hbm, aa.at[mine], ld_sem.at[2]),
        pltpu.make_async_copy(wd_hbm, wd32, ld_sem.at[1]),
        pltpu.make_async_copy(gu_hbm.at[:, own_ff], gu_own, ld_sem.at[4]),
        pltpu.make_async_copy(gd_hbm.at[own_ff, :], gd_own, ld_sem.at[5]),
    ]
    dy_load = pltpu.make_async_copy(dy_hbm, gg.at[mine], ld_sem.at[3])
    gu_load = pltpu.make_async_copy(gu_hbm.at[:, oth_ff], gu_oth, ld_sem.at[6])
    gd_load = pltpu.make_async_copy(gd_hbm.at[oth_ff, :], gd_oth, ld_sem.at[7])
    for copy in loads[:3]:
        copy.start()

    @pl.when(p == last)
    def _():
        dy_load.start()
    for copy in loads[3:]:
        copy.start()

    @pl.when(by_sums)
    def _():
        gd_load.start()
        gu_load.start()

    whole_barrier(n_model, n_data, n_stage)
    send_acts = remote(acts_hbm, aa.at[theirs], ysend.at[0], yrecv.at[0], ypeer)
    raw_gu = remote(gu_hbm.at[:, oth_ff], gu_rcv, ysend.at[1], yrecv.at[1], ypeer)
    raw_gd = remote(gd_hbm.at[oth_ff, :], gd_rcv, ysend.at[2], yrecv.at[2], ypeer)
    sum_gu = remote(gu_oth, gu_rcv, ysend.at[1], yrecv.at[1], ypeer)
    sum_gd = remote(gd_oth, gd_rcv, ysend.at[2], yrecv.at[2], ypeer)
    send_g = remote(gg.at[mine], gg.at[theirs], ysend.at[3], yrecv.at[3], ypeer)

    @pl.when(by_rows)
    def _():
        send_acts.start()
        raw_gd.start()
        raw_gu.start()

    loads[0].wait()
    loads[1].wait()

    def cast_up(i, carry):
        at = pl.ds(pl.multiple_of(i * 128, 128), 128)
        wu_bf[at, :] = wu32[at, :].astype(BF16)
        return carry
    lax.fori_loop(0, width // 128, cast_up, 0)

    def own_pre(i, carry):
        at = pl.ds(pl.multiple_of(i * rb, rb), rb)
        val, slp = gelu_both(mm(aa[at, :], wu_bf[...], NN))
        h_own[at, :] = val.astype(BF16)
        slope[at, :] = slp
        return carry
    lax.fori_loop(0, nb, own_pre, 0)
    loads[2].wait()

    def cast_down(i, carry):
        at = pl.ds(pl.multiple_of(i * 128, 128), 128)
        wd_bf[at, :] = wd32[at, :].astype(BF16)
        return carry
    lax.fori_loop(0, 2 * half // 128, cast_down, 0)

    @pl.when(p == last)
    def _():
        dy_load.wait()

    def g_at(c, zi):
        return gg.at[pl.ds(pl.multiple_of(c * rb + zi * hb, hb), hb)]

    def part_copy(c):
        return remote(part.at[c, pl.ds(pl.multiple_of(zo * hb, hb), hb)], part_rcv.at[c], psend.at[c], precv.at[c], zpeer)

    def fin_copy(c, zi):
        return remote(fin.at[c], g_at(c, z), fsend.at[c, zi], frecv.at[c, z], (zi, d, lax.max(p - 1, 0)))

    def compute(c):
        @pl.when(p < last)
        def _():
            for zi in range(n_model):
                pltpu.make_async_copy(fin.at[c], g_at(c, zi), frecv.at[c, zi]).wait()
        at = pl.ds(pl.multiple_of(c * rb, rb), rb)
        grad_hid = mm(gg[at, :], wd_bf[...], NT)
        dz_own[at, :] = (slope[at, :] * grad_hid).astype(BF16)

        @pl.when(p > 0)
        def _():
            part[c] = mm(dz_own[at, :], wu_bf[...], NT)
            part_copy(c).start()

    def finalize(c):
        part_copy(c).wait_recv()
        at = pl.ds(pl.multiple_of(c * rb + z * hb, hb), hb)
        total = part[c, pl.ds(pl.multiple_of(z * hb, hb), hb), :] + part_rcv[c]
        fin[c] = (gg[at, :].astype(F32) + total).astype(BF16)
        for zi in range(n_model):
            fin_copy(c, zi).start()

    def chain(i, carry):
        @pl.when(i < nb)
        def _():
            compute(i)

        @pl.when((i >= 1) & (p > 0))
        def _():
            finalize(i - 1)
        return carry
    lax.fori_loop(0, nb + 1, chain, 0)

    def down_block(j, base):
        at = pl.ds(pl.multiple_of(base * half + j * 128, 128), 128)
        return mm(h_own[:, at], gg[mine, :], TN)

    def up_block(j, ff_at):
        at = pl.ds(pl.multiple_of(j * 128, 128), 128)
        return mm(aa[mine, at], dz_own[:, ff_at], TN)

    @pl.when(by_sums)
    def _():
        gd_load.wait()

        def down_oth(j, carry):
            gd_oth[pl.ds(pl.multiple_of(j * 128, 128), 128), :] += down_block(j, do)
            return carry
        lax.fori_loop(0, half // 128, down_oth, 0)
        gu_load.wait()
        sum_gd.start()

        def up_oth(j, carry):
            gu_oth[pl.ds(pl.multiple_of(j * 128, 128), 128), :] += up_block(j, oth_ff)
            return carry
        lax.fori_loop(0, width // 128, up_oth, 0)

    @pl.when(by_rows)
    def _():
        send_g.start()
    loads[3].wait()
    loads[4].wait()

    def down_own(j, carry):
        gd_own[pl.ds(pl.multiple_of(j * 128, 128), 128), :] += down_block(j, d)
        return carry
    lax.fori_loop(0, half // 128, down_own, 0)

    @pl.when(by_sums)
    def _():
        sum_gu.start()

    def up_own(j, carry):
        gu_own[pl.ds(pl.multiple_of(j * 128, 128), 128), :] += up_block(j, own_ff)
        return carry
    lax.fori_loop(0, width // 128, up_own, 0)

    @pl.when(by_rows)
    def _():
        send_acts.wait_recv()

        def oth_pre(i, carry):
            at = pl.ds(pl.multiple_of(i * rb, rb), rb)
            val, slp = gelu_both(mm(aa[pl.ds(pl.multiple_of(rows + i * rb, rb), rb), :], wu_bf[:, own_ff], NN))
            hid_o[at, :] = val.astype(BF16)
            slope_o[at, :] = slp
            return carry
        lax.fori_loop(0, nb, oth_pre, 0)
        send_g.wait_recv()

        def oth_dz(i, carry):
            at = pl.ds(pl.multiple_of(i * rb, rb), rb)
            grad_hid = mm(gg[pl.ds(pl.multiple_of(rows + i * rb, rb), rb), :], wd_bf[own_ff, :], NT)
            dz_o[at, :] = (slope_o[at, :] * grad_hid).astype(BF16)
            return carry
        lax.fori_loop(0, nb, oth_dz, 0)

        def oth_grads(j, carry):
            at = pl.ds(pl.multiple_of(j * 128, 128), 128)
            gd_own[at, :] += mm(hid_o[:, at], gg[theirs, :], TN)
            gu_own[at, :] += mm(aa[theirs, at], dz_o[...], TN)
            return carry
        lax.fori_loop(0, half // 128, oth_grads, 0)

    def combine(own, rcv):
        def body(i, acc):
            at = pl.ds(pl.multiple_of(i * 32, 32), 32)
            mean = (own[at, :] + rcv[at, :]) * 0.5
            own[at, :] = mean
            return acc + jnp.sum((mean * mean).reshape(4, 8, mean.shape[1]), axis=0)
        return body

    def combine_up(acc):
        raw_gu.wait_recv()
        return lax.fori_loop(0, gu_own.shape[0] // 32, combine(gu_own, gu_rcv), acc)

    def combine_down(acc):
        raw_gd.wait_recv()
        return lax.fori_loop(0, gd_own.shape[0] // 32, combine(gd_own, gd_rcv), acc)
    acc = jnp.zeros((8, half), F32)
    acc = combine_down(acc)
    store_d = pltpu.make_async_copy(gd_own, gbd_hbm, st_sem.at[1])
    store_d.start()
    store_early = pltpu.make_async_copy(gd_own.at[pl.ds(0, early_hbm.shape[0])], early_hbm, st_sem.at[2])
    store_early.start()
    acc = combine_up(acc)
    store_u = pltpu.make_async_copy(gu_own, gbu_hbm, st_sem.at[0])
    store_u.start()
    tile = acc[:, 0:128]
    for k in range(1, half // 128):
        tile = tile + acc[:, k * 128:(k + 1) * 128]
    n_all = n_model * n_data * n_stage
    my_id = (z * n_data + d) * n_stage + p
    norm_buf[my_id] = tile

    def norm_copy(k):
        peer = lax.rem(my_id + k, n_all)
        device = (peer // (n_data * n_stage), lax.rem(peer // n_stage, n_data), lax.rem(peer, n_stage))
        return remote(norm_buf.at[my_id], norm_buf.at[my_id], nsend.at[k], nrecv.at[my_id], device)
    for k in range(1, n_all):
        norm_copy(k).start()
    for k in range(1, n_all):
        peer = lax.rem(my_id + k, n_all)
        pltpu.make_async_copy(norm_buf.at[peer], norm_buf.at[peer], nrecv.at[peer]).wait()
    total = norm_buf[0]
    for k in range(1, n_all):
        total = total + norm_buf[k]
    norm_out[...] = total

    for k in range(1, n_all):
        norm_copy(k).wait_send()

    @pl.when(by_rows)
    def _():
        for copy in (send_acts, raw_gu, raw_gd, send_g):
            copy.wait_send()

    @pl.when(by_sums)
    def _():
        sum_gu.wait_send()
        sum_gd.wait_send()

    @pl.when(p > 0)
    def _():
        for c in range(nb):
            part_copy(c).wait_send()
            for zi in range(n_model):
                fin_copy(c, zi).wait_send()
    store_u.wait()
    store_d.wait()
    store_early.wait()


def update_kernel(d_ref, lr_ref, mn_ref, norm_ref, gu, gd, wu, wd, mu, md, vu, vd, *rest):
    owu, owd, omu, omd, ovu, ovd = rest[:6]
    clip = clip_of(norm_ref[...], mn_ref[0])
    rate = lr_ref[0]
    owu[...], omu[...], ovu[...] = adamw_update(wu[...], mu[...], vu[...], clip * gu[...], rate)
    owd[...], omd[...], ovd[...] = adamw_update(wd[...], md[...], vd[...], clip * gd[...], rate)
    if len(rest) == 8:
        rest[6][...] = owu[...].astype(BF16)
        rest[7][...] = owd[...].astype(BF16)


def fill_kernel(d_ref, lr_ref, mn_ref, norm_ref, gu, gd_early, gd_late, y_in, wu, wd, mu, md, vu, vd, *rest):
    owu, owd, omu, omd, ovu, ovd, y_out = rest[6:]
    clip = clip_of(norm_ref[...], mn_ref[0])
    rate = lr_ref[0]
    gd = jnp.where(pl.program_id(0) < EARLY_ROWS // UPD_ROWS, gd_early[...], gd_late[...])
    owu[...], omu[...], ovu[...] = adamw_update(wu[...], mu[...], vu[...], clip * gu[...], rate)
    owd[...], omd[...], ovd[...] = adamw_update(wd[...], md[...], vd[...], clip * gd, rate)
    y_out[...] = y_in[...]


def fwd_kernel(dims, bu_hbm, bd_hbm, gbu_hbm, gbd_hbm, x_hbm,
               gu_oth, gd_oth, y_hbm,
               wu_bf, wd_bf, wu_z, wd_z, a_buf, y_buf, part, part_rcv, fin,
               ld_sem, ysend, yrecv, zsend, zrecv, psend, precv, fsend, frecv, agsend, agrecv, outsend, outrecv, turn):
    n_model, n_data, n_stage = dims
    z, d, p = lax.axis_index('model'), lax.axis_index('data'), lax.axis_index('stage')
    zo, do = 1 - z, 1 - d
    ypeer, zpeer = (z, do, p), (zo, d, p)
    last = n_stage - 1
    nc, rb, width = a_buf.shape
    half = wu_bf.shape[1] // 2
    hb = rb // 2
    own_ff = pl.ds(pl.multiple_of(d * half, 128), half)
    oth_ff = pl.ds(pl.multiple_of(do * half, 128), half)
    first = (p == 0) | (p == last)
    partner = (z, d, p + 1 - 2 * lax.rem(p, 2))

    load_u = pltpu.make_async_copy(bu_hbm, wu_bf.at[:, own_ff], ld_sem.at[0])
    load_d = pltpu.make_async_copy(bd_hbm, wd_bf.at[own_ff, :], ld_sem.at[1])
    load_u.start()
    load_d.start()
    x_load = pltpu.make_async_copy(x_hbm, a_buf, ld_sem.at[2])

    @pl.when(p == 0)
    def _():
        x_load.start()
    whole_barrier(n_model, n_data, n_stage)

    send_wu = remote(wu_bf.at[:, own_ff], wu_bf.at[:, own_ff], ysend.at[0], yrecv.at[0], ypeer)
    send_wd = remote(wd_bf.at[own_ff, :], wd_bf.at[own_ff, :], ysend.at[1], yrecv.at[1], ypeer)
    send_gu = remote(gbu_hbm, gu_oth, ysend.at[2], yrecv.at[2], ypeer)
    send_gd = remote(gbd_hbm.at[pl.ds(half - gd_oth.shape[0], gd_oth.shape[0])], gd_oth, ysend.at[3], yrecv.at[3], ypeer)
    load_u.wait()
    load_d.wait()

    shard = [
        remote(wu_bf.at[:, own_ff], wu_z.at[:, own_ff], zsend.at[0], zrecv.at[0], zpeer),
        remote(wd_bf.at[own_ff, :], wd_z.at[own_ff, :], zsend.at[1], zrecv.at[1], zpeer),
        remote(wu_bf.at[:, oth_ff], wu_z.at[:, oth_ff], zsend.at[2], zrecv.at[2], zpeer),
        remote(wd_bf.at[oth_ff, :], wd_z.at[oth_ff, :], zsend.at[3], zrecv.at[3], zpeer),
    ]

    @pl.when(p == last)
    def _():
        shard[0].start()
        shard[1].start()

    @pl.when(first)
    def _():
        send_wu.start()
        send_wd.start()
        send_wu.wait_send()
        send_wd.wait_send()
        pl.semaphore_signal(turn, inc=1, device_id=partner, device_id_type=MESH)

    @pl.when(jnp.logical_not(first))
    def _():
        pl.semaphore_wait(turn, 1)
        send_wu.start()
        send_wd.start()
        send_gu.start()
        send_gd.start()
        send_wu.wait_send()
        send_wd.wait_send()
        pl.semaphore_signal(turn, inc=1, device_id=partner, device_id_type=MESH)

    @pl.when(p == 0)
    def _():
        x_load.wait()
    send_wu.wait_recv()

    @pl.when(p == last)
    def _():
        shard[2].start()
    send_wd.wait_recv()

    @pl.when(p == last)
    def _():
        shard[3].start()
        for copy in shard:
            copy.wait_recv()

    def half_rows(zi):
        return pl.ds(pl.multiple_of(zi * hb, hb), hb)

    def part_copy(c):
        return remote(part.at[c, half_rows(zo)], part_rcv.at[c], psend.at[c], precv.at[c], zpeer)

    def fin_copy(c, zi):
        return remote(fin.at[c], a_buf.at[c, half_rows(z)], fsend.at[c, zi], frecv.at[c, z], (zi, d, lax.min(p + 1, last)))

    def gather_copy(c):
        return remote(fin.at[c], y_buf.at[c, half_rows(z)], agsend.at[c], agrecv.at[c], zpeer)

    def out_copy(c, q):
        return remote(y_buf.at[c], y_hbm.at[c], outsend.at[c, q], outrecv.at[c], (z, d, q))

    def out_local(c):
        return pltpu.make_async_copy(y_buf.at[c], y_hbm.at[c], outsend.at[c, last])

    def arrived(c, zi):
        pltpu.make_async_copy(fin.at[c], a_buf.at[c, half_rows(zi)], frecv.at[c, zi]).wait()

    def branch(rows_in, w_up, w_down):
        hid = gelu_val(mm(rows_in, w_up[...], NN)).astype(BF16)
        return mm(hid, w_down[...], NN)

    def compute(c):
        @pl.when(p < last)
        def _():
            @pl.when(p > 0)
            def _():
                for zi in range(n_model):
                    arrived(c, zi)
            part[c] = branch(a_buf[c], wu_bf, wd_bf)
            part_copy(c).start()

        @pl.when(p == last)
        def _():
            arrived(c, z)
            at = half_rows(z)
            rows_in = a_buf[c, at, :]
            total = branch(rows_in, wu_bf, wd_bf) + branch(rows_in, wu_z, wd_z)
            new = (rows_in.astype(F32) + total).astype(BF16)
            fin[c] = new
            y_buf[c, at, :] = new
            gather_copy(c).start()

    def finalize(c):
        part_copy(c).wait_recv()
        total = part[c, half_rows(z), :] + part_rcv[c]
        fin[c] = (a_buf[c, half_rows(z), :].astype(F32) + total).astype(BF16)
        fin_copy(c, z).start()

        @pl.when(p < last - 1)
        def _():
            fin_copy(c, zo).start()

    def publish(c):
        gather_copy(c).wait_recv()
        out_local(c).start()
        for q in range(last):
            out_copy(c, q).start()

    def chain(i, carry):
        @pl.when(i < nc)
        def _():
            compute(i)

        @pl.when((i >= 1) & (i <= nc) & (p < last))
        def _():
            finalize(i - 1)

        @pl.when((i >= 1) & (i <= nc) & (p == last))
        def _():
            publish(i - 1)

        @pl.when((i == TURN_STEP) & first)
        def _():
            pl.semaphore_wait(turn, 1)
            send_gu.start()
            send_gd.start()
        return carry
    lax.fori_loop(0, nc + 1, chain, 0)

    def drain(c, carry):
        @pl.when(p < last)
        def _():
            part_copy(c).wait_send()
            fin_copy(c, z).wait_send()

            @pl.when(p < last - 1)
            def _():
                fin_copy(c, zo).wait_send()
            pltpu.make_async_copy(y_buf.at[c], y_hbm.at[c], outrecv.at[c]).wait()

        @pl.when(p == last)
        def _():
            gather_copy(c).wait_send()
            out_local(c).wait()
            for q in range(last):
                out_copy(c, q).wait_send()
        return carry
    lax.fori_loop(0, nc, drain, 0)

    @pl.when(p == last)
    def _():
        for copy in shard:
            copy.wait_send()
    send_gu.wait()
    send_gd.wait()


def solution(mesh):
    n_model, n_data, n_stage = (mesh.shape[k] for k in ('model', 'data', 'stage'))
    dims = (n_model, n_data, n_stage)
    n_all = n_model * n_data * n_stage
    up_spec = P('stage', None, 'model')
    down_spec = P('stage', 'model', None)
    row_spec = P(None, 'data', None)
    in_specs = (up_spec, down_spec, up_spec, down_spec, up_spec, down_spec, P('data', 'stage', None, 'model'), P('data', 'stage', 'model', None), P('stage', 'data', None), P('data', None), row_spec, P(None), P(None))
    out_specs = (up_spec, down_spec, up_spec, down_spec, up_spec, down_spec, row_spec)
    any_spec = pl.BlockSpec(memory_space=pl.ANY)
    vmem_spec = pl.BlockSpec(memory_space=pltpu.VMEM)
    smem_spec = pl.BlockSpec(memory_space=pltpu.SMEM)
    dma = pltpu.SemaphoreType.DMA

    def device_step(w_up, w_down, m_up, m_down, v_up, v_down, g_up, g_down, acts_last, grad_out, x_next, learn_rate, max_norm):
        rows, width = grad_out.shape
        ff = w_up.shape[2]
        half = ff // 2
        nb = rows // BACK_ROWS
        hb = BACK_ROWS // 2
        sds = jax.ShapeDtypeStruct
        gbar_u, gbar_d, early, norm_tile = pl.pallas_call(
            functools.partial(bwd_kernel, dims),
            out_shape=(sds((width, half), F32), sds((half, width), F32), sds((EARLY_ROWS, width), F32), sds((8, 128), F32)),
            in_specs=[any_spec] * 6,
            out_specs=(any_spec, any_spec, any_spec, vmem_spec),
            scratch_shapes=[
                pltpu.VMEM((width, ff), F32), pltpu.VMEM((ff, width), F32),
                pltpu.VMEM((width, ff), BF16), pltpu.VMEM((ff, width), BF16),
                pltpu.VMEM((2 * rows, width), BF16), pltpu.VMEM((2 * rows, width), BF16),
                pltpu.VMEM((rows, half), BF16), pltpu.VMEM((rows, half), BF16),
                pltpu.VMEM((rows, ff), F32), pltpu.VMEM((rows, half), F32),
                pltpu.VMEM((rows, ff), BF16), pltpu.VMEM((rows, ff), BF16),
            ] + [pltpu.VMEM((width, half), F32), pltpu.VMEM((half, width), F32)] * 3 + [
                pltpu.VMEM((nb, BACK_ROWS, width), F32), pltpu.VMEM((nb, hb, width), F32),
                pltpu.VMEM((nb, hb, width), BF16), pltpu.VMEM((n_all, 8, 128), F32),
                dma((8,)), dma((4,)), dma((4,)), dma((nb,)), dma((nb,)), dma((nb, 2)), dma((nb, 2)),
                dma((n_all,)), dma((n_all,)), dma((3,)),
            ],
            compiler_params=pltpu.CompilerParams(collective_id=0, has_side_effects=True, vmem_limit_bytes=VMEM_LIMIT),
            name='backward',
        )(w_up[0], w_down[0], acts_last[0], grad_out, g_up[0, 0], g_down[0, 0])

        early_oth = lax.ppermute(early, 'data', [(k, 1 - k) for k in range(n_data)])
        blocks = half // UPD_ROWS
        state = (w_up[0], w_down[0], m_up[0], m_down[0], v_up[0], v_down[0])
        state_shapes = tuple(sds(s.shape, F32) for s in state)
        which = lax.axis_index('data').astype(jnp.int32).reshape(1)

        def update_specs(pick):
            up = pl.BlockSpec((UPD_ROWS, half), lambda i, w: (i, pick(w[0])))
            down = pl.BlockSpec((UPD_ROWS, width), lambda i, w: (pick(w[0]) * blocks + i, 0))
            return [up, down]
        plain_up = pl.BlockSpec((UPD_ROWS, half), lambda i, w: (i, 0))
        plain_down = pl.BlockSpec((UPD_ROWS, width), lambda i, w: (i, 0))
        small = [smem_spec, smem_spec, pl.BlockSpec((8, 128), lambda i, w: (0, 0))]
        own = update_specs(lambda w: w)
        *fresh, b_up, b_down = pl.pallas_call(
            update_kernel,
            out_shape=state_shapes + (sds((width, half), BF16), sds((half, width), BF16)),
            grid_spec=pltpu.PrefetchScalarGridSpec(
                num_scalar_prefetch=1, grid=(width // UPD_ROWS,),
                in_specs=small + [plain_up, plain_down] + own * 3,
                out_specs=own * 3 + [plain_up, plain_down]),
            compiler_params=pltpu.CompilerParams(dimension_semantics=('arbitrary',), vmem_limit_bytes=VMEM_LIMIT),
            name='update_own',
        )(which, learn_rate, max_norm, norm_tile, gbar_u, gbar_d, *state)

        n_micro = x_next.shape[0]
        nc = n_micro * rows // FWD_ROWS
        fb = FWD_ROWS // 2
        gu_oth, gd_oth, y_next = pl.pallas_call(
            functools.partial(fwd_kernel, dims),
            out_shape=(sds((width, half), F32), sds((half - EARLY_ROWS, width), F32), sds((nc, FWD_ROWS, width), BF16)),
            in_specs=[any_spec] * 5,
            out_specs=(any_spec, any_spec, any_spec),
            scratch_shapes=[pltpu.VMEM((width, ff), BF16), pltpu.VMEM((ff, width), BF16)] * 2 + [
                pltpu.VMEM((nc, FWD_ROWS, width), BF16), pltpu.VMEM((nc, FWD_ROWS, width), BF16),
                pltpu.VMEM((nc, FWD_ROWS, width), F32), pltpu.VMEM((nc, fb, width), F32),
                pltpu.VMEM((nc, fb, width), BF16),
                dma((3,)), dma((4,)), dma((4,)), dma((4,)), dma((4,)), dma((nc,)), dma((nc,)), dma((nc, 2)), dma((nc, 2)),
                dma((nc,)), dma((nc,)), dma((nc, n_stage)), dma((nc,)), pltpu.SemaphoreType.REGULAR,
            ],
            compiler_params=pltpu.CompilerParams(collective_id=1, has_side_effects=True, vmem_limit_bytes=VMEM_LIMIT),
            name='forward',
        )(b_up, b_down, gbar_u, gbar_d, x_next.reshape(nc, FWD_ROWS, width))

        other = update_specs(lambda w: 1 - w)
        ne = EARLY_ROWS // UPD_ROWS
        steps = width // UPD_ROWS
        early_spec = pl.BlockSpec((UPD_ROWS, width), lambda i, w: (jnp.minimum(i, ne - 1), 0))
        late_spec = pl.BlockSpec((UPD_ROWS, width), lambda i, w: (jnp.maximum(i - ne, 0), 0))
        y_spec = pl.BlockSpec((nc // steps, FWD_ROWS, width), lambda i, w: (i, 0, 0))
        *filled, y_next = pl.pallas_call(
            fill_kernel,
            out_shape=state_shapes + (sds(y_next.shape, BF16),),
            grid_spec=pltpu.PrefetchScalarGridSpec(
                num_scalar_prefetch=1, grid=(steps,),
                in_specs=small + [plain_up, early_spec, late_spec, y_spec] + other * 3 + [any_spec] * 6,
                out_specs=other * 3 + [y_spec]),
            input_output_aliases={14 + k: k for k in range(6)},
            compiler_params=pltpu.CompilerParams(dimension_semantics=('arbitrary',), vmem_limit_bytes=VMEM_LIMIT),
            name='update_other',
        )(which, learn_rate, max_norm, norm_tile, gu_oth, early_oth, gd_oth, y_next, *state, *fresh)
        return tuple(s[None] for s in filled) + (y_next.reshape(n_micro, rows, width),)

    return jax.shard_map(device_step, mesh=mesh, in_specs=in_specs, out_specs=out_specs, check_vma=False)
```

```python
import functools

import jax
import jax.numpy as jnp
from jax import lax
from jax.experimental import pallas as pl
from jax.experimental.pallas import tpu as pltpu
from jax.sharding import PartitionSpec as P

ADAM_STEP = 10
BETA_ONE = 0.9
BETA_TWO = 0.95
ADAM_EPS = 1e-8
WEIGHT_DECAY = 0.1
NORM_EPS = 1e-6
ONE_CORR = 1.0 - BETA_ONE ** ADAM_STEP
TWO_CORR = 1.0 - BETA_TWO ** ADAM_STEP
GELU_SCALE = (2.0 / 3.141592653589793) ** 0.5
GELU_CUBE = 0.044715
NN = (((1,), (0,)), ((), ()))
NT = (((1,), (1,)), ((), ()))
TN = (((0,), (0,)), ((), ()))
F32 = jnp.float32
BF16 = jnp.bfloat16
MESH = pl.DeviceIdType.MESH
BACK_ROWS = 128
FWD_ROWS = 64
UPD_ROWS = 128
PRE_ROWS = 128
EARLY_ROWS = 256
LATE_ROWS = 128
TURN_STEP = 8
VMEM_LIMIT = 66_000_000


def mm(lhs, rhs, dims):
    return lax.dot_general(lhs, rhs, dims, preferred_element_type=F32)


def gelu_val(pre):
    return pre * (0.5 * (1.0 + jnp.tanh(GELU_SCALE * (pre + GELU_CUBE * (pre * pre * pre)))))


def gelu_both(pre):
    sq = pre * pre
    tan = jnp.tanh(GELU_SCALE * (pre + GELU_CUBE * (sq * pre)))
    cdf = 0.5 * (1.0 + tan)
    slope = cdf + 0.5 * pre * (1.0 - tan * tan) * (GELU_SCALE * (1.0 + (3.0 * GELU_CUBE) * sq))
    return pre * cdf, slope


def adamw_update(weight, moment_one, moment_two, grad_step, step_rate):
    mom_new = BETA_ONE * moment_one + (1.0 - BETA_ONE) * grad_step
    sec_new = BETA_TWO * moment_two + (1.0 - BETA_TWO) * grad_step * grad_step
    direction = (mom_new / ONE_CORR) / (jnp.sqrt(sec_new / TWO_CORR) + ADAM_EPS)
    weight_new = weight - step_rate * (direction + WEIGHT_DECAY * weight)
    return weight_new, mom_new, sec_new


def clip_of(norm_tile, max_norm):
    total = jnp.sum(jnp.sum(norm_tile, axis=0, keepdims=True), axis=1, keepdims=True)
    return jnp.minimum(1.0, max_norm / (jnp.sqrt(total) + NORM_EPS))


def whole_barrier(n_model, n_data, n_stage):
    barrier = pltpu.get_barrier_semaphore()
    me = (lax.axis_index('model'), lax.axis_index('data'), lax.axis_index('stage'))
    for dm in range(n_model):
        for dd in range(n_data):
            for ds in range(n_stage):
                if dm or dd or ds:
                    peer = (lax.rem(me[0] + dm, n_model), lax.rem(me[1] + dd, n_data), lax.rem(me[2] + ds, n_stage))
                    pl.semaphore_signal(barrier, inc=1, device_id=peer, device_id_type=MESH)
    pl.semaphore_wait(barrier, n_model * n_data * n_stage - 1)


def remote(src, dst, send_sem, recv_sem, device):
    return pltpu.make_async_remote_copy(src_ref=src, dst_ref=dst, send_sem=send_sem, recv_sem=recv_sem, device_id=device, device_id_type=MESH)


def bwd_kernel(dims, wu_hbm, wd_hbm, acts_hbm, dy_hbm, gu_hbm, gd_hbm,
               gbu_hbm, gbd_hbm, early_hbm, late_hbm, pre_oth, norm_out,
               wu32, wd32, wu_bf, wd_bf, aa, gg, hid_o, dz_o, slope, slope_o, dz_own, h_own,
               gu_own, gd_own, gu_oth, gd_oth, gu_rcv, gd_rcv, part, part_rcv, fin, norm_buf,
               ld_sem, ysend, yrecv, psend, precv, fsend, frecv, nsend, nrecv, st_sem):
    n_model, n_data, n_stage = dims
    z, d, p = lax.axis_index('model'), lax.axis_index('data'), lax.axis_index('stage')
    zo, do = 1 - z, 1 - d
    ypeer, zpeer = (z, do, p), (zo, d, p)
    last = n_stage - 1
    by_rows = lax.rem(p, 2) == 0
    by_sums = lax.rem(p, 2) == 1
    rows = aa.shape[0] // 2
    width = aa.shape[1]
    half = hid_o.shape[1]
    rb = BACK_ROWS
    hb = rb // 2
    nb = rows // rb
    own_ff = pl.ds(pl.multiple_of(d * half, 128), half)
    oth_ff = pl.ds(pl.multiple_of(do * half, 128), half)
    mine, theirs = pl.ds(0, rows), pl.ds(rows, rows)

    loads = [
        pltpu.make_async_copy(wu_hbm, wu32, ld_sem.at[0]),
        pltpu.make_async_copy(acts_hbm, aa.at[mine], ld_sem.at[2]),
        pltpu.make_async_copy(wd_hbm, wd32, ld_sem.at[1]),
        pltpu.make_async_copy(gu_hbm.at[:, own_ff], gu_own, ld_sem.at[4]),
        pltpu.make_async_copy(gd_hbm.at[own_ff, :], gd_own, ld_sem.at[5]),
    ]
    dy_load = pltpu.make_async_copy(dy_hbm, gg.at[mine], ld_sem.at[3])
    gu_load = pltpu.make_async_copy(gu_hbm.at[:, oth_ff], gu_oth, ld_sem.at[6])
    gd_load = pltpu.make_async_copy(gd_hbm.at[oth_ff, :], gd_oth, ld_sem.at[7])
    for copy in loads[:3]:
        copy.start()

    @pl.when(p == last)
    def _():
        dy_load.start()
    for copy in loads[3:]:
        copy.start()

    @pl.when(by_sums)
    def _():
        gd_load.start()
        gu_load.start()

    whole_barrier(n_model, n_data, n_stage)
    send_acts = remote(acts_hbm, aa.at[theirs], ysend.at[0], yrecv.at[0], ypeer)
    raw_gu = remote(gu_hbm.at[:, oth_ff], gu_rcv, ysend.at[1], yrecv.at[1], ypeer)
    raw_gd = remote(gd_hbm.at[oth_ff, :], gd_rcv, ysend.at[2], yrecv.at[2], ypeer)
    sum_gu = remote(gu_oth, gu_rcv, ysend.at[1], yrecv.at[1], ypeer)
    sum_gd = remote(gd_oth, gd_rcv, ysend.at[2], yrecv.at[2], ypeer)
    send_g = remote(gg.at[mine], gg.at[theirs], ysend.at[3], yrecv.at[3], ypeer)

    @pl.when(by_rows)
    def _():
        send_acts.start()
        raw_gd.start()
        raw_gu.start()

    loads[0].wait()
    loads[1].wait()

    def cast_up(i, carry):
        at = pl.ds(pl.multiple_of(i * 128, 128), 128)
        wu_bf[at, :] = wu32[at, :].astype(BF16)
        return carry
    lax.fori_loop(0, width // 128, cast_up, 0)

    def own_pre(i, carry):
        at = pl.ds(pl.multiple_of(i * rb, rb), rb)
        val, slp = gelu_both(mm(aa[at, :], wu_bf[...], NN))
        h_own[at, :] = val.astype(BF16)
        slope[at, :] = slp
        return carry
    lax.fori_loop(0, nb, own_pre, 0)
    loads[2].wait()

    def cast_down(i, carry):
        at = pl.ds(pl.multiple_of(i * 128, 128), 128)
        wd_bf[at, :] = wd32[at, :].astype(BF16)
        return carry
    lax.fori_loop(0, 2 * half // 128, cast_down, 0)

    @pl.when(p == last)
    def _():
        dy_load.wait()

    def g_at(c, zi):
        return gg.at[pl.ds(pl.multiple_of(c * rb + zi * hb, hb), hb)]

    def part_copy(c):
        return remote(part.at[c, pl.ds(pl.multiple_of(zo * hb, hb), hb)], part_rcv.at[c], psend.at[c], precv.at[c], zpeer)

    def fin_copy(c, zi):
        return remote(fin.at[c], g_at(c, z), fsend.at[c, zi], frecv.at[c, z], (zi, d, lax.max(p - 1, 0)))

    def compute(c):
        @pl.when(p < last)
        def _():
            for zi in range(n_model):
                pltpu.make_async_copy(fin.at[c], g_at(c, zi), frecv.at[c, zi]).wait()
        at = pl.ds(pl.multiple_of(c * rb, rb), rb)
        grad_hid = mm(gg[at, :], wd_bf[...], NT)
        dz_own[at, :] = (slope[at, :] * grad_hid).astype(BF16)

        @pl.when(p > 0)
        def _():
            part[c] = mm(dz_own[at, :], wu_bf[...], NT)
            part_copy(c).start()

    def finalize(c):
        part_copy(c).wait_recv()
        at = pl.ds(pl.multiple_of(c * rb + z * hb, hb), hb)
        total = part[c, pl.ds(pl.multiple_of(z * hb, hb), hb), :] + part_rcv[c]
        fin[c] = (gg[at, :].astype(F32) + total).astype(BF16)
        for zi in range(n_model):
            fin_copy(c, zi).start()

    def chain(i, carry):
        @pl.when(i < nb)
        def _():
            compute(i)

        @pl.when((i >= 1) & (p > 0))
        def _():
            finalize(i - 1)
        return carry
    lax.fori_loop(0, nb + 1, chain, 0)

    def down_block(j, base):
        at = pl.ds(pl.multiple_of(base * half + j * 128, 128), 128)
        return mm(h_own[:, at], gg[mine, :], TN)

    def up_block(j, ff_at):
        at = pl.ds(pl.multiple_of(j * 128, 128), 128)
        return mm(aa[mine, at], dz_own[:, ff_at], TN)

    @pl.when(by_sums)
    def _():
        gd_load.wait()

        def down_oth(j, carry):
            gd_oth[pl.ds(pl.multiple_of(j * 128, 128), 128), :] += down_block(j, do)
            return carry
        lax.fori_loop(0, half // 128, down_oth, 0)
        gu_load.wait()
        sum_gd.start()

        def up_oth(j, carry):
            gu_oth[pl.ds(pl.multiple_of(j * 128, 128), 128), :] += up_block(j, oth_ff)
            return carry
        lax.fori_loop(0, width // 128, up_oth, 0)

    @pl.when(by_rows)
    def _():
        send_g.start()
    loads[3].wait()
    loads[4].wait()

    def down_own(j, carry):
        gd_own[pl.ds(pl.multiple_of(j * 128, 128), 128), :] += down_block(j, d)
        return carry
    lax.fori_loop(0, half // 128, down_own, 0)

    @pl.when(by_sums)
    def _():
        sum_gu.start()

    def up_own(j, carry):
        gu_own[pl.ds(pl.multiple_of(j * 128, 128), 128), :] += up_block(j, own_ff)
        return carry
    lax.fori_loop(0, width // 128, up_own, 0)

    @pl.when(by_rows)
    def _():
        send_acts.wait_recv()

        def oth_pre(i, carry):
            at = pl.ds(pl.multiple_of(i * rb, rb), rb)
            val, slp = gelu_both(mm(aa[pl.ds(pl.multiple_of(rows + i * rb, rb), rb), :], wu_bf[:, own_ff], NN))
            hid_o[at, :] = val.astype(BF16)
            slope_o[at, :] = slp
            return carry
        lax.fori_loop(0, nb, oth_pre, 0)
        send_g.wait_recv()

        def oth_dz(i, carry):
            at = pl.ds(pl.multiple_of(i * rb, rb), rb)
            grad_hid = mm(gg[pl.ds(pl.multiple_of(rows + i * rb, rb), rb), :], wd_bf[own_ff, :], NT)
            dz_o[at, :] = (slope_o[at, :] * grad_hid).astype(BF16)
            return carry
        lax.fori_loop(0, nb, oth_dz, 0)

        def oth_grads(j, carry):
            at = pl.ds(pl.multiple_of(j * 128, 128), 128)
            gd_own[at, :] += mm(hid_o[:, at], gg[theirs, :], TN)
            gu_own[at, :] += mm(aa[theirs, at], dz_o[...], TN)
            return carry
        lax.fori_loop(0, half // 128, oth_grads, 0)

    def combine(own, rcv):
        def body(i, acc):
            at = pl.ds(pl.multiple_of(i * 32, 32), 32)
            mean = (own[at, :] + rcv[at, :]) * 0.5
            own[at, :] = mean
            return acc + jnp.sum((mean * mean).reshape(4, 8, mean.shape[1]), axis=0)
        return body

    def combine_up(acc):
        raw_gu.wait_recv()
        return lax.fori_loop(0, gu_own.shape[0] // 32, combine(gu_own, gu_rcv), acc)

    def combine_down(acc):
        raw_gd.wait_recv()
        return lax.fori_loop(0, gd_own.shape[0] // 32, combine(gd_own, gd_rcv), acc)
    acc = jnp.zeros((8, half), F32)
    acc = combine_down(acc)
    store_d = pltpu.make_async_copy(gd_own, gbd_hbm, st_sem.at[1])
    store_d.start()
    store_early = pltpu.make_async_copy(gd_own.at[pl.ds(PRE_ROWS, EARLY_ROWS)], early_hbm, st_sem.at[2])
    store_early.start()
    send_pre = remote(gd_own.at[pl.ds(0, PRE_ROWS)], pre_oth, ysend.at[4], yrecv.at[4], ypeer)
    send_pre.start()
    acc = combine_up(acc)
    store_u = pltpu.make_async_copy(gu_own, gbu_hbm, st_sem.at[0])
    store_u.start()
    store_late = pltpu.make_async_copy(gu_own.at[pl.ds(width - LATE_ROWS, LATE_ROWS)], late_hbm, st_sem.at[3])
    store_late.start()
    tile = acc[:, 0:128]
    for k in range(1, half // 128):
        tile = tile + acc[:, k * 128:(k + 1) * 128]
    n_all = n_model * n_data * n_stage
    my_id = (z * n_data + d) * n_stage + p
    norm_buf[my_id] = tile

    def norm_copy(k):
        peer = lax.rem(my_id + k, n_all)
        device = (peer // (n_data * n_stage), lax.rem(peer // n_stage, n_data), lax.rem(peer, n_stage))
        return remote(norm_buf.at[my_id], norm_buf.at[my_id], nsend.at[k], nrecv.at[my_id], device)
    for k in range(1, n_all):
        norm_copy(k).start()
    for k in range(1, n_all):
        peer = lax.rem(my_id + k, n_all)
        pltpu.make_async_copy(norm_buf.at[peer], norm_buf.at[peer], nrecv.at[peer]).wait()
    total = norm_buf[0]
    for k in range(1, n_all):
        total = total + norm_buf[k]
    norm_out[...] = total

    for k in range(1, n_all):
        norm_copy(k).wait_send()

    @pl.when(by_rows)
    def _():
        for copy in (send_acts, raw_gu, raw_gd, send_g):
            copy.wait_send()

    @pl.when(by_sums)
    def _():
        sum_gu.wait_send()
        sum_gd.wait_send()

    @pl.when(p > 0)
    def _():
        for c in range(nb):
            part_copy(c).wait_send()
            for zi in range(n_model):
                fin_copy(c, zi).wait_send()
    store_u.wait()
    store_d.wait()
    store_early.wait()
    store_late.wait()
    send_pre.wait()


def update_kernel(d_ref, lr_ref, mn_ref, norm_ref, gu, gd, wu, wd, mu, md, vu, vd, *rest):
    owu, owd, omu, omd, ovu, ovd = rest[:6]
    clip = clip_of(norm_ref[...], mn_ref[0])
    rate = lr_ref[0]
    owu[...], omu[...], ovu[...] = adamw_update(wu[...], mu[...], vu[...], clip * gu[...], rate)
    owd[...], omd[...], ovd[...] = adamw_update(wd[...], md[...], vd[...], clip * gd[...], rate)
    if len(rest) == 8:
        rest[6][...] = owu[...].astype(BF16)
        rest[7][...] = owd[...].astype(BF16)


def fill_kernel(d_ref, lr_ref, mn_ref, norm_ref, gu, gd_pre, gd_early, gd_rest, y_in, wu, wd, mu, md, vu, vd, *rest):
    owu, owd, omu, omd, ovu, ovd, y_out = rest[6:]
    clip = clip_of(norm_ref[...], mn_ref[0])
    rate = lr_ref[0]
    step = pl.program_id(0)
    gd = jnp.where(step < PRE_ROWS // UPD_ROWS, gd_pre[...], jnp.where(step < (PRE_ROWS + EARLY_ROWS) // UPD_ROWS, gd_early[...], gd_rest[...]))
    owu[...], omu[...], ovu[...] = adamw_update(wu[...], mu[...], vu[...], clip * gu[...], rate)
    owd[...], omd[...], ovd[...] = adamw_update(wd[...], md[...], vd[...], clip * gd, rate)
    y_out[...] = y_in[...]


def late_kernel(d_ref, lr_ref, mn_ref, norm_ref, gu, wu, mu, vu, *rest):
    owu, omu, ovu = rest[3:]
    clip = clip_of(norm_ref[...], mn_ref[0])
    owu[...], omu[...], ovu[...] = adamw_update(wu[...], mu[...], vu[...], clip * gu[...], lr_ref[0])


def fwd_kernel(dims, bu_hbm, bd_hbm, gbu_hbm, gbd_hbm, x_hbm,
               gu_oth, gd_oth, y_hbm,
               wu_bf, wd_bf, wu_z, wd_z, a_buf, y_buf, part, part_rcv, fin,
               ld_sem, ysend, yrecv, zsend, zrecv, psend, precv, fsend, frecv, agsend, agrecv, outsend, outrecv, turn):
    n_model, n_data, n_stage = dims
    z, d, p = lax.axis_index('model'), lax.axis_index('data'), lax.axis_index('stage')
    zo, do = 1 - z, 1 - d
    ypeer, zpeer = (z, do, p), (zo, d, p)
    last = n_stage - 1
    nc, rb, width = a_buf.shape
    half = wu_bf.shape[1] // 2
    hb = rb // 2
    own_ff = pl.ds(pl.multiple_of(d * half, 128), half)
    oth_ff = pl.ds(pl.multiple_of(do * half, 128), half)
    first = (p == 0) | (p == last)
    partner = (z, d, p + 1 - 2 * lax.rem(p, 2))

    load_u = pltpu.make_async_copy(bu_hbm, wu_bf.at[:, own_ff], ld_sem.at[0])
    load_d = pltpu.make_async_copy(bd_hbm, wd_bf.at[own_ff, :], ld_sem.at[1])
    load_u.start()
    load_d.start()
    x_load = pltpu.make_async_copy(x_hbm, a_buf, ld_sem.at[2])

    @pl.when(p == 0)
    def _():
        x_load.start()
    whole_barrier(n_model, n_data, n_stage)

    send_wu = remote(bu_hbm, wu_bf.at[:, own_ff], ysend.at[0], yrecv.at[0], ypeer)
    send_wd = remote(bd_hbm, wd_bf.at[own_ff, :], ysend.at[1], yrecv.at[1], ypeer)
    send_gu = remote(gbu_hbm.at[pl.ds(0, gu_oth.shape[0])], gu_oth, ysend.at[2], yrecv.at[2], ypeer)
    send_gd = remote(gbd_hbm.at[pl.ds(half - gd_oth.shape[0], gd_oth.shape[0])], gd_oth, ysend.at[3], yrecv.at[3], ypeer)

    shard = [
        remote(bu_hbm, wu_z.at[:, own_ff], zsend.at[0], zrecv.at[0], zpeer),
        remote(bd_hbm, wd_z.at[own_ff, :], zsend.at[1], zrecv.at[1], zpeer),
        remote(wu_bf.at[:, oth_ff], wu_z.at[:, oth_ff], zsend.at[2], zrecv.at[2], zpeer),
        remote(wd_bf.at[oth_ff, :], wd_z.at[oth_ff, :], zsend.at[3], zrecv.at[3], zpeer),
    ]

    @pl.when(p == last)
    def _():
        shard[0].start()
        shard[1].start()

    @pl.when(first)
    def _():
        send_wu.start()
        send_wd.start()
        send_wu.wait_send()
        send_wd.wait_send()
        pl.semaphore_signal(turn, inc=1, device_id=partner, device_id_type=MESH)

    @pl.when(jnp.logical_not(first))
    def _():
        pl.semaphore_wait(turn, 1)
        send_wu.start()
        send_wd.start()
        send_gu.start()
        send_gd.start()
        send_wu.wait_send()
        send_wd.wait_send()
        pl.semaphore_signal(turn, inc=1, device_id=partner, device_id_type=MESH)

    @pl.when(p == 0)
    def _():
        x_load.wait()
    load_u.wait()
    load_d.wait()
    send_wu.wait_recv()

    @pl.when(p == last)
    def _():
        shard[2].start()
    send_wd.wait_recv()

    @pl.when(p == last)
    def _():
        shard[3].start()
        for copy in shard:
            copy.wait_recv()

    def half_rows(zi):
        return pl.ds(pl.multiple_of(zi * hb, hb), hb)

    def part_copy(c):
        return remote(part.at[c, half_rows(zo)], part_rcv.at[c], psend.at[c], precv.at[c], zpeer)

    def fin_copy(c, zi):
        return remote(fin.at[c], a_buf.at[c, half_rows(z)], fsend.at[c, zi], frecv.at[c, z], (zi, d, lax.min(p + 1, last)))

    def gather_copy(c):
        return remote(fin.at[c], y_buf.at[c, half_rows(z)], agsend.at[c], agrecv.at[c], zpeer)

    def out_copy(c, q):
        return remote(y_buf.at[c], y_hbm.at[c], outsend.at[c, q], outrecv.at[c], (z, d, q))

    def out_local(c):
        return pltpu.make_async_copy(y_buf.at[c], y_hbm.at[c], outsend.at[c, last])

    def arrived(c, zi):
        pltpu.make_async_copy(fin.at[c], a_buf.at[c, half_rows(zi)], frecv.at[c, zi]).wait()

    def branch(rows_in, w_up, w_down):
        hid = gelu_val(mm(rows_in, w_up[...], NN)).astype(BF16)
        return mm(hid, w_down[...], NN)

    def compute(c):
        @pl.when(p < last)
        def _():
            @pl.when(p > 0)
            def _():
                for zi in range(n_model):
                    arrived(c, zi)
            part[c] = branch(a_buf[c], wu_bf, wd_bf)
            part_copy(c).start()

        @pl.when(p == last)
        def _():
            arrived(c, z)
            at = half_rows(z)
            rows_in = a_buf[c, at, :]
            total = branch(rows_in, wu_bf, wd_bf) + branch(rows_in, wu_z, wd_z)
            new = (rows_in.astype(F32) + total).astype(BF16)
            fin[c] = new
            y_buf[c, at, :] = new
            gather_copy(c).start()

    def finalize(c):
        part_copy(c).wait_recv()
        total = part[c, half_rows(z), :] + part_rcv[c]
        fin[c] = (a_buf[c, half_rows(z), :].astype(F32) + total).astype(BF16)
        fin_copy(c, z).start()

        @pl.when(p < last - 1)
        def _():
            fin_copy(c, zo).start()

    def publish(c):
        gather_copy(c).wait_recv()
        out_local(c).start()
        for q in range(last):
            out_copy(c, q).start()

    def chain(i, carry):
        @pl.when(i < nc)
        def _():
            compute(i)

        @pl.when((i >= 1) & (i <= nc) & (p < last))
        def _():
            finalize(i - 1)

        @pl.when((i >= 1) & (i <= nc) & (p == last))
        def _():
            publish(i - 1)

        @pl.when((i == TURN_STEP) & first)
        def _():
            pl.semaphore_wait(turn, 1)
            send_gu.start()
            send_gd.start()
        return carry
    lax.fori_loop(0, nc + 1, chain, 0)

    def drain(c, carry):
        @pl.when(p < last)
        def _():
            part_copy(c).wait_send()
            fin_copy(c, z).wait_send()

            @pl.when(p < last - 1)
            def _():
                fin_copy(c, zo).wait_send()
            pltpu.make_async_copy(y_buf.at[c], y_hbm.at[c], outrecv.at[c]).wait()

        @pl.when(p == last)
        def _():
            gather_copy(c).wait_send()
            out_local(c).wait()
            for q in range(last):
                out_copy(c, q).wait_send()
        return carry
    lax.fori_loop(0, nc, drain, 0)

    @pl.when(p == last)
    def _():
        for copy in shard:
            copy.wait_send()
    send_gu.wait()
    send_gd.wait()


def solution(mesh):
    n_model, n_data, n_stage = (mesh.shape[k] for k in ('model', 'data', 'stage'))
    dims = (n_model, n_data, n_stage)
    n_all = n_model * n_data * n_stage
    up_spec = P('stage', None, 'model')
    down_spec = P('stage', 'model', None)
    row_spec = P(None, 'data', None)
    in_specs = (up_spec, down_spec, up_spec, down_spec, up_spec, down_spec, P('data', 'stage', None, 'model'), P('data', 'stage', 'model', None), P('stage', 'data', None), P('data', None), row_spec, P(None), P(None))
    out_specs = (up_spec, down_spec, up_spec, down_spec, up_spec, down_spec, row_spec)
    any_spec = pl.BlockSpec(memory_space=pl.ANY)
    vmem_spec = pl.BlockSpec(memory_space=pltpu.VMEM)
    smem_spec = pl.BlockSpec(memory_space=pltpu.SMEM)
    dma = pltpu.SemaphoreType.DMA

    def device_step(w_up, w_down, m_up, m_down, v_up, v_down, g_up, g_down, acts_last, grad_out, x_next, learn_rate, max_norm):
        rows, width = grad_out.shape
        ff = w_up.shape[2]
        half = ff // 2
        nb = rows // BACK_ROWS
        hb = BACK_ROWS // 2
        sds = jax.ShapeDtypeStruct
        gbar_u, gbar_d, early, late, pre_oth, norm_tile = pl.pallas_call(
            functools.partial(bwd_kernel, dims),
            out_shape=(sds((width, half), F32), sds((half, width), F32), sds((EARLY_ROWS, width), F32), sds((LATE_ROWS, half), F32), sds((PRE_ROWS, width), F32), sds((8, 128), F32)),
            in_specs=[any_spec] * 6,
            out_specs=(any_spec,) * 5 + (vmem_spec,),
            scratch_shapes=[
                pltpu.VMEM((width, ff), F32), pltpu.VMEM((ff, width), F32),
                pltpu.VMEM((width, ff), BF16), pltpu.VMEM((ff, width), BF16),
                pltpu.VMEM((2 * rows, width), BF16), pltpu.VMEM((2 * rows, width), BF16),
                pltpu.VMEM((rows, half), BF16), pltpu.VMEM((rows, half), BF16),
                pltpu.VMEM((rows, ff), F32), pltpu.VMEM((rows, half), F32),
                pltpu.VMEM((rows, ff), BF16), pltpu.VMEM((rows, ff), BF16),
            ] + [pltpu.VMEM((width, half), F32), pltpu.VMEM((half, width), F32)] * 3 + [
                pltpu.VMEM((nb, BACK_ROWS, width), F32), pltpu.VMEM((nb, hb, width), F32),
                pltpu.VMEM((nb, hb, width), BF16), pltpu.VMEM((n_all, 8, 128), F32),
                dma((8,)), dma((5,)), dma((5,)), dma((nb,)), dma((nb,)), dma((nb, 2)), dma((nb, 2)),
                dma((n_all,)), dma((n_all,)), dma((4,)),
            ],
            compiler_params=pltpu.CompilerParams(collective_id=0, has_side_effects=True, vmem_limit_bytes=VMEM_LIMIT),
            name='backward',
        )(w_up[0], w_down[0], acts_last[0], grad_out, g_up[0, 0], g_down[0, 0])

        early_oth = lax.ppermute(early, 'data', [(k, 1 - k) for k in range(n_data)])
        blocks = half // UPD_ROWS
        state = (w_up[0], w_down[0], m_up[0], m_down[0], v_up[0], v_down[0])
        state_shapes = tuple(sds(s.shape, F32) for s in state)
        which = lax.axis_index('data').astype(jnp.int32).reshape(1)

        def update_specs(pick):
            up = pl.BlockSpec((UPD_ROWS, half), lambda i, w: (i, pick(w[0])))
            down = pl.BlockSpec((UPD_ROWS, width), lambda i, w: (pick(w[0]) * blocks + i, 0))
            return [up, down]
        plain_up = pl.BlockSpec((UPD_ROWS, half), lambda i, w: (i, 0))
        plain_down = pl.BlockSpec((UPD_ROWS, width), lambda i, w: (i, 0))
        small = [smem_spec, smem_spec, pl.BlockSpec((8, 128), lambda i, w: (0, 0))]
        own = update_specs(lambda w: w)
        *fresh, b_up, b_down = pl.pallas_call(
            update_kernel,
            out_shape=state_shapes + (sds((width, half), BF16), sds((half, width), BF16)),
            grid_spec=pltpu.PrefetchScalarGridSpec(
                num_scalar_prefetch=1, grid=(width // UPD_ROWS,),
                in_specs=small + [plain_up, plain_down] + own * 3,
                out_specs=own * 3 + [plain_up, plain_down]),
            compiler_params=pltpu.CompilerParams(dimension_semantics=('arbitrary',), vmem_limit_bytes=VMEM_LIMIT),
            name='update_own',
        )(which, learn_rate, max_norm, norm_tile, gbar_u, gbar_d, *state)

        n_micro = x_next.shape[0]
        nc = n_micro * rows // FWD_ROWS
        fb = FWD_ROWS // 2
        gu_oth, gd_oth, y_next = pl.pallas_call(
            functools.partial(fwd_kernel, dims),
            out_shape=(sds((width - LATE_ROWS, half), F32), sds((half - PRE_ROWS - EARLY_ROWS, width), F32), sds((nc, FWD_ROWS, width), BF16)),
            in_specs=[any_spec] * 5,
            out_specs=(any_spec, any_spec, any_spec),
            scratch_shapes=[pltpu.VMEM((width, ff), BF16), pltpu.VMEM((ff, width), BF16)] * 2 + [
                pltpu.VMEM((nc, FWD_ROWS, width), BF16), pltpu.VMEM((nc, FWD_ROWS, width), BF16),
                pltpu.VMEM((nc, FWD_ROWS, width), F32), pltpu.VMEM((nc, fb, width), F32),
                pltpu.VMEM((nc, fb, width), BF16),
                dma((3,)), dma((4,)), dma((4,)), dma((4,)), dma((4,)), dma((nc,)), dma((nc,)), dma((nc, 2)), dma((nc, 2)),
                dma((nc,)), dma((nc,)), dma((nc, n_stage)), dma((nc,)), pltpu.SemaphoreType.REGULAR,
            ],
            compiler_params=pltpu.CompilerParams(collective_id=1, has_side_effects=True, vmem_limit_bytes=VMEM_LIMIT),
            name='forward',
        )(b_up, b_down, gbar_u, gbar_d, x_next.reshape(nc, FWD_ROWS, width))

        other = update_specs(lambda w: 1 - w)
        gu_oth, late = lax.optimization_barrier((gu_oth, late))
        late_oth = lax.ppermute(late, 'data', [(k, 1 - k) for k in range(n_data)])
        npre, nearly, nlate = PRE_ROWS // UPD_ROWS, EARLY_ROWS // UPD_ROWS, LATE_ROWS // UPD_ROWS
        steps = width // UPD_ROWS
        lastup = steps - nlate - 1

        def rows_spec(start, count):
            return pl.BlockSpec((UPD_ROWS, width), lambda i, w: (jnp.clip(i - start, 0, count - 1), 0))
        y_spec = pl.BlockSpec((nc // steps, FWD_ROWS, width), lambda i, w: (i, 0, 0))
        up_oth = pl.BlockSpec((UPD_ROWS, half), lambda i, w: (jnp.minimum(i, lastup), 1 - w[0]))
        down_oth = pl.BlockSpec((UPD_ROWS, width), lambda i, w: ((1 - w[0]) * blocks + i, 0))
        other = [up_oth, down_oth]
        *filled, y_next = pl.pallas_call(
            fill_kernel,
            out_shape=state_shapes + (sds(y_next.shape, BF16),),
            grid_spec=pltpu.PrefetchScalarGridSpec(
                num_scalar_prefetch=1, grid=(steps,),
                in_specs=small + [rows_spec(0, lastup + 1), rows_spec(0, npre), rows_spec(npre, nearly), rows_spec(npre + nearly, blocks - npre - nearly), y_spec] + other * 3 + [any_spec] * 6,
                out_specs=other * 3 + [y_spec]),
            input_output_aliases={15 + k: k for k in range(6)},
            compiler_params=pltpu.CompilerParams(dimension_semantics=('arbitrary',), vmem_limit_bytes=VMEM_LIMIT),
            cost_estimate=pl.CostEstimate(flops=10**10, bytes_accessed=40 * 10**6, transcendentals=0),
            name='update_other',
        )(which, learn_rate, max_norm, norm_tile, gu_oth, pre_oth, early_oth, gd_oth, y_next, *state, *fresh)
        up_late = pl.BlockSpec((UPD_ROWS, half), lambda i, w: (steps - nlate + i, 1 - w[0]))
        filled[0], filled[2], filled[4] = pl.pallas_call(
            late_kernel,
            out_shape=(state_shapes[0],) * 3,
            grid_spec=pltpu.PrefetchScalarGridSpec(
                num_scalar_prefetch=1, grid=(nlate,),
                in_specs=small + [plain_up] + [up_late] * 3 + [any_spec] * 3,
                out_specs=[up_late] * 3),
            input_output_aliases={8 + k: k for k in range(3)},
            compiler_params=pltpu.CompilerParams(dimension_semantics=('arbitrary',), vmem_limit_bytes=VMEM_LIMIT),
            name='update_late',
        )(which, learn_rate, max_norm, norm_tile, late_oth, state[0], state[2], state[4], filled[0], filled[2], filled[4])
        return tuple(s[None] for s in filled) + (y_next.reshape(n_micro, rows, width),)

    return jax.shard_map(device_step, mesh=mesh, in_specs=in_specs, out_specs=out_specs, check_vma=False)
```

```python
import functools

import jax
import jax.numpy as jnp
from jax import lax
from jax.experimental import pallas as pl
from jax.experimental.pallas import tpu as pltpu
from jax.sharding import PartitionSpec as P

ADAM_STEP = 10
BETA_ONE = 0.9
BETA_TWO = 0.95
ADAM_EPS = 1e-8
WEIGHT_DECAY = 0.1
NORM_EPS = 1e-6
ONE_CORR = 1.0 - BETA_ONE ** ADAM_STEP
TWO_CORR = 1.0 - BETA_TWO ** ADAM_STEP
GELU_SCALE = (2.0 / 3.141592653589793) ** 0.5
GELU_CUBE = 0.044715
NN = (((1,), (0,)), ((), ()))
NT = (((1,), (1,)), ((), ()))
TN = (((0,), (0,)), ((), ()))
F32 = jnp.float32
BF16 = jnp.bfloat16
MESH = pl.DeviceIdType.MESH
BACK_ROWS = 128
FWD_ROWS = 96
UPD_ROWS = 128
PRE_ROWS = 64
EARLY_ROWS = 192
LATE_ROWS = 128
TURN_STEP = 5
VMEM_LIMIT = 66_000_000


def mm(lhs, rhs, dims):
    return lax.dot_general(lhs, rhs, dims, preferred_element_type=F32)


def gelu_val(pre):
    return pre * (0.5 * (1.0 + jnp.tanh(GELU_SCALE * (pre + GELU_CUBE * (pre * pre * pre)))))


def gelu_both(pre):
    sq = pre * pre
    tan = jnp.tanh(GELU_SCALE * (pre + GELU_CUBE * (sq * pre)))
    cdf = 0.5 * (1.0 + tan)
    slope = cdf + 0.5 * pre * (1.0 - tan * tan) * (GELU_SCALE * (1.0 + (3.0 * GELU_CUBE) * sq))
    return pre * cdf, slope


def adamw_update(weight, moment_one, moment_two, grad_step, step_rate):
    mom_new = BETA_ONE * moment_one + (1.0 - BETA_ONE) * grad_step
    sec_new = BETA_TWO * moment_two + (1.0 - BETA_TWO) * grad_step * grad_step
    direction = (mom_new / ONE_CORR) / (jnp.sqrt(sec_new / TWO_CORR) + ADAM_EPS)
    weight_new = weight - step_rate * (direction + WEIGHT_DECAY * weight)
    return weight_new, mom_new, sec_new


def clip_of(norm_tile, max_norm):
    total = jnp.sum(jnp.sum(norm_tile, axis=0, keepdims=True), axis=1, keepdims=True)
    return jnp.minimum(1.0, max_norm / (jnp.sqrt(total) + NORM_EPS))


def whole_barrier(n_model, n_data, n_stage):
    barrier = pltpu.get_barrier_semaphore()
    me = (lax.axis_index('model'), lax.axis_index('data'), lax.axis_index('stage'))
    for dm in range(n_model):
        for dd in range(n_data):
            for ds in range(n_stage):
                if dm or dd or ds:
                    peer = (lax.rem(me[0] + dm, n_model), lax.rem(me[1] + dd, n_data), lax.rem(me[2] + ds, n_stage))
                    pl.semaphore_signal(barrier, inc=1, device_id=peer, device_id_type=MESH)
    pl.semaphore_wait(barrier, n_model * n_data * n_stage - 1)


def remote(src, dst, send_sem, recv_sem, device):
    return pltpu.make_async_remote_copy(src_ref=src, dst_ref=dst, send_sem=send_sem, recv_sem=recv_sem, device_id=device, device_id_type=MESH)


def bwd_kernel(dims, wu_hbm, wd_hbm, acts_hbm, dy_hbm, gu_hbm, gd_hbm,
               gbu_hbm, gbd_hbm, early_hbm, late_hbm, pre_oth, norm_out,
               wu32, wd32, wu_bf, wd_bf, aa, gg, hid_o, dz_o, slope, slope_o, dz_own, h_own,
               gu_own, gd_own, gu_oth, gd_oth, gu_rcv, gd_rcv, part, part_rcv, fin, norm_buf,
               ld_sem, ysend, yrecv, psend, precv, fsend, frecv, nsend, nrecv, st_sem):
    n_model, n_data, n_stage = dims
    z, d, p = lax.axis_index('model'), lax.axis_index('data'), lax.axis_index('stage')
    zo, do = 1 - z, 1 - d
    ypeer, zpeer = (z, do, p), (zo, d, p)
    last = n_stage - 1
    by_rows = lax.rem(p, 2) == 0
    by_sums = lax.rem(p, 2) == 1
    rows = aa.shape[0] // 2
    width = aa.shape[1]
    half = hid_o.shape[1]
    rb = BACK_ROWS
    hb = rb // 2
    nb = rows // rb
    own_ff = pl.ds(pl.multiple_of(d * half, 128), half)
    oth_ff = pl.ds(pl.multiple_of(do * half, 128), half)
    mine, theirs = pl.ds(0, rows), pl.ds(rows, rows)

    loads = [
        pltpu.make_async_copy(wu_hbm, wu32, ld_sem.at[0]),
        pltpu.make_async_copy(acts_hbm, aa.at[mine], ld_sem.at[2]),
        pltpu.make_async_copy(wd_hbm, wd32, ld_sem.at[1]),
        pltpu.make_async_copy(gu_hbm.at[:, own_ff], gu_own, ld_sem.at[4]),
        pltpu.make_async_copy(gd_hbm.at[own_ff, :], gd_own, ld_sem.at[5]),
    ]
    dy_load = pltpu.make_async_copy(dy_hbm, gg.at[mine], ld_sem.at[3])
    gu_load = pltpu.make_async_copy(gu_hbm.at[:, oth_ff], gu_oth, ld_sem.at[6])
    gd_load = pltpu.make_async_copy(gd_hbm.at[oth_ff, :], gd_oth, ld_sem.at[7])
    for copy in loads[:3]:
        copy.start()

    @pl.when(p == last)
    def _():
        dy_load.start()
    for copy in loads[3:]:
        copy.start()

    @pl.when(by_sums)
    def _():
        gd_load.start()
        gu_load.start()

    whole_barrier(n_model, n_data, n_stage)
    send_acts = remote(acts_hbm, aa.at[theirs], ysend.at[0], yrecv.at[0], ypeer)
    raw_gu = remote(gu_hbm.at[:, oth_ff], gu_rcv, ysend.at[1], yrecv.at[1], ypeer)
    raw_gd = remote(gd_hbm.at[oth_ff, :], gd_rcv, ysend.at[2], yrecv.at[2], ypeer)
    sum_gu = remote(gu_oth, gu_rcv, ysend.at[1], yrecv.at[1], ypeer)
    sum_gd = remote(gd_oth, gd_rcv, ysend.at[2], yrecv.at[2], ypeer)
    send_g = remote(gg.at[mine], gg.at[theirs], ysend.at[3], yrecv.at[3], ypeer)

    @pl.when(by_rows)
    def _():
        send_acts.start()
        raw_gd.start()
        raw_gu.start()

    loads[0].wait()
    loads[1].wait()

    def cast_up(i, carry):
        at = pl.ds(pl.multiple_of(i * 128, 128), 128)
        wu_bf[at, :] = wu32[at, :].astype(BF16)
        return carry
    lax.fori_loop(0, width // 128, cast_up, 0)

    def own_pre(i, carry):
        at = pl.ds(pl.multiple_of(i * rb, rb), rb)
        val, slp = gelu_both(mm(aa[at, :], wu_bf[...], NN))
        h_own[at, :] = val.astype(BF16)
        slope[at, :] = slp
        return carry
    lax.fori_loop(0, nb, own_pre, 0)
    loads[2].wait()

    def cast_down(i, carry):
        at = pl.ds(pl.multiple_of(i * 128, 128), 128)
        wd_bf[at, :] = wd32[at, :].astype(BF16)
        return carry
    lax.fori_loop(0, 2 * half // 128, cast_down, 0)

    @pl.when(p == last)
    def _():
        dy_load.wait()

    def g_at(c, zi):
        return gg.at[pl.ds(pl.multiple_of(c * rb + zi * hb, hb), hb)]

    def part_copy(c):
        return remote(part.at[c, pl.ds(pl.multiple_of(zo * hb, hb), hb)], part_rcv.at[c], psend.at[c], precv.at[c], zpeer)

    def fin_copy(c, zi):
        return remote(fin.at[c], g_at(c, z), fsend.at[c, zi], frecv.at[c, z], (zi, d, lax.max(p - 1, 0)))

    def compute(c):
        @pl.when(p < last)
        def _():
            for zi in range(n_model):
                pltpu.make_async_copy(fin.at[c], g_at(c, zi), frecv.at[c, zi]).wait()
        at = pl.ds(pl.multiple_of(c * rb, rb), rb)
        grad_hid = mm(gg[at, :], wd_bf[...], NT)
        dz_own[at, :] = (slope[at, :] * grad_hid).astype(BF16)

        @pl.when(p > 0)
        def _():
            part[c] = mm(dz_own[at, :], wu_bf[...], NT)
            part_copy(c).start()

    def finalize(c):
        part_copy(c).wait_recv()
        at = pl.ds(pl.multiple_of(c * rb + z * hb, hb), hb)
        total = part[c, pl.ds(pl.multiple_of(z * hb, hb), hb), :] + part_rcv[c]
        fin[c] = (gg[at, :].astype(F32) + total).astype(BF16)
        for zi in range(n_model):
            fin_copy(c, zi).start()

    def chain(i, carry):
        @pl.when(i < nb)
        def _():
            compute(i)

        @pl.when((i >= 1) & (p > 0))
        def _():
            finalize(i - 1)
        return carry
    lax.fori_loop(0, nb + 1, chain, 0)

    def down_block(j, base):
        at = pl.ds(pl.multiple_of(base * half + j * 128, 128), 128)
        return mm(h_own[:, at], gg[mine, :], TN)

    def up_block(j, ff_at):
        at = pl.ds(pl.multiple_of(j * 128, 128), 128)
        return mm(aa[mine, at], dz_own[:, ff_at], TN)

    @pl.when(by_sums)
    def _():
        gd_load.wait()

        def down_oth(j, carry):
            gd_oth[pl.ds(pl.multiple_of(j * 128, 128), 128), :] += down_block(j, do)
            return carry
        lax.fori_loop(0, half // 128, down_oth, 0)
        gu_load.wait()
        sum_gd.start()

        def up_oth(j, carry):
            gu_oth[pl.ds(pl.multiple_of(j * 128, 128), 128), :] += up_block(j, oth_ff)
            return carry
        lax.fori_loop(0, width // 128, up_oth, 0)

    @pl.when(by_rows)
    def _():
        send_g.start()
    loads[3].wait()
    loads[4].wait()

    def down_own(j, carry):
        gd_own[pl.ds(pl.multiple_of(j * 128, 128), 128), :] += down_block(j, d)
        return carry
    lax.fori_loop(0, half // 128, down_own, 0)

    @pl.when(by_sums)
    def _():
        sum_gu.start()

    def up_own(j, carry):
        gu_own[pl.ds(pl.multiple_of(j * 128, 128), 128), :] += up_block(j, own_ff)
        return carry
    lax.fori_loop(0, width // 128, up_own, 0)

    @pl.when(by_rows)
    def _():
        send_acts.wait_recv()

        def oth_pre(i, carry):
            at = pl.ds(pl.multiple_of(i * rb, rb), rb)
            val, slp = gelu_both(mm(aa[pl.ds(pl.multiple_of(rows + i * rb, rb), rb), :], wu_bf[:, own_ff], NN))
            hid_o[at, :] = val.astype(BF16)
            slope_o[at, :] = slp
            return carry
        lax.fori_loop(0, nb, oth_pre, 0)
        send_g.wait_recv()

        def oth_dz(i, carry):
            at = pl.ds(pl.multiple_of(i * rb, rb), rb)
            grad_hid = mm(gg[pl.ds(pl.multiple_of(rows + i * rb, rb), rb), :], wd_bf[own_ff, :], NT)
            dz_o[at, :] = (slope_o[at, :] * grad_hid).astype(BF16)
            return carry
        lax.fori_loop(0, nb, oth_dz, 0)

        def oth_grads(j, carry):
            at = pl.ds(pl.multiple_of(j * 128, 128), 128)
            gd_own[at, :] += mm(hid_o[:, at], gg[theirs, :], TN)
            gu_own[at, :] += mm(aa[theirs, at], dz_o[...], TN)
            return carry
        lax.fori_loop(0, half // 128, oth_grads, 0)

    def combine(own, rcv):
        def body(i, acc):
            at = pl.ds(pl.multiple_of(i * 32, 32), 32)
            mean = (own[at, :] + rcv[at, :]) * 0.5
            own[at, :] = mean
            return acc + jnp.sum((mean * mean).reshape(4, 8, mean.shape[1]), axis=0)
        return body

    def combine_up(acc):
        raw_gu.wait_recv()
        return lax.fori_loop(0, gu_own.shape[0] // 32, combine(gu_own, gu_rcv), acc)

    def combine_down(acc):
        raw_gd.wait_recv()
        return lax.fori_loop(0, gd_own.shape[0] // 32, combine(gd_own, gd_rcv), acc)
    acc = jnp.zeros((8, half), F32)
    acc = combine_down(acc)
    store_d = pltpu.make_async_copy(gd_own, gbd_hbm, st_sem.at[1])
    store_d.start()
    store_early = pltpu.make_async_copy(gd_own.at[pl.ds(PRE_ROWS, EARLY_ROWS)], early_hbm, st_sem.at[2])
    store_early.start()
    send_pre = remote(gd_own.at[pl.ds(0, PRE_ROWS)], pre_oth, ysend.at[4], yrecv.at[4], ypeer)
    send_pre.start()
    acc = combine_up(acc)
    store_u = pltpu.make_async_copy(gu_own, gbu_hbm, st_sem.at[0])
    store_u.start()
    store_late = pltpu.make_async_copy(gu_own.at[pl.ds(width - LATE_ROWS, LATE_ROWS)], late_hbm, st_sem.at[3])
    store_late.start()
    tile = acc[:, 0:128]
    for k in range(1, half // 128):
        tile = tile + acc[:, k * 128:(k + 1) * 128]
    n_all = n_model * n_data * n_stage
    my_id = (z * n_data + d) * n_stage + p
    norm_buf[my_id] = tile

    def norm_copy(k):
        peer = lax.rem(my_id + k, n_all)
        device = (peer // (n_data * n_stage), lax.rem(peer // n_stage, n_data), lax.rem(peer, n_stage))
        return remote(norm_buf.at[my_id], norm_buf.at[my_id], nsend.at[k], nrecv.at[my_id], device)
    for k in range(1, n_all):
        norm_copy(k).start()
    for k in range(1, n_all):
        peer = lax.rem(my_id + k, n_all)
        pltpu.make_async_copy(norm_buf.at[peer], norm_buf.at[peer], nrecv.at[peer]).wait()
    total = norm_buf[0]
    for k in range(1, n_all):
        total = total + norm_buf[k]
    norm_out[...] = total

    for k in range(1, n_all):
        norm_copy(k).wait_send()

    @pl.when(by_rows)
    def _():
        for copy in (send_acts, raw_gu, raw_gd, send_g):
            copy.wait_send()

    @pl.when(by_sums)
    def _():
        sum_gu.wait_send()
        sum_gd.wait_send()

    @pl.when(p > 0)
    def _():
        for c in range(nb):
            part_copy(c).wait_send()
            for zi in range(n_model):
                fin_copy(c, zi).wait_send()
    store_u.wait()
    store_d.wait()
    store_early.wait()
    store_late.wait()
    send_pre.wait()


def update_kernel(d_ref, lr_ref, mn_ref, norm_ref, gu, gd, wu, wd, mu, md, vu, vd, *rest):
    owu, owd, omu, omd, ovu, ovd = rest[:6]
    clip = clip_of(norm_ref[...], mn_ref[0])
    rate = lr_ref[0]
    owu[...], omu[...], ovu[...] = adamw_update(wu[...], mu[...], vu[...], clip * gu[...], rate)
    owd[...], omd[...], ovd[...] = adamw_update(wd[...], md[...], vd[...], clip * gd[...], rate)
    if len(rest) == 8:
        rest[6][...] = owu[...].astype(BF16)
        rest[7][...] = owd[...].astype(BF16)


def fill_kernel(d_ref, lr_ref, mn_ref, norm_ref, gu, gd_early, gd_rest, y_in, wu, wd, mu, md, vu, vd, *rest):
    owu, owd, omu, omd, ovu, ovd, y_out = rest[6:]
    clip = clip_of(norm_ref[...], mn_ref[0])
    rate = lr_ref[0]
    step = pl.program_id(0)
    gd = jnp.where(step < (PRE_ROWS + EARLY_ROWS) // UPD_ROWS, gd_early[...], gd_rest[...])
    owu[...], omu[...], ovu[...] = adamw_update(wu[...], mu[...], vu[...], clip * gu[...], rate)
    owd[...], omd[...], ovd[...] = adamw_update(wd[...], md[...], vd[...], clip * gd, rate)
    y_out[...] = y_in[...]


def late_kernel(d_ref, lr_ref, mn_ref, norm_ref, gu, wu, mu, vu, *rest):
    owu, omu, ovu = rest[3:]
    clip = clip_of(norm_ref[...], mn_ref[0])
    owu[...], omu[...], ovu[...] = adamw_update(wu[...], mu[...], vu[...], clip * gu[...], lr_ref[0])


def fwd_kernel(dims, bu_hbm, bd_hbm, gbu_hbm, gbd_hbm, x_hbm,
               gu_oth, gd_oth, y_hbm,
               wu_bf, wd_bf, wu_z, wd_z, a_buf, y_buf, part, part_rcv, fin,
               ld_sem, ysend, yrecv, zsend, zrecv, psend, precv, fsend, frecv, agsend, agrecv, outsend, outrecv, turn):
    n_model, n_data, n_stage = dims
    z, d, p = lax.axis_index('model'), lax.axis_index('data'), lax.axis_index('stage')
    zo, do = 1 - z, 1 - d
    ypeer, zpeer = (z, do, p), (zo, d, p)
    last = n_stage - 1
    nc, rb, width = a_buf.shape
    half = wu_bf.shape[1] // 2
    hb = rb // 2
    own_ff = pl.ds(pl.multiple_of(d * half, 128), half)
    oth_ff = pl.ds(pl.multiple_of(do * half, 128), half)
    first = (p == 0) | (p == last)
    partner = (z, d, p + 1 - 2 * lax.rem(p, 2))

    load_u = pltpu.make_async_copy(bu_hbm, wu_bf.at[:, own_ff], ld_sem.at[0])
    load_d = pltpu.make_async_copy(bd_hbm, wd_bf.at[own_ff, :], ld_sem.at[1])
    load_u.start()
    load_d.start()
    x_load = pltpu.make_async_copy(x_hbm, a_buf, ld_sem.at[2])

    @pl.when(p == 0)
    def _():
        x_load.start()
    whole_barrier(n_model, n_data, n_stage)

    send_wu = remote(bu_hbm, wu_bf.at[:, own_ff], ysend.at[0], yrecv.at[0], ypeer)
    send_wd = remote(bd_hbm, wd_bf.at[own_ff, :], ysend.at[1], yrecv.at[1], ypeer)
    send_gu = remote(gbu_hbm.at[pl.ds(0, gu_oth.shape[0])], gu_oth, ysend.at[2], yrecv.at[2], ypeer)
    send_gd = remote(gbd_hbm.at[pl.ds(half - gd_oth.shape[0], gd_oth.shape[0])], gd_oth, ysend.at[3], yrecv.at[3], ypeer)

    shard = [
        remote(bu_hbm, wu_z.at[:, own_ff], zsend.at[0], zrecv.at[0], zpeer),
        remote(bd_hbm, wd_z.at[own_ff, :], zsend.at[1], zrecv.at[1], zpeer),
        remote(wu_bf.at[:, oth_ff], wu_z.at[:, oth_ff], zsend.at[2], zrecv.at[2], zpeer),
        remote(wd_bf.at[oth_ff, :], wd_z.at[oth_ff, :], zsend.at[3], zrecv.at[3], zpeer),
    ]

    @pl.when(p == last)
    def _():
        shard[0].start()
        shard[1].start()

    @pl.when(first)
    def _():
        send_wu.start()
        send_wd.start()
        send_wu.wait_send()
        send_wd.wait_send()
        pl.semaphore_signal(turn, inc=1, device_id=partner, device_id_type=MESH)

    @pl.when(jnp.logical_not(first))
    def _():
        pl.semaphore_wait(turn, 1)
        send_wu.start()
        send_wd.start()
        send_gu.start()
        send_gd.start()
        send_wu.wait_send()
        send_wd.wait_send()
        pl.semaphore_signal(turn, inc=1, device_id=partner, device_id_type=MESH)

    @pl.when(p == 0)
    def _():
        x_load.wait()
    load_u.wait()
    load_d.wait()
    send_wu.wait_recv()

    @pl.when(p == last)
    def _():
        shard[2].start()
    send_wd.wait_recv()

    @pl.when(p == last)
    def _():
        shard[3].start()
        for copy in shard:
            copy.wait_recv()

    def half_rows(zi):
        return pl.ds(pl.multiple_of(zi * hb, hb), hb)

    def part_copy(c):
        return remote(part.at[c, half_rows(zo)], part_rcv.at[c], psend.at[c], precv.at[c], zpeer)

    def fin_copy(c, zi):
        return remote(fin.at[c], a_buf.at[c, half_rows(z)], fsend.at[c, zi], frecv.at[c, z], (zi, d, lax.min(p + 1, last)))

    def gather_copy(c):
        return remote(fin.at[c], y_buf.at[c, half_rows(z)], agsend.at[c], agrecv.at[c], zpeer)

    def out_copy(c, q):
        return remote(y_buf.at[c], y_hbm.at[c], outsend.at[c, q], outrecv.at[c], (z, d, q))

    def out_local(c):
        return pltpu.make_async_copy(y_buf.at[c], y_hbm.at[c], outsend.at[c, last])

    def arrived(c, zi):
        pltpu.make_async_copy(fin.at[c], a_buf.at[c, half_rows(zi)], frecv.at[c, zi]).wait()

    def branch(rows_in, w_up, w_down):
        hid = gelu_val(mm(rows_in, w_up[...], NN)).astype(BF16)
        return mm(hid, w_down[...], NN)

    def compute(c):
        @pl.when(p < last)
        def _():
            @pl.when(p > 0)
            def _():
                for zi in range(n_model):
                    arrived(c, zi)
            part[c] = branch(a_buf[c], wu_bf, wd_bf)
            part_copy(c).start()

        @pl.when(p == last)
        def _():
            arrived(c, z)
            at = half_rows(z)
            rows_in = a_buf[c, at, :]
            total = branch(rows_in, wu_bf, wd_bf) + branch(rows_in, wu_z, wd_z)
            new = (rows_in.astype(F32) + total).astype(BF16)
            fin[c] = new
            y_buf[c, at, :] = new
            gather_copy(c).start()

    def finalize(c):
        part_copy(c).wait_recv()
        total = part[c, half_rows(z), :] + part_rcv[c]
        fin[c] = (a_buf[c, half_rows(z), :].astype(F32) + total).astype(BF16)
        fin_copy(c, z).start()

        @pl.when(p < last - 1)
        def _():
            fin_copy(c, zo).start()

    def publish(c):
        gather_copy(c).wait_recv()
        out_local(c).start()
        for q in range(last):
            out_copy(c, q).start()

    def chain(i, carry):
        @pl.when(i < nc)
        def _():
            compute(i)

        @pl.when((i >= 1) & (i <= nc) & (p < last))
        def _():
            finalize(i - 1)

        @pl.when((i >= 1) & (i <= nc) & (p == last))
        def _():
            publish(i - 1)

        @pl.when((i == TURN_STEP) & first)
        def _():
            pl.semaphore_wait(turn, 1)
            send_gu.start()
            send_gd.start()
        return carry
    lax.fori_loop(0, nc + 1, chain, 0)

    def drain(c, carry):
        @pl.when(p < last)
        def _():
            part_copy(c).wait_send()
            fin_copy(c, z).wait_send()

            @pl.when(p < last - 1)
            def _():
                fin_copy(c, zo).wait_send()
            pltpu.make_async_copy(y_buf.at[c], y_hbm.at[c], outrecv.at[c]).wait()

        @pl.when(p == last)
        def _():
            gather_copy(c).wait_send()
            out_local(c).wait()
            for q in range(last):
                out_copy(c, q).wait_send()
        return carry
    lax.fori_loop(0, nc, drain, 0)

    @pl.when(p == last)
    def _():
        for copy in shard:
            copy.wait_send()
    send_gu.wait()
    send_gd.wait()


def solution(mesh):
    n_model, n_data, n_stage = (mesh.shape[k] for k in ('model', 'data', 'stage'))
    dims = (n_model, n_data, n_stage)
    n_all = n_model * n_data * n_stage
    up_spec = P('stage', None, 'model')
    down_spec = P('stage', 'model', None)
    row_spec = P(None, 'data', None)
    in_specs = (up_spec, down_spec, up_spec, down_spec, up_spec, down_spec, P('data', 'stage', None, 'model'), P('data', 'stage', 'model', None), P('stage', 'data', None), P('data', None), row_spec, P(None), P(None))
    out_specs = (up_spec, down_spec, up_spec, down_spec, up_spec, down_spec, row_spec)
    any_spec = pl.BlockSpec(memory_space=pl.ANY)
    vmem_spec = pl.BlockSpec(memory_space=pltpu.VMEM)
    smem_spec = pl.BlockSpec(memory_space=pltpu.SMEM)
    dma = pltpu.SemaphoreType.DMA

    def device_step(w_up, w_down, m_up, m_down, v_up, v_down, g_up, g_down, acts_last, grad_out, x_next, learn_rate, max_norm):
        rows, width = grad_out.shape
        ff = w_up.shape[2]
        half = ff // 2
        nb = rows // BACK_ROWS
        hb = BACK_ROWS // 2
        sds = jax.ShapeDtypeStruct
        gbar_u, gbar_d, early, late, pre_oth, norm_tile = pl.pallas_call(
            functools.partial(bwd_kernel, dims),
            out_shape=(sds((width, half), F32), sds((half, width), F32), sds((EARLY_ROWS, width), F32), sds((LATE_ROWS, half), F32), sds((PRE_ROWS, width), F32), sds((8, 128), F32)),
            in_specs=[any_spec] * 6,
            out_specs=(any_spec,) * 5 + (vmem_spec,),
            scratch_shapes=[
                pltpu.VMEM((width, ff), F32), pltpu.VMEM((ff, width), F32),
                pltpu.VMEM((width, ff), BF16), pltpu.VMEM((ff, width), BF16),
                pltpu.VMEM((2 * rows, width), BF16), pltpu.VMEM((2 * rows, width), BF16),
                pltpu.VMEM((rows, half), BF16), pltpu.VMEM((rows, half), BF16),
                pltpu.VMEM((rows, ff), F32), pltpu.VMEM((rows, half), F32),
                pltpu.VMEM((rows, ff), BF16), pltpu.VMEM((rows, ff), BF16),
            ] + [pltpu.VMEM((width, half), F32), pltpu.VMEM((half, width), F32)] * 3 + [
                pltpu.VMEM((nb, BACK_ROWS, width), F32), pltpu.VMEM((nb, hb, width), F32),
                pltpu.VMEM((nb, hb, width), BF16), pltpu.VMEM((n_all, 8, 128), F32),
                dma((8,)), dma((5,)), dma((5,)), dma((nb,)), dma((nb,)), dma((nb, 2)), dma((nb, 2)),
                dma((n_all,)), dma((n_all,)), dma((4,)),
            ],
            compiler_params=pltpu.CompilerParams(collective_id=0, has_side_effects=True, vmem_limit_bytes=VMEM_LIMIT),
            name='backward',
        )(w_up[0], w_down[0], acts_last[0], grad_out, g_up[0, 0], g_down[0, 0])

        early_oth = lax.ppermute(early, 'data', [(k, 1 - k) for k in range(n_data)])
        blocks = half // UPD_ROWS
        state = (w_up[0], w_down[0], m_up[0], m_down[0], v_up[0], v_down[0])
        state_shapes = tuple(sds(s.shape, F32) for s in state)
        which = lax.axis_index('data').astype(jnp.int32).reshape(1)

        def update_specs(pick):
            up = pl.BlockSpec((UPD_ROWS, half), lambda i, w: (i, pick(w[0])))
            down = pl.BlockSpec((UPD_ROWS, width), lambda i, w: (pick(w[0]) * blocks + i, 0))
            return [up, down]
        plain_up = pl.BlockSpec((UPD_ROWS, half), lambda i, w: (i, 0))
        plain_down = pl.BlockSpec((UPD_ROWS, width), lambda i, w: (i, 0))
        small = [smem_spec, smem_spec, pl.BlockSpec((8, 128), lambda i, w: (0, 0))]
        own = update_specs(lambda w: w)
        *fresh, b_up, b_down = pl.pallas_call(
            update_kernel,
            out_shape=state_shapes + (sds((width, half), BF16), sds((half, width), BF16)),
            grid_spec=pltpu.PrefetchScalarGridSpec(
                num_scalar_prefetch=1, grid=(width // UPD_ROWS,),
                in_specs=small + [plain_up, plain_down] + own * 3,
                out_specs=own * 3 + [plain_up, plain_down]),
            compiler_params=pltpu.CompilerParams(dimension_semantics=('arbitrary',), vmem_limit_bytes=VMEM_LIMIT),
            name='update_own',
        )(which, learn_rate, max_norm, norm_tile, gbar_u, gbar_d, *state)

        n_micro = x_next.shape[0]
        nc = n_micro * rows // FWD_ROWS
        fb = FWD_ROWS // 2
        gu_oth, gd_oth, y_next = pl.pallas_call(
            functools.partial(fwd_kernel, dims),
            out_shape=(sds((width - LATE_ROWS, half), F32), sds((half - PRE_ROWS - EARLY_ROWS, width), F32), sds((nc, FWD_ROWS, width), BF16)),
            in_specs=[any_spec] * 5,
            out_specs=(any_spec, any_spec, any_spec),
            scratch_shapes=[pltpu.VMEM((width, ff), BF16), pltpu.VMEM((ff, width), BF16)] * 2 + [
                pltpu.VMEM((nc, FWD_ROWS, width), BF16), pltpu.VMEM((nc, FWD_ROWS, width), BF16),
                pltpu.VMEM((nc, FWD_ROWS, width), F32), pltpu.VMEM((nc, fb, width), F32),
                pltpu.VMEM((nc, fb, width), BF16),
                dma((3,)), dma((4,)), dma((4,)), dma((4,)), dma((4,)), dma((nc,)), dma((nc,)), dma((nc, 2)), dma((nc, 2)),
                dma((nc,)), dma((nc,)), dma((nc, n_stage)), dma((nc,)), pltpu.SemaphoreType.REGULAR,
            ],
            compiler_params=pltpu.CompilerParams(collective_id=1, has_side_effects=True, vmem_limit_bytes=VMEM_LIMIT),
            name='forward',
        )(b_up, b_down, gbar_u, gbar_d, x_next.reshape(nc, FWD_ROWS, width))

        other = update_specs(lambda w: 1 - w)
        gu_oth, late = lax.optimization_barrier((gu_oth, late))
        late_oth = lax.ppermute(late, 'data', [(k, 1 - k) for k in range(n_data)])
        early_oth = jnp.concatenate([pre_oth, early_oth])
        y_next = y_next.reshape(n_micro * rows, width)
        nearly, nlate = (PRE_ROWS + EARLY_ROWS) // UPD_ROWS, LATE_ROWS // UPD_ROWS
        steps = width // UPD_ROWS
        lastup = steps - nlate - 1

        def rows_spec(start, count):
            return pl.BlockSpec((UPD_ROWS, width), lambda i, w: (jnp.clip(i - start, 0, count - 1), 0))
        y_spec = pl.BlockSpec((n_micro * rows // steps, width), lambda i, w: (i, 0))
        up_oth = pl.BlockSpec((UPD_ROWS, half), lambda i, w: (jnp.minimum(i, lastup), 1 - w[0]))
        down_oth = pl.BlockSpec((UPD_ROWS, width), lambda i, w: ((1 - w[0]) * blocks + i, 0))
        other = [up_oth, down_oth]
        *filled, y_next = pl.pallas_call(
            fill_kernel,
            out_shape=state_shapes + (sds(y_next.shape, BF16),),
            grid_spec=pltpu.PrefetchScalarGridSpec(
                num_scalar_prefetch=1, grid=(steps,),
                in_specs=small + [rows_spec(0, lastup + 1), rows_spec(0, nearly), rows_spec(nearly, blocks - nearly), y_spec] + other * 3 + [any_spec] * 6,
                out_specs=other * 3 + [y_spec]),
            input_output_aliases={14 + k: k for k in range(6)},
            compiler_params=pltpu.CompilerParams(dimension_semantics=('arbitrary',), vmem_limit_bytes=VMEM_LIMIT),
            cost_estimate=pl.CostEstimate(flops=10**10, bytes_accessed=40 * 10**6, transcendentals=0),
            name='update_other',
        )(which, learn_rate, max_norm, norm_tile, gu_oth, early_oth, gd_oth, y_next, *state, *fresh)
        up_late = pl.BlockSpec((UPD_ROWS, half), lambda i, w: (steps - nlate + i, 1 - w[0]))
        filled[0], filled[2], filled[4] = pl.pallas_call(
            late_kernel,
            out_shape=(state_shapes[0],) * 3,
            grid_spec=pltpu.PrefetchScalarGridSpec(
                num_scalar_prefetch=1, grid=(nlate,),
                in_specs=small + [plain_up] + [up_late] * 3 + [any_spec] * 3,
                out_specs=[up_late] * 3),
            input_output_aliases={8 + k: k for k in range(3)},
            compiler_params=pltpu.CompilerParams(dimension_semantics=('arbitrary',), vmem_limit_bytes=VMEM_LIMIT),
            name='update_late',
        )(which, learn_rate, max_norm, norm_tile, late_oth, state[0], state[2], state[4], filled[0], filled[2], filled[4])
        return tuple(s[None] for s in filled) + (y_next.reshape(n_micro, rows, width),)

    return jax.shard_map(device_step, mesh=mesh, in_specs=in_specs, out_specs=out_specs, check_vma=False)
```

```python
import functools

import jax
import jax.numpy as jnp
from jax import lax
from jax.experimental import pallas as pl
from jax.experimental.pallas import tpu as pltpu
from jax.sharding import PartitionSpec as P

ADAM_STEP = 10
BETA_ONE = 0.9
BETA_TWO = 0.95
ADAM_EPS = 1e-8
WEIGHT_DECAY = 0.1
NORM_EPS = 1e-6
ONE_CORR = 1.0 - BETA_ONE ** ADAM_STEP
TWO_CORR = 1.0 - BETA_TWO ** ADAM_STEP
GELU_SCALE = (2.0 / 3.141592653589793) ** 0.5
GELU_CUBE = 0.044715
NN = (((1,), (0,)), ((), ()))
NT = (((1,), (1,)), ((), ()))
TN = (((0,), (0,)), ((), ()))
F32 = jnp.float32
BF16 = jnp.bfloat16
MESH = pl.DeviceIdType.MESH
BACK_ROWS = 128
FWD_ROWS = 96
UPD_ROWS = 128
PRE_ROWS = 128
LATE_ROWS = 256
TURN_STEP = 8
VMEM_LIMIT = 66_000_000


def mm(lhs, rhs, dims):
    return lax.dot_general(lhs, rhs, dims, preferred_element_type=F32)


def gelu_val(pre):
    return pre * (0.5 * (1.0 + jnp.tanh(GELU_SCALE * (pre + GELU_CUBE * (pre * pre * pre)))))


def gelu_both(pre):
    sq = pre * pre
    tan = jnp.tanh(GELU_SCALE * (pre + GELU_CUBE * (sq * pre)))
    cdf = 0.5 * (1.0 + tan)
    slope = cdf + 0.5 * pre * (1.0 - tan * tan) * (GELU_SCALE * (1.0 + (3.0 * GELU_CUBE) * sq))
    return pre * cdf, slope


def adamw_update(weight, moment_one, moment_two, grad_step, step_rate):
    mom_new = BETA_ONE * moment_one + (1.0 - BETA_ONE) * grad_step
    sec_new = BETA_TWO * moment_two + (1.0 - BETA_TWO) * grad_step * grad_step
    direction = (mom_new / ONE_CORR) / (jnp.sqrt(sec_new / TWO_CORR) + ADAM_EPS)
    weight_new = weight - step_rate * (direction + WEIGHT_DECAY * weight)
    return weight_new, mom_new, sec_new


def clip_of(norm_tile, max_norm):
    total = jnp.sum(jnp.sum(norm_tile, axis=0, keepdims=True), axis=1, keepdims=True)
    return jnp.minimum(1.0, max_norm / (jnp.sqrt(total) + NORM_EPS))


def whole_barrier(n_model, n_data, n_stage):
    barrier = pltpu.get_barrier_semaphore()
    me = (lax.axis_index('model'), lax.axis_index('data'), lax.axis_index('stage'))
    for dm in range(n_model):
        for dd in range(n_data):
            for ds in range(n_stage):
                if dm or dd or ds:
                    peer = (lax.rem(me[0] + dm, n_model), lax.rem(me[1] + dd, n_data), lax.rem(me[2] + ds, n_stage))
                    pl.semaphore_signal(barrier, inc=1, device_id=peer, device_id_type=MESH)
    pl.semaphore_wait(barrier, n_model * n_data * n_stage - 1)


def remote(src, dst, send_sem, recv_sem, device):
    return pltpu.make_async_remote_copy(src_ref=src, dst_ref=dst, send_sem=send_sem, recv_sem=recv_sem, device_id=device, device_id_type=MESH)


def bwd_kernel(dims, lr_ref, mn_ref, wu_hbm, wd_hbm, mu_hbm, md_hbm, vu_hbm, vd_hbm, acts_hbm, dy_hbm, gu_hbm, gd_hbm,
               gbu_hbm, gbd_hbm, late_hbm, pre_oth, own_hbm, norm_out,
               wu32, wd32, wu_bf, wd_bf, aa, gg, hid_o, dz_o, slope, slope_o, dz_own, h_own,
               gu_own, gd_own, gu_oth, gd_oth, gu_rcv, gd_rcv, mu32, md32, vu32, vd32, new_bf, part, part_rcv, fin, norm_buf,
               ld_sem, ysend, yrecv, psend, precv, fsend, frecv, nsend, nrecv, st_sem):
    n_model, n_data, n_stage = dims
    z, d, p = lax.axis_index('model'), lax.axis_index('data'), lax.axis_index('stage')
    zo, do = 1 - z, 1 - d
    ypeer, zpeer = (z, do, p), (zo, d, p)
    last = n_stage - 1
    by_rows = lax.rem(p, 2) == 0
    by_sums = lax.rem(p, 2) == 1
    rows = aa.shape[0] // 2
    width = aa.shape[1]
    half = hid_o.shape[1]
    rb = BACK_ROWS
    hb = rb // 2
    nb = rows // rb
    own_ff = pl.ds(pl.multiple_of(d * half, 128), half)
    oth_ff = pl.ds(pl.multiple_of(do * half, 128), half)
    mine, theirs = pl.ds(0, rows), pl.ds(rows, rows)

    loads = [
        pltpu.make_async_copy(wu_hbm, wu32, ld_sem.at[0]),
        pltpu.make_async_copy(acts_hbm, aa.at[mine], ld_sem.at[2]),
        pltpu.make_async_copy(wd_hbm, wd32, ld_sem.at[1]),
        pltpu.make_async_copy(gu_hbm.at[:, own_ff], gu_own, ld_sem.at[4]),
        pltpu.make_async_copy(gd_hbm.at[own_ff, :], gd_own, ld_sem.at[5]),
    ]
    dy_load = pltpu.make_async_copy(dy_hbm, gg.at[mine], ld_sem.at[3])
    gu_load = pltpu.make_async_copy(gu_hbm.at[:, oth_ff], gu_oth, ld_sem.at[6])
    gd_load = pltpu.make_async_copy(gd_hbm.at[oth_ff, :], gd_oth, ld_sem.at[7])
    for copy in loads[:3]:
        copy.start()

    @pl.when(p == last)
    def _():
        dy_load.start()
    for copy in loads[3:]:
        copy.start()

    @pl.when(by_sums)
    def _():
        gd_load.start()
        gu_load.start()

    moments = [
        pltpu.make_async_copy(mu_hbm.at[:, own_ff], mu32, ld_sem.at[8]),
        pltpu.make_async_copy(md_hbm.at[own_ff, :], md32, ld_sem.at[9]),
        pltpu.make_async_copy(vu_hbm.at[:, own_ff], vu32, ld_sem.at[10]),
        pltpu.make_async_copy(vd_hbm.at[own_ff, :], vd32, ld_sem.at[11]),
    ]
    for copy in moments:
        copy.start()
    whole_barrier(n_model, n_data, n_stage)
    send_acts = remote(acts_hbm, aa.at[theirs], ysend.at[0], yrecv.at[0], ypeer)
    raw_gu = remote(gu_hbm.at[:, oth_ff], gu_rcv, ysend.at[1], yrecv.at[1], ypeer)
    raw_gd = remote(gd_hbm.at[oth_ff, :], gd_rcv, ysend.at[2], yrecv.at[2], ypeer)
    sum_gu = remote(gu_oth, gu_rcv, ysend.at[1], yrecv.at[1], ypeer)
    sum_gd = remote(gd_oth, gd_rcv, ysend.at[2], yrecv.at[2], ypeer)
    send_g = remote(gg.at[mine], gg.at[theirs], ysend.at[3], yrecv.at[3], ypeer)

    @pl.when(by_rows)
    def _():
        send_acts.start()
        raw_gd.start()
        raw_gu.start()

    loads[0].wait()
    loads[1].wait()

    def cast_up(i, carry):
        at = pl.ds(pl.multiple_of(i * 128, 128), 128)
        wu_bf[at, :] = wu32[at, :].astype(BF16)
        return carry
    lax.fori_loop(0, width // 128, cast_up, 0)

    def own_pre(i, carry):
        at = pl.ds(pl.multiple_of(i * rb, rb), rb)
        val, slp = gelu_both(mm(aa[at, :], wu_bf[...], NN))
        h_own[at, :] = val.astype(BF16)
        slope[at, :] = slp
        return carry
    lax.fori_loop(0, nb, own_pre, 0)
    loads[2].wait()

    def cast_down(i, carry):
        at = pl.ds(pl.multiple_of(i * 128, 128), 128)
        wd_bf[at, :] = wd32[at, :].astype(BF16)
        return carry
    lax.fori_loop(0, 2 * half // 128, cast_down, 0)

    @pl.when(p == last)
    def _():
        dy_load.wait()

    def g_at(c, zi):
        return gg.at[pl.ds(pl.multiple_of(c * rb + zi * hb, hb), hb)]

    def part_copy(c):
        return remote(part.at[c, pl.ds(pl.multiple_of(zo * hb, hb), hb)], part_rcv.at[c], psend.at[c], precv.at[c], zpeer)

    def fin_copy(c, zi):
        return remote(fin.at[c], g_at(c, z), fsend.at[c, zi], frecv.at[c, z], (zi, d, lax.max(p - 1, 0)))

    def compute(c):
        @pl.when(p < last)
        def _():
            for zi in range(n_model):
                pltpu.make_async_copy(fin.at[c], g_at(c, zi), frecv.at[c, zi]).wait()
        at = pl.ds(pl.multiple_of(c * rb, rb), rb)
        grad_hid = mm(gg[at, :], wd_bf[...], NT)
        dz_own[at, :] = (slope[at, :] * grad_hid).astype(BF16)

        @pl.when(p > 0)
        def _():
            part[c] = mm(dz_own[at, :], wu_bf[...], NT)
            part_copy(c).start()

    def finalize(c):
        part_copy(c).wait_recv()
        at = pl.ds(pl.multiple_of(c * rb + z * hb, hb), hb)
        total = part[c, pl.ds(pl.multiple_of(z * hb, hb), hb), :] + part_rcv[c]
        fin[c] = (gg[at, :].astype(F32) + total).astype(BF16)
        for zi in range(n_model):
            fin_copy(c, zi).start()

    def chain(i, carry):
        @pl.when(i < nb)
        def _():
            compute(i)

        @pl.when((i >= 1) & (p > 0))
        def _():
            finalize(i - 1)
        return carry
    lax.fori_loop(0, nb + 1, chain, 0)

    def down_block(j, base):
        at = pl.ds(pl.multiple_of(base * half + j * 128, 128), 128)
        return mm(h_own[:, at], gg[mine, :], TN)

    def up_block(j, ff_at):
        at = pl.ds(pl.multiple_of(j * 128, 128), 128)
        return mm(aa[mine, at], dz_own[:, ff_at], TN)

    @pl.when(by_sums)
    def _():
        gd_load.wait()

        def down_oth(j, carry):
            gd_oth[pl.ds(pl.multiple_of(j * 128, 128), 128), :] += down_block(j, do)
            return carry
        lax.fori_loop(0, half // 128, down_oth, 0)
        gu_load.wait()
        sum_gd.start()

        def up_oth(j, carry):
            gu_oth[pl.ds(pl.multiple_of(j * 128, 128), 128), :] += up_block(j, oth_ff)
            return carry
        lax.fori_loop(0, width // 128, up_oth, 0)

    @pl.when(by_rows)
    def _():
        send_g.start()
    loads[3].wait()
    loads[4].wait()

    def down_own(j, carry):
        gd_own[pl.ds(pl.multiple_of(j * 128, 128), 128), :] += down_block(j, d)
        return carry
    lax.fori_loop(0, half // 128, down_own, 0)

    @pl.when(by_sums)
    def _():
        sum_gu.start()

    def up_own(j, carry):
        gu_own[pl.ds(pl.multiple_of(j * 128, 128), 128), :] += up_block(j, own_ff)
        return carry
    lax.fori_loop(0, width // 128, up_own, 0)

    @pl.when(by_rows)
    def _():
        send_acts.wait_recv()

        def oth_pre(i, carry):
            at = pl.ds(pl.multiple_of(i * rb, rb), rb)
            val, slp = gelu_both(mm(aa[pl.ds(pl.multiple_of(rows + i * rb, rb), rb), :], wu_bf[:, own_ff], NN))
            hid_o[at, :] = val.astype(BF16)
            slope_o[at, :] = slp
            return carry
        lax.fori_loop(0, nb, oth_pre, 0)
        send_g.wait_recv()

        def oth_dz(i, carry):
            at = pl.ds(pl.multiple_of(i * rb, rb), rb)
            grad_hid = mm(gg[pl.ds(pl.multiple_of(rows + i * rb, rb), rb), :], wd_bf[own_ff, :], NT)
            dz_o[at, :] = (slope_o[at, :] * grad_hid).astype(BF16)
            return carry
        lax.fori_loop(0, nb, oth_dz, 0)

        def oth_grads(j, carry):
            at = pl.ds(pl.multiple_of(j * 128, 128), 128)
            gd_own[at, :] += mm(hid_o[:, at], gg[theirs, :], TN)
            gu_own[at, :] += mm(aa[theirs, at], dz_o[...], TN)
            return carry
        lax.fori_loop(0, half // 128, oth_grads, 0)

    def combine(own, rcv):
        def body(i, acc):
            at = pl.ds(pl.multiple_of(i * 32, 32), 32)
            mean = (own[at, :] + rcv[at, :]) * 0.5
            own[at, :] = mean
            return acc + jnp.sum((mean * mean).reshape(4, 8, mean.shape[1]), axis=0)
        return body

    def combine_up(acc):
        raw_gu.wait_recv()
        return lax.fori_loop(0, gu_own.shape[0] // 32, combine(gu_own, gu_rcv), acc)

    def combine_down(acc):
        raw_gd.wait_recv()
        return lax.fori_loop(0, gd_own.shape[0] // 32, combine(gd_own, gd_rcv), acc)
    acc = jnp.zeros((8, half), F32)
    acc = combine_down(acc)
    store_d = pltpu.make_async_copy(gd_own, gbd_hbm, st_sem.at[1])
    store_d.start()
    send_pre = remote(gd_own.at[pl.ds(0, PRE_ROWS)], pre_oth, ysend.at[4], yrecv.at[4], ypeer)
    send_pre.start()
    acc = combine_up(acc)
    store_u = pltpu.make_async_copy(gu_own, gbu_hbm, st_sem.at[0])
    store_u.start()
    store_late = pltpu.make_async_copy(gu_own.at[pl.ds(width - LATE_ROWS, LATE_ROWS)], late_hbm, st_sem.at[3])
    store_late.start()
    tile = acc[:, 0:128]
    for k in range(1, half // 128):
        tile = tile + acc[:, k * 128:(k + 1) * 128]
    n_all = n_model * n_data * n_stage
    my_id = (z * n_data + d) * n_stage + p
    norm_buf[my_id] = tile

    def norm_copy(k):
        peer = lax.rem(my_id + k, n_all)
        device = (peer // (n_data * n_stage), lax.rem(peer // n_stage, n_data), lax.rem(peer, n_stage))
        return remote(norm_buf.at[my_id], norm_buf.at[my_id], nsend.at[k], nrecv.at[my_id], device)
    for k in range(1, n_all):
        norm_copy(k).start()
    for k in range(1, n_all):
        peer = lax.rem(my_id + k, n_all)
        pltpu.make_async_copy(norm_buf.at[peer], norm_buf.at[peer], nrecv.at[peer]).wait()
    total = norm_buf[0]
    for k in range(1, n_all):
        total = total + norm_buf[k]
    norm_out[...] = total

    for copy in moments:
        copy.wait()
    clip = clip_of(total, mn_ref[0])
    rate = lr_ref[0]

    def new_up(i, carry):
        at = pl.ds(pl.multiple_of(i * 32, 32), 32)
        new_bf[at, :] = adamw_update(wu32[at, own_ff], mu32[at, :], vu32[at, :], clip * gu_own[at, :], rate)[0].astype(BF16)
        return carry
    lax.fori_loop(0, width // 32, new_up, 0)
    store_bu = pltpu.make_async_copy(new_bf.at[pl.ds(0, width)], own_hbm.at[pl.ds(0, width)], st_sem.at[2])
    store_bu.start()

    def new_down(i, carry):
        at = pl.ds(pl.multiple_of(i * 32, 32), 32)
        weight = wd32[pl.ds(pl.multiple_of(d * half + i * 32, 32), 32), :]
        new_bf[pl.ds(pl.multiple_of(width + i * 32, 32), 32), :] = adamw_update(weight, md32[at, :], vd32[at, :], clip * gd_own[at, :], rate)[0].astype(BF16)
        return carry
    lax.fori_loop(0, half // 32, new_down, 0)
    store_bd = pltpu.make_async_copy(new_bf.at[pl.ds(width, half)], own_hbm.at[pl.ds(width, half)], st_sem.at[4])
    store_bd.start()

    for k in range(1, n_all):
        norm_copy(k).wait_send()

    @pl.when(by_rows)
    def _():
        for copy in (send_acts, raw_gu, raw_gd, send_g):
            copy.wait_send()

    @pl.when(by_sums)
    def _():
        sum_gu.wait_send()
        sum_gd.wait_send()

    @pl.when(p > 0)
    def _():
        for c in range(nb):
            part_copy(c).wait_send()
            for zi in range(n_model):
                fin_copy(c, zi).wait_send()
    store_u.wait()
    store_d.wait()
    store_late.wait()
    send_pre.wait()
    store_bu.wait()
    store_bd.wait()


def update_kernel(d_ref, lr_ref, mn_ref, norm_ref, gu, gd, wu, wd, mu, md, vu, vd, *rest):
    owu, owd, omu, omd, ovu, ovd = rest[:6]
    clip = clip_of(norm_ref[...], mn_ref[0])
    rate = lr_ref[0]
    owu[...], omu[...], ovu[...] = adamw_update(wu[...], mu[...], vu[...], clip * gu[...], rate)
    owd[...], omd[...], ovd[...] = adamw_update(wd[...], md[...], vd[...], clip * gd[...], rate)


def fill_kernel(d_ref, lr_ref, mn_ref, norm_ref, gu, gd_pre, gd_rest, y_in, wu, wd, mu, md, vu, vd, *rest):
    owu, owd, omu, omd, ovu, ovd, y_out = rest[6:]
    clip = clip_of(norm_ref[...], mn_ref[0])
    rate = lr_ref[0]
    step = pl.program_id(0)
    gd = jnp.where(step < PRE_ROWS // UPD_ROWS, gd_pre[...], gd_rest[...])
    owu[...], omu[...], ovu[...] = adamw_update(wu[...], mu[...], vu[...], clip * gu[...], rate)
    owd[...], omd[...], ovd[...] = adamw_update(wd[...], md[...], vd[...], clip * gd, rate)
    y_out[...] = y_in[...]


def late_kernel(d_ref, lr_ref, mn_ref, norm_ref, gu, wu, mu, vu, *rest):
    owu, omu, ovu = rest[3:]
    clip = clip_of(norm_ref[...], mn_ref[0])
    owu[...], omu[...], ovu[...] = adamw_update(wu[...], mu[...], vu[...], clip * gu[...], lr_ref[0])


def fwd_kernel(dims, own_hbm, first_hbm, shard_hbm, gbu_hbm, gbd_hbm, x_hbm, after_hbm,
               gu_oth, gd_oth, y_hbm,
               wu_bf, wd_bf, wu_z, wd_z, a_buf, y_buf, part, part_rcv, fin,
               ld_sem, ysend, yrecv, zsend, zrecv, psend, precv, fsend, frecv, agsend, agrecv, outsend, outrecv, turn):
    n_model, n_data, n_stage = dims
    z, d, p = lax.axis_index('model'), lax.axis_index('data'), lax.axis_index('stage')
    zo, do = 1 - z, 1 - d
    ypeer, zpeer = (z, do, p), (zo, d, p)
    last = n_stage - 1
    nc, rb, width = a_buf.shape
    half = wu_bf.shape[1] // 2
    hb = rb // 2
    own_ff = pl.ds(pl.multiple_of(d * half, 128), half)
    oth_ff = pl.ds(pl.multiple_of(do * half, 128), half)
    first = (p == 0) | (p == last)
    partner = (z, d, p + 1 - 2 * lax.rem(p, 2))

    up_rows, down_rows = pl.ds(0, width), pl.ds(width, half)
    loads = [
        pltpu.make_async_copy(own_hbm.at[up_rows], wu_bf.at[:, own_ff], ld_sem.at[0]),
        pltpu.make_async_copy(own_hbm.at[down_rows], wd_bf.at[own_ff, :], ld_sem.at[1]),
    ]
    first_loads = [
        pltpu.make_async_copy(first_hbm.at[up_rows], wu_bf.at[:, oth_ff], ld_sem.at[3]),
        pltpu.make_async_copy(first_hbm.at[down_rows], wd_bf.at[oth_ff, :], ld_sem.at[4]),
    ]
    shard_loads = [
        pltpu.make_async_copy(shard_hbm.at[up_rows], wu_z.at[:, own_ff], ld_sem.at[5]),
        pltpu.make_async_copy(shard_hbm.at[down_rows], wd_z.at[own_ff, :], ld_sem.at[6]),
    ]
    for copy in loads:
        copy.start()

    @pl.when(first)
    def _():
        for copy in first_loads:
            copy.start()

    @pl.when(p == last)
    def _():
        for copy in shard_loads:
            copy.start()
    x_load = pltpu.make_async_copy(x_hbm, a_buf, ld_sem.at[2])

    @pl.when(p == 0)
    def _():
        x_load.start()
    whole_barrier(n_model, n_data, n_stage)

    send_wu = remote(own_hbm.at[up_rows], wu_bf.at[:, own_ff], ysend.at[0], yrecv.at[0], ypeer)
    send_wd = remote(own_hbm.at[down_rows], wd_bf.at[own_ff, :], ysend.at[1], yrecv.at[1], ypeer)
    send_gu = remote(gbu_hbm.at[pl.ds(0, gu_oth.shape[0])], gu_oth, ysend.at[2], yrecv.at[2], ypeer)
    send_gd = remote(gbd_hbm.at[pl.ds(half - gd_oth.shape[0], gd_oth.shape[0])], gd_oth, ysend.at[3], yrecv.at[3], ypeer)

    shard = [
        remote(first_hbm.at[up_rows], wu_z.at[:, oth_ff], zsend.at[0], zrecv.at[0], zpeer),
        remote(first_hbm.at[down_rows], wd_z.at[oth_ff, :], zsend.at[1], zrecv.at[1], zpeer),
    ]

    @pl.when(p == last)
    def _():
        for copy in shard:
            copy.start()

    @pl.when(jnp.logical_not(first))
    def _():
        send_wu.start()
        send_wd.start()
        send_gu.start()
        send_gd.start()
        send_wu.wait()
        send_wd.wait()
        pl.semaphore_signal(turn, inc=1, device_id=partner, device_id_type=MESH)
    for copy in loads:
        copy.wait()

    @pl.when(first)
    def _():
        for copy in first_loads:
            copy.wait()

    @pl.when(p == 0)
    def _():
        x_load.wait()

    @pl.when(p == last)
    def _():
        for copy in shard_loads:
            copy.wait()
        for copy in shard:
            copy.wait_recv()

    def half_rows(zi):
        return pl.ds(pl.multiple_of(zi * hb, hb), hb)

    def part_copy(c):
        return remote(part.at[c, half_rows(zo)], part_rcv.at[c], psend.at[c], precv.at[c], zpeer)

    def fin_copy(c, zi):
        return remote(fin.at[c], a_buf.at[c, half_rows(z)], fsend.at[c, zi], frecv.at[c, z], (zi, d, lax.min(p + 1, last)))

    def gather_copy(c):
        return remote(fin.at[c], y_buf.at[c, half_rows(z)], agsend.at[c], agrecv.at[c], zpeer)

    def out_copy(c, q):
        return remote(y_buf.at[c], y_hbm.at[c], outsend.at[c, q], outrecv.at[c], (z, d, q))

    def out_local(c):
        return pltpu.make_async_copy(y_buf.at[c], y_hbm.at[c], outsend.at[c, last])

    def arrived(c, zi):
        pltpu.make_async_copy(fin.at[c], a_buf.at[c, half_rows(zi)], frecv.at[c, zi]).wait()

    def branch(rows_in, w_up, w_down):
        hid = gelu_val(mm(rows_in, w_up[...], NN)).astype(BF16)
        return mm(hid, w_down[...], NN)

    def compute(c):
        @pl.when(p < last)
        def _():
            @pl.when(p > 0)
            def _():
                for zi in range(n_model):
                    arrived(c, zi)
            part[c] = branch(a_buf[c], wu_bf, wd_bf)
            part_copy(c).start()

        @pl.when(p == last)
        def _():
            arrived(c, z)
            at = half_rows(z)
            rows_in = a_buf[c, at, :]
            total = branch(rows_in, wu_bf, wd_bf) + branch(rows_in, wu_z, wd_z)
            new = (rows_in.astype(F32) + total).astype(BF16)
            fin[c] = new
            y_buf[c, at, :] = new
            gather_copy(c).start()

    def finalize(c):
        part_copy(c).wait_recv()
        total = part[c, half_rows(z), :] + part_rcv[c]
        fin[c] = (a_buf[c, half_rows(z), :].astype(F32) + total).astype(BF16)
        fin_copy(c, z).start()

        @pl.when(p < last - 1)
        def _():
            fin_copy(c, zo).start()

    def publish(c):
        gather_copy(c).wait_recv()
        out_local(c).start()
        for q in range(last):
            out_copy(c, q).start()

    def chain(i, carry):
        @pl.when(i < nc)
        def _():
            compute(i)

        @pl.when((i >= 1) & (i <= nc) & (p < last))
        def _():
            finalize(i - 1)

        @pl.when((i >= 1) & (i <= nc) & (p == last))
        def _():
            publish(i - 1)

        @pl.when((i == TURN_STEP) & first)
        def _():
            pl.semaphore_wait(turn, 1)
            send_gu.start()
            send_gd.start()
        return carry
    lax.fori_loop(0, nc + 1, chain, 0)

    def drain(c, carry):
        @pl.when(p < last)
        def _():
            part_copy(c).wait_send()
            fin_copy(c, z).wait_send()

            @pl.when(p < last - 1)
            def _():
                fin_copy(c, zo).wait_send()
            pltpu.make_async_copy(y_buf.at[c], y_hbm.at[c], outrecv.at[c]).wait()

        @pl.when(p == last)
        def _():
            gather_copy(c).wait_send()
            out_local(c).wait()
            for q in range(last):
                out_copy(c, q).wait_send()
        return carry
    lax.fori_loop(0, nc, drain, 0)

    @pl.when(p == last)
    def _():
        for copy in shard:
            copy.wait_send()
    send_gu.wait()
    send_gd.wait()


def solution(mesh):
    n_model, n_data, n_stage = (mesh.shape[k] for k in ('model', 'data', 'stage'))
    dims = (n_model, n_data, n_stage)
    n_all = n_model * n_data * n_stage
    up_spec = P('stage', None, 'model')
    down_spec = P('stage', 'model', None)
    row_spec = P(None, 'data', None)
    in_specs = (up_spec, down_spec, up_spec, down_spec, up_spec, down_spec, P('data', 'stage', None, 'model'), P('data', 'stage', 'model', None), P('stage', 'data', None), P('data', None), row_spec, P(None), P(None))
    out_specs = (up_spec, down_spec, up_spec, down_spec, up_spec, down_spec, row_spec)
    any_spec = pl.BlockSpec(memory_space=pl.ANY)
    vmem_spec = pl.BlockSpec(memory_space=pltpu.VMEM)
    smem_spec = pl.BlockSpec(memory_space=pltpu.SMEM)
    dma = pltpu.SemaphoreType.DMA

    def device_step(w_up, w_down, m_up, m_down, v_up, v_down, g_up, g_down, acts_last, grad_out, x_next, learn_rate, max_norm):
        rows, width = grad_out.shape
        ff = w_up.shape[2]
        half = ff // 2
        nb = rows // BACK_ROWS
        hb = BACK_ROWS // 2
        sds = jax.ShapeDtypeStruct
        gbar_u, gbar_d, late, pre_oth, b_own, norm_tile = pl.pallas_call(
            functools.partial(bwd_kernel, dims),
            out_shape=(sds((width, half), F32), sds((half, width), F32), sds((LATE_ROWS, half), F32), sds((PRE_ROWS, width), F32), sds((width + half, width), BF16), sds((8, 128), F32)),
            in_specs=[smem_spec] * 2 + [any_spec] * 10,
            out_specs=(any_spec,) * 5 + (vmem_spec,),
            scratch_shapes=[
                pltpu.VMEM((width, ff), F32), pltpu.VMEM((ff, width), F32),
                pltpu.VMEM((width, ff), BF16), pltpu.VMEM((ff, width), BF16),
                pltpu.VMEM((2 * rows, width), BF16), pltpu.VMEM((2 * rows, width), BF16),
                pltpu.VMEM((rows, half), BF16), pltpu.VMEM((rows, half), BF16),
                pltpu.VMEM((rows, ff), F32), pltpu.VMEM((rows, half), F32),
                pltpu.VMEM((rows, ff), BF16), pltpu.VMEM((rows, ff), BF16),
            ] + [pltpu.VMEM((width, half), F32), pltpu.VMEM((half, width), F32)] * 5 + [
                pltpu.VMEM((width + half, width), BF16),
                pltpu.VMEM((nb, BACK_ROWS, width), F32), pltpu.VMEM((nb, hb, width), F32),
                pltpu.VMEM((nb, hb, width), BF16), pltpu.VMEM((n_all, 8, 128), F32),
                dma((12,)), dma((5,)), dma((5,)), dma((nb,)), dma((nb,)), dma((nb, 2)), dma((nb, 2)),
                dma((n_all,)), dma((n_all,)), dma((5,)),
            ],
            compiler_params=pltpu.CompilerParams(collective_id=0, has_side_effects=True, vmem_limit_bytes=VMEM_LIMIT),
            name='backward',
        )(learn_rate, max_norm, w_up[0], w_down[0], m_up[0], m_down[0], v_up[0], v_down[0], acts_last[0], grad_out, g_up[0, 0], g_down[0, 0])

        ends = (0, n_stage - 1)
        b_first = lax.ppermute(b_own, ('data', 'stage'), [(k * n_stage + q, (1 - k) * n_stage + q) for k in range(n_data) for q in ends])
        b_shard = lax.ppermute(b_own, ('model', 'stage'), [(k * n_stage + ends[1], (1 - k) * n_stage + ends[1]) for k in range(n_model)])
        blocks = half // UPD_ROWS
        state = (w_up[0], w_down[0], m_up[0], m_down[0], v_up[0], v_down[0])
        state_shapes = tuple(sds(s.shape, F32) for s in state)
        which = lax.axis_index('data').astype(jnp.int32).reshape(1)

        def update_specs(pick):
            up = pl.BlockSpec((UPD_ROWS, half), lambda i, w: (i, pick(w[0])))
            down = pl.BlockSpec((UPD_ROWS, width), lambda i, w: (pick(w[0]) * blocks + i, 0))
            return [up, down]
        plain_up = pl.BlockSpec((UPD_ROWS, half), lambda i, w: (i, 0))
        plain_down = pl.BlockSpec((UPD_ROWS, width), lambda i, w: (i, 0))
        small = [smem_spec, smem_spec, pl.BlockSpec((8, 128), lambda i, w: (0, 0))]
        own = update_specs(lambda w: w)
        fresh = pl.pallas_call(
            update_kernel,
            out_shape=state_shapes,
            grid_spec=pltpu.PrefetchScalarGridSpec(
                num_scalar_prefetch=1, grid=(width // UPD_ROWS,),
                in_specs=small + [plain_up, plain_down] + own * 3,
                out_specs=own * 3),
            compiler_params=pltpu.CompilerParams(dimension_semantics=('arbitrary',), vmem_limit_bytes=VMEM_LIMIT),
            cost_estimate=pl.CostEstimate(flops=10**10, bytes_accessed=34 * 10**6, transcendentals=0),
            name='update_own',
        )(which, learn_rate, max_norm, norm_tile, gbar_u, gbar_d, *state)

        n_micro = x_next.shape[0]
        nc = n_micro * rows // FWD_ROWS
        fb = FWD_ROWS // 2
        gu_oth, gd_oth, y_next = pl.pallas_call(
            functools.partial(fwd_kernel, dims),
            out_shape=(sds((width - LATE_ROWS, half), F32), sds((half - PRE_ROWS, width), F32), sds((nc, FWD_ROWS, width), BF16)),
            in_specs=[any_spec] * 7,
            out_specs=(any_spec, any_spec, any_spec),
            scratch_shapes=[pltpu.VMEM((width, ff), BF16), pltpu.VMEM((ff, width), BF16)] * 2 + [
                pltpu.VMEM((nc, FWD_ROWS, width), BF16), pltpu.VMEM((nc, FWD_ROWS, width), BF16),
                pltpu.VMEM((nc, FWD_ROWS, width), F32), pltpu.VMEM((nc, fb, width), F32),
                pltpu.VMEM((nc, fb, width), BF16),
                dma((7,)), dma((4,)), dma((4,)), dma((2,)), dma((2,)), dma((nc,)), dma((nc,)), dma((nc, 2)), dma((nc, 2)),
                dma((nc,)), dma((nc,)), dma((nc, n_stage)), dma((nc,)), pltpu.SemaphoreType.REGULAR,
            ],
            compiler_params=pltpu.CompilerParams(collective_id=1, has_side_effects=True, vmem_limit_bytes=VMEM_LIMIT),
            name='forward',
        )(b_own, b_first, b_shard, gbar_u, gbar_d, x_next.reshape(nc, FWD_ROWS, width), fresh[0])

        other = update_specs(lambda w: 1 - w)
        gu_oth, late = lax.optimization_barrier((gu_oth, late))
        late_oth = lax.ppermute(late, 'data', [(k, 1 - k) for k in range(n_data)])
        y_next = y_next.reshape(n_micro * rows, width)
        npre, nlate = PRE_ROWS // UPD_ROWS, LATE_ROWS // UPD_ROWS
        steps = width // UPD_ROWS
        lastup = steps - nlate - 1

        def rows_spec(start, count):
            return pl.BlockSpec((UPD_ROWS, width), lambda i, w: (jnp.clip(i - start, 0, count - 1), 0))
        y_spec = pl.BlockSpec((n_micro * rows // steps, width), lambda i, w: (i, 0))
        up_oth = pl.BlockSpec((UPD_ROWS, half), lambda i, w: (jnp.minimum(i, lastup), 1 - w[0]))
        down_oth = pl.BlockSpec((UPD_ROWS, width), lambda i, w: ((1 - w[0]) * blocks + i, 0))
        other = [up_oth, down_oth]
        *filled, y_next = pl.pallas_call(
            fill_kernel,
            out_shape=state_shapes + (sds(y_next.shape, BF16),),
            grid_spec=pltpu.PrefetchScalarGridSpec(
                num_scalar_prefetch=1, grid=(steps,),
                in_specs=small + [rows_spec(0, lastup + 1), rows_spec(0, npre), rows_spec(npre, blocks - npre), y_spec] + other * 3 + [any_spec] * 6,
                out_specs=other * 3 + [y_spec]),
            input_output_aliases={14 + k: k for k in range(6)},
            compiler_params=pltpu.CompilerParams(dimension_semantics=('arbitrary',), vmem_limit_bytes=VMEM_LIMIT),
            cost_estimate=pl.CostEstimate(flops=10**10, bytes_accessed=40 * 10**6, transcendentals=0),
            name='update_other',
        )(which, learn_rate, max_norm, norm_tile, gu_oth, pre_oth, gd_oth, y_next, *state, *fresh)
        up_late = pl.BlockSpec((UPD_ROWS, half), lambda i, w: (steps - nlate + i, 1 - w[0]))
        filled[0], filled[2], filled[4] = pl.pallas_call(
            late_kernel,
            out_shape=(state_shapes[0],) * 3,
            grid_spec=pltpu.PrefetchScalarGridSpec(
                num_scalar_prefetch=1, grid=(nlate,),
                in_specs=small + [plain_up] + [up_late] * 3 + [any_spec] * 3,
                out_specs=[up_late] * 3),
            input_output_aliases={8 + k: k for k in range(3)},
            compiler_params=pltpu.CompilerParams(dimension_semantics=('arbitrary',), vmem_limit_bytes=VMEM_LIMIT),
            name='update_late',
        )(which, learn_rate, max_norm, norm_tile, late_oth, state[0], state[2], state[4], filled[0], filled[2], filled[4])
        return tuple(s[None] for s in filled) + (y_next.reshape(n_micro, rows, width),)

    return jax.shard_map(device_step, mesh=mesh, in_specs=in_specs, out_specs=out_specs, check_vma=False)
```

```python
import functools

import jax
import jax.numpy as jnp
from jax import lax
from jax.experimental import pallas as pl
from jax.experimental.pallas import tpu as pltpu
from jax.sharding import PartitionSpec as P

ADAM_STEP = 10
BETA_ONE = 0.9
BETA_TWO = 0.95
ADAM_EPS = 1e-8
WEIGHT_DECAY = 0.1
NORM_EPS = 1e-6
ONE_CORR = 1.0 - BETA_ONE ** ADAM_STEP
TWO_CORR = 1.0 - BETA_TWO ** ADAM_STEP
GELU_SCALE = (2.0 / 3.141592653589793) ** 0.5
GELU_CUBE = 0.044715
NN = (((1,), (0,)), ((), ()))
NT = (((1,), (1,)), ((), ()))
TN = (((0,), (0,)), ((), ()))
F32 = jnp.float32
BF16 = jnp.bfloat16
MESH = pl.DeviceIdType.MESH
BACK_ROWS = 128
FWD_ROWS = 96
UPD_ROWS = 128
PRE_ROWS = 128
TURN_STEP = 8
VMEM_LIMIT = 66_000_000


def mm(lhs, rhs, dims):
    return lax.dot_general(lhs, rhs, dims, preferred_element_type=F32)


def gelu_val(pre):
    return pre * (0.5 * (1.0 + jnp.tanh(GELU_SCALE * (pre + GELU_CUBE * (pre * pre * pre)))))


def gelu_both(pre):
    sq = pre * pre
    tan = jnp.tanh(GELU_SCALE * (pre + GELU_CUBE * (sq * pre)))
    cdf = 0.5 * (1.0 + tan)
    slope = cdf + 0.5 * pre * (1.0 - tan * tan) * (GELU_SCALE * (1.0 + (3.0 * GELU_CUBE) * sq))
    return pre * cdf, slope


def adamw_update(weight, moment_one, moment_two, grad_step, step_rate):
    mom_new = BETA_ONE * moment_one + (1.0 - BETA_ONE) * grad_step
    sec_new = BETA_TWO * moment_two + (1.0 - BETA_TWO) * grad_step * grad_step
    direction = (mom_new * (1.0 / ONE_CORR)) / (jnp.sqrt(sec_new * (1.0 / TWO_CORR)) + ADAM_EPS)
    weight_new = weight - step_rate * (direction + WEIGHT_DECAY * weight)
    return weight_new, mom_new, sec_new


def clip_of(norm_tile, max_norm):
    total = jnp.sum(jnp.sum(norm_tile, axis=0, keepdims=True), axis=1, keepdims=True)
    return jnp.minimum(1.0, max_norm / (jnp.sqrt(total) + NORM_EPS))


def whole_barrier(n_model, n_data, n_stage):
    barrier = pltpu.get_barrier_semaphore()
    me = (lax.axis_index('model'), lax.axis_index('data'), lax.axis_index('stage'))
    for dm in range(n_model):
        for dd in range(n_data):
            for ds in range(n_stage):
                if dm or dd or ds:
                    peer = (lax.rem(me[0] + dm, n_model), lax.rem(me[1] + dd, n_data), lax.rem(me[2] + ds, n_stage))
                    pl.semaphore_signal(barrier, inc=1, device_id=peer, device_id_type=MESH)
    pl.semaphore_wait(barrier, n_model * n_data * n_stage - 1)


def remote(src, dst, send_sem, recv_sem, device):
    return pltpu.make_async_remote_copy(src_ref=src, dst_ref=dst, send_sem=send_sem, recv_sem=recv_sem, device_id=device, device_id_type=MESH)


def bwd_kernel(dims, lr_ref, mn_ref, wu_hbm, wd_hbm, mu_hbm, md_hbm, vu_hbm, vd_hbm, acts_hbm, dy_hbm, gu_hbm, gd_hbm,
               gbu_hbm, gbd_hbm, pre_oth, own_hbm, norm_out,
               wu32, wd32, wu_bf, wd_bf, aa, gg, hid_o, dz_o, slope, slope_o, dz_own, h_own,
               gu_own, gd_own, gu_oth, gd_oth, gu_rcv, gd_rcv, mu32, md32, vu32, vd32, new_bf, part, part_rcv, fin, norm_buf,
               ld_sem, ysend, yrecv, psend, precv, fsend, frecv, nsend, nrecv, st_sem):
    n_model, n_data, n_stage = dims
    z, d, p = lax.axis_index('model'), lax.axis_index('data'), lax.axis_index('stage')
    zo, do = 1 - z, 1 - d
    ypeer, zpeer = (z, do, p), (zo, d, p)
    last = n_stage - 1
    by_rows = lax.rem(p, 2) == 0
    by_sums = lax.rem(p, 2) == 1
    rows = aa.shape[0] // 2
    width = aa.shape[1]
    half = hid_o.shape[1]
    rb = BACK_ROWS
    hb = rb // 2
    nb = rows // rb
    own_ff = pl.ds(pl.multiple_of(d * half, 128), half)
    oth_ff = pl.ds(pl.multiple_of(do * half, 128), half)
    mine, theirs = pl.ds(0, rows), pl.ds(rows, rows)

    loads = [
        pltpu.make_async_copy(wu_hbm, wu32, ld_sem.at[0]),
        pltpu.make_async_copy(acts_hbm, aa.at[mine], ld_sem.at[2]),
        pltpu.make_async_copy(wd_hbm, wd32, ld_sem.at[1]),
        pltpu.make_async_copy(gu_hbm.at[:, own_ff], gu_own, ld_sem.at[4]),
        pltpu.make_async_copy(gd_hbm.at[own_ff, :], gd_own, ld_sem.at[5]),
    ]
    dy_load = pltpu.make_async_copy(dy_hbm, gg.at[mine], ld_sem.at[3])
    gu_load = pltpu.make_async_copy(gu_hbm.at[:, oth_ff], gu_oth, ld_sem.at[6])
    gd_load = pltpu.make_async_copy(gd_hbm.at[oth_ff, :], gd_oth, ld_sem.at[7])
    for copy in loads[:3]:
        copy.start()

    @pl.when(p == last)
    def _():
        dy_load.start()
    for copy in loads[3:]:
        copy.start()

    @pl.when(by_sums)
    def _():
        gd_load.start()
        gu_load.start()

    moments = [
        pltpu.make_async_copy(mu_hbm.at[:, own_ff], mu32, ld_sem.at[8]),
        pltpu.make_async_copy(md_hbm.at[own_ff, :], md32, ld_sem.at[9]),
        pltpu.make_async_copy(vu_hbm.at[:, own_ff], vu32, ld_sem.at[10]),
        pltpu.make_async_copy(vd_hbm.at[own_ff, :], vd32, ld_sem.at[11]),
    ]
    for copy in moments:
        copy.start()
    whole_barrier(n_model, n_data, n_stage)
    send_acts = remote(acts_hbm, aa.at[theirs], ysend.at[0], yrecv.at[0], ypeer)
    raw_gu = remote(gu_hbm.at[:, oth_ff], gu_rcv, ysend.at[1], yrecv.at[1], ypeer)
    raw_gd = remote(gd_hbm.at[oth_ff, :], gd_rcv, ysend.at[2], yrecv.at[2], ypeer)
    sum_gu = remote(gu_oth, gu_rcv, ysend.at[1], yrecv.at[1], ypeer)
    sum_gd = remote(gd_oth, gd_rcv, ysend.at[2], yrecv.at[2], ypeer)
    send_g = remote(gg.at[mine], gg.at[theirs], ysend.at[3], yrecv.at[3], ypeer)

    @pl.when(by_rows)
    def _():
        send_acts.start()
        raw_gd.start()
        raw_gu.start()

    loads[0].wait()
    loads[1].wait()

    def cast_up(i, carry):
        at = pl.ds(pl.multiple_of(i * 128, 128), 128)
        wu_bf[at, :] = wu32[at, :].astype(BF16)
        return carry
    lax.fori_loop(0, width // 128, cast_up, 0)

    def own_pre(i, carry):
        at = pl.ds(pl.multiple_of(i * rb, rb), rb)
        val, slp = gelu_both(mm(aa[at, :], wu_bf[...], NN))
        h_own[at, :] = val.astype(BF16)
        slope[at, :] = slp
        return carry
    lax.fori_loop(0, nb, own_pre, 0)
    loads[2].wait()

    def cast_down(i, carry):
        at = pl.ds(pl.multiple_of(i * 128, 128), 128)
        wd_bf[at, :] = wd32[at, :].astype(BF16)
        return carry
    lax.fori_loop(0, 2 * half // 128, cast_down, 0)

    @pl.when(p == last)
    def _():
        dy_load.wait()

    def g_at(c, zi):
        return gg.at[pl.ds(pl.multiple_of(c * rb + zi * hb, hb), hb)]

    def part_copy(c):
        return remote(part.at[c, pl.ds(pl.multiple_of(zo * hb, hb), hb)], part_rcv.at[c], psend.at[c], precv.at[c], zpeer)

    def fin_copy(c, zi):
        return remote(fin.at[c], g_at(c, z), fsend.at[c, zi], frecv.at[c, z], (zi, d, lax.max(p - 1, 0)))

    def compute(c):
        @pl.when(p < last)
        def _():
            for zi in range(n_model):
                pltpu.make_async_copy(fin.at[c], g_at(c, zi), frecv.at[c, zi]).wait()
        at = pl.ds(pl.multiple_of(c * rb, rb), rb)
        grad_hid = mm(gg[at, :], wd_bf[...], NT)
        dz_own[at, :] = (slope[at, :] * grad_hid).astype(BF16)

        @pl.when(p > 0)
        def _():
            part[c] = mm(dz_own[at, :], wu_bf[...], NT)
            part_copy(c).start()

    def finalize(c):
        part_copy(c).wait_recv()
        at = pl.ds(pl.multiple_of(c * rb + z * hb, hb), hb)
        total = part[c, pl.ds(pl.multiple_of(z * hb, hb), hb), :] + part_rcv[c]
        fin[c] = (gg[at, :].astype(F32) + total).astype(BF16)
        for zi in range(n_model):
            fin_copy(c, zi).start()

    def chain(i, carry):
        @pl.when(i < nb)
        def _():
            compute(i)

        @pl.when((i >= 1) & (p > 0))
        def _():
            finalize(i - 1)
        return carry
    lax.fori_loop(0, nb + 1, chain, 0)

    def down_block(j, base):
        at = pl.ds(pl.multiple_of(base * half + j * 128, 128), 128)
        return mm(h_own[:, at], gg[mine, :], TN)

    def up_block(j, ff_at):
        at = pl.ds(pl.multiple_of(j * 128, 128), 128)
        return mm(aa[mine, at], dz_own[:, ff_at], TN)

    @pl.when(by_sums)
    def _():
        gd_load.wait()

        def down_oth(j, carry):
            gd_oth[pl.ds(pl.multiple_of(j * 128, 128), 128), :] += down_block(j, do)
            return carry
        lax.fori_loop(0, half // 128, down_oth, 0)
        gu_load.wait()
        sum_gd.start()

        def up_oth(j, carry):
            gu_oth[pl.ds(pl.multiple_of(j * 128, 128), 128), :] += up_block(j, oth_ff)
            return carry
        lax.fori_loop(0, width // 128, up_oth, 0)

    @pl.when(by_rows)
    def _():
        send_g.start()
    loads[3].wait()
    loads[4].wait()

    def down_own(j, carry):
        gd_own[pl.ds(pl.multiple_of(j * 128, 128), 128), :] += down_block(j, d)
        return carry
    lax.fori_loop(0, half // 128, down_own, 0)

    @pl.when(by_sums)
    def _():
        sum_gu.start()

    def up_own(j, carry):
        gu_own[pl.ds(pl.multiple_of(j * 128, 128), 128), :] += up_block(j, own_ff)
        return carry
    lax.fori_loop(0, width // 128, up_own, 0)

    @pl.when(by_rows)
    def _():
        send_acts.wait_recv()

        def oth_pre(i, carry):
            at = pl.ds(pl.multiple_of(i * rb, rb), rb)
            val, slp = gelu_both(mm(aa[pl.ds(pl.multiple_of(rows + i * rb, rb), rb), :], wu_bf[:, own_ff], NN))
            hid_o[at, :] = val.astype(BF16)
            slope_o[at, :] = slp
            return carry
        lax.fori_loop(0, nb, oth_pre, 0)
        send_g.wait_recv()

        def oth_dz(i, carry):
            at = pl.ds(pl.multiple_of(i * rb, rb), rb)
            grad_hid = mm(gg[pl.ds(pl.multiple_of(rows + i * rb, rb), rb), :], wd_bf[own_ff, :], NT)
            dz_o[at, :] = (slope_o[at, :] * grad_hid).astype(BF16)
            return carry
        lax.fori_loop(0, nb, oth_dz, 0)

        def oth_grads(j, carry):
            at = pl.ds(pl.multiple_of(j * 128, 128), 128)
            gd_own[at, :] += mm(hid_o[:, at], gg[theirs, :], TN)
            gu_own[at, :] += mm(aa[theirs, at], dz_o[...], TN)
            return carry
        lax.fori_loop(0, half // 128, oth_grads, 0)

    def combine(own, rcv):
        def body(i, acc):
            at = pl.ds(pl.multiple_of(i * 32, 32), 32)
            mean = (own[at, :] + rcv[at, :]) * 0.5
            own[at, :] = mean
            return acc + jnp.sum((mean * mean).reshape(4, 8, mean.shape[1]), axis=0)
        return body

    def combine_up(acc):
        raw_gu.wait_recv()
        return lax.fori_loop(0, gu_own.shape[0] // 32, combine(gu_own, gu_rcv), acc)

    def combine_down(acc):
        raw_gd.wait_recv()
        return lax.fori_loop(0, gd_own.shape[0] // 32, combine(gd_own, gd_rcv), acc)
    acc = jnp.zeros((8, half), F32)
    acc = combine_down(acc)
    store_d = pltpu.make_async_copy(gd_own, gbd_hbm, st_sem.at[1])
    store_d.start()
    send_pre = remote(gd_own.at[pl.ds(0, PRE_ROWS)], pre_oth, ysend.at[4], yrecv.at[4], ypeer)
    send_pre.start()
    acc = combine_up(acc)
    store_u = pltpu.make_async_copy(gu_own, gbu_hbm, st_sem.at[0])
    store_u.start()
    tile = acc[:, 0:128]
    for k in range(1, half // 128):
        tile = tile + acc[:, k * 128:(k + 1) * 128]
    n_all = n_model * n_data * n_stage
    my_id = (z * n_data + d) * n_stage + p
    norm_buf[my_id] = tile

    def norm_copy(k):
        peer = lax.rem(my_id + k, n_all)
        device = (peer // (n_data * n_stage), lax.rem(peer // n_stage, n_data), lax.rem(peer, n_stage))
        return remote(norm_buf.at[my_id], norm_buf.at[my_id], nsend.at[k], nrecv.at[my_id], device)
    for k in range(1, n_all):
        norm_copy(k).start()
    for k in range(1, n_all):
        peer = lax.rem(my_id + k, n_all)
        pltpu.make_async_copy(norm_buf.at[peer], norm_buf.at[peer], nrecv.at[peer]).wait()
    total = norm_buf[0]
    for k in range(1, n_all):
        total = total + norm_buf[k]
    norm_out[...] = total

    for copy in moments:
        copy.wait()
    clip = clip_of(total, mn_ref[0])
    rate = lr_ref[0]

    def new_up(i, carry):
        at = pl.ds(pl.multiple_of(i * 32, 32), 32)
        new_bf[at, :] = adamw_update(wu32[at, own_ff], mu32[at, :], vu32[at, :], clip * gu_own[at, :], rate)[0].astype(BF16)
        return carry
    lax.fori_loop(0, width // 32, new_up, 0)
    store_bu = pltpu.make_async_copy(new_bf.at[pl.ds(0, width)], own_hbm.at[pl.ds(0, width)], st_sem.at[2])
    store_bu.start()

    def new_down(i, carry):
        at = pl.ds(pl.multiple_of(i * 32, 32), 32)
        weight = wd32[pl.ds(pl.multiple_of(d * half + i * 32, 32), 32), :]
        new_bf[pl.ds(pl.multiple_of(width + i * 32, 32), 32), :] = adamw_update(weight, md32[at, :], vd32[at, :], clip * gd_own[at, :], rate)[0].astype(BF16)
        return carry
    lax.fori_loop(0, half // 32, new_down, 0)
    store_bd = pltpu.make_async_copy(new_bf.at[pl.ds(width, half)], own_hbm.at[pl.ds(width, half)], st_sem.at[3])
    store_bd.start()

    for k in range(1, n_all):
        norm_copy(k).wait_send()

    @pl.when(by_rows)
    def _():
        for copy in (send_acts, raw_gu, raw_gd, send_g):
            copy.wait_send()

    @pl.when(by_sums)
    def _():
        sum_gu.wait_send()
        sum_gd.wait_send()

    @pl.when(p > 0)
    def _():
        for c in range(nb):
            part_copy(c).wait_send()
            for zi in range(n_model):
                fin_copy(c, zi).wait_send()
    store_u.wait()
    store_d.wait()
    send_pre.wait()
    store_bu.wait()
    store_bd.wait()


def update_kernel(d_ref, lr_ref, mn_ref, norm_ref, gu, gd, wu, wd, mu, md, vu, vd, *rest):
    owu, owd, omu, omd, ovu, ovd = rest[:6]
    clip = clip_of(norm_ref[...], mn_ref[0])
    rate = lr_ref[0]
    owu[...], omu[...], ovu[...] = adamw_update(wu[...], mu[...], vu[...], clip * gu[...], rate)
    owd[...], omd[...], ovd[...] = adamw_update(wd[...], md[...], vd[...], clip * gd[...], rate)


def fill_kernel(d_ref, lr_ref, mn_ref, norm_ref, gu, gd_pre, gd_rest, y_in, wu, wd, mu, md, vu, vd, *rest):
    owu, owd, omu, omd, ovu, ovd, y_out = rest[6:]
    clip = clip_of(norm_ref[...], mn_ref[0])
    rate = lr_ref[0]
    step = pl.program_id(0)
    gd = jnp.where(step < PRE_ROWS // UPD_ROWS, gd_pre[...], gd_rest[...])
    owu[...], omu[...], ovu[...] = adamw_update(wu[...], mu[...], vu[...], clip * gu[...], rate)
    owd[...], omd[...], ovd[...] = adamw_update(wd[...], md[...], vd[...], clip * gd, rate)
    y_out[...] = y_in[...]


def fwd_kernel(dims, own_hbm, first_hbm, gbu_hbm, gbd_hbm, x_hbm, after_hbm,
               gu_oth, gd_oth, y_hbm,
               wu_bf, wd_bf, wu_z, wd_z, a_buf, y_buf, part, part_rcv, fin,
               ld_sem, ysend, yrecv, zsend, zrecv, psend, precv, fsend, frecv, agsend, agrecv, outsend, outrecv, turn):
    n_model, n_data, n_stage = dims
    z, d, p = lax.axis_index('model'), lax.axis_index('data'), lax.axis_index('stage')
    zo, do = 1 - z, 1 - d
    ypeer, zpeer = (z, do, p), (zo, d, p)
    last = n_stage - 1
    nc, rb, width = a_buf.shape
    half = wu_bf.shape[1] // 2
    hb = rb // 2
    own_ff = pl.ds(pl.multiple_of(d * half, 128), half)
    oth_ff = pl.ds(pl.multiple_of(do * half, 128), half)
    first = (p == 0) | (p == last)
    partner = (z, d, p + 1 - 2 * lax.rem(p, 2))

    up_rows, down_rows = pl.ds(0, width), pl.ds(width, half)
    loads = [
        pltpu.make_async_copy(own_hbm.at[up_rows], wu_bf.at[:, own_ff], ld_sem.at[0]),
        pltpu.make_async_copy(own_hbm.at[down_rows], wd_bf.at[own_ff, :], ld_sem.at[1]),
    ]
    first_loads = [
        pltpu.make_async_copy(first_hbm.at[up_rows], wu_bf.at[:, oth_ff], ld_sem.at[3]),
        pltpu.make_async_copy(first_hbm.at[down_rows], wd_bf.at[oth_ff, :], ld_sem.at[4]),
    ]
    for copy in loads:
        copy.start()

    @pl.when(first)
    def _():
        for copy in first_loads:
            copy.start()

    x_load = pltpu.make_async_copy(x_hbm, a_buf, ld_sem.at[2])

    @pl.when(p == 0)
    def _():
        x_load.start()
    whole_barrier(n_model, n_data, n_stage)

    send_wu = remote(own_hbm.at[up_rows], wu_bf.at[:, own_ff], ysend.at[0], yrecv.at[0], ypeer)
    send_wd = remote(own_hbm.at[down_rows], wd_bf.at[own_ff, :], ysend.at[1], yrecv.at[1], ypeer)
    send_gu = remote(gbu_hbm, gu_oth, ysend.at[2], yrecv.at[2], ypeer)
    send_gd = remote(gbd_hbm.at[pl.ds(half - gd_oth.shape[0], gd_oth.shape[0])], gd_oth, ysend.at[3], yrecv.at[3], ypeer)

    shard = [
        remote(own_hbm.at[up_rows], wu_z.at[:, own_ff], zsend.at[0], zrecv.at[0], zpeer),
        remote(own_hbm.at[down_rows], wd_z.at[own_ff, :], zsend.at[1], zrecv.at[1], zpeer),
        remote(first_hbm.at[up_rows], wu_z.at[:, oth_ff], zsend.at[2], zrecv.at[2], zpeer),
        remote(first_hbm.at[down_rows], wd_z.at[oth_ff, :], zsend.at[3], zrecv.at[3], zpeer),
    ]

    @pl.when(p == last)
    def _():
        for copy in shard:
            copy.start()

    @pl.when(jnp.logical_not(first))
    def _():
        send_wu.start()
        send_wd.start()
        send_gu.start()
        send_gd.start()
        send_wu.wait()
        send_wd.wait()
        pl.semaphore_signal(turn, inc=1, device_id=partner, device_id_type=MESH)
    for copy in loads:
        copy.wait()

    @pl.when(first)
    def _():
        for copy in first_loads:
            copy.wait()

    @pl.when(p == 0)
    def _():
        x_load.wait()

    @pl.when(p == last)
    def _():
        pl.semaphore_wait(turn, 1)
        send_gu.start()
        send_gd.start()
        for copy in shard:
            copy.wait_recv()

    def half_rows(zi):
        return pl.ds(pl.multiple_of(zi * hb, hb), hb)

    def part_copy(c):
        return remote(part.at[c, half_rows(zo)], part_rcv.at[c], psend.at[c], precv.at[c], zpeer)

    def fin_copy(c, zi):
        return remote(fin.at[c], a_buf.at[c, half_rows(z)], fsend.at[c, zi], frecv.at[c, z], (zi, d, lax.min(p + 1, last)))

    def gather_copy(c):
        return remote(fin.at[c], y_buf.at[c, half_rows(z)], agsend.at[c], agrecv.at[c], zpeer)

    def out_copy(c, q):
        return remote(y_buf.at[c], y_hbm.at[c], outsend.at[c, q], outrecv.at[c], (z, d, q))

    def out_local(c):
        return pltpu.make_async_copy(y_buf.at[c], y_hbm.at[c], outsend.at[c, last])

    def arrived(c, zi):
        pltpu.make_async_copy(fin.at[c], a_buf.at[c, half_rows(zi)], frecv.at[c, zi]).wait()

    def branch(rows_in, w_up, w_down):
        hid = gelu_val(mm(rows_in, w_up[...], NN)).astype(BF16)
        return mm(hid, w_down[...], NN)

    def compute(c):
        @pl.when(p < last)
        def _():
            @pl.when(p > 0)
            def _():
                for zi in range(n_model):
                    arrived(c, zi)
            part[c] = branch(a_buf[c], wu_bf, wd_bf)
            part_copy(c).start()

        @pl.when(p == last)
        def _():
            arrived(c, z)
            at = half_rows(z)
            rows_in = a_buf[c, at, :]
            total = branch(rows_in, wu_bf, wd_bf) + branch(rows_in, wu_z, wd_z)
            new = (rows_in.astype(F32) + total).astype(BF16)
            fin[c] = new
            y_buf[c, at, :] = new
            gather_copy(c).start()

    def finalize(c):
        part_copy(c).wait_recv()
        total = part[c, half_rows(z), :] + part_rcv[c]
        fin[c] = (a_buf[c, half_rows(z), :].astype(F32) + total).astype(BF16)
        fin_copy(c, z).start()

        @pl.when(p < last - 1)
        def _():
            fin_copy(c, zo).start()

    def publish(c):
        gather_copy(c).wait_recv()
        out_local(c).start()
        for q in range(last):
            out_copy(c, q).start()

    def chain(i, carry):
        @pl.when(i < nc)
        def _():
            compute(i)

        @pl.when((i >= 1) & (i <= nc) & (p < last))
        def _():
            finalize(i - 1)

        @pl.when((i >= 1) & (i <= nc) & (p == last))
        def _():
            publish(i - 1)

        @pl.when((i == TURN_STEP) & (p == 0))
        def _():
            pl.semaphore_wait(turn, 1)
            send_gu.start()
            send_gd.start()
        return carry
    lax.fori_loop(0, nc + 1, chain, 0)

    def drain(c, carry):
        @pl.when(p < last)
        def _():
            part_copy(c).wait_send()
            fin_copy(c, z).wait_send()

            @pl.when(p < last - 1)
            def _():
                fin_copy(c, zo).wait_send()
            pltpu.make_async_copy(y_buf.at[c], y_hbm.at[c], outrecv.at[c]).wait()

        @pl.when(p == last)
        def _():
            gather_copy(c).wait_send()
            out_local(c).wait()
            for q in range(last):
                out_copy(c, q).wait_send()
        return carry
    lax.fori_loop(0, nc, drain, 0)

    @pl.when(p == last)
    def _():
        for copy in shard:
            copy.wait_send()
    send_gu.wait()
    send_gd.wait()


def solution(mesh):
    n_model, n_data, n_stage = (mesh.shape[k] for k in ('model', 'data', 'stage'))
    dims = (n_model, n_data, n_stage)
    n_all = n_model * n_data * n_stage
    up_spec = P('stage', None, 'model')
    down_spec = P('stage', 'model', None)
    row_spec = P(None, 'data', None)
    in_specs = (up_spec, down_spec, up_spec, down_spec, up_spec, down_spec, P('data', 'stage', None, 'model'), P('data', 'stage', 'model', None), P('stage', 'data', None), P('data', None), row_spec, P(None), P(None))
    out_specs = (up_spec, down_spec, up_spec, down_spec, up_spec, down_spec, row_spec)
    any_spec = pl.BlockSpec(memory_space=pl.ANY)
    vmem_spec = pl.BlockSpec(memory_space=pltpu.VMEM)
    smem_spec = pl.BlockSpec(memory_space=pltpu.SMEM)
    dma = pltpu.SemaphoreType.DMA

    def device_step(w_up, w_down, m_up, m_down, v_up, v_down, g_up, g_down, acts_last, grad_out, x_next, learn_rate, max_norm):
        rows, width = grad_out.shape
        ff = w_up.shape[2]
        half = ff // 2
        nb = rows // BACK_ROWS
        hb = BACK_ROWS // 2
        sds = jax.ShapeDtypeStruct
        gbar_u, gbar_d, pre_oth, b_own, norm_tile = pl.pallas_call(
            functools.partial(bwd_kernel, dims),
            out_shape=(sds((width, half), F32), sds((half, width), F32), sds((PRE_ROWS, width), F32), sds((width + half, width), BF16), sds((8, 128), F32)),
            in_specs=[smem_spec] * 2 + [any_spec] * 10,
            out_specs=(any_spec,) * 4 + (vmem_spec,),
            scratch_shapes=[
                pltpu.VMEM((width, ff), F32), pltpu.VMEM((ff, width), F32),
                pltpu.VMEM((width, ff), BF16), pltpu.VMEM((ff, width), BF16),
                pltpu.VMEM((2 * rows, width), BF16), pltpu.VMEM((2 * rows, width), BF16),
                pltpu.VMEM((rows, half), BF16), pltpu.VMEM((rows, half), BF16),
                pltpu.VMEM((rows, ff), F32), pltpu.VMEM((rows, half), F32),
                pltpu.VMEM((rows, ff), BF16), pltpu.VMEM((rows, ff), BF16),
            ] + [pltpu.VMEM((width, half), F32), pltpu.VMEM((half, width), F32)] * 5 + [
                pltpu.VMEM((width + half, width), BF16),
                pltpu.VMEM((nb, BACK_ROWS, width), F32), pltpu.VMEM((nb, hb, width), F32),
                pltpu.VMEM((nb, hb, width), BF16), pltpu.VMEM((n_all, 8, 128), F32),
                dma((12,)), dma((5,)), dma((5,)), dma((nb,)), dma((nb,)), dma((nb, 2)), dma((nb, 2)),
                dma((n_all,)), dma((n_all,)), dma((4,)),
            ],
            compiler_params=pltpu.CompilerParams(collective_id=0, has_side_effects=True, vmem_limit_bytes=VMEM_LIMIT),
            name='backward',
        )(learn_rate, max_norm, w_up[0], w_down[0], m_up[0], m_down[0], v_up[0], v_down[0], acts_last[0], grad_out, g_up[0, 0], g_down[0, 0])

        ends = (0, n_stage - 1)
        b_first = lax.ppermute(b_own, ('data', 'stage'), [(k * n_stage + q, (1 - k) * n_stage + q) for k in range(n_data) for q in ends])
        blocks = half // UPD_ROWS
        state = (w_up[0], w_down[0], m_up[0], m_down[0], v_up[0], v_down[0])
        state_shapes = tuple(sds(s.shape, F32) for s in state)
        which = lax.axis_index('data').astype(jnp.int32).reshape(1)

        def update_specs(pick):
            up = pl.BlockSpec((UPD_ROWS, half), lambda i, w: (i, pick(w[0])))
            down = pl.BlockSpec((UPD_ROWS, width), lambda i, w: (pick(w[0]) * blocks + i, 0))
            return [up, down]
        plain_up = pl.BlockSpec((UPD_ROWS, half), lambda i, w: (i, 0))
        plain_down = pl.BlockSpec((UPD_ROWS, width), lambda i, w: (i, 0))
        small = [smem_spec, smem_spec, pl.BlockSpec((8, 128), lambda i, w: (0, 0))]
        own = update_specs(lambda w: w)
        fresh = pl.pallas_call(
            update_kernel,
            out_shape=state_shapes,
            grid_spec=pltpu.PrefetchScalarGridSpec(
                num_scalar_prefetch=1, grid=(width // UPD_ROWS,),
                in_specs=small + [plain_up, plain_down] + own * 3,
                out_specs=own * 3),
            compiler_params=pltpu.CompilerParams(dimension_semantics=('arbitrary',), vmem_limit_bytes=VMEM_LIMIT),
            cost_estimate=pl.CostEstimate(flops=10**10, bytes_accessed=34 * 10**6, transcendentals=0),
            name='update_own',
        )(which, learn_rate, max_norm, norm_tile, gbar_u, gbar_d, *state)

        n_micro = x_next.shape[0]
        nc = n_micro * rows // FWD_ROWS
        fb = FWD_ROWS // 2
        gu_oth, gd_oth, y_next = pl.pallas_call(
            functools.partial(fwd_kernel, dims),
            out_shape=(sds((width, half), F32), sds((half - PRE_ROWS, width), F32), sds((nc, FWD_ROWS, width), BF16)),
            in_specs=[any_spec] * 6,
            out_specs=(any_spec, any_spec, any_spec),
            scratch_shapes=[pltpu.VMEM((width, ff), BF16), pltpu.VMEM((ff, width), BF16)] * 2 + [
                pltpu.VMEM((nc, FWD_ROWS, width), BF16), pltpu.VMEM((nc, FWD_ROWS, width), BF16),
                pltpu.VMEM((nc, FWD_ROWS, width), F32), pltpu.VMEM((nc, fb, width), F32),
                pltpu.VMEM((nc, fb, width), BF16),
                dma((5,)), dma((4,)), dma((4,)), dma((4,)), dma((4,)), dma((nc,)), dma((nc,)), dma((nc, 2)), dma((nc, 2)),
                dma((nc,)), dma((nc,)), dma((nc, n_stage)), dma((nc,)), pltpu.SemaphoreType.REGULAR,
            ],
            compiler_params=pltpu.CompilerParams(collective_id=1, has_side_effects=True, vmem_limit_bytes=VMEM_LIMIT),
            name='forward',
        )(b_own, b_first, gbar_u, gbar_d, x_next.reshape(nc, FWD_ROWS, width), fresh[0])

        other = update_specs(lambda w: 1 - w)
        y_next = y_next.reshape(n_micro * rows, width)
        npre = PRE_ROWS // UPD_ROWS
        steps = width // UPD_ROWS

        def rows_spec(start, count):
            return pl.BlockSpec((UPD_ROWS, width), lambda i, w: (jnp.clip(i - start, 0, count - 1), 0))
        y_spec = pl.BlockSpec((n_micro * rows // steps, width), lambda i, w: (i, 0))
        other = update_specs(lambda w: 1 - w)
        *filled, y_next = pl.pallas_call(
            fill_kernel,
            out_shape=state_shapes + (sds(y_next.shape, BF16),),
            grid_spec=pltpu.PrefetchScalarGridSpec(
                num_scalar_prefetch=1, grid=(steps,),
                in_specs=small + [plain_up, rows_spec(0, npre), rows_spec(npre, blocks - npre), y_spec] + other * 3 + [any_spec] * 6,
                out_specs=other * 3 + [y_spec]),
            input_output_aliases={14 + k: k for k in range(6)},
            compiler_params=pltpu.CompilerParams(dimension_semantics=('arbitrary',), vmem_limit_bytes=VMEM_LIMIT),
            cost_estimate=pl.CostEstimate(flops=10**10, bytes_accessed=40 * 10**6, transcendentals=0),
            name='update_other',
        )(which, learn_rate, max_norm, norm_tile, gu_oth, pre_oth, gd_oth, y_next, *state, *fresh)
        return tuple(s[None] for s in filled) + (y_next.reshape(n_micro, rows, width),)

    return jax.shard_map(device_step, mesh=mesh, in_specs=in_specs, out_specs=out_specs, check_vma=False)
```

```python
import functools

import jax
import jax.numpy as jnp
from jax import lax
from jax.experimental import pallas as pl
from jax.experimental.pallas import tpu as pltpu
from jax.sharding import PartitionSpec as P

ADAM_STEP = 10
BETA_ONE = 0.9
BETA_TWO = 0.95
ADAM_EPS = 1e-8
WEIGHT_DECAY = 0.1
NORM_EPS = 1e-6
ONE_CORR = 1.0 - BETA_ONE ** ADAM_STEP
TWO_CORR = 1.0 - BETA_TWO ** ADAM_STEP
GELU_SCALE = (2.0 / 3.141592653589793) ** 0.5
GELU_CUBE = 0.044715
NN = (((1,), (0,)), ((), ()))
NT = (((1,), (1,)), ((), ()))
TN = (((0,), (0,)), ((), ()))
F32 = jnp.float32
BF16 = jnp.bfloat16
MESH = pl.DeviceIdType.MESH
BACK_ROWS = 128
FWD_ROWS = 96
UPD_ROWS = 128
EARLY_ROWS = 256
LATE_ROWS = 128
TURN_STEP = 5
VMEM_LIMIT = 66_000_000


def mm(lhs, rhs, dims):
    return lax.dot_general(lhs, rhs, dims, preferred_element_type=F32)


def gelu_val(pre):
    return pre * (0.5 * (1.0 + jnp.tanh(GELU_SCALE * (pre + GELU_CUBE * (pre * pre * pre)))))


def gelu_both(pre):
    sq = pre * pre
    tan = jnp.tanh(GELU_SCALE * (pre + GELU_CUBE * (sq * pre)))
    cdf = 0.5 * (1.0 + tan)
    slope = cdf + 0.5 * pre * (1.0 - tan * tan) * (GELU_SCALE * (1.0 + (3.0 * GELU_CUBE) * sq))
    return pre * cdf, slope


def adamw_update(weight, moment_one, moment_two, grad_step, step_rate):
    mom_new = BETA_ONE * moment_one + (1.0 - BETA_ONE) * grad_step
    sec_new = BETA_TWO * moment_two + (1.0 - BETA_TWO) * grad_step * grad_step
    direction = (mom_new * (1.0 / ONE_CORR)) / (jnp.sqrt(sec_new * (1.0 / TWO_CORR)) + ADAM_EPS)
    weight_new = weight - step_rate * (direction + WEIGHT_DECAY * weight)
    return weight_new, mom_new, sec_new


def clip_of(norm_tile, max_norm):
    total = jnp.sum(jnp.sum(norm_tile, axis=0, keepdims=True), axis=1, keepdims=True)
    return jnp.minimum(1.0, max_norm / (jnp.sqrt(total) + NORM_EPS))


def whole_barrier(n_model, n_data, n_stage):
    barrier = pltpu.get_barrier_semaphore()
    me = (lax.axis_index('model'), lax.axis_index('data'), lax.axis_index('stage'))
    for dm in range(n_model):
        for dd in range(n_data):
            for ds in range(n_stage):
                if dm or dd or ds:
                    peer = (lax.rem(me[0] + dm, n_model), lax.rem(me[1] + dd, n_data), lax.rem(me[2] + ds, n_stage))
                    pl.semaphore_signal(barrier, inc=1, device_id=peer, device_id_type=MESH)
    pl.semaphore_wait(barrier, n_model * n_data * n_stage - 1)


def remote(src, dst, send_sem, recv_sem, device):
    return pltpu.make_async_remote_copy(src_ref=src, dst_ref=dst, send_sem=send_sem, recv_sem=recv_sem, device_id=device, device_id_type=MESH)


def bwd_kernel(dims, wu_hbm, wd_hbm, acts_hbm, dy_hbm, gu_hbm, gd_hbm,
               gbu_hbm, gbd_hbm, early_hbm, late_hbm, norm_out,
               wu32, wd32, wu_bf, wd_bf, aa, gg, hid_o, dz_o, slope, slope_o, dz_own, h_own,
               gu_own, gd_own, gu_oth, gd_oth, gu_rcv, gd_rcv, part, part_rcv, fin, norm_buf,
               ld_sem, ysend, yrecv, rsend, rrecv, psend, precv, fsend, frecv, nsend, nrecv, st_sem):
    n_model, n_data, n_stage = dims
    z, d, p = lax.axis_index('model'), lax.axis_index('data'), lax.axis_index('stage')
    zo, do = 1 - z, 1 - d
    ypeer, zpeer = (z, do, p), (zo, d, p)
    last = n_stage - 1
    by_rows = p == 0
    by_sums = p > 0
    hub = n_stage // 2
    rows = aa.shape[0] // 2
    width = aa.shape[1]
    half = hid_o.shape[1]
    rb = BACK_ROWS
    hb = rb // 2
    nb = rows // rb
    own_ff = pl.ds(pl.multiple_of(d * half, 128), half)
    oth_ff = pl.ds(pl.multiple_of(do * half, 128), half)
    mine, theirs = pl.ds(0, rows), pl.ds(rows, rows)

    loads = [
        pltpu.make_async_copy(wu_hbm, wu32, ld_sem.at[0]),
        pltpu.make_async_copy(acts_hbm, aa.at[mine], ld_sem.at[2]),
        pltpu.make_async_copy(wd_hbm, wd32, ld_sem.at[1]),
        pltpu.make_async_copy(gu_hbm.at[:, own_ff], gu_own, ld_sem.at[4]),
        pltpu.make_async_copy(gd_hbm.at[own_ff, :], gd_own, ld_sem.at[5]),
    ]
    dy_load = pltpu.make_async_copy(dy_hbm, gg.at[mine], ld_sem.at[3])
    gu_load = pltpu.make_async_copy(gu_hbm.at[:, oth_ff], gu_oth, ld_sem.at[6])
    gd_load = pltpu.make_async_copy(gd_hbm.at[oth_ff, :], gd_oth, ld_sem.at[7])
    for copy in loads[:3]:
        copy.start()

    @pl.when(p == last)
    def _():
        dy_load.start()
    for copy in loads[3:]:
        copy.start()

    @pl.when(by_sums)
    def _():
        gd_load.start()
        gu_load.start()

    whole_barrier(n_model, n_data, n_stage)
    send_acts = remote(acts_hbm, hid_o, ysend.at[0], rrecv.at[0], (z, d, hub))
    relay_over = remote(hid_o, dz_o, rsend.at[0], rrecv.at[1], ypeer)
    relay_back = remote(dz_o, aa.at[theirs], rsend.at[1], yrecv.at[0], (z, d, 0))
    raw_gu = remote(gu_hbm.at[:, oth_ff], gu_rcv, ysend.at[1], yrecv.at[1], ypeer)
    raw_gd = remote(gd_hbm.at[oth_ff, :], gd_rcv, ysend.at[2], yrecv.at[2], ypeer)
    sum_gu = remote(gu_oth, gu_rcv, ysend.at[1], yrecv.at[1], ypeer)
    sum_gd = remote(gd_oth, gd_rcv, ysend.at[2], yrecv.at[2], ypeer)
    send_g = remote(gg.at[mine], gg.at[theirs], ysend.at[3], yrecv.at[3], ypeer)

    @pl.when(by_rows)
    def _():
        send_acts.start()
        raw_gd.start()
        raw_gu.start()

    loads[0].wait()
    loads[1].wait()

    def cast_up(i, carry):
        at = pl.ds(pl.multiple_of(i * 128, 128), 128)
        wu_bf[at, :] = wu32[at, :].astype(BF16)
        return carry
    lax.fori_loop(0, width // 128, cast_up, 0)

    def own_pre(i, carry):
        at = pl.ds(pl.multiple_of(i * rb, rb), rb)
        val, slp = gelu_both(mm(aa[at, :], wu_bf[...], NN))
        h_own[at, :] = val.astype(BF16)
        slope[at, :] = slp
        return carry
    lax.fori_loop(0, nb, own_pre, 0)
    loads[2].wait()

    def cast_down(i, carry):
        at = pl.ds(pl.multiple_of(i * 128, 128), 128)
        wd_bf[at, :] = wd32[at, :].astype(BF16)
        return carry
    lax.fori_loop(0, 2 * half // 128, cast_down, 0)

    @pl.when(p == last)
    def _():
        dy_load.wait()

    @pl.when(p == hub)
    def _():
        pltpu.make_async_copy(hid_o, hid_o, rrecv.at[0]).wait()
        relay_over.start()
        pltpu.make_async_copy(dz_o, dz_o, rrecv.at[1]).wait()
        relay_back.start()

    def down_block(j, base):
        at = pl.ds(pl.multiple_of(base * half + j * 128, 128), 128)
        return mm(h_own[:, at], gg[mine, :], TN)

    def up_block(j, ff_at):
        at = pl.ds(pl.multiple_of(j * 128, 128), 128)
        return mm(aa[mine, at], dz_own[:, ff_at], TN)

    def send_down():
        gd_load.wait()

        def down_oth(j, carry):
            gd_oth[pl.ds(pl.multiple_of(j * 128, 128), 128), :] += down_block(j, do)
            return carry
        lax.fori_loop(0, half // 128, down_oth, 0)
        gu_load.wait()
        sum_gd.start()

    @pl.when(p == last)
    def _():
        send_down()

    def g_at(c, zi):
        return gg.at[pl.ds(pl.multiple_of(c * rb + zi * hb, hb), hb)]

    def part_copy(c):
        return remote(part.at[c, pl.ds(pl.multiple_of(zo * hb, hb), hb)], part_rcv.at[c], psend.at[c], precv.at[c], zpeer)

    def fin_copy(c, zi):
        return remote(fin.at[c], g_at(c, z), fsend.at[c, zi], frecv.at[c, z], (zi, d, lax.max(p - 1, 0)))

    def compute(c):
        @pl.when(p < last)
        def _():
            for zi in range(n_model):
                pltpu.make_async_copy(fin.at[c], g_at(c, zi), frecv.at[c, zi]).wait()
        at = pl.ds(pl.multiple_of(c * rb, rb), rb)
        grad_hid = mm(gg[at, :], wd_bf[...], NT)
        dz_own[at, :] = (slope[at, :] * grad_hid).astype(BF16)

        @pl.when(p > 0)
        def _():
            part[c] = mm(dz_own[at, :], wu_bf[...], NT)
            part_copy(c).start()

    def finalize(c):
        part_copy(c).wait_recv()
        at = pl.ds(pl.multiple_of(c * rb + z * hb, hb), hb)
        total = part[c, pl.ds(pl.multiple_of(z * hb, hb), hb), :] + part_rcv[c]
        fin[c] = (gg[at, :].astype(F32) + total).astype(BF16)
        for zi in range(n_model):
            fin_copy(c, zi).start()

    def chain(i, carry):
        @pl.when(i < nb)
        def _():
            compute(i)

        @pl.when((i >= 1) & (p > 0))
        def _():
            finalize(i - 1)
        return carry
    lax.fori_loop(0, nb + 1, chain, 0)

    @pl.when(by_sums & (p < last))
    def _():
        send_down()

    @pl.when(by_sums)
    def _():
        def up_oth(j, carry):
            gu_oth[pl.ds(pl.multiple_of(j * 128, 128), 128), :] += up_block(j, oth_ff)
            return carry
        lax.fori_loop(0, width // 128, up_oth, 0)

    @pl.when(by_rows)
    def _():
        send_g.start()
    loads[3].wait()
    loads[4].wait()

    def down_own(j, carry):
        gd_own[pl.ds(pl.multiple_of(j * 128, 128), 128), :] += down_block(j, d)
        return carry
    lax.fori_loop(0, half // 128, down_own, 0)

    @pl.when(by_sums)
    def _():
        sum_gu.start()

    def up_own(j, carry):
        gu_own[pl.ds(pl.multiple_of(j * 128, 128), 128), :] += up_block(j, own_ff)
        return carry
    lax.fori_loop(0, width // 128, up_own, 0)

    @pl.when(by_rows)
    def _():
        pltpu.make_async_copy(aa.at[theirs], aa.at[theirs], yrecv.at[0]).wait()

        def oth_pre(i, carry):
            at = pl.ds(pl.multiple_of(i * rb, rb), rb)
            val, slp = gelu_both(mm(aa[pl.ds(pl.multiple_of(rows + i * rb, rb), rb), :], wu_bf[:, own_ff], NN))
            hid_o[at, :] = val.astype(BF16)
            slope_o[at, :] = slp
            return carry
        lax.fori_loop(0, nb, oth_pre, 0)
        send_g.wait_recv()

        def oth_dz(i, carry):
            at = pl.ds(pl.multiple_of(i * rb, rb), rb)
            grad_hid = mm(gg[pl.ds(pl.multiple_of(rows + i * rb, rb), rb), :], wd_bf[own_ff, :], NT)
            dz_o[at, :] = (slope_o[at, :] * grad_hid).astype(BF16)
            return carry
        lax.fori_loop(0, nb, oth_dz, 0)

        def oth_grads(j, carry):
            at = pl.ds(pl.multiple_of(j * 128, 128), 128)
            gd_own[at, :] += mm(hid_o[:, at], gg[theirs, :], TN)
            gu_own[at, :] += mm(aa[theirs, at], dz_o[...], TN)
            return carry
        lax.fori_loop(0, half // 128, oth_grads, 0)

    def combine(own, rcv):
        def body(i, acc):
            at = pl.ds(pl.multiple_of(i * 32, 32), 32)
            mean = (own[at, :] + rcv[at, :]) * 0.5
            own[at, :] = mean
            return acc + jnp.sum((mean * mean).reshape(4, 8, mean.shape[1]), axis=0)
        return body

    def combine_up(acc):
        raw_gu.wait_recv()
        return lax.fori_loop(0, gu_own.shape[0] // 32, combine(gu_own, gu_rcv), acc)

    def combine_down(acc):
        raw_gd.wait_recv()
        return lax.fori_loop(0, gd_own.shape[0] // 32, combine(gd_own, gd_rcv), acc)
    acc = jnp.zeros((8, half), F32)
    acc = combine_down(acc)
    store_d = pltpu.make_async_copy(gd_own, gbd_hbm, st_sem.at[1])
    store_d.start()
    store_early = pltpu.make_async_copy(gd_own.at[pl.ds(0, EARLY_ROWS)], early_hbm, st_sem.at[2])
    store_early.start()
    acc = combine_up(acc)
    store_u = pltpu.make_async_copy(gu_own, gbu_hbm, st_sem.at[0])
    store_u.start()
    store_late = pltpu.make_async_copy(gu_own.at[pl.ds(width - LATE_ROWS, LATE_ROWS)], late_hbm, st_sem.at[3])
    store_late.start()
    tile = acc[:, 0:128]
    for k in range(1, half // 128):
        tile = tile + acc[:, k * 128:(k + 1) * 128]
    n_all = n_model * n_data * n_stage
    my_id = (z * n_data + d) * n_stage + p
    norm_buf[my_id] = tile

    def norm_copy(k):
        peer = lax.rem(my_id + k, n_all)
        device = (peer // (n_data * n_stage), lax.rem(peer // n_stage, n_data), lax.rem(peer, n_stage))
        return remote(norm_buf.at[my_id], norm_buf.at[my_id], nsend.at[k], nrecv.at[my_id], device)
    for k in range(1, n_all):
        norm_copy(k).start()
    for k in range(1, n_all):
        peer = lax.rem(my_id + k, n_all)
        pltpu.make_async_copy(norm_buf.at[peer], norm_buf.at[peer], nrecv.at[peer]).wait()
    total = norm_buf[0]
    for k in range(1, n_all):
        total = total + norm_buf[k]
    norm_out[...] = total

    for k in range(1, n_all):
        norm_copy(k).wait_send()

    @pl.when(by_rows)
    def _():
        for copy in (send_acts, raw_gu, raw_gd, send_g):
            copy.wait_send()

    @pl.when(p == hub)
    def _():
        relay_over.wait_send()
        relay_back.wait_send()

    @pl.when(by_sums)
    def _():
        sum_gu.wait_send()
        sum_gd.wait_send()

    @pl.when(p > 0)
    def _():
        for c in range(nb):
            part_copy(c).wait_send()
            for zi in range(n_model):
                fin_copy(c, zi).wait_send()
    store_u.wait()
    store_d.wait()
    store_early.wait()
    store_late.wait()


def update_kernel(d_ref, lr_ref, mn_ref, norm_ref, gu, gd, wu, wd, mu, md, vu, vd, *rest):
    owu, owd, omu, omd, ovu, ovd = rest[:6]
    clip = clip_of(norm_ref[...], mn_ref[0])
    rate = lr_ref[0]
    owu[...], omu[...], ovu[...] = adamw_update(wu[...], mu[...], vu[...], clip * gu[...], rate)
    owd[...], omd[...], ovd[...] = adamw_update(wd[...], md[...], vd[...], clip * gd[...], rate)
    if len(rest) == 8:
        rest[6][...] = owu[...].astype(BF16)
        rest[7][...] = owd[...].astype(BF16)


def fill_kernel(d_ref, lr_ref, mn_ref, norm_ref, gu, gd_early, gd_rest, y_in, wu, wd, mu, md, vu, vd, *rest):
    owu, owd, omu, omd, ovu, ovd, y_out = rest[6:]
    clip = clip_of(norm_ref[...], mn_ref[0])
    rate = lr_ref[0]
    step = pl.program_id(0)
    gd = jnp.where(step < EARLY_ROWS // UPD_ROWS, gd_early[...], gd_rest[...])
    owu[...], omu[...], ovu[...] = adamw_update(wu[...], mu[...], vu[...], clip * gu[...], rate)
    owd[...], omd[...], ovd[...] = adamw_update(wd[...], md[...], vd[...], clip * gd, rate)
    y_out[...] = y_in[...]


def late_kernel(d_ref, lr_ref, mn_ref, norm_ref, gu, wu, mu, vu, *rest):
    owu, omu, ovu = rest[3:]
    clip = clip_of(norm_ref[...], mn_ref[0])
    owu[...], omu[...], ovu[...] = adamw_update(wu[...], mu[...], vu[...], clip * gu[...], lr_ref[0])


def fwd_kernel(dims, bu_hbm, bd_hbm, gbu_hbm, gbd_hbm, x_hbm,
               gu_oth, gd_oth, y_hbm,
               wu_bf, wd_bf, wu_z, wd_z, a_buf, y_buf, part, part_rcv, fin,
               ld_sem, ysend, yrecv, zsend, zrecv, psend, precv, fsend, frecv, agsend, agrecv, outsend, outrecv, turn):
    n_model, n_data, n_stage = dims
    z, d, p = lax.axis_index('model'), lax.axis_index('data'), lax.axis_index('stage')
    zo, do = 1 - z, 1 - d
    ypeer, zpeer = (z, do, p), (zo, d, p)
    last = n_stage - 1
    nc, rb, width = a_buf.shape
    half = wu_bf.shape[1] // 2
    hb = rb // 2
    own_ff = pl.ds(pl.multiple_of(d * half, 128), half)
    oth_ff = pl.ds(pl.multiple_of(do * half, 128), half)
    first = (p == 0) | (p == last)
    partner = (z, d, p + 1 - 2 * lax.rem(p, 2))

    load_u = pltpu.make_async_copy(bu_hbm, wu_bf.at[:, own_ff], ld_sem.at[0])
    load_d = pltpu.make_async_copy(bd_hbm, wd_bf.at[own_ff, :], ld_sem.at[1])
    load_u.start()
    load_d.start()
    x_load = pltpu.make_async_copy(x_hbm, a_buf, ld_sem.at[2])

    @pl.when(p == 0)
    def _():
        x_load.start()
    whole_barrier(n_model, n_data, n_stage)

    send_wu = remote(bu_hbm, wu_bf.at[:, own_ff], ysend.at[0], yrecv.at[0], ypeer)
    send_wd = remote(bd_hbm, wd_bf.at[own_ff, :], ysend.at[1], yrecv.at[1], ypeer)
    send_gu = remote(gbu_hbm.at[pl.ds(0, gu_oth.shape[0])], gu_oth, ysend.at[2], yrecv.at[2], ypeer)
    send_gd = remote(gbd_hbm.at[pl.ds(half - gd_oth.shape[0], gd_oth.shape[0])], gd_oth, ysend.at[3], yrecv.at[3], ypeer)

    shard = [
        remote(bu_hbm, wu_z.at[:, own_ff], zsend.at[0], zrecv.at[0], zpeer),
        remote(bd_hbm, wd_z.at[own_ff, :], zsend.at[1], zrecv.at[1], zpeer),
        remote(wu_bf.at[:, oth_ff], wu_z.at[:, oth_ff], zsend.at[2], zrecv.at[2], zpeer),
        remote(wd_bf.at[oth_ff, :], wd_z.at[oth_ff, :], zsend.at[3], zrecv.at[3], zpeer),
    ]

    @pl.when(p == last)
    def _():
        shard[0].start()
        shard[1].start()

    @pl.when(first)
    def _():
        send_wu.start()
        send_wd.start()
        send_wu.wait_send()
        send_wd.wait_send()
        pl.semaphore_signal(turn, inc=1, device_id=partner, device_id_type=MESH)

    @pl.when(jnp.logical_not(first))
    def _():
        pl.semaphore_wait(turn, 1)
        send_wu.start()
        send_wd.start()
        send_gu.start()
        send_gd.start()
        send_wu.wait_send()
        send_wd.wait_send()
        pl.semaphore_signal(turn, inc=1, device_id=partner, device_id_type=MESH)

    @pl.when(p == 0)
    def _():
        x_load.wait()
    load_u.wait()
    load_d.wait()
    send_wu.wait_recv()

    @pl.when(p == last)
    def _():
        shard[2].start()
    send_wd.wait_recv()

    @pl.when(p == last)
    def _():
        shard[3].start()
        for copy in shard:
            copy.wait_recv()

    def half_rows(zi):
        return pl.ds(pl.multiple_of(zi * hb, hb), hb)

    def part_copy(c):
        return remote(part.at[c, half_rows(zo)], part_rcv.at[c], psend.at[c], precv.at[c], zpeer)

    def fin_copy(c, zi):
        return remote(fin.at[c], a_buf.at[c, half_rows(z)], fsend.at[c, zi], frecv.at[c, z], (zi, d, lax.min(p + 1, last)))

    def gather_copy(c):
        return remote(fin.at[c], y_buf.at[c, half_rows(z)], agsend.at[c], agrecv.at[c], zpeer)

    def out_copy(c, q):
        return remote(y_buf.at[c], y_hbm.at[c], outsend.at[c, q], outrecv.at[c], (z, d, q))

    def out_local(c):
        return pltpu.make_async_copy(y_buf.at[c], y_hbm.at[c], outsend.at[c, last])

    def arrived(c, zi):
        pltpu.make_async_copy(fin.at[c], a_buf.at[c, half_rows(zi)], frecv.at[c, zi]).wait()

    def branch(rows_in, w_up, w_down):
        hid = gelu_val(mm(rows_in, w_up[...], NN)).astype(BF16)
        return mm(hid, w_down[...], NN)

    def compute(c):
        @pl.when(p < last)
        def _():
            @pl.when(p > 0)
            def _():
                for zi in range(n_model):
                    arrived(c, zi)
            part[c] = branch(a_buf[c], wu_bf, wd_bf)
            part_copy(c).start()

        @pl.when(p == last)
        def _():
            arrived(c, z)
            at = half_rows(z)
            rows_in = a_buf[c, at, :]
            total = branch(rows_in, wu_bf, wd_bf) + branch(rows_in, wu_z, wd_z)
            new = (rows_in.astype(F32) + total).astype(BF16)
            fin[c] = new
            y_buf[c, at, :] = new
            gather_copy(c).start()

    def finalize(c):
        part_copy(c).wait_recv()
        total = part[c, half_rows(z), :] + part_rcv[c]
        fin[c] = (a_buf[c, half_rows(z), :].astype(F32) + total).astype(BF16)
        fin_copy(c, z).start()

        @pl.when(p < last - 1)
        def _():
            fin_copy(c, zo).start()

    def publish(c):
        gather_copy(c).wait_recv()
        out_local(c).start()
        for q in range(last):
            out_copy(c, q).start()

    def chain(i, carry):
        @pl.when(i < nc)
        def _():
            compute(i)

        @pl.when((i >= 1) & (i <= nc) & (p < last))
        def _():
            finalize(i - 1)

        @pl.when((i >= 1) & (i <= nc) & (p == last))
        def _():
            publish(i - 1)

        @pl.when((i == TURN_STEP) & first)
        def _():
            pl.semaphore_wait(turn, 1)
            send_gu.start()
            send_gd.start()
        return carry
    lax.fori_loop(0, nc + 1, chain, 0)

    def drain(c, carry):
        @pl.when(p < last)
        def _():
            part_copy(c).wait_send()
            fin_copy(c, z).wait_send()

            @pl.when(p < last - 1)
            def _():
                fin_copy(c, zo).wait_send()
            pltpu.make_async_copy(y_buf.at[c], y_hbm.at[c], outrecv.at[c]).wait()

        @pl.when(p == last)
        def _():
            gather_copy(c).wait_send()
            out_local(c).wait()
            for q in range(last):
                out_copy(c, q).wait_send()
        return carry
    lax.fori_loop(0, nc, drain, 0)

    @pl.when(p == last)
    def _():
        for copy in shard:
            copy.wait_send()
    send_gu.wait()
    send_gd.wait()


def solution(mesh):
    n_model, n_data, n_stage = (mesh.shape[k] for k in ('model', 'data', 'stage'))
    dims = (n_model, n_data, n_stage)
    n_all = n_model * n_data * n_stage
    up_spec = P('stage', None, 'model')
    down_spec = P('stage', 'model', None)
    row_spec = P(None, 'data', None)
    in_specs = (up_spec, down_spec, up_spec, down_spec, up_spec, down_spec, P('data', 'stage', None, 'model'), P('data', 'stage', 'model', None), P('stage', 'data', None), P('data', None), row_spec, P(None), P(None))
    out_specs = (up_spec, down_spec, up_spec, down_spec, up_spec, down_spec, row_spec)
    any_spec = pl.BlockSpec(memory_space=pl.ANY)
    vmem_spec = pl.BlockSpec(memory_space=pltpu.VMEM)
    smem_spec = pl.BlockSpec(memory_space=pltpu.SMEM)
    dma = pltpu.SemaphoreType.DMA

    def device_step(w_up, w_down, m_up, m_down, v_up, v_down, g_up, g_down, acts_last, grad_out, x_next, learn_rate, max_norm):
        rows, width = grad_out.shape
        ff = w_up.shape[2]
        half = ff // 2
        nb = rows // BACK_ROWS
        hb = BACK_ROWS // 2
        sds = jax.ShapeDtypeStruct
        gbar_u, gbar_d, early, late, norm_tile = pl.pallas_call(
            functools.partial(bwd_kernel, dims),
            out_shape=(sds((width, half), F32), sds((half, width), F32), sds((EARLY_ROWS, width), F32), sds((LATE_ROWS, half), F32), sds((8, 128), F32)),
            in_specs=[any_spec] * 6,
            out_specs=(any_spec,) * 4 + (vmem_spec,),
            scratch_shapes=[
                pltpu.VMEM((width, ff), F32), pltpu.VMEM((ff, width), F32),
                pltpu.VMEM((width, ff), BF16), pltpu.VMEM((ff, width), BF16),
                pltpu.VMEM((2 * rows, width), BF16), pltpu.VMEM((2 * rows, width), BF16),
                pltpu.VMEM((rows, half), BF16), pltpu.VMEM((rows, half), BF16),
                pltpu.VMEM((rows, ff), F32), pltpu.VMEM((rows, half), F32),
                pltpu.VMEM((rows, ff), BF16), pltpu.VMEM((rows, ff), BF16),
            ] + [pltpu.VMEM((width, half), F32), pltpu.VMEM((half, width), F32)] * 3 + [
                pltpu.VMEM((nb, BACK_ROWS, width), F32), pltpu.VMEM((nb, hb, width), F32),
                pltpu.VMEM((nb, hb, width), BF16), pltpu.VMEM((n_all, 8, 128), F32),
                dma((8,)), dma((4,)), dma((4,)), dma((2,)), dma((2,)), dma((nb,)), dma((nb,)), dma((nb, 2)), dma((nb, 2)),
                dma((n_all,)), dma((n_all,)), dma((4,)),
            ],
            compiler_params=pltpu.CompilerParams(collective_id=0, has_side_effects=True, vmem_limit_bytes=VMEM_LIMIT),
            name='backward',
        )(w_up[0], w_down[0], acts_last[0], grad_out, g_up[0, 0], g_down[0, 0])

        early_oth = lax.ppermute(early, 'data', [(k, 1 - k) for k in range(n_data)])
        blocks = half // UPD_ROWS
        state = (w_up[0], w_down[0], m_up[0], m_down[0], v_up[0], v_down[0])
        state_shapes = tuple(sds(s.shape, F32) for s in state)
        which = lax.axis_index('data').astype(jnp.int32).reshape(1)

        def update_specs(pick):
            up = pl.BlockSpec((UPD_ROWS, half), lambda i, w: (i, pick(w[0])))
            down = pl.BlockSpec((UPD_ROWS, width), lambda i, w: (pick(w[0]) * blocks + i, 0))
            return [up, down]
        plain_up = pl.BlockSpec((UPD_ROWS, half), lambda i, w: (i, 0))
        plain_down = pl.BlockSpec((UPD_ROWS, width), lambda i, w: (i, 0))
        small = [smem_spec, smem_spec, pl.BlockSpec((8, 128), lambda i, w: (0, 0))]
        own = update_specs(lambda w: w)
        *fresh, b_up, b_down = pl.pallas_call(
            update_kernel,
            out_shape=state_shapes + (sds((width, half), BF16), sds((half, width), BF16)),
            grid_spec=pltpu.PrefetchScalarGridSpec(
                num_scalar_prefetch=1, grid=(width // UPD_ROWS,),
                in_specs=small + [plain_up, plain_down] + own * 3,
                out_specs=own * 3 + [plain_up, plain_down]),
            compiler_params=pltpu.CompilerParams(dimension_semantics=('arbitrary',), vmem_limit_bytes=VMEM_LIMIT),
            name='update_own',
        )(which, learn_rate, max_norm, norm_tile, gbar_u, gbar_d, *state)

        n_micro = x_next.shape[0]
        nc = n_micro * rows // FWD_ROWS
        fb = FWD_ROWS // 2
        gu_oth, gd_oth, y_next = pl.pallas_call(
            functools.partial(fwd_kernel, dims),
            out_shape=(sds((width - LATE_ROWS, half), F32), sds((half - EARLY_ROWS, width), F32), sds((nc, FWD_ROWS, width), BF16)),
            in_specs=[any_spec] * 5,
            out_specs=(any_spec, any_spec, any_spec),
            scratch_shapes=[pltpu.VMEM((width, ff), BF16), pltpu.VMEM((ff, width), BF16)] * 2 + [
                pltpu.VMEM((nc, FWD_ROWS, width), BF16), pltpu.VMEM((nc, FWD_ROWS, width), BF16),
                pltpu.VMEM((nc, FWD_ROWS, width), F32), pltpu.VMEM((nc, fb, width), F32),
                pltpu.VMEM((nc, fb, width), BF16),
                dma((3,)), dma((4,)), dma((4,)), dma((4,)), dma((4,)), dma((nc,)), dma((nc,)), dma((nc, 2)), dma((nc, 2)),
                dma((nc,)), dma((nc,)), dma((nc, n_stage)), dma((nc,)), pltpu.SemaphoreType.REGULAR,
            ],
            compiler_params=pltpu.CompilerParams(collective_id=1, has_side_effects=True, vmem_limit_bytes=VMEM_LIMIT),
            name='forward',
        )(b_up, b_down, gbar_u, gbar_d, x_next.reshape(nc, FWD_ROWS, width))

        other = update_specs(lambda w: 1 - w)
        gu_oth, late = lax.optimization_barrier((gu_oth, late))
        late_oth = lax.ppermute(late, 'data', [(k, 1 - k) for k in range(n_data)])
        y_next = y_next.reshape(n_micro * rows, width)
        nearly, nlate = EARLY_ROWS // UPD_ROWS, LATE_ROWS // UPD_ROWS
        steps = width // UPD_ROWS
        lastup = steps - nlate - 1

        def rows_spec(start, count):
            return pl.BlockSpec((UPD_ROWS, width), lambda i, w: (jnp.clip(i - start, 0, count - 1), 0))
        y_spec = pl.BlockSpec((n_micro * rows // steps, width), lambda i, w: (i, 0))
        up_oth = pl.BlockSpec((UPD_ROWS, half), lambda i, w: (jnp.minimum(i, lastup), 1 - w[0]))
        down_oth = pl.BlockSpec((UPD_ROWS, width), lambda i, w: ((1 - w[0]) * blocks + i, 0))
        other = [up_oth, down_oth]
        *filled, y_next = pl.pallas_call(
            fill_kernel,
            out_shape=state_shapes + (sds(y_next.shape, BF16),),
            grid_spec=pltpu.PrefetchScalarGridSpec(
                num_scalar_prefetch=1, grid=(steps,),
                in_specs=small + [rows_spec(0, lastup + 1), rows_spec(0, nearly), rows_spec(nearly, blocks - nearly), y_spec] + other * 3 + [any_spec] * 6,
                out_specs=other * 3 + [y_spec]),
            input_output_aliases={14 + k: k for k in range(6)},
            compiler_params=pltpu.CompilerParams(dimension_semantics=('arbitrary',), vmem_limit_bytes=VMEM_LIMIT),
            cost_estimate=pl.CostEstimate(flops=10**10, bytes_accessed=40 * 10**6, transcendentals=0),
            name='update_other',
        )(which, learn_rate, max_norm, norm_tile, gu_oth, early_oth, gd_oth, y_next, *state, *fresh)
        up_late = pl.BlockSpec((UPD_ROWS, half), lambda i, w: (steps - nlate + i, 1 - w[0]))
        filled[0], filled[2], filled[4] = pl.pallas_call(
            late_kernel,
            out_shape=(state_shapes[0],) * 3,
            grid_spec=pltpu.PrefetchScalarGridSpec(
                num_scalar_prefetch=1, grid=(nlate,),
                in_specs=small + [plain_up] + [up_late] * 3 + [any_spec] * 3,
                out_specs=[up_late] * 3),
            input_output_aliases={8 + k: k for k in range(3)},
            compiler_params=pltpu.CompilerParams(dimension_semantics=('arbitrary',), vmem_limit_bytes=VMEM_LIMIT),
            name='update_late',
        )(which, learn_rate, max_norm, norm_tile, late_oth, state[0], state[2], state[4], filled[0], filled[2], filled[4])
        return tuple(s[None] for s in filled) + (y_next.reshape(n_micro, rows, width),)

    return jax.shard_map(device_step, mesh=mesh, in_specs=in_specs, out_specs=out_specs, check_vma=False)
```

```python
import functools

import jax
import jax.numpy as jnp
from jax import lax
from jax.experimental import pallas as pl
from jax.experimental.pallas import tpu as pltpu
from jax.sharding import PartitionSpec as P

ADAM_STEP = 10
BETA_ONE = 0.9
BETA_TWO = 0.95
ADAM_EPS = 1e-8
WEIGHT_DECAY = 0.1
NORM_EPS = 1e-6
ONE_CORR = 1.0 - BETA_ONE ** ADAM_STEP
TWO_CORR = 1.0 - BETA_TWO ** ADAM_STEP
GELU_SCALE = (2.0 / 3.141592653589793) ** 0.5
GELU_CUBE = 0.044715
NN = (((1,), (0,)), ((), ()))
NT = (((1,), (1,)), ((), ()))
TN = (((0,), (0,)), ((), ()))
F32 = jnp.float32
BF16 = jnp.bfloat16
MESH = pl.DeviceIdType.MESH
BACK_ROWS = 64
PRE_BLOCK = 128
FWD_ROWS = 96
UPD_ROWS = 128
EARLY_ROWS = 256
LATE_ROWS = 128
TURN_STEP = 5
VMEM_LIMIT = 66_000_000


def mm(lhs, rhs, dims):
    return lax.dot_general(lhs, rhs, dims, preferred_element_type=F32)


def gelu_val(pre):
    return pre * (0.5 * (1.0 + jnp.tanh(GELU_SCALE * (pre + GELU_CUBE * (pre * pre * pre)))))


def gelu_both(pre):
    sq = pre * pre
    tan = jnp.tanh(GELU_SCALE * (pre + GELU_CUBE * (sq * pre)))
    cdf = 0.5 * (1.0 + tan)
    slope = cdf + 0.5 * pre * (1.0 - tan * tan) * (GELU_SCALE * (1.0 + (3.0 * GELU_CUBE) * sq))
    return pre * cdf, slope


def adamw_update(weight, moment_one, moment_two, grad_step, step_rate):
    mom_new = BETA_ONE * moment_one + (1.0 - BETA_ONE) * grad_step
    sec_new = BETA_TWO * moment_two + (1.0 - BETA_TWO) * grad_step * grad_step
    direction = (mom_new * (1.0 / ONE_CORR)) / (jnp.sqrt(sec_new * (1.0 / TWO_CORR)) + ADAM_EPS)
    weight_new = weight - step_rate * (direction + WEIGHT_DECAY * weight)
    return weight_new, mom_new, sec_new


def clip_of(norm_tile, max_norm):
    total = jnp.sum(jnp.sum(norm_tile, axis=0, keepdims=True), axis=1, keepdims=True)
    return jnp.minimum(1.0, max_norm / (jnp.sqrt(total) + NORM_EPS))


def whole_barrier(n_model, n_data, n_stage):
    barrier = pltpu.get_barrier_semaphore()
    me = (lax.axis_index('model'), lax.axis_index('data'), lax.axis_index('stage'))
    for dm in range(n_model):
        for dd in range(n_data):
            for ds in range(n_stage):
                if dm or dd or ds:
                    peer = (lax.rem(me[0] + dm, n_model), lax.rem(me[1] + dd, n_data), lax.rem(me[2] + ds, n_stage))
                    pl.semaphore_signal(barrier, inc=1, device_id=peer, device_id_type=MESH)
    pl.semaphore_wait(barrier, n_model * n_data * n_stage - 1)


def remote(src, dst, send_sem, recv_sem, device):
    return pltpu.make_async_remote_copy(src_ref=src, dst_ref=dst, send_sem=send_sem, recv_sem=recv_sem, device_id=device, device_id_type=MESH)


def bwd_kernel(dims, wu_hbm, wd_hbm, acts_hbm, dy_hbm, gu_hbm, gd_hbm,
               gbu_hbm, gbd_hbm, early_hbm, late_hbm, norm_out,
               wu32, wd32, wu_bf, wd_bf, aa, gg, hid_o, dz_o, slope, slope_o, dz_own, h_own,
               gu_own, gd_own, gu_oth, gd_oth, gu_rcv, gd_rcv, part, part_rcv, fin, norm_buf,
               ld_sem, ysend, yrecv, rsend, rrecv, psend, precv, fsend, frecv, nsend, nrecv, st_sem):
    n_model, n_data, n_stage = dims
    z, d, p = lax.axis_index('model'), lax.axis_index('data'), lax.axis_index('stage')
    zo, do = 1 - z, 1 - d
    ypeer, zpeer = (z, do, p), (zo, d, p)
    last = n_stage - 1
    by_rows = p == 0
    by_sums = p > 0
    hub = n_stage // 2
    rows = aa.shape[0] // 2
    width = aa.shape[1]
    half = hid_o.shape[1]
    rb = BACK_ROWS
    hb = rb // 2
    nb = rows // rb
    pb = PRE_BLOCK
    own_ff = pl.ds(pl.multiple_of(d * half, 128), half)
    oth_ff = pl.ds(pl.multiple_of(do * half, 128), half)
    mine, theirs = pl.ds(0, rows), pl.ds(rows, rows)

    loads = [
        pltpu.make_async_copy(wu_hbm, wu32, ld_sem.at[0]),
        pltpu.make_async_copy(acts_hbm, aa.at[mine], ld_sem.at[2]),
        pltpu.make_async_copy(wd_hbm, wd32, ld_sem.at[1]),
        pltpu.make_async_copy(gu_hbm.at[:, own_ff], gu_own, ld_sem.at[4]),
        pltpu.make_async_copy(gd_hbm.at[own_ff, :], gd_own, ld_sem.at[5]),
    ]
    dy_load = pltpu.make_async_copy(dy_hbm, gg.at[mine], ld_sem.at[3])
    gu_load = pltpu.make_async_copy(gu_hbm.at[:, oth_ff], gu_oth, ld_sem.at[6])
    gd_load = pltpu.make_async_copy(gd_hbm.at[oth_ff, :], gd_oth, ld_sem.at[7])
    for copy in loads[:3]:
        copy.start()

    @pl.when(p == last)
    def _():
        dy_load.start()
    for copy in loads[3:]:
        copy.start()

    @pl.when(by_sums)
    def _():
        gd_load.start()
        gu_load.start()

    whole_barrier(n_model, n_data, n_stage)
    send_acts = remote(acts_hbm, hid_o, ysend.at[0], rrecv.at[0], (z, d, hub))
    relay_over = remote(hid_o, dz_o, rsend.at[0], rrecv.at[1], ypeer)
    relay_back = remote(dz_o, aa.at[theirs], rsend.at[1], yrecv.at[0], (z, d, 0))
    raw_gu = remote(gu_hbm.at[:, oth_ff], gu_rcv, ysend.at[1], yrecv.at[1], ypeer)
    raw_gd = remote(gd_hbm.at[oth_ff, :], gd_rcv, ysend.at[2], yrecv.at[2], ypeer)
    sum_gu = remote(gu_oth, gu_rcv, ysend.at[1], yrecv.at[1], ypeer)
    sum_gd = remote(gd_oth, gd_rcv, ysend.at[2], yrecv.at[2], ypeer)
    send_g = remote(gg.at[mine], gg.at[theirs], ysend.at[3], yrecv.at[3], ypeer)

    @pl.when(by_rows)
    def _():
        send_acts.start()
        raw_gd.start()
        raw_gu.start()

    loads[0].wait()
    loads[1].wait()

    def cast_up(i, carry):
        at = pl.ds(pl.multiple_of(i * 128, 128), 128)
        wu_bf[at, :] = wu32[at, :].astype(BF16)
        return carry
    lax.fori_loop(0, width // 128, cast_up, 0)

    def own_pre(i, carry):
        at = pl.ds(pl.multiple_of(i * pb, pb), pb)
        val, slp = gelu_both(mm(aa[at, :], wu_bf[...], NN))
        h_own[at, :] = val.astype(BF16)
        slope[at, :] = slp
        return carry
    lax.fori_loop(0, rows // pb, own_pre, 0)
    loads[2].wait()

    def cast_down(i, carry):
        at = pl.ds(pl.multiple_of(i * 128, 128), 128)
        wd_bf[at, :] = wd32[at, :].astype(BF16)
        return carry
    lax.fori_loop(0, 2 * half // 128, cast_down, 0)

    @pl.when(p == last)
    def _():
        dy_load.wait()

    @pl.when(p == hub)
    def _():
        pltpu.make_async_copy(hid_o, hid_o, rrecv.at[0]).wait()
        relay_over.start()
        pltpu.make_async_copy(dz_o, dz_o, rrecv.at[1]).wait()
        relay_back.start()

    def down_block(j, base):
        at = pl.ds(pl.multiple_of(base * half + j * 128, 128), 128)
        return mm(h_own[:, at], gg[mine, :], TN)

    def up_block(j, ff_at):
        at = pl.ds(pl.multiple_of(j * 128, 128), 128)
        return mm(aa[mine, at], dz_own[:, ff_at], TN)

    def send_down():
        gd_load.wait()

        def down_oth(j, carry):
            gd_oth[pl.ds(pl.multiple_of(j * 128, 128), 128), :] += down_block(j, do)
            return carry
        lax.fori_loop(0, half // 128, down_oth, 0)
        gu_load.wait()
        sum_gd.start()

    @pl.when(p == last)
    def _():
        send_down()

    def g_at(c, zi):
        return gg.at[pl.ds(pl.multiple_of(c * rb + zi * hb, hb), hb)]

    def part_copy(c):
        return remote(part.at[c, pl.ds(pl.multiple_of(zo * hb, hb), hb)], part_rcv.at[c], psend.at[c], precv.at[c], zpeer)

    def fin_copy(c, zi):
        return remote(fin.at[c], g_at(c, z), fsend.at[c, zi], frecv.at[c, z], (zi, d, lax.max(p - 1, 0)))

    def compute(c):
        @pl.when(p < last)
        def _():
            for zi in range(n_model):
                pltpu.make_async_copy(fin.at[c], g_at(c, zi), frecv.at[c, zi]).wait()
        at = pl.ds(pl.multiple_of(c * rb, rb), rb)
        grad_hid = mm(gg[at, :], wd_bf[...], NT)
        dz_own[at, :] = (slope[at, :] * grad_hid).astype(BF16)

        @pl.when(p > 0)
        def _():
            part[c] = mm(dz_own[at, :], wu_bf[...], NT)
            part_copy(c).start()

    def finalize(c):
        part_copy(c).wait_recv()
        at = pl.ds(pl.multiple_of(c * rb + z * hb, hb), hb)
        total = part[c, pl.ds(pl.multiple_of(z * hb, hb), hb), :] + part_rcv[c]
        fin[c] = (gg[at, :].astype(F32) + total).astype(BF16)
        for zi in range(n_model):
            fin_copy(c, zi).start()

    def chain(i, carry):
        @pl.when(i < nb)
        def _():
            compute(i)

        @pl.when((i >= 1) & (p > 0))
        def _():
            finalize(i - 1)
        return carry
    lax.fori_loop(0, nb + 1, chain, 0)

    @pl.when(by_sums & (p < last))
    def _():
        send_down()

    @pl.when(by_sums)
    def _():
        def up_oth(j, carry):
            gu_oth[pl.ds(pl.multiple_of(j * 128, 128), 128), :] += up_block(j, oth_ff)
            return carry
        lax.fori_loop(0, width // 128, up_oth, 0)

    @pl.when(by_rows)
    def _():
        send_g.start()
    loads[3].wait()
    loads[4].wait()

    def down_own(j, carry):
        gd_own[pl.ds(pl.multiple_of(j * 128, 128), 128), :] += down_block(j, d)
        return carry
    lax.fori_loop(0, half // 128, down_own, 0)

    @pl.when(by_sums)
    def _():
        sum_gu.start()

    def up_own(j, carry):
        gu_own[pl.ds(pl.multiple_of(j * 128, 128), 128), :] += up_block(j, own_ff)
        return carry
    lax.fori_loop(0, width // 128, up_own, 0)

    @pl.when(by_rows)
    def _():
        pltpu.make_async_copy(aa.at[theirs], aa.at[theirs], yrecv.at[0]).wait()

        def oth_pre(i, carry):
            at = pl.ds(pl.multiple_of(i * pb, pb), pb)
            val, slp = gelu_both(mm(aa[pl.ds(pl.multiple_of(rows + i * pb, pb), pb), :], wu_bf[:, own_ff], NN))
            hid_o[at, :] = val.astype(BF16)
            slope_o[at, :] = slp
            return carry
        lax.fori_loop(0, rows // pb, oth_pre, 0)
        send_g.wait_recv()

        def oth_dz(i, carry):
            at = pl.ds(pl.multiple_of(i * pb, pb), pb)
            grad_hid = mm(gg[pl.ds(pl.multiple_of(rows + i * pb, pb), pb), :], wd_bf[own_ff, :], NT)
            dz_o[at, :] = (slope_o[at, :] * grad_hid).astype(BF16)
            return carry
        lax.fori_loop(0, rows // pb, oth_dz, 0)

        def oth_grads(j, carry):
            at = pl.ds(pl.multiple_of(j * 128, 128), 128)
            gd_own[at, :] += mm(hid_o[:, at], gg[theirs, :], TN)
            gu_own[at, :] += mm(aa[theirs, at], dz_o[...], TN)
            return carry
        lax.fori_loop(0, half // 128, oth_grads, 0)

    def combine(own, rcv):
        def body(i, acc):
            at = pl.ds(pl.multiple_of(i * 32, 32), 32)
            mean = (own[at, :] + rcv[at, :]) * 0.5
            own[at, :] = mean
            return acc + jnp.sum((mean * mean).reshape(4, 8, mean.shape[1]), axis=0)
        return body

    def combine_up(acc):
        raw_gu.wait_recv()
        return lax.fori_loop(0, gu_own.shape[0] // 32, combine(gu_own, gu_rcv), acc)

    def combine_down(acc):
        raw_gd.wait_recv()
        return lax.fori_loop(0, gd_own.shape[0] // 32, combine(gd_own, gd_rcv), acc)
    acc = jnp.zeros((8, half), F32)
    acc = combine_down(acc)
    store_d = pltpu.make_async_copy(gd_own, gbd_hbm, st_sem.at[1])
    store_d.start()
    store_early = pltpu.make_async_copy(gd_own.at[pl.ds(0, EARLY_ROWS)], early_hbm, st_sem.at[2])
    store_early.start()
    acc = combine_up(acc)
    store_u = pltpu.make_async_copy(gu_own, gbu_hbm, st_sem.at[0])
    store_u.start()
    store_late = pltpu.make_async_copy(gu_own.at[pl.ds(width - LATE_ROWS, LATE_ROWS)], late_hbm, st_sem.at[3])
    store_late.start()
    tile = acc[:, 0:128]
    for k in range(1, half // 128):
        tile = tile + acc[:, k * 128:(k + 1) * 128]
    n_all = n_model * n_data * n_stage
    my_id = (z * n_data + d) * n_stage + p
    norm_buf[my_id] = tile

    def norm_copy(k):
        peer = lax.rem(my_id + k, n_all)
        device = (peer // (n_data * n_stage), lax.rem(peer // n_stage, n_data), lax.rem(peer, n_stage))
        return remote(norm_buf.at[my_id], norm_buf.at[my_id], nsend.at[k], nrecv.at[my_id], device)
    for k in range(1, n_all):
        norm_copy(k).start()
    for k in range(1, n_all):
        peer = lax.rem(my_id + k, n_all)
        pltpu.make_async_copy(norm_buf.at[peer], norm_buf.at[peer], nrecv.at[peer]).wait()
    total = norm_buf[0]
    for k in range(1, n_all):
        total = total + norm_buf[k]
    norm_out[...] = total

    for k in range(1, n_all):
        norm_copy(k).wait_send()

    @pl.when(by_rows)
    def _():
        for copy in (send_acts, raw_gu, raw_gd, send_g):
            copy.wait_send()

    @pl.when(p == hub)
    def _():
        relay_over.wait_send()
        relay_back.wait_send()

    @pl.when(by_sums)
    def _():
        sum_gu.wait_send()
        sum_gd.wait_send()

    @pl.when(p > 0)
    def _():
        for c in range(nb):
            part_copy(c).wait_send()
            for zi in range(n_model):
                fin_copy(c, zi).wait_send()
    store_u.wait()
    store_d.wait()
    store_early.wait()
    store_late.wait()


def update_kernel(d_ref, lr_ref, mn_ref, norm_ref, gu, gd, wu, wd, mu, md, vu, vd, *rest):
    owu, owd, omu, omd, ovu, ovd = rest[:6]
    clip = clip_of(norm_ref[...], mn_ref[0])
    rate = lr_ref[0]
    owu[...], omu[...], ovu[...] = adamw_update(wu[...], mu[...], vu[...], clip * gu[...], rate)
    owd[...], omd[...], ovd[...] = adamw_update(wd[...], md[...], vd[...], clip * gd[...], rate)
    if len(rest) == 8:
        rest[6][...] = owu[...].astype(BF16)
        rest[7][...] = owd[...].astype(BF16)


def fill_kernel(d_ref, lr_ref, mn_ref, norm_ref, gu, gd_early, gd_rest, y_in, wu, wd, mu, md, vu, vd, *rest):
    owu, owd, omu, omd, ovu, ovd, y_out = rest[6:]
    clip = clip_of(norm_ref[...], mn_ref[0])
    rate = lr_ref[0]
    step = pl.program_id(0)
    gd = jnp.where(step < EARLY_ROWS // UPD_ROWS, gd_early[...], gd_rest[...])
    owu[...], omu[...], ovu[...] = adamw_update(wu[...], mu[...], vu[...], clip * gu[...], rate)
    owd[...], omd[...], ovd[...] = adamw_update(wd[...], md[...], vd[...], clip * gd, rate)
    y_out[...] = y_in[...]


def late_kernel(d_ref, lr_ref, mn_ref, norm_ref, gu, wu, mu, vu, *rest):
    owu, omu, ovu = rest[3:]
    clip = clip_of(norm_ref[...], mn_ref[0])
    owu[...], omu[...], ovu[...] = adamw_update(wu[...], mu[...], vu[...], clip * gu[...], lr_ref[0])


def fwd_kernel(dims, bu_hbm, bd_hbm, gbu_hbm, gbd_hbm, x_hbm,
               gu_oth, gd_oth, y_hbm,
               wu_bf, wd_bf, wu_z, wd_z, a_buf, y_buf, part, part_rcv, fin,
               ld_sem, ysend, yrecv, zsend, zrecv, psend, precv, fsend, frecv, agsend, agrecv, outsend, outrecv, turn):
    n_model, n_data, n_stage = dims
    z, d, p = lax.axis_index('model'), lax.axis_index('data'), lax.axis_index('stage')
    zo, do = 1 - z, 1 - d
    ypeer, zpeer = (z, do, p), (zo, d, p)
    last = n_stage - 1
    nc, rb, width = a_buf.shape
    half = wu_bf.shape[1] // 2
    hb = rb // 2
    own_ff = pl.ds(pl.multiple_of(d * half, 128), half)
    oth_ff = pl.ds(pl.multiple_of(do * half, 128), half)
    first = (p == 0) | (p == last)
    partner = (z, d, p + 1 - 2 * lax.rem(p, 2))

    load_u = pltpu.make_async_copy(bu_hbm, wu_bf.at[:, own_ff], ld_sem.at[0])
    load_d = pltpu.make_async_copy(bd_hbm, wd_bf.at[own_ff, :], ld_sem.at[1])
    load_u.start()
    load_d.start()
    x_load = pltpu.make_async_copy(x_hbm, a_buf, ld_sem.at[2])

    @pl.when(p == 0)
    def _():
        x_load.start()
    whole_barrier(n_model, n_data, n_stage)

    send_wu = remote(bu_hbm, wu_bf.at[:, own_ff], ysend.at[0], yrecv.at[0], ypeer)
    send_wd = remote(bd_hbm, wd_bf.at[own_ff, :], ysend.at[1], yrecv.at[1], ypeer)
    send_gu = remote(gbu_hbm.at[pl.ds(0, gu_oth.shape[0])], gu_oth, ysend.at[2], yrecv.at[2], ypeer)
    send_gd = remote(gbd_hbm.at[pl.ds(half - gd_oth.shape[0], gd_oth.shape[0])], gd_oth, ysend.at[3], yrecv.at[3], ypeer)

    shard = [
        remote(bu_hbm, wu_z.at[:, own_ff], zsend.at[0], zrecv.at[0], zpeer),
        remote(bd_hbm, wd_z.at[own_ff, :], zsend.at[1], zrecv.at[1], zpeer),
        remote(wu_bf.at[:, oth_ff], wu_z.at[:, oth_ff], zsend.at[2], zrecv.at[2], zpeer),
        remote(wd_bf.at[oth_ff, :], wd_z.at[oth_ff, :], zsend.at[3], zrecv.at[3], zpeer),
    ]

    @pl.when(p == last)
    def _():
        shard[0].start()
        shard[1].start()

    @pl.when(first)
    def _():
        send_wu.start()
        send_wd.start()
        send_wu.wait_send()
        send_wd.wait_send()
        pl.semaphore_signal(turn, inc=1, device_id=partner, device_id_type=MESH)

    @pl.when(jnp.logical_not(first))
    def _():
        pl.semaphore_wait(turn, 1)
        send_wu.start()
        send_wd.start()
        send_gu.start()
        send_gd.start()
        send_wu.wait_send()
        send_wd.wait_send()
        pl.semaphore_signal(turn, inc=1, device_id=partner, device_id_type=MESH)

    @pl.when(p == 0)
    def _():
        x_load.wait()
    load_u.wait()
    load_d.wait()
    send_wu.wait_recv()

    @pl.when(p == last)
    def _():
        shard[2].start()
    send_wd.wait_recv()

    @pl.when(p == last)
    def _():
        shard[3].start()
        for copy in shard:
            copy.wait_recv()

    def half_rows(zi):
        return pl.ds(pl.multiple_of(zi * hb, hb), hb)

    def part_copy(c):
        return remote(part.at[c, half_rows(zo)], part_rcv.at[c], psend.at[c], precv.at[c], zpeer)

    def fin_copy(c, zi):
        return remote(fin.at[c], a_buf.at[c, half_rows(z)], fsend.at[c, zi], frecv.at[c, z], (zi, d, lax.min(p + 1, last)))

    def gather_copy(c):
        return remote(fin.at[c], y_buf.at[c, half_rows(z)], agsend.at[c], agrecv.at[c], zpeer)

    def out_copy(c, q):
        return remote(y_buf.at[c], y_hbm.at[c], outsend.at[c, q], outrecv.at[c], (z, d, q))

    def out_local(c):
        return pltpu.make_async_copy(y_buf.at[c], y_hbm.at[c], outsend.at[c, last])

    def arrived(c, zi):
        pltpu.make_async_copy(fin.at[c], a_buf.at[c, half_rows(zi)], frecv.at[c, zi]).wait()

    def branch(rows_in, w_up, w_down):
        hid = gelu_val(mm(rows_in, w_up[...], NN)).astype(BF16)
        return mm(hid, w_down[...], NN)

    def compute(c):
        @pl.when(p < last)
        def _():
            @pl.when(p > 0)
            def _():
                for zi in range(n_model):
                    arrived(c, zi)
            part[c] = branch(a_buf[c], wu_bf, wd_bf)
            part_copy(c).start()

        @pl.when(p == last)
        def _():
            arrived(c, z)
            at = half_rows(z)
            rows_in = a_buf[c, at, :]
            total = branch(rows_in, wu_bf, wd_bf) + branch(rows_in, wu_z, wd_z)
            new = (rows_in.astype(F32) + total).astype(BF16)
            fin[c] = new
            y_buf[c, at, :] = new
            gather_copy(c).start()

    def finalize(c):
        part_copy(c).wait_recv()
        total = part[c, half_rows(z), :] + part_rcv[c]
        fin[c] = (a_buf[c, half_rows(z), :].astype(F32) + total).astype(BF16)
        fin_copy(c, z).start()

        @pl.when(p < last - 1)
        def _():
            fin_copy(c, zo).start()

    def publish(c):
        gather_copy(c).wait_recv()
        out_local(c).start()
        for q in range(last):
            out_copy(c, q).start()

    def chain(i, carry):
        @pl.when(i < nc)
        def _():
            compute(i)

        @pl.when((i >= 1) & (i <= nc) & (p < last))
        def _():
            finalize(i - 1)

        @pl.when((i >= 1) & (i <= nc) & (p == last))
        def _():
            publish(i - 1)

        @pl.when((i == TURN_STEP) & first)
        def _():
            pl.semaphore_wait(turn, 1)
            send_gu.start()
            send_gd.start()
        return carry
    lax.fori_loop(0, nc + 1, chain, 0)

    def drain(c, carry):
        @pl.when(p < last)
        def _():
            part_copy(c).wait_send()
            fin_copy(c, z).wait_send()

            @pl.when(p < last - 1)
            def _():
                fin_copy(c, zo).wait_send()
            pltpu.make_async_copy(y_buf.at[c], y_hbm.at[c], outrecv.at[c]).wait()

        @pl.when(p == last)
        def _():
            gather_copy(c).wait_send()
            out_local(c).wait()
            for q in range(last):
                out_copy(c, q).wait_send()
        return carry
    lax.fori_loop(0, nc, drain, 0)

    @pl.when(p == last)
    def _():
        for copy in shard:
            copy.wait_send()
    send_gu.wait()
    send_gd.wait()


def solution(mesh):
    n_model, n_data, n_stage = (mesh.shape[k] for k in ('model', 'data', 'stage'))
    dims = (n_model, n_data, n_stage)
    n_all = n_model * n_data * n_stage
    up_spec = P('stage', None, 'model')
    down_spec = P('stage', 'model', None)
    row_spec = P(None, 'data', None)
    in_specs = (up_spec, down_spec, up_spec, down_spec, up_spec, down_spec, P('data', 'stage', None, 'model'), P('data', 'stage', 'model', None), P('stage', 'data', None), P('data', None), row_spec, P(None), P(None))
    out_specs = (up_spec, down_spec, up_spec, down_spec, up_spec, down_spec, row_spec)
    any_spec = pl.BlockSpec(memory_space=pl.ANY)
    vmem_spec = pl.BlockSpec(memory_space=pltpu.VMEM)
    smem_spec = pl.BlockSpec(memory_space=pltpu.SMEM)
    dma = pltpu.SemaphoreType.DMA

    def device_step(w_up, w_down, m_up, m_down, v_up, v_down, g_up, g_down, acts_last, grad_out, x_next, learn_rate, max_norm):
        rows, width = grad_out.shape
        ff = w_up.shape[2]
        half = ff // 2
        nb = rows // BACK_ROWS
        hb = BACK_ROWS // 2
        sds = jax.ShapeDtypeStruct
        gbar_u, gbar_d, early, late, norm_tile = pl.pallas_call(
            functools.partial(bwd_kernel, dims),
            out_shape=(sds((width, half), F32), sds((half, width), F32), sds((EARLY_ROWS, width), F32), sds((LATE_ROWS, half), F32), sds((8, 128), F32)),
            in_specs=[any_spec] * 6,
            out_specs=(any_spec,) * 4 + (vmem_spec,),
            scratch_shapes=[
                pltpu.VMEM((width, ff), F32), pltpu.VMEM((ff, width), F32),
                pltpu.VMEM((width, ff), BF16), pltpu.VMEM((ff, width), BF16),
                pltpu.VMEM((2 * rows, width), BF16), pltpu.VMEM((2 * rows, width), BF16),
                pltpu.VMEM((rows, half), BF16), pltpu.VMEM((rows, half), BF16),
                pltpu.VMEM((rows, ff), F32), pltpu.VMEM((rows, half), F32),
                pltpu.VMEM((rows, ff), BF16), pltpu.VMEM((rows, ff), BF16),
            ] + [pltpu.VMEM((width, half), F32), pltpu.VMEM((half, width), F32)] * 3 + [
                pltpu.VMEM((nb, BACK_ROWS, width), F32), pltpu.VMEM((nb, hb, width), F32),
                pltpu.VMEM((nb, hb, width), BF16), pltpu.VMEM((n_all, 8, 128), F32),
                dma((8,)), dma((4,)), dma((4,)), dma((2,)), dma((2,)), dma((nb,)), dma((nb,)), dma((nb, 2)), dma((nb, 2)),
                dma((n_all,)), dma((n_all,)), dma((4,)),
            ],
            compiler_params=pltpu.CompilerParams(collective_id=0, has_side_effects=True, vmem_limit_bytes=VMEM_LIMIT),
            name='backward',
        )(w_up[0], w_down[0], acts_last[0], grad_out, g_up[0, 0], g_down[0, 0])

        early_oth = lax.ppermute(early, 'data', [(k, 1 - k) for k in range(n_data)])
        blocks = half // UPD_ROWS
        state = (w_up[0], w_down[0], m_up[0], m_down[0], v_up[0], v_down[0])
        state_shapes = tuple(sds(s.shape, F32) for s in state)
        which = lax.axis_index('data').astype(jnp.int32).reshape(1)

        def update_specs(pick):
            up = pl.BlockSpec((UPD_ROWS, half), lambda i, w: (i, pick(w[0])))
            down = pl.BlockSpec((UPD_ROWS, width), lambda i, w: (pick(w[0]) * blocks + i, 0))
            return [up, down]
        plain_up = pl.BlockSpec((UPD_ROWS, half), lambda i, w: (i, 0))
        plain_down = pl.BlockSpec((UPD_ROWS, width), lambda i, w: (i, 0))
        small = [smem_spec, smem_spec, pl.BlockSpec((8, 128), lambda i, w: (0, 0))]
        own = update_specs(lambda w: w)
        *fresh, b_up, b_down = pl.pallas_call(
            update_kernel,
            out_shape=state_shapes + (sds((width, half), BF16), sds((half, width), BF16)),
            grid_spec=pltpu.PrefetchScalarGridSpec(
                num_scalar_prefetch=1, grid=(width // UPD_ROWS,),
                in_specs=small + [plain_up, plain_down] + own * 3,
                out_specs=own * 3 + [plain_up, plain_down]),
            compiler_params=pltpu.CompilerParams(dimension_semantics=('arbitrary',), vmem_limit_bytes=VMEM_LIMIT),
            name='update_own',
        )(which, learn_rate, max_norm, norm_tile, gbar_u, gbar_d, *state)

        n_micro = x_next.shape[0]
        nc = n_micro * rows // FWD_ROWS
        fb = FWD_ROWS // 2
        gu_oth, gd_oth, y_next = pl.pallas_call(
            functools.partial(fwd_kernel, dims),
            out_shape=(sds((width - LATE_ROWS, half), F32), sds((half - EARLY_ROWS, width), F32), sds((nc, FWD_ROWS, width), BF16)),
            in_specs=[any_spec] * 5,
            out_specs=(any_spec, any_spec, any_spec),
            scratch_shapes=[pltpu.VMEM((width, ff), BF16), pltpu.VMEM((ff, width), BF16)] * 2 + [
                pltpu.VMEM((nc, FWD_ROWS, width), BF16), pltpu.VMEM((nc, FWD_ROWS, width), BF16),
                pltpu.VMEM((nc, FWD_ROWS, width), F32), pltpu.VMEM((nc, fb, width), F32),
                pltpu.VMEM((nc, fb, width), BF16),
                dma((3,)), dma((4,)), dma((4,)), dma((4,)), dma((4,)), dma((nc,)), dma((nc,)), dma((nc, 2)), dma((nc, 2)),
                dma((nc,)), dma((nc,)), dma((nc, n_stage)), dma((nc,)), pltpu.SemaphoreType.REGULAR,
            ],
            compiler_params=pltpu.CompilerParams(collective_id=1, has_side_effects=True, vmem_limit_bytes=VMEM_LIMIT),
            name='forward',
        )(b_up, b_down, gbar_u, gbar_d, x_next.reshape(nc, FWD_ROWS, width))

        other = update_specs(lambda w: 1 - w)
        gu_oth, late = lax.optimization_barrier((gu_oth, late))
        late_oth = lax.ppermute(late, 'data', [(k, 1 - k) for k in range(n_data)])
        y_next = y_next.reshape(n_micro * rows, width)
        nearly, nlate = EARLY_ROWS // UPD_ROWS, LATE_ROWS // UPD_ROWS
        steps = width // UPD_ROWS
        lastup = steps - nlate - 1

        def rows_spec(start, count):
            return pl.BlockSpec((UPD_ROWS, width), lambda i, w: (jnp.clip(i - start, 0, count - 1), 0))
        y_spec = pl.BlockSpec((n_micro * rows // steps, width), lambda i, w: (i, 0))
        up_oth = pl.BlockSpec((UPD_ROWS, half), lambda i, w: (jnp.minimum(i, lastup), 1 - w[0]))
        down_oth = pl.BlockSpec((UPD_ROWS, width), lambda i, w: ((1 - w[0]) * blocks + i, 0))
        other = [up_oth, down_oth]
        *filled, y_next = pl.pallas_call(
            fill_kernel,
            out_shape=state_shapes + (sds(y_next.shape, BF16),),
            grid_spec=pltpu.PrefetchScalarGridSpec(
                num_scalar_prefetch=1, grid=(steps,),
                in_specs=small + [rows_spec(0, lastup + 1), rows_spec(0, nearly), rows_spec(nearly, blocks - nearly), y_spec] + other * 3 + [any_spec] * 6,
                out_specs=other * 3 + [y_spec]),
            input_output_aliases={14 + k: k for k in range(6)},
            compiler_params=pltpu.CompilerParams(dimension_semantics=('arbitrary',), vmem_limit_bytes=VMEM_LIMIT),
            cost_estimate=pl.CostEstimate(flops=10**10, bytes_accessed=40 * 10**6, transcendentals=0),
            name='update_other',
        )(which, learn_rate, max_norm, norm_tile, gu_oth, early_oth, gd_oth, y_next, *state, *fresh)
        up_late = pl.BlockSpec((UPD_ROWS, half), lambda i, w: (steps - nlate + i, 1 - w[0]))
        filled[0], filled[2], filled[4] = pl.pallas_call(
            late_kernel,
            out_shape=(state_shapes[0],) * 3,
            grid_spec=pltpu.PrefetchScalarGridSpec(
                num_scalar_prefetch=1, grid=(nlate,),
                in_specs=small + [plain_up] + [up_late] * 3 + [any_spec] * 3,
                out_specs=[up_late] * 3),
            input_output_aliases={8 + k: k for k in range(3)},
            compiler_params=pltpu.CompilerParams(dimension_semantics=('arbitrary',), vmem_limit_bytes=VMEM_LIMIT),
            name='update_late',
        )(which, learn_rate, max_norm, norm_tile, late_oth, state[0], state[2], state[4], filled[0], filled[2], filled[4])
        return tuple(s[None] for s in filled) + (y_next.reshape(n_micro, rows, width),)

    return jax.shard_map(device_step, mesh=mesh, in_specs=in_specs, out_specs=out_specs, check_vma=False)
```

```python
import functools

import jax
import jax.numpy as jnp
from jax import lax
from jax.experimental import pallas as pl
from jax.experimental.pallas import tpu as pltpu
from jax.sharding import PartitionSpec as P

ADAM_STEP = 10
BETA_ONE = 0.9
BETA_TWO = 0.95
ADAM_EPS = 1e-8
WEIGHT_DECAY = 0.1
NORM_EPS = 1e-6
ONE_CORR = 1.0 - BETA_ONE ** ADAM_STEP
TWO_CORR = 1.0 - BETA_TWO ** ADAM_STEP
GELU_SCALE = (2.0 / 3.141592653589793) ** 0.5
GELU_CUBE = 0.044715
NN = (((1,), (0,)), ((), ()))
NT = (((1,), (1,)), ((), ()))
TN = (((0,), (0,)), ((), ()))
F32 = jnp.float32
BF16 = jnp.bfloat16
MESH = pl.DeviceIdType.MESH
BACK_ROWS = 128
FWD_ROWS = 96
UPD_ROWS = 128
EARLY_ROWS = 256
LATE_ROWS = 128
TURN_STEP = 5
VMEM_LIMIT = 66_000_000


def mm(lhs, rhs, dims):
    return lax.dot_general(lhs, rhs, dims, preferred_element_type=F32)


def gelu_val(pre):
    return pre * (0.5 * (1.0 + jnp.tanh(GELU_SCALE * (pre + GELU_CUBE * (pre * pre * pre)))))


def gelu_both(pre):
    sq = pre * pre
    tan = jnp.tanh(GELU_SCALE * (pre + GELU_CUBE * (sq * pre)))
    cdf = 0.5 * (1.0 + tan)
    slope = cdf + 0.5 * pre * (1.0 - tan * tan) * (GELU_SCALE * (1.0 + (3.0 * GELU_CUBE) * sq))
    return pre * cdf, slope


def adamw_update(weight, moment_one, moment_two, grad_step, step_rate):
    mom_new = BETA_ONE * moment_one + (1.0 - BETA_ONE) * grad_step
    sec_new = BETA_TWO * moment_two + (1.0 - BETA_TWO) * grad_step * grad_step
    direction = (mom_new * (1.0 / ONE_CORR)) / (jnp.sqrt(sec_new * (1.0 / TWO_CORR)) + ADAM_EPS)
    weight_new = weight - step_rate * (direction + WEIGHT_DECAY * weight)
    return weight_new, mom_new, sec_new


def clip_of(norm_tile, max_norm):
    total = jnp.sum(jnp.sum(norm_tile, axis=0, keepdims=True), axis=1, keepdims=True)
    return jnp.minimum(1.0, max_norm / (jnp.sqrt(total) + NORM_EPS))


def whole_barrier(n_model, n_data, n_stage):
    barrier = pltpu.get_barrier_semaphore()
    me = (lax.axis_index('model'), lax.axis_index('data'), lax.axis_index('stage'))
    for dm in range(n_model):
        for dd in range(n_data):
            for ds in range(n_stage):
                if dm or dd or ds:
                    peer = (lax.rem(me[0] + dm, n_model), lax.rem(me[1] + dd, n_data), lax.rem(me[2] + ds, n_stage))
                    pl.semaphore_signal(barrier, inc=1, device_id=peer, device_id_type=MESH)
    pl.semaphore_wait(barrier, n_model * n_data * n_stage - 1)


def remote(src, dst, send_sem, recv_sem, device):
    return pltpu.make_async_remote_copy(src_ref=src, dst_ref=dst, send_sem=send_sem, recv_sem=recv_sem, device_id=device, device_id_type=MESH)


def bwd_kernel(dims, wu_hbm, wd_hbm, acts_hbm, dy_hbm, gu_hbm, gd_hbm,
               gbu_hbm, gbd_hbm, early_hbm, late_hbm, norm_out,
               wu32, wd32, wu_bf, wd_bf, aa, gg, hid_o, dz_o, slope, slope_o, dz_own, h_own,
               gu_own, gd_own, gu_oth, gd_oth, gu_rcv, gd_rcv, part, part_rcv, fin, norm_buf,
               ld_sem, ysend, yrecv, rsend, rrecv, psend, precv, fsend, frecv, nsend, nrecv, st_sem):
    n_model, n_data, n_stage = dims
    z, d, p = lax.axis_index('model'), lax.axis_index('data'), lax.axis_index('stage')
    zo, do = 1 - z, 1 - d
    ypeer, zpeer = (z, do, p), (zo, d, p)
    last = n_stage - 1
    by_rows = p == 0
    by_sums = p > 0
    hub = n_stage // 2
    rows = aa.shape[0] // 2
    width = aa.shape[1]
    half = hid_o.shape[1]
    rb = BACK_ROWS
    hb = rb // 2
    nb = rows // rb
    own_ff = pl.ds(pl.multiple_of(d * half, 128), half)
    oth_ff = pl.ds(pl.multiple_of(do * half, 128), half)
    mine, theirs = pl.ds(0, rows), pl.ds(rows, rows)

    loads = [
        pltpu.make_async_copy(wu_hbm, wu32, ld_sem.at[0]),
        pltpu.make_async_copy(acts_hbm, aa.at[mine], ld_sem.at[2]),
        pltpu.make_async_copy(wd_hbm, wd32, ld_sem.at[1]),
        pltpu.make_async_copy(gu_hbm.at[:, own_ff], gu_own, ld_sem.at[4]),
        pltpu.make_async_copy(gd_hbm.at[own_ff, :], gd_own, ld_sem.at[5]),
    ]
    dy_load = pltpu.make_async_copy(dy_hbm, gg.at[mine], ld_sem.at[3])
    gu_load = pltpu.make_async_copy(gu_hbm.at[:, oth_ff], gu_oth, ld_sem.at[6])
    gd_load = pltpu.make_async_copy(gd_hbm.at[oth_ff, :], gd_oth, ld_sem.at[7])
    for copy in loads[:3]:
        copy.start()

    @pl.when(p == last)
    def _():
        dy_load.start()
    whole_barrier(n_model, n_data, n_stage)
    send_acts = remote(acts_hbm, hid_o, ysend.at[0], rrecv.at[0], (z, d, hub))
    relay_over = remote(hid_o, dz_o, rsend.at[0], rrecv.at[1], ypeer)
    relay_back = remote(dz_o, aa.at[theirs], rsend.at[1], yrecv.at[0], (z, d, 0))
    raw_gu = remote(gu_hbm.at[:, oth_ff], gu_rcv, ysend.at[1], yrecv.at[1], ypeer)
    raw_gd = remote(gd_hbm.at[oth_ff, :], gd_rcv, ysend.at[2], yrecv.at[2], ypeer)
    sum_gu = remote(gu_oth, gu_rcv, ysend.at[1], yrecv.at[1], ypeer)
    sum_gd = remote(gd_oth, gd_rcv, ysend.at[2], yrecv.at[2], ypeer)
    send_g = remote(gg.at[mine], gg.at[theirs], ysend.at[3], yrecv.at[3], ypeer)

    @pl.when(by_rows)
    def _():
        send_acts.start()
        raw_gd.start()
        raw_gu.start()

    loads[0].wait()
    loads[1].wait()

    def cast_up(i, carry):
        at = pl.ds(pl.multiple_of(i * 128, 128), 128)
        wu_bf[at, :] = wu32[at, :].astype(BF16)
        return carry
    lax.fori_loop(0, width // 128, cast_up, 0)

    def own_pre(i, carry):
        at = pl.ds(pl.multiple_of(i * rb, rb), rb)
        val, slp = gelu_both(mm(aa[at, :], wu_bf[...], NN))
        h_own[at, :] = val.astype(BF16)
        slope[at, :] = slp
        return carry
    loads[2].wait()

    @pl.when(by_sums)
    def _():
        gd_load.start()
        gu_load.start()
    for copy in loads[3:]:
        copy.start()
    lax.fori_loop(0, nb, own_pre, 0)

    def cast_down(i, carry):
        at = pl.ds(pl.multiple_of(i * 128, 128), 128)
        wd_bf[at, :] = wd32[at, :].astype(BF16)
        return carry
    lax.fori_loop(0, 2 * half // 128, cast_down, 0)

    @pl.when(p == last)
    def _():
        dy_load.wait()

    @pl.when(p == hub)
    def _():
        pltpu.make_async_copy(hid_o, hid_o, rrecv.at[0]).wait()
        relay_over.start()
        pltpu.make_async_copy(dz_o, dz_o, rrecv.at[1]).wait()
        relay_back.start()

    def down_block(j, base):
        at = pl.ds(pl.multiple_of(base * half + j * 128, 128), 128)
        return mm(h_own[:, at], gg[mine, :], TN)

    def up_block(j, ff_at):
        at = pl.ds(pl.multiple_of(j * 128, 128), 128)
        return mm(aa[mine, at], dz_own[:, ff_at], TN)

    def send_down():
        gd_load.wait()

        def down_oth(j, carry):
            gd_oth[pl.ds(pl.multiple_of(j * 128, 128), 128), :] += down_block(j, do)
            return carry
        lax.fori_loop(0, half // 128, down_oth, 0)
        gu_load.wait()
        sum_gd.start()

    @pl.when(p == last)
    def _():
        send_down()

    def g_at(c, zi):
        return gg.at[pl.ds(pl.multiple_of(c * rb + zi * hb, hb), hb)]

    def part_copy(c):
        return remote(part.at[c, pl.ds(pl.multiple_of(zo * hb, hb), hb)], part_rcv.at[c], psend.at[c], precv.at[c], zpeer)

    def fin_copy(c, zi):
        return remote(fin.at[c], g_at(c, z), fsend.at[c, zi], frecv.at[c, z], (zi, d, lax.max(p - 1, 0)))

    def compute(c):
        @pl.when(p < last)
        def _():
            for zi in range(n_model):
                pltpu.make_async_copy(fin.at[c], g_at(c, zi), frecv.at[c, zi]).wait()
        at = pl.ds(pl.multiple_of(c * rb, rb), rb)
        grad_hid = mm(gg[at, :], wd_bf[...], NT)
        dz_own[at, :] = (slope[at, :] * grad_hid).astype(BF16)

        @pl.when(p > 0)
        def _():
            part[c] = mm(dz_own[at, :], wu_bf[...], NT)
            part_copy(c).start()

    def finalize(c):
        part_copy(c).wait_recv()
        at = pl.ds(pl.multiple_of(c * rb + z * hb, hb), hb)
        total = part[c, pl.ds(pl.multiple_of(z * hb, hb), hb), :] + part_rcv[c]
        fin[c] = (gg[at, :].astype(F32) + total).astype(BF16)
        for zi in range(n_model):
            fin_copy(c, zi).start()

    def chain(i, carry):
        compute(i)

        @pl.when((i >= 1) & (p > 0))
        def _():
            finalize(i - 1)
        return carry
    lax.fori_loop(0, nb, chain, 0)

    @pl.when(by_sums & (p < hub))
    def _():
        send_down()

    @pl.when(p > 0)
    def _():
        finalize(nb - 1)

    @pl.when((p >= hub) & (p < last))
    def _():
        send_down()

    @pl.when(by_sums)
    def _():
        def up_oth(j, carry):
            gu_oth[pl.ds(pl.multiple_of(j * 128, 128), 128), :] += up_block(j, oth_ff)
            return carry
        lax.fori_loop(0, width // 128, up_oth, 0)

    @pl.when(by_rows)
    def _():
        send_g.start()
    loads[3].wait()
    loads[4].wait()

    def down_own(j, carry):
        gd_own[pl.ds(pl.multiple_of(j * 128, 128), 128), :] += down_block(j, d)
        return carry
    lax.fori_loop(0, half // 128, down_own, 0)

    @pl.when(by_sums)
    def _():
        sum_gu.start()

    def up_own(j, carry):
        gu_own[pl.ds(pl.multiple_of(j * 128, 128), 128), :] += up_block(j, own_ff)
        return carry
    lax.fori_loop(0, width // 128, up_own, 0)

    @pl.when(by_rows)
    def _():
        pltpu.make_async_copy(aa.at[theirs], aa.at[theirs], yrecv.at[0]).wait()

        def oth_pre(i, carry):
            at = pl.ds(pl.multiple_of(i * rb, rb), rb)
            val, slp = gelu_both(mm(aa[pl.ds(pl.multiple_of(rows + i * rb, rb), rb), :], wu_bf[:, own_ff], NN))
            hid_o[at, :] = val.astype(BF16)
            slope_o[at, :] = slp
            return carry
        lax.fori_loop(0, nb, oth_pre, 0)
        send_g.wait_recv()

        def oth_dz(i, carry):
            at = pl.ds(pl.multiple_of(i * rb, rb), rb)
            grad_hid = mm(gg[pl.ds(pl.multiple_of(rows + i * rb, rb), rb), :], wd_bf[own_ff, :], NT)
            dz_o[at, :] = (slope_o[at, :] * grad_hid).astype(BF16)
            return carry
        lax.fori_loop(0, nb, oth_dz, 0)

        def oth_grads(j, carry):
            at = pl.ds(pl.multiple_of(j * 128, 128), 128)
            gd_own[at, :] += mm(hid_o[:, at], gg[theirs, :], TN)
            gu_own[at, :] += mm(aa[theirs, at], dz_o[...], TN)
            return carry
        lax.fori_loop(0, half // 128, oth_grads, 0)

    def combine(own, rcv):
        def body(i, acc):
            at = pl.ds(pl.multiple_of(i * 32, 32), 32)
            mean = (own[at, :] + rcv[at, :]) * 0.5
            own[at, :] = mean
            return acc + jnp.sum((mean * mean).reshape(4, 8, mean.shape[1]), axis=0)
        return body

    def combine_up(acc):
        raw_gu.wait_recv()
        return lax.fori_loop(0, gu_own.shape[0] // 32, combine(gu_own, gu_rcv), acc)

    def combine_down(acc):
        raw_gd.wait_recv()
        return lax.fori_loop(0, gd_own.shape[0] // 32, combine(gd_own, gd_rcv), acc)
    acc = jnp.zeros((8, half), F32)
    acc = combine_down(acc)
    store_d = pltpu.make_async_copy(gd_own, gbd_hbm, st_sem.at[1])
    store_d.start()
    store_early = pltpu.make_async_copy(gd_own.at[pl.ds(0, EARLY_ROWS)], early_hbm, st_sem.at[2])
    store_early.start()
    acc = combine_up(acc)
    store_u = pltpu.make_async_copy(gu_own, gbu_hbm, st_sem.at[0])
    store_u.start()
    store_late = pltpu.make_async_copy(gu_own.at[pl.ds(width - LATE_ROWS, LATE_ROWS)], late_hbm, st_sem.at[3])
    store_late.start()
    tile = acc[:, 0:128]
    for k in range(1, half // 128):
        tile = tile + acc[:, k * 128:(k + 1) * 128]
    n_all = n_model * n_data * n_stage
    my_id = (z * n_data + d) * n_stage + p
    norm_buf[my_id] = tile

    def norm_copy(k):
        peer = lax.rem(my_id + k, n_all)
        device = (peer // (n_data * n_stage), lax.rem(peer // n_stage, n_data), lax.rem(peer, n_stage))
        return remote(norm_buf.at[my_id], norm_buf.at[my_id], nsend.at[k], nrecv.at[my_id], device)
    for k in range(1, n_all):
        norm_copy(k).start()
    for k in range(1, n_all):
        peer = lax.rem(my_id + k, n_all)
        pltpu.make_async_copy(norm_buf.at[peer], norm_buf.at[peer], nrecv.at[peer]).wait()
    total = norm_buf[0]
    for k in range(1, n_all):
        total = total + norm_buf[k]
    norm_out[...] = total

    for k in range(1, n_all):
        norm_copy(k).wait_send()

    @pl.when(by_rows)
    def _():
        for copy in (send_acts, raw_gu, raw_gd, send_g):
            copy.wait_send()

    @pl.when(p == hub)
    def _():
        relay_over.wait_send()
        relay_back.wait_send()

    @pl.when(by_sums)
    def _():
        sum_gu.wait_send()
        sum_gd.wait_send()

    @pl.when(p > 0)
    def _():
        for c in range(nb):
            part_copy(c).wait_send()
            for zi in range(n_model):
                fin_copy(c, zi).wait_send()
    store_u.wait()
    store_d.wait()
    store_early.wait()
    store_late.wait()


def update_kernel(d_ref, lr_ref, mn_ref, norm_ref, gu, gd, wu, wd, mu, md, vu, vd, *rest):
    owu, owd, omu, omd, ovu, ovd = rest[:6]
    clip = clip_of(norm_ref[...], mn_ref[0])
    rate = lr_ref[0]
    owu[...], omu[...], ovu[...] = adamw_update(wu[...], mu[...], vu[...], clip * gu[...], rate)
    owd[...], omd[...], ovd[...] = adamw_update(wd[...], md[...], vd[...], clip * gd[...], rate)
    if len(rest) == 8:
        rest[6][...] = owu[...].astype(BF16)
        rest[7][...] = owd[...].astype(BF16)


def fill_kernel(d_ref, lr_ref, mn_ref, norm_ref, gu, gd_early, gd_rest, y_in, wu, wd, mu, md, vu, vd, *rest):
    owu, owd, omu, omd, ovu, ovd, y_out = rest[6:]
    clip = clip_of(norm_ref[...], mn_ref[0])
    rate = lr_ref[0]
    step = pl.program_id(0)
    gd = jnp.where(step < EARLY_ROWS // UPD_ROWS, gd_early[...], gd_rest[...])
    owu[...], omu[...], ovu[...] = adamw_update(wu[...], mu[...], vu[...], clip * gu[...], rate)
    owd[...], omd[...], ovd[...] = adamw_update(wd[...], md[...], vd[...], clip * gd, rate)
    y_out[...] = y_in[...]


def late_kernel(d_ref, lr_ref, mn_ref, norm_ref, gu, wu, mu, vu, *rest):
    owu, omu, ovu = rest[3:]
    clip = clip_of(norm_ref[...], mn_ref[0])
    owu[...], omu[...], ovu[...] = adamw_update(wu[...], mu[...], vu[...], clip * gu[...], lr_ref[0])


def fwd_kernel(dims, bu_hbm, bd_hbm, gbu_hbm, gbd_hbm, x_hbm,
               gu_oth, gd_oth, y_hbm,
               wu_bf, wd_bf, wu_z, wd_z, a_buf, y_buf, part, part_rcv, fin,
               ld_sem, ysend, yrecv, zsend, zrecv, psend, precv, fsend, frecv, agsend, agrecv, outsend, outrecv, turn):
    n_model, n_data, n_stage = dims
    z, d, p = lax.axis_index('model'), lax.axis_index('data'), lax.axis_index('stage')
    zo, do = 1 - z, 1 - d
    ypeer, zpeer = (z, do, p), (zo, d, p)
    last = n_stage - 1
    nc, rb, width = a_buf.shape
    half = wu_bf.shape[1] // 2
    hb = rb // 2
    own_ff = pl.ds(pl.multiple_of(d * half, 128), half)
    oth_ff = pl.ds(pl.multiple_of(do * half, 128), half)
    first = (p == 0) | (p == last)
    partner = (z, d, p + 1 - 2 * lax.rem(p, 2))

    load_u = pltpu.make_async_copy(bu_hbm, wu_bf.at[:, own_ff], ld_sem.at[0])
    load_d = pltpu.make_async_copy(bd_hbm, wd_bf.at[own_ff, :], ld_sem.at[1])
    load_u.start()
    load_d.start()
    x_load = pltpu.make_async_copy(x_hbm, a_buf, ld_sem.at[2])

    @pl.when(p == 0)
    def _():
        x_load.start()
    whole_barrier(n_model, n_data, n_stage)

    send_wu = remote(bu_hbm, wu_bf.at[:, own_ff], ysend.at[0], yrecv.at[0], ypeer)
    send_wd = remote(bd_hbm, wd_bf.at[own_ff, :], ysend.at[1], yrecv.at[1], ypeer)
    send_gu = remote(gbu_hbm.at[pl.ds(0, gu_oth.shape[0])], gu_oth, ysend.at[2], yrecv.at[2], ypeer)
    send_gd = remote(gbd_hbm.at[pl.ds(half - gd_oth.shape[0], gd_oth.shape[0])], gd_oth, ysend.at[3], yrecv.at[3], ypeer)

    shard = [
        remote(bu_hbm, wu_z.at[:, own_ff], zsend.at[0], zrecv.at[0], zpeer),
        remote(bd_hbm, wd_z.at[own_ff, :], zsend.at[1], zrecv.at[1], zpeer),
        remote(wu_bf.at[:, oth_ff], wu_z.at[:, oth_ff], zsend.at[2], zrecv.at[2], zpeer),
        remote(wd_bf.at[oth_ff, :], wd_z.at[oth_ff, :], zsend.at[3], zrecv.at[3], zpeer),
    ]

    @pl.when(p == last)
    def _():
        shard[0].start()
        shard[1].start()

    @pl.when(first)
    def _():
        send_wu.start()
        send_wd.start()
        send_wu.wait_send()
        send_wd.wait_send()
        pl.semaphore_signal(turn, inc=1, device_id=partner, device_id_type=MESH)

    @pl.when(jnp.logical_not(first))
    def _():
        pl.semaphore_wait(turn, 1)
        send_wu.start()
        send_wd.start()
        send_gu.start()
        send_gd.start()
        send_wu.wait_send()
        send_wd.wait_send()
        pl.semaphore_signal(turn, inc=1, device_id=partner, device_id_type=MESH)

    @pl.when(p == 0)
    def _():
        x_load.wait()
    load_u.wait()
    load_d.wait()
    send_wu.wait_recv()

    @pl.when(p == last)
    def _():
        shard[2].start()
    send_wd.wait_recv()

    @pl.when(p == last)
    def _():
        shard[3].start()
        for copy in shard:
            copy.wait_recv()

    def half_rows(zi):
        return pl.ds(pl.multiple_of(zi * hb, hb), hb)

    def part_copy(c):
        return remote(part.at[c, half_rows(zo)], part_rcv.at[c], psend.at[c], precv.at[c], zpeer)

    def fin_copy(c, zi):
        return remote(fin.at[c], a_buf.at[c, half_rows(z)], fsend.at[c, zi], frecv.at[c, z], (zi, d, lax.min(p + 1, last)))

    def gather_copy(c):
        return remote(fin.at[c], y_buf.at[c, half_rows(z)], agsend.at[c], agrecv.at[c], zpeer)

    def out_copy(c, q):
        return remote(y_buf.at[c], y_hbm.at[c], outsend.at[c, q], outrecv.at[c], (z, d, q))

    def out_local(c):
        return pltpu.make_async_copy(y_buf.at[c], y_hbm.at[c], outsend.at[c, last])

    def arrived(c, zi):
        pltpu.make_async_copy(fin.at[c], a_buf.at[c, half_rows(zi)], frecv.at[c, zi]).wait()

    def branch(rows_in, w_up, w_down):
        hid = gelu_val(mm(rows_in, w_up[...], NN)).astype(BF16)
        return mm(hid, w_down[...], NN)

    def compute(c):
        @pl.when(p < last)
        def _():
            @pl.when(p > 0)
            def _():
                for zi in range(n_model):
                    arrived(c, zi)
            part[c] = branch(a_buf[c], wu_bf, wd_bf)
            part_copy(c).start()

        @pl.when(p == last)
        def _():
            arrived(c, z)
            at = half_rows(z)
            rows_in = a_buf[c, at, :]
            total = branch(rows_in, wu_bf, wd_bf) + branch(rows_in, wu_z, wd_z)
            new = (rows_in.astype(F32) + total).astype(BF16)
            fin[c] = new
            y_buf[c, at, :] = new
            gather_copy(c).start()

    def finalize(c):
        part_copy(c).wait_recv()
        total = part[c, half_rows(z), :] + part_rcv[c]
        fin[c] = (a_buf[c, half_rows(z), :].astype(F32) + total).astype(BF16)
        fin_copy(c, z).start()

        @pl.when(p < last - 1)
        def _():
            fin_copy(c, zo).start()

    def publish(c):
        gather_copy(c).wait_recv()
        out_local(c).start()
        for q in range(last):
            out_copy(c, q).start()

    def chain(i, carry):
        @pl.when(i < nc)
        def _():
            compute(i)

        @pl.when((i >= 1) & (i <= nc) & (p < last))
        def _():
            finalize(i - 1)

        @pl.when((i >= 1) & (i <= nc) & (p == last))
        def _():
            publish(i - 1)

        @pl.when((i == TURN_STEP) & first)
        def _():
            pl.semaphore_wait(turn, 1)
            send_gu.start()
            send_gd.start()
        return carry
    lax.fori_loop(0, nc + 1, chain, 0)

    def drain(c, carry):
        @pl.when(p < last)
        def _():
            part_copy(c).wait_send()
            fin_copy(c, z).wait_send()

            @pl.when(p < last - 1)
            def _():
                fin_copy(c, zo).wait_send()
            pltpu.make_async_copy(y_buf.at[c], y_hbm.at[c], outrecv.at[c]).wait()

        @pl.when(p == last)
        def _():
            gather_copy(c).wait_send()
            out_local(c).wait()
            for q in range(last):
                out_copy(c, q).wait_send()
        return carry
    lax.fori_loop(0, nc, drain, 0)

    @pl.when(p == last)
    def _():
        for copy in shard:
            copy.wait_send()
    send_gu.wait()
    send_gd.wait()


def solution(mesh):
    n_model, n_data, n_stage = (mesh.shape[k] for k in ('model', 'data', 'stage'))
    dims = (n_model, n_data, n_stage)
    n_all = n_model * n_data * n_stage
    up_spec = P('stage', None, 'model')
    down_spec = P('stage', 'model', None)
    row_spec = P(None, 'data', None)
    in_specs = (up_spec, down_spec, up_spec, down_spec, up_spec, down_spec, P('data', 'stage', None, 'model'), P('data', 'stage', 'model', None), P('stage', 'data', None), P('data', None), row_spec, P(None), P(None))
    out_specs = (up_spec, down_spec, up_spec, down_spec, up_spec, down_spec, row_spec)
    any_spec = pl.BlockSpec(memory_space=pl.ANY)
    vmem_spec = pl.BlockSpec(memory_space=pltpu.VMEM)
    smem_spec = pl.BlockSpec(memory_space=pltpu.SMEM)
    dma = pltpu.SemaphoreType.DMA

    def device_step(w_up, w_down, m_up, m_down, v_up, v_down, g_up, g_down, acts_last, grad_out, x_next, learn_rate, max_norm):
        rows, width = grad_out.shape
        ff = w_up.shape[2]
        half = ff // 2
        nb = rows // BACK_ROWS
        hb = BACK_ROWS // 2
        sds = jax.ShapeDtypeStruct
        gbar_u, gbar_d, early, late, norm_tile = pl.pallas_call(
            functools.partial(bwd_kernel, dims),
            out_shape=(sds((width, half), F32), sds((half, width), F32), sds((EARLY_ROWS, width), F32), sds((LATE_ROWS, half), F32), sds((8, 128), F32)),
            in_specs=[any_spec] * 6,
            out_specs=(any_spec,) * 4 + (vmem_spec,),
            scratch_shapes=[
                pltpu.VMEM((width, ff), F32), pltpu.VMEM((ff, width), F32),
                pltpu.VMEM((width, ff), BF16), pltpu.VMEM((ff, width), BF16),
                pltpu.VMEM((2 * rows, width), BF16), pltpu.VMEM((2 * rows, width), BF16),
                pltpu.VMEM((rows, half), BF16), pltpu.VMEM((rows, half), BF16),
                pltpu.VMEM((rows, ff), F32), pltpu.VMEM((rows, half), F32),
                pltpu.VMEM((rows, ff), BF16), pltpu.VMEM((rows, ff), BF16),
            ] + [pltpu.VMEM((width, half), F32), pltpu.VMEM((half, width), F32)] * 3 + [
                pltpu.VMEM((nb, BACK_ROWS, width), F32), pltpu.VMEM((nb, hb, width), F32),
                pltpu.VMEM((nb, hb, width), BF16), pltpu.VMEM((n_all, 8, 128), F32),
                dma((8,)), dma((4,)), dma((4,)), dma((2,)), dma((2,)), dma((nb,)), dma((nb,)), dma((nb, 2)), dma((nb, 2)),
                dma((n_all,)), dma((n_all,)), dma((4,)),
            ],
            compiler_params=pltpu.CompilerParams(collective_id=0, has_side_effects=True, vmem_limit_bytes=VMEM_LIMIT),
            name='backward',
        )(w_up[0], w_down[0], acts_last[0], grad_out, g_up[0, 0], g_down[0, 0])

        early_oth = lax.ppermute(early, 'data', [(k, 1 - k) for k in range(n_data)])
        blocks = half // UPD_ROWS
        state = (w_up[0], w_down[0], m_up[0], m_down[0], v_up[0], v_down[0])
        state_shapes = tuple(sds(s.shape, F32) for s in state)
        which = lax.axis_index('data').astype(jnp.int32).reshape(1)

        def update_specs(pick):
            up = pl.BlockSpec((UPD_ROWS, half), lambda i, w: (i, pick(w[0])))
            down = pl.BlockSpec((UPD_ROWS, width), lambda i, w: (pick(w[0]) * blocks + i, 0))
            return [up, down]
        plain_up = pl.BlockSpec((UPD_ROWS, half), lambda i, w: (i, 0))
        plain_down = pl.BlockSpec((UPD_ROWS, width), lambda i, w: (i, 0))
        small = [smem_spec, smem_spec, pl.BlockSpec((8, 128), lambda i, w: (0, 0))]
        own = update_specs(lambda w: w)
        *fresh, b_up, b_down = pl.pallas_call(
            update_kernel,
            out_shape=state_shapes + (sds((width, half), BF16), sds((half, width), BF16)),
            grid_spec=pltpu.PrefetchScalarGridSpec(
                num_scalar_prefetch=1, grid=(width // UPD_ROWS,),
                in_specs=small + [plain_up, plain_down] + own * 3,
                out_specs=own * 3 + [plain_up, plain_down]),
            compiler_params=pltpu.CompilerParams(dimension_semantics=('arbitrary',), vmem_limit_bytes=VMEM_LIMIT),
            name='update_own',
        )(which, learn_rate, max_norm, norm_tile, gbar_u, gbar_d, *state)

        n_micro = x_next.shape[0]
        nc = n_micro * rows // FWD_ROWS
        fb = FWD_ROWS // 2
        gu_oth, gd_oth, y_next = pl.pallas_call(
            functools.partial(fwd_kernel, dims),
            out_shape=(sds((width - LATE_ROWS, half), F32), sds((half - EARLY_ROWS, width), F32), sds((nc, FWD_ROWS, width), BF16)),
            in_specs=[any_spec] * 5,
            out_specs=(any_spec, any_spec, any_spec),
            scratch_shapes=[pltpu.VMEM((width, ff), BF16), pltpu.VMEM((ff, width), BF16)] * 2 + [
                pltpu.VMEM((nc, FWD_ROWS, width), BF16), pltpu.VMEM((nc, FWD_ROWS, width), BF16),
                pltpu.VMEM((nc, FWD_ROWS, width), F32), pltpu.VMEM((nc, fb, width), F32),
                pltpu.VMEM((nc, fb, width), BF16),
                dma((3,)), dma((4,)), dma((4,)), dma((4,)), dma((4,)), dma((nc,)), dma((nc,)), dma((nc, 2)), dma((nc, 2)),
                dma((nc,)), dma((nc,)), dma((nc, n_stage)), dma((nc,)), pltpu.SemaphoreType.REGULAR,
            ],
            compiler_params=pltpu.CompilerParams(collective_id=1, has_side_effects=True, vmem_limit_bytes=VMEM_LIMIT),
            name='forward',
        )(b_up, b_down, gbar_u, gbar_d, x_next.reshape(nc, FWD_ROWS, width))

        other = update_specs(lambda w: 1 - w)
        gu_oth, late = lax.optimization_barrier((gu_oth, late))
        late_oth = lax.ppermute(late, 'data', [(k, 1 - k) for k in range(n_data)])
        y_next = y_next.reshape(n_micro * rows, width)
        nearly, nlate = EARLY_ROWS // UPD_ROWS, LATE_ROWS // UPD_ROWS
        steps = width // UPD_ROWS
        lastup = steps - nlate - 1

        def rows_spec(start, count):
            return pl.BlockSpec((UPD_ROWS, width), lambda i, w: (jnp.clip(i - start, 0, count - 1), 0))
        y_spec = pl.BlockSpec((n_micro * rows // steps, width), lambda i, w: (i, 0))
        up_oth = pl.BlockSpec((UPD_ROWS, half), lambda i, w: (jnp.minimum(i, lastup), 1 - w[0]))
        down_oth = pl.BlockSpec((UPD_ROWS, width), lambda i, w: ((1 - w[0]) * blocks + i, 0))
        other = [up_oth, down_oth]
        *filled, y_next = pl.pallas_call(
            fill_kernel,
            out_shape=state_shapes + (sds(y_next.shape, BF16),),
            grid_spec=pltpu.PrefetchScalarGridSpec(
                num_scalar_prefetch=1, grid=(steps,),
                in_specs=small + [rows_spec(0, lastup + 1), rows_spec(0, nearly), rows_spec(nearly, blocks - nearly), y_spec] + other * 3 + [any_spec] * 6,
                out_specs=other * 3 + [y_spec]),
            input_output_aliases={14 + k: k for k in range(6)},
            compiler_params=pltpu.CompilerParams(dimension_semantics=('arbitrary',), vmem_limit_bytes=VMEM_LIMIT),
            cost_estimate=pl.CostEstimate(flops=10**10, bytes_accessed=40 * 10**6, transcendentals=0),
            name='update_other',
        )(which, learn_rate, max_norm, norm_tile, gu_oth, early_oth, gd_oth, y_next, *state, *fresh)
        up_late = pl.BlockSpec((UPD_ROWS, half), lambda i, w: (steps - nlate + i, 1 - w[0]))
        filled[0], filled[2], filled[4] = pl.pallas_call(
            late_kernel,
            out_shape=(state_shapes[0],) * 3,
            grid_spec=pltpu.PrefetchScalarGridSpec(
                num_scalar_prefetch=1, grid=(nlate,),
                in_specs=small + [plain_up] + [up_late] * 3 + [any_spec] * 3,
                out_specs=[up_late] * 3),
            input_output_aliases={8 + k: k for k in range(3)},
            compiler_params=pltpu.CompilerParams(dimension_semantics=('arbitrary',), vmem_limit_bytes=VMEM_LIMIT),
            name='update_late',
        )(which, learn_rate, max_norm, norm_tile, late_oth, state[0], state[2], state[4], filled[0], filled[2], filled[4])
        return tuple(s[None] for s in filled) + (y_next.reshape(n_micro, rows, width),)

    return jax.shard_map(device_step, mesh=mesh, in_specs=in_specs, out_specs=out_specs, check_vma=False)
```

```python
import functools

import jax
import jax.numpy as jnp
from jax import lax
from jax.experimental import pallas as pl
from jax.experimental.pallas import tpu as pltpu
from jax.sharding import PartitionSpec as P

ADAM_STEP = 10
BETA_ONE = 0.9
BETA_TWO = 0.95
ADAM_EPS = 1e-8
WEIGHT_DECAY = 0.1
NORM_EPS = 1e-6
ONE_CORR = 1.0 - BETA_ONE ** ADAM_STEP
TWO_CORR = 1.0 - BETA_TWO ** ADAM_STEP
GELU_SCALE = (2.0 / 3.141592653589793) ** 0.5
GELU_CUBE = 0.044715
NN = (((1,), (0,)), ((), ()))
NT = (((1,), (1,)), ((), ()))
TN = (((0,), (0,)), ((), ()))
F32 = jnp.float32
BF16 = jnp.bfloat16
MESH = pl.DeviceIdType.MESH
BACK_ROWS = 128
FWD_ROWS = 96
UPD_ROWS = 128
EARLY_ROWS = 256
LATE_ROWS = 128
TURN_STEP = 5
VMEM_LIMIT = 66_000_000


def mm(lhs, rhs, dims):
    return lax.dot_general(lhs, rhs, dims, preferred_element_type=F32)


def gelu_val(pre):
    return pre * (0.5 * (1.0 + jnp.tanh(GELU_SCALE * (pre + GELU_CUBE * (pre * pre * pre)))))


def gelu_both(pre):
    sq = pre * pre
    tan = jnp.tanh(GELU_SCALE * (pre + GELU_CUBE * (sq * pre)))
    cdf = 0.5 * (1.0 + tan)
    slope = cdf + 0.5 * pre * (1.0 - tan * tan) * (GELU_SCALE * (1.0 + (3.0 * GELU_CUBE) * sq))
    return pre * cdf, slope


def adamw_update(weight, moment_one, moment_two, grad_step, step_rate):
    mom_new = BETA_ONE * moment_one + (1.0 - BETA_ONE) * grad_step
    sec_new = BETA_TWO * moment_two + (1.0 - BETA_TWO) * grad_step * grad_step
    direction = (mom_new * (1.0 / ONE_CORR)) / (jnp.sqrt(sec_new * (1.0 / TWO_CORR)) + ADAM_EPS)
    weight_new = weight - step_rate * (direction + WEIGHT_DECAY * weight)
    return weight_new, mom_new, sec_new


def clip_of(norm_tile, max_norm):
    total = jnp.sum(jnp.sum(norm_tile, axis=0, keepdims=True), axis=1, keepdims=True)
    return jnp.minimum(1.0, max_norm / (jnp.sqrt(total) + NORM_EPS))


def whole_barrier(n_model, n_data, n_stage):
    barrier = pltpu.get_barrier_semaphore()
    me = (lax.axis_index('model'), lax.axis_index('data'), lax.axis_index('stage'))
    for dm in range(n_model):
        for dd in range(n_data):
            for ds in range(n_stage):
                if dm or dd or ds:
                    peer = (lax.rem(me[0] + dm, n_model), lax.rem(me[1] + dd, n_data), lax.rem(me[2] + ds, n_stage))
                    pl.semaphore_signal(barrier, inc=1, device_id=peer, device_id_type=MESH)
    pl.semaphore_wait(barrier, n_model * n_data * n_stage - 1)


def remote(src, dst, send_sem, recv_sem, device):
    return pltpu.make_async_remote_copy(src_ref=src, dst_ref=dst, send_sem=send_sem, recv_sem=recv_sem, device_id=device, device_id_type=MESH)


def bwd_kernel(dims, wu_hbm, wd_hbm, acts_hbm, dy_hbm, gu_hbm, gd_hbm,
               gbu_hbm, gbd_hbm, early_hbm, late_hbm, norm_out,
               wu32, wd32, wu_bf, wd_bf, aa, gg, hid_o, dz_o, slope, slope_o, dz_own, h_own,
               gu_own, gd_own, gu_oth, gd_oth, gu_rcv, gd_rcv, part, part_rcv, fin, norm_buf,
               ld_sem, ysend, yrecv, rsend, rrecv, psend, precv, fsend, frecv, nsend, nrecv, st_sem):
    n_model, n_data, n_stage = dims
    z, d, p = lax.axis_index('model'), lax.axis_index('data'), lax.axis_index('stage')
    zo, do = 1 - z, 1 - d
    ypeer, zpeer = (z, do, p), (zo, d, p)
    last = n_stage - 1
    by_rows = p == 0
    by_sums = p > 0
    hub = n_stage // 2
    rows = aa.shape[0] // 2
    width = aa.shape[1]
    half = hid_o.shape[1]
    rb = BACK_ROWS
    hb = rb // 2
    nb = rows // rb
    own_ff = pl.ds(pl.multiple_of(d * half, 128), half)
    oth_ff = pl.ds(pl.multiple_of(do * half, 128), half)
    mine, theirs = pl.ds(0, rows), pl.ds(rows, rows)

    loads = [
        pltpu.make_async_copy(wu_hbm, wu32, ld_sem.at[0]),
        pltpu.make_async_copy(acts_hbm, aa.at[mine], ld_sem.at[2]),
        pltpu.make_async_copy(wd_hbm, wd32, ld_sem.at[1]),
        pltpu.make_async_copy(gu_hbm.at[:, own_ff], gu_own, ld_sem.at[4]),
        pltpu.make_async_copy(gd_hbm.at[own_ff, :], gd_own, ld_sem.at[5]),
    ]
    dy_load = pltpu.make_async_copy(dy_hbm, gg.at[mine], ld_sem.at[3])
    gu_load = pltpu.make_async_copy(gu_hbm.at[:, oth_ff], gu_oth, ld_sem.at[6])
    gd_load = pltpu.make_async_copy(gd_hbm.at[oth_ff, :], gd_oth, ld_sem.at[7])
    for copy in loads[:3]:
        copy.start()

    @pl.when(p == last)
    def _():
        dy_load.start()
    whole_barrier(n_model, n_data, n_stage)
    low, high = pl.ds(0, rows // 2), pl.ds(rows // 2, rows // 2)
    late_rows = pl.ds(rows + rows // 2, rows // 2)
    send_low = remote(acts_hbm.at[low], aa.at[pl.ds(rows, rows // 2)], ysend.at[0], yrecv.at[0], ypeer)
    send_acts = remote(acts_hbm.at[high], hid_o.at[low], rsend.at[2], rrecv.at[0], (z, d, hub))
    relay_over = remote(hid_o.at[low], dz_o.at[low], rsend.at[0], rrecv.at[1], ypeer)
    relay_back = remote(dz_o.at[low], aa.at[late_rows], rsend.at[1], rrecv.at[2], (z, d, 0))
    raw_gu = remote(gu_hbm.at[:, oth_ff], gu_rcv, ysend.at[1], yrecv.at[1], ypeer)
    raw_gd = remote(gd_hbm.at[oth_ff, :], gd_rcv, ysend.at[2], yrecv.at[2], ypeer)
    sum_gu = remote(gu_oth, gu_rcv, ysend.at[1], yrecv.at[1], ypeer)
    sum_gd = remote(gd_oth, gd_rcv, ysend.at[2], yrecv.at[2], ypeer)
    send_g = remote(gg.at[mine], gg.at[theirs], ysend.at[3], yrecv.at[3], ypeer)

    @pl.when(by_rows)
    def _():
        send_acts.start()
        send_low.start()
        raw_gd.start()
        raw_gu.start()

    loads[0].wait()
    loads[1].wait()

    def cast_up(i, carry):
        at = pl.ds(pl.multiple_of(i * 128, 128), 128)
        wu_bf[at, :] = wu32[at, :].astype(BF16)
        return carry
    lax.fori_loop(0, width // 128, cast_up, 0)

    def own_pre(i, carry):
        at = pl.ds(pl.multiple_of(i * rb, rb), rb)
        val, slp = gelu_both(mm(aa[at, :], wu_bf[...], NN))
        h_own[at, :] = val.astype(BF16)
        slope[at, :] = slp
        return carry
    loads[2].wait()

    @pl.when(by_sums)
    def _():
        gd_load.start()
        gu_load.start()
    for copy in loads[3:]:
        copy.start()
    lax.fori_loop(0, nb, own_pre, 0)

    def down_block(j, base):
        at = pl.ds(pl.multiple_of(base * half + j * 128, 128), 128)
        return mm(h_own[:, at], gg[mine, :], TN)

    def up_block(j, ff_at):
        at = pl.ds(pl.multiple_of(j * 128, 128), 128)
        return mm(aa[mine, at], dz_own[:, ff_at], TN)

    def send_down():
        gd_load.wait()

        def down_oth(j, carry):
            gd_oth[pl.ds(pl.multiple_of(j * 128, 128), 128), :] += down_block(j, do)
            return carry
        lax.fori_loop(0, half // 128, down_oth, 0)
        gu_load.wait()
        sum_gd.start()

    @pl.when(p == last)
    def _():
        dy_load.wait()
        send_down()


    def cast_down(i, carry):
        at = pl.ds(pl.multiple_of(i * 128, 128), 128)
        wd_bf[at, :] = wd32[at, :].astype(BF16)
        return carry
    lax.fori_loop(0, 2 * half // 128, cast_down, 0)

    @pl.when(p == hub)
    def _():
        pltpu.make_async_copy(hid_o.at[low], hid_o.at[low], rrecv.at[0]).wait()
        relay_over.start()
        pltpu.make_async_copy(dz_o.at[low], dz_o.at[low], rrecv.at[1]).wait()
        relay_back.start()

    def g_at(c, zi):
        return gg.at[pl.ds(pl.multiple_of(c * rb + zi * hb, hb), hb)]

    def part_copy(c):
        return remote(part.at[c, pl.ds(pl.multiple_of(zo * hb, hb), hb)], part_rcv.at[c], psend.at[c], precv.at[c], zpeer)

    def fin_copy(c, zi):
        return remote(fin.at[c], g_at(c, z), fsend.at[c, zi], frecv.at[c, z], (zi, d, lax.max(p - 1, 0)))

    def compute(c):
        @pl.when(p < last)
        def _():
            for zi in range(n_model):
                pltpu.make_async_copy(fin.at[c], g_at(c, zi), frecv.at[c, zi]).wait()
        at = pl.ds(pl.multiple_of(c * rb, rb), rb)
        grad_hid = mm(gg[at, :], wd_bf[...], NT)
        dz_own[at, :] = (slope[at, :] * grad_hid).astype(BF16)

        @pl.when(p > 0)
        def _():
            part[c] = mm(dz_own[at, :], wu_bf[...], NT)
            part_copy(c).start()

    def finalize(c):
        part_copy(c).wait_recv()
        at = pl.ds(pl.multiple_of(c * rb + z * hb, hb), hb)
        total = part[c, pl.ds(pl.multiple_of(z * hb, hb), hb), :] + part_rcv[c]
        fin[c] = (gg[at, :].astype(F32) + total).astype(BF16)
        for zi in range(n_model):
            fin_copy(c, zi).start()

    def chain(i, carry):
        compute(i)

        @pl.when((i >= 1) & (p > 0))
        def _():
            finalize(i - 1)
        return carry
    lax.fori_loop(0, nb, chain, 0)

    @pl.when(by_sums & (p < hub))
    def _():
        send_down()

    @pl.when(p > 0)
    def _():
        finalize(nb - 1)

    @pl.when((p >= hub) & (p < last))
    def _():
        send_down()

    @pl.when(by_sums)
    def _():
        def up_oth(j, carry):
            gu_oth[pl.ds(pl.multiple_of(j * 128, 128), 128), :] += up_block(j, oth_ff)
            return carry
        lax.fori_loop(0, width // 128, up_oth, 0)

    @pl.when(by_rows)
    def _():
        send_g.start()
    loads[3].wait()
    loads[4].wait()

    def down_own(j, carry):
        gd_own[pl.ds(pl.multiple_of(j * 128, 128), 128), :] += down_block(j, d)
        return carry
    lax.fori_loop(0, half // 128, down_own, 0)

    @pl.when(by_sums)
    def _():
        sum_gu.start()

    def up_own(j, carry):
        gu_own[pl.ds(pl.multiple_of(j * 128, 128), 128), :] += up_block(j, own_ff)
        return carry
    lax.fori_loop(0, width // 128, up_own, 0)

    @pl.when(by_rows)
    def _():
        send_low.wait_recv()
        pltpu.make_async_copy(aa.at[late_rows], aa.at[late_rows], rrecv.at[2]).wait()

        def oth_pre(i, carry):
            at = pl.ds(pl.multiple_of(i * rb, rb), rb)
            val, slp = gelu_both(mm(aa[pl.ds(pl.multiple_of(rows + i * rb, rb), rb), :], wu_bf[:, own_ff], NN))
            hid_o[at, :] = val.astype(BF16)
            slope_o[at, :] = slp
            return carry
        lax.fori_loop(0, nb, oth_pre, 0)
        send_g.wait_recv()

        def oth_dz(i, carry):
            at = pl.ds(pl.multiple_of(i * rb, rb), rb)
            grad_hid = mm(gg[pl.ds(pl.multiple_of(rows + i * rb, rb), rb), :], wd_bf[own_ff, :], NT)
            dz_o[at, :] = (slope_o[at, :] * grad_hid).astype(BF16)
            return carry
        lax.fori_loop(0, nb, oth_dz, 0)

        def oth_grads(j, carry):
            at = pl.ds(pl.multiple_of(j * 128, 128), 128)
            gd_own[at, :] += mm(hid_o[:, at], gg[theirs, :], TN)
            gu_own[at, :] += mm(aa[theirs, at], dz_o[...], TN)
            return carry
        lax.fori_loop(0, half // 128, oth_grads, 0)

    def combine(own, rcv):
        def body(i, acc):
            at = pl.ds(pl.multiple_of(i * 32, 32), 32)
            mean = (own[at, :] + rcv[at, :]) * 0.5
            own[at, :] = mean
            return acc + jnp.sum((mean * mean).reshape(4, 8, mean.shape[1]), axis=0)
        return body

    def combine_up(acc):
        raw_gu.wait_recv()
        return lax.fori_loop(0, gu_own.shape[0] // 32, combine(gu_own, gu_rcv), acc)

    def combine_down(acc):
        raw_gd.wait_recv()
        return lax.fori_loop(0, gd_own.shape[0] // 32, combine(gd_own, gd_rcv), acc)
    acc = jnp.zeros((8, half), F32)
    acc = combine_down(acc)
    store_d = pltpu.make_async_copy(gd_own, gbd_hbm, st_sem.at[1])
    store_d.start()
    store_early = pltpu.make_async_copy(gd_own.at[pl.ds(0, EARLY_ROWS)], early_hbm, st_sem.at[2])
    store_early.start()
    acc = combine_up(acc)
    store_u = pltpu.make_async_copy(gu_own, gbu_hbm, st_sem.at[0])
    store_u.start()
    store_late = pltpu.make_async_copy(gu_own.at[pl.ds(width - LATE_ROWS, LATE_ROWS)], late_hbm, st_sem.at[3])
    store_late.start()
    tile = acc[:, 0:128]
    for k in range(1, half // 128):
        tile = tile + acc[:, k * 128:(k + 1) * 128]
    n_all = n_model * n_data * n_stage
    my_id = (z * n_data + d) * n_stage + p
    norm_buf[my_id] = tile

    def norm_copy(k):
        peer = lax.rem(my_id + k, n_all)
        device = (peer // (n_data * n_stage), lax.rem(peer // n_stage, n_data), lax.rem(peer, n_stage))
        return remote(norm_buf.at[my_id], norm_buf.at[my_id], nsend.at[k], nrecv.at[my_id], device)
    for k in range(1, n_all):
        norm_copy(k).start()
    for k in range(1, n_all):
        peer = lax.rem(my_id + k, n_all)
        pltpu.make_async_copy(norm_buf.at[peer], norm_buf.at[peer], nrecv.at[peer]).wait()
    total = norm_buf[0]
    for k in range(1, n_all):
        total = total + norm_buf[k]
    norm_out[...] = total

    for k in range(1, n_all):
        norm_copy(k).wait_send()

    @pl.when(by_rows)
    def _():
        for copy in (send_acts, send_low, raw_gu, raw_gd, send_g):
            copy.wait_send()

    @pl.when(p == hub)
    def _():
        relay_over.wait_send()
        relay_back.wait_send()

    @pl.when(by_sums)
    def _():
        sum_gu.wait_send()
        sum_gd.wait_send()

    @pl.when(p > 0)
    def _():
        for c in range(nb):
            part_copy(c).wait_send()
            for zi in range(n_model):
                fin_copy(c, zi).wait_send()
    store_u.wait()
    store_d.wait()
    store_early.wait()
    store_late.wait()


def update_kernel(d_ref, lr_ref, mn_ref, norm_ref, gu, gd, wu, wd, mu, md, vu, vd, *rest):
    owu, owd, omu, omd, ovu, ovd = rest[:6]
    clip = clip_of(norm_ref[...], mn_ref[0])
    rate = lr_ref[0]
    owu[...], omu[...], ovu[...] = adamw_update(wu[...], mu[...], vu[...], clip * gu[...], rate)
    owd[...], omd[...], ovd[...] = adamw_update(wd[...], md[...], vd[...], clip * gd[...], rate)
    if len(rest) == 8:
        rest[6][...] = owu[...].astype(BF16)
        rest[7][...] = owd[...].astype(BF16)


def fill_kernel(d_ref, lr_ref, mn_ref, norm_ref, gu, gd_early, gd_rest, y_in, wu, wd, mu, md, vu, vd, *rest):
    owu, owd, omu, omd, ovu, ovd, y_out = rest[6:]
    clip = clip_of(norm_ref[...], mn_ref[0])
    rate = lr_ref[0]
    step = pl.program_id(0)
    early_at = pl.ds(pl.multiple_of(jnp.minimum(step, EARLY_ROWS // UPD_ROWS - 1) * UPD_ROWS, UPD_ROWS), UPD_ROWS)
    gd = jnp.where(step < EARLY_ROWS // UPD_ROWS, gd_early[early_at, :], gd_rest[...])
    owu[...], omu[...], ovu[...] = adamw_update(wu[...], mu[...], vu[...], clip * gu[...], rate)
    owd[...], omd[...], ovd[...] = adamw_update(wd[...], md[...], vd[...], clip * gd, rate)
    y_out[...] = y_in[...]


def late_kernel(d_ref, lr_ref, mn_ref, norm_ref, gu, wu, mu, vu, *rest):
    owu, omu, ovu = rest[3:]
    clip = clip_of(norm_ref[...], mn_ref[0])
    owu[...], omu[...], ovu[...] = adamw_update(wu[...], mu[...], vu[...], clip * gu[...], lr_ref[0])


def fwd_kernel(dims, bu_hbm, bd_hbm, gbu_hbm, gbd_hbm, x_hbm,
               gu_oth, gd_oth, y_hbm,
               wu_bf, wd_bf, wu_z, wd_z, a_buf, y_buf, part, part_rcv, fin,
               ld_sem, ysend, yrecv, zsend, zrecv, psend, precv, fsend, frecv, agsend, agrecv, outsend, outrecv, turn):
    n_model, n_data, n_stage = dims
    z, d, p = lax.axis_index('model'), lax.axis_index('data'), lax.axis_index('stage')
    zo, do = 1 - z, 1 - d
    ypeer, zpeer = (z, do, p), (zo, d, p)
    last = n_stage - 1
    nc, rb, width = a_buf.shape
    half = wu_bf.shape[1] // 2
    hb = rb // 2
    own_ff = pl.ds(pl.multiple_of(d * half, 128), half)
    oth_ff = pl.ds(pl.multiple_of(do * half, 128), half)
    first = (p == 0) | (p == last)
    partner = (z, d, p + 1 - 2 * lax.rem(p, 2))

    load_u = pltpu.make_async_copy(bu_hbm, wu_bf.at[:, own_ff], ld_sem.at[0])
    load_d = pltpu.make_async_copy(bd_hbm, wd_bf.at[own_ff, :], ld_sem.at[1])
    load_u.start()
    load_d.start()
    x_load = pltpu.make_async_copy(x_hbm, a_buf, ld_sem.at[2])

    @pl.when(p == 0)
    def _():
        x_load.start()
    whole_barrier(n_model, n_data, n_stage)

    send_wu = remote(bu_hbm, wu_bf.at[:, own_ff], ysend.at[0], yrecv.at[0], ypeer)
    send_wd = remote(bd_hbm, wd_bf.at[own_ff, :], ysend.at[1], yrecv.at[1], ypeer)
    send_gu = remote(gbu_hbm.at[pl.ds(0, gu_oth.shape[0])], gu_oth, ysend.at[2], yrecv.at[2], ypeer)
    send_gd = remote(gbd_hbm.at[pl.ds(half - gd_oth.shape[0], gd_oth.shape[0])], gd_oth, ysend.at[3], yrecv.at[3], ypeer)

    shard = [
        remote(bu_hbm, wu_z.at[:, own_ff], zsend.at[0], zrecv.at[0], zpeer),
        remote(bd_hbm, wd_z.at[own_ff, :], zsend.at[1], zrecv.at[1], zpeer),
        remote(wu_bf.at[:, oth_ff], wu_z.at[:, oth_ff], zsend.at[2], zrecv.at[2], zpeer),
        remote(wd_bf.at[oth_ff, :], wd_z.at[oth_ff, :], zsend.at[3], zrecv.at[3], zpeer),
    ]

    @pl.when(p == last)
    def _():
        shard[0].start()
        shard[1].start()

    @pl.when(first)
    def _():
        send_wu.start()
        send_wd.start()
        send_wu.wait_send()
        send_wd.wait_send()
        pl.semaphore_signal(turn, inc=1, device_id=partner, device_id_type=MESH)

    @pl.when(jnp.logical_not(first))
    def _():
        pl.semaphore_wait(turn, 1)
        send_wu.start()
        send_wd.start()
        send_gu.start()
        send_gd.start()
        send_wu.wait_send()
        send_wd.wait_send()
        pl.semaphore_signal(turn, inc=1, device_id=partner, device_id_type=MESH)

    @pl.when(p == 0)
    def _():
        x_load.wait()
    load_u.wait()
    load_d.wait()
    send_wu.wait_recv()

    @pl.when(p == last)
    def _():
        shard[2].start()
    send_wd.wait_recv()

    @pl.when(p == last)
    def _():
        shard[3].start()
        for copy in shard:
            copy.wait_recv()

    def half_rows(zi):
        return pl.ds(pl.multiple_of(zi * hb, hb), hb)

    def part_copy(c):
        return remote(part.at[c, half_rows(zo)], part_rcv.at[c], psend.at[c], precv.at[c], zpeer)

    def fin_copy(c, zi):
        return remote(fin.at[c], a_buf.at[c, half_rows(z)], fsend.at[c, zi], frecv.at[c, z], (zi, d, lax.min(p + 1, last)))

    def gather_copy(c):
        return remote(fin.at[c], y_buf.at[c, half_rows(z)], agsend.at[c], agrecv.at[c], zpeer)

    def out_copy(c, q):
        return remote(y_buf.at[c], y_hbm.at[c], outsend.at[c, q], outrecv.at[c], (z, d, q))

    def out_local(c):
        return pltpu.make_async_copy(y_buf.at[c], y_hbm.at[c], outsend.at[c, last])

    def arrived(c, zi):
        pltpu.make_async_copy(fin.at[c], a_buf.at[c, half_rows(zi)], frecv.at[c, zi]).wait()

    def branch(rows_in, w_up, w_down):
        hid = gelu_val(mm(rows_in, w_up[...], NN)).astype(BF16)
        return mm(hid, w_down[...], NN)

    def compute(c):
        @pl.when(p < last)
        def _():
            @pl.when(p > 0)
            def _():
                for zi in range(n_model):
                    arrived(c, zi)
            part[c] = branch(a_buf[c], wu_bf, wd_bf)
            part_copy(c).start()

        @pl.when(p == last)
        def _():
            arrived(c, z)
            at = half_rows(z)
            rows_in = a_buf[c, at, :]
            total = branch(rows_in, wu_bf, wd_bf) + branch(rows_in, wu_z, wd_z)
            new = (rows_in.astype(F32) + total).astype(BF16)
            fin[c] = new
            y_buf[c, at, :] = new
            gather_copy(c).start()

    def finalize(c):
        part_copy(c).wait_recv()
        total = part[c, half_rows(z), :] + part_rcv[c]
        fin[c] = (a_buf[c, half_rows(z), :].astype(F32) + total).astype(BF16)
        fin_copy(c, z).start()

        @pl.when(p < last - 1)
        def _():
            fin_copy(c, zo).start()

    def publish(c):
        gather_copy(c).wait_recv()
        out_local(c).start()
        for q in range(last):
            out_copy(c, q).start()

    def chain(i, carry):
        @pl.when(i < nc)
        def _():
            compute(i)

        @pl.when((i >= 1) & (i <= nc) & (p < last))
        def _():
            finalize(i - 1)

        @pl.when((i >= 1) & (i <= nc) & (p == last))
        def _():
            publish(i - 1)

        @pl.when((i == TURN_STEP) & first)
        def _():
            pl.semaphore_wait(turn, 1)
            send_gu.start()
            send_gd.start()
        return carry
    lax.fori_loop(0, nc + 1, chain, 0)

    def drain(c, carry):
        @pl.when(p < last)
        def _():
            part_copy(c).wait_send()
            fin_copy(c, z).wait_send()

            @pl.when(p < last - 1)
            def _():
                fin_copy(c, zo).wait_send()
            pltpu.make_async_copy(y_buf.at[c], y_hbm.at[c], outrecv.at[c]).wait()

        @pl.when(p == last)
        def _():
            gather_copy(c).wait_send()
            out_local(c).wait()
            for q in range(last):
                out_copy(c, q).wait_send()
        return carry
    lax.fori_loop(0, nc, drain, 0)

    @pl.when(p == last)
    def _():
        for copy in shard:
            copy.wait_send()
    send_gu.wait()
    send_gd.wait()


def solution(mesh):
    n_model, n_data, n_stage = (mesh.shape[k] for k in ('model', 'data', 'stage'))
    dims = (n_model, n_data, n_stage)
    n_all = n_model * n_data * n_stage
    up_spec = P('stage', None, 'model')
    down_spec = P('stage', 'model', None)
    row_spec = P(None, 'data', None)
    in_specs = (up_spec, down_spec, up_spec, down_spec, up_spec, down_spec, P('data', 'stage', None, 'model'), P('data', 'stage', 'model', None), P('stage', 'data', None), P('data', None), row_spec, P(None), P(None))
    out_specs = (up_spec, down_spec, up_spec, down_spec, up_spec, down_spec, row_spec)
    any_spec = pl.BlockSpec(memory_space=pl.ANY)
    vmem_spec = pl.BlockSpec(memory_space=pltpu.VMEM)
    smem_spec = pl.BlockSpec(memory_space=pltpu.SMEM)
    dma = pltpu.SemaphoreType.DMA

    def device_step(w_up, w_down, m_up, m_down, v_up, v_down, g_up, g_down, acts_last, grad_out, x_next, learn_rate, max_norm):
        rows, width = grad_out.shape
        ff = w_up.shape[2]
        half = ff // 2
        nb = rows // BACK_ROWS
        hb = BACK_ROWS // 2
        sds = jax.ShapeDtypeStruct
        gbar_u, gbar_d, early, late, norm_tile = pl.pallas_call(
            functools.partial(bwd_kernel, dims),
            out_shape=(sds((width, half), F32), sds((half, width), F32), sds((EARLY_ROWS, width), F32), sds((LATE_ROWS, half), F32), sds((8, 128), F32)),
            in_specs=[any_spec] * 6,
            out_specs=(any_spec,) * 4 + (vmem_spec,),
            scratch_shapes=[
                pltpu.VMEM((width, ff), F32), pltpu.VMEM((ff, width), F32),
                pltpu.VMEM((width, ff), BF16), pltpu.VMEM((ff, width), BF16),
                pltpu.VMEM((2 * rows, width), BF16), pltpu.VMEM((2 * rows, width), BF16),
                pltpu.VMEM((rows, half), BF16), pltpu.VMEM((rows, half), BF16),
                pltpu.VMEM((rows, ff), F32), pltpu.VMEM((rows, half), F32),
                pltpu.VMEM((rows, ff), BF16), pltpu.VMEM((rows, ff), BF16),
            ] + [pltpu.VMEM((width, half), F32), pltpu.VMEM((half, width), F32)] * 3 + [
                pltpu.VMEM((nb, BACK_ROWS, width), F32), pltpu.VMEM((nb, hb, width), F32),
                pltpu.VMEM((nb, hb, width), BF16), pltpu.VMEM((n_all, 8, 128), F32),
                dma((8,)), dma((4,)), dma((4,)), dma((3,)), dma((3,)), dma((nb,)), dma((nb,)), dma((nb, 2)), dma((nb, 2)),
                dma((n_all,)), dma((n_all,)), dma((4,)),
            ],
            compiler_params=pltpu.CompilerParams(collective_id=0, has_side_effects=True, vmem_limit_bytes=VMEM_LIMIT),
            name='backward',
        )(w_up[0], w_down[0], acts_last[0], grad_out, g_up[0, 0], g_down[0, 0])

        early_oth = lax.ppermute(early, 'data', [(k, 1 - k) for k in range(n_data)])
        blocks = half // UPD_ROWS
        state = (w_up[0], w_down[0], m_up[0], m_down[0], v_up[0], v_down[0])
        state_shapes = tuple(sds(s.shape, F32) for s in state)
        which = lax.axis_index('data').astype(jnp.int32).reshape(1)

        def update_specs(pick):
            up = pl.BlockSpec((UPD_ROWS, half), lambda i, w: (i, pick(w[0])))
            down = pl.BlockSpec((UPD_ROWS, width), lambda i, w: (pick(w[0]) * blocks + i, 0))
            return [up, down]
        plain_up = pl.BlockSpec((UPD_ROWS, half), lambda i, w: (i, 0))
        plain_down = pl.BlockSpec((UPD_ROWS, width), lambda i, w: (i, 0))
        small = [smem_spec, smem_spec, pl.BlockSpec((8, 128), lambda i, w: (0, 0))]
        own = update_specs(lambda w: w)
        *fresh, b_up, b_down = pl.pallas_call(
            update_kernel,
            out_shape=state_shapes + (sds((width, half), BF16), sds((half, width), BF16)),
            grid_spec=pltpu.PrefetchScalarGridSpec(
                num_scalar_prefetch=1, grid=(width // UPD_ROWS,),
                in_specs=small + [plain_up, plain_down] + own * 3,
                out_specs=own * 3 + [plain_up, plain_down]),
            compiler_params=pltpu.CompilerParams(dimension_semantics=('arbitrary',), vmem_limit_bytes=VMEM_LIMIT),
            name='update_own',
        )(which, learn_rate, max_norm, norm_tile, gbar_u, gbar_d, *state)

        n_micro = x_next.shape[0]
        nc = n_micro * rows // FWD_ROWS
        fb = FWD_ROWS // 2
        gu_oth, gd_oth, y_next = pl.pallas_call(
            functools.partial(fwd_kernel, dims),
            out_shape=(sds((width - LATE_ROWS, half), F32), sds((half - EARLY_ROWS, width), F32), sds((nc, FWD_ROWS, width), BF16)),
            in_specs=[any_spec] * 5,
            out_specs=(any_spec, any_spec, any_spec),
            scratch_shapes=[pltpu.VMEM((width, ff), BF16), pltpu.VMEM((ff, width), BF16)] * 2 + [
                pltpu.VMEM((nc, FWD_ROWS, width), BF16), pltpu.VMEM((nc, FWD_ROWS, width), BF16),
                pltpu.VMEM((nc, FWD_ROWS, width), F32), pltpu.VMEM((nc, fb, width), F32),
                pltpu.VMEM((nc, fb, width), BF16),
                dma((3,)), dma((4,)), dma((4,)), dma((4,)), dma((4,)), dma((nc,)), dma((nc,)), dma((nc, 2)), dma((nc, 2)),
                dma((nc,)), dma((nc,)), dma((nc, n_stage)), dma((nc,)), pltpu.SemaphoreType.REGULAR,
            ],
            compiler_params=pltpu.CompilerParams(collective_id=1, has_side_effects=True, vmem_limit_bytes=VMEM_LIMIT),
            name='forward',
        )(b_up, b_down, gbar_u, gbar_d, x_next.reshape(nc, FWD_ROWS, width))

        other = update_specs(lambda w: 1 - w)
        gu_oth, late = lax.optimization_barrier((gu_oth, late))
        late_oth = lax.ppermute(late, 'data', [(k, 1 - k) for k in range(n_data)])
        y_next = y_next.reshape(n_micro * rows, width)
        nearly, nlate = EARLY_ROWS // UPD_ROWS, LATE_ROWS // UPD_ROWS
        steps = width // UPD_ROWS
        lastup = steps - nlate - 1

        def rows_spec(start, count):
            return pl.BlockSpec((UPD_ROWS, width), lambda i, w: (jnp.clip(i - start, 0, count - 1), 0))
        y_spec = pl.BlockSpec((n_micro * rows // steps, width), lambda i, w: (i, 0))
        up_oth = pl.BlockSpec((UPD_ROWS, half), lambda i, w: (jnp.minimum(i, lastup), 1 - w[0]))
        down_oth = pl.BlockSpec((UPD_ROWS, width), lambda i, w: ((1 - w[0]) * blocks + i, 0))
        other = [up_oth, down_oth]
        *filled, y_next = pl.pallas_call(
            fill_kernel,
            out_shape=state_shapes + (sds(y_next.shape, BF16),),
            grid_spec=pltpu.PrefetchScalarGridSpec(
                num_scalar_prefetch=1, grid=(steps,),
                in_specs=small + [rows_spec(0, lastup + 1), vmem_spec, rows_spec(nearly, blocks - nearly), y_spec] + other * 3 + [any_spec] * 6,
                out_specs=other * 3 + [y_spec]),
            input_output_aliases={14 + k: k for k in range(6)},
            compiler_params=pltpu.CompilerParams(dimension_semantics=('arbitrary',), vmem_limit_bytes=VMEM_LIMIT),
            cost_estimate=pl.CostEstimate(flops=10**10, bytes_accessed=40 * 10**6, transcendentals=0),
            name='update_other',
        )(which, learn_rate, max_norm, norm_tile, gu_oth, early_oth, gd_oth, y_next, *state, *fresh)
        up_late = pl.BlockSpec((UPD_ROWS, half), lambda i, w: (steps - nlate + i, 1 - w[0]))
        filled[0], filled[2], filled[4] = pl.pallas_call(
            late_kernel,
            out_shape=(state_shapes[0],) * 3,
            grid_spec=pltpu.PrefetchScalarGridSpec(
                num_scalar_prefetch=1, grid=(nlate,),
                in_specs=small + [plain_up] + [up_late] * 3 + [any_spec] * 3,
                out_specs=[up_late] * 3),
            input_output_aliases={8 + k: k for k in range(3)},
            compiler_params=pltpu.CompilerParams(dimension_semantics=('arbitrary',), vmem_limit_bytes=VMEM_LIMIT),
            name='update_late',
        )(which, learn_rate, max_norm, norm_tile, late_oth, state[0], state[2], state[4], filled[0], filled[2], filled[4])
        return tuple(s[None] for s in filled) + (y_next.reshape(n_micro, rows, width),)

    return jax.shard_map(device_step, mesh=mesh, in_specs=in_specs, out_specs=out_specs, check_vma=False)
```

```python
import functools

import jax
import jax.numpy as jnp
from jax import lax
from jax.experimental import pallas as pl
from jax.experimental.pallas import tpu as pltpu
from jax.sharding import PartitionSpec as P

ADAM_STEP = 10
BETA_ONE = 0.9
BETA_TWO = 0.95
ADAM_EPS = 1e-8
WEIGHT_DECAY = 0.1
NORM_EPS = 1e-6
ONE_CORR = 1.0 - BETA_ONE ** ADAM_STEP
TWO_CORR = 1.0 - BETA_TWO ** ADAM_STEP
GELU_SCALE = (2.0 / 3.141592653589793) ** 0.5
GELU_CUBE = 0.044715
NN = (((1,), (0,)), ((), ()))
NT = (((1,), (1,)), ((), ()))
TN = (((0,), (0,)), ((), ()))
F32 = jnp.float32
BF16 = jnp.bfloat16
MESH = pl.DeviceIdType.MESH
BACK_ROWS = 128
FWD_ROWS = 96
UPD_ROWS = 128
EARLY_ROWS = 256
LATE_ROWS = 128
TURN_STEP = 8
VMEM_LIMIT = 66_000_000


def mm(lhs, rhs, dims):
    return lax.dot_general(lhs, rhs, dims, preferred_element_type=F32)


def gelu_val(pre):
    return pre * (0.5 * (1.0 + jnp.tanh(GELU_SCALE * (pre + GELU_CUBE * (pre * pre * pre)))))


def gelu_both(pre):
    sq = pre * pre
    tan = jnp.tanh(GELU_SCALE * (pre + GELU_CUBE * (sq * pre)))
    cdf = 0.5 * (1.0 + tan)
    slope = cdf + 0.5 * pre * (1.0 - tan * tan) * (GELU_SCALE * (1.0 + (3.0 * GELU_CUBE) * sq))
    return pre * cdf, slope


def adamw_update(weight, moment_one, moment_two, grad_step, step_rate):
    mom_new = BETA_ONE * moment_one + (1.0 - BETA_ONE) * grad_step
    sec_new = BETA_TWO * moment_two + (1.0 - BETA_TWO) * grad_step * grad_step
    direction = (mom_new * (1.0 / ONE_CORR)) / (jnp.sqrt(sec_new * (1.0 / TWO_CORR)) + ADAM_EPS)
    weight_new = weight - step_rate * (direction + WEIGHT_DECAY * weight)
    return weight_new, mom_new, sec_new


def clip_of(norm_tile, max_norm):
    total = jnp.sum(jnp.sum(norm_tile, axis=0, keepdims=True), axis=1, keepdims=True)
    return jnp.minimum(1.0, max_norm / (jnp.sqrt(total) + NORM_EPS))


def whole_barrier(n_model, n_data, n_stage):
    barrier = pltpu.get_barrier_semaphore()
    me = (lax.axis_index('model'), lax.axis_index('data'), lax.axis_index('stage'))
    for dm in range(n_model):
        for dd in range(n_data):
            for ds in range(n_stage):
                if dm or dd or ds:
                    peer = (lax.rem(me[0] + dm, n_model), lax.rem(me[1] + dd, n_data), lax.rem(me[2] + ds, n_stage))
                    pl.semaphore_signal(barrier, inc=1, device_id=peer, device_id_type=MESH)
    pl.semaphore_wait(barrier, n_model * n_data * n_stage - 1)


def remote(src, dst, send_sem, recv_sem, device):
    return pltpu.make_async_remote_copy(src_ref=src, dst_ref=dst, send_sem=send_sem, recv_sem=recv_sem, device_id=device, device_id_type=MESH)


def bwd_kernel(dims, wu_hbm, wd_hbm, acts_hbm, dy_hbm, gu_hbm, gd_hbm,
               gbu_hbm, gbd_hbm, early_hbm, late_hbm, norm_out,
               wu32, wd32, wu_bf, wd_bf, aa, gg, hid_o, dz_o, slope, slope_o, dz_own, h_own,
               gu_own, gd_own, gu_oth, gd_oth, gu_rcv, gd_rcv, part, part_rcv, fin, norm_buf,
               ld_sem, ysend, yrecv, rsend, rrecv, psend, precv, fsend, frecv, nsend, nrecv, st_sem):
    n_model, n_data, n_stage = dims
    z, d, p = lax.axis_index('model'), lax.axis_index('data'), lax.axis_index('stage')
    zo, do = 1 - z, 1 - d
    ypeer, zpeer = (z, do, p), (zo, d, p)
    last = n_stage - 1
    by_rows = p == 0
    by_sums = p > 0
    hub = n_stage // 2
    rows = aa.shape[0] // 2
    width = aa.shape[1]
    half = hid_o.shape[1]
    rb = BACK_ROWS
    hb = rb // 2
    nb = rows // rb
    own_ff = pl.ds(pl.multiple_of(d * half, 128), half)
    oth_ff = pl.ds(pl.multiple_of(do * half, 128), half)
    mine, theirs = pl.ds(0, rows), pl.ds(rows, rows)

    loads = [
        pltpu.make_async_copy(wu_hbm, wu32, ld_sem.at[0]),
        pltpu.make_async_copy(acts_hbm, aa.at[mine], ld_sem.at[2]),
        pltpu.make_async_copy(wd_hbm, wd32, ld_sem.at[1]),
        pltpu.make_async_copy(gu_hbm.at[:, own_ff], gu_own, ld_sem.at[4]),
        pltpu.make_async_copy(gd_hbm.at[own_ff, :], gd_own, ld_sem.at[5]),
    ]
    dy_load = pltpu.make_async_copy(dy_hbm, gg.at[mine], ld_sem.at[3])
    gu_load = pltpu.make_async_copy(gu_hbm.at[:, oth_ff], gu_oth, ld_sem.at[6])
    gd_load = pltpu.make_async_copy(gd_hbm.at[oth_ff, :], gd_oth, ld_sem.at[7])
    for copy in loads[:3]:
        copy.start()

    @pl.when(p == last)
    def _():
        dy_load.start()
    whole_barrier(n_model, n_data, n_stage)
    low, high = pl.ds(0, rows // 2), pl.ds(rows // 2, rows // 2)
    late_rows = pl.ds(rows + rows // 2, rows // 2)
    send_low = remote(acts_hbm.at[low], aa.at[pl.ds(rows, rows // 2)], ysend.at[0], yrecv.at[0], ypeer)
    send_acts = remote(acts_hbm.at[high], hid_o.at[low], rsend.at[2], rrecv.at[0], (z, d, hub))
    relay_over = remote(hid_o.at[low], dz_o.at[low], rsend.at[0], rrecv.at[1], ypeer)
    relay_back = remote(dz_o.at[low], aa.at[late_rows], rsend.at[1], rrecv.at[2], (z, d, 0))
    raw_gu = remote(gu_hbm.at[:, oth_ff], gu_rcv, ysend.at[1], yrecv.at[1], ypeer)
    raw_gd = remote(gd_hbm.at[oth_ff, :], gd_rcv, ysend.at[2], yrecv.at[2], ypeer)
    sum_gu = remote(gu_oth, gu_rcv, ysend.at[1], yrecv.at[1], ypeer)
    sum_gd = remote(gd_oth, gd_rcv, ysend.at[2], yrecv.at[2], ypeer)
    send_g = remote(gg.at[mine], gg.at[theirs], ysend.at[3], yrecv.at[3], ypeer)

    @pl.when(by_rows)
    def _():
        send_acts.start()
        send_low.start()
        raw_gd.start()
        raw_gu.start()

    loads[0].wait()
    loads[1].wait()

    def cast_up(i, carry):
        at = pl.ds(pl.multiple_of(i * 128, 128), 128)
        wu_bf[at, :] = wu32[at, :].astype(BF16)
        return carry
    lax.fori_loop(0, width // 128, cast_up, 0)

    def own_pre(i, carry):
        at = pl.ds(pl.multiple_of(i * rb, rb), rb)
        val, slp = gelu_both(mm(aa[at, :], wu_bf[...], NN))
        h_own[at, :] = val.astype(BF16)
        slope[at, :] = slp
        return carry
    loads[2].wait()

    @pl.when(by_sums)
    def _():
        gd_load.start()
        gu_load.start()
    for copy in loads[3:]:
        copy.start()
    lax.fori_loop(0, nb, own_pre, 0)

    def down_block(j, base):
        at = pl.ds(pl.multiple_of(base * half + j * 128, 128), 128)
        return mm(h_own[:, at], gg[mine, :], TN)

    def up_block(j, ff_at):
        at = pl.ds(pl.multiple_of(j * 128, 128), 128)
        return mm(aa[mine, at], dz_own[:, ff_at], TN)

    def send_down():
        gd_load.wait()

        def down_oth(j, carry):
            gd_oth[pl.ds(pl.multiple_of(j * 128, 128), 128), :] += down_block(j, do)
            return carry
        lax.fori_loop(0, half // 128, down_oth, 0)
        gu_load.wait()
        sum_gd.start()

    @pl.when(p == last)
    def _():
        dy_load.wait()
        send_down()


    def cast_down(i, carry):
        at = pl.ds(pl.multiple_of(i * 128, 128), 128)
        wd_bf[at, :] = wd32[at, :].astype(BF16)
        return carry
    lax.fori_loop(0, 2 * half // 128, cast_down, 0)

    @pl.when(p == hub)
    def _():
        pltpu.make_async_copy(hid_o.at[low], hid_o.at[low], rrecv.at[0]).wait()
        relay_over.start()
        pltpu.make_async_copy(dz_o.at[low], dz_o.at[low], rrecv.at[1]).wait()
        relay_back.start()

    def g_at(c, zi):
        return gg.at[pl.ds(pl.multiple_of(c * rb + zi * hb, hb), hb)]

    def part_copy(c):
        return remote(part.at[c, pl.ds(pl.multiple_of(zo * hb, hb), hb)], part_rcv.at[c], psend.at[c], precv.at[c], zpeer)

    def fin_copy(c, zi):
        return remote(fin.at[c], g_at(c, z), fsend.at[c, zi], frecv.at[c, z], (zi, d, lax.max(p - 1, 0)))

    def compute(c):
        @pl.when(p < last)
        def _():
            for zi in range(n_model):
                pltpu.make_async_copy(fin.at[c], g_at(c, zi), frecv.at[c, zi]).wait()
        at = pl.ds(pl.multiple_of(c * rb, rb), rb)
        grad_hid = mm(gg[at, :], wd_bf[...], NT)
        dz_own[at, :] = (slope[at, :] * grad_hid).astype(BF16)

        @pl.when(p > 0)
        def _():
            part[c] = mm(dz_own[at, :], wu_bf[...], NT)
            part_copy(c).start()

    def finalize(c):
        part_copy(c).wait_recv()
        at = pl.ds(pl.multiple_of(c * rb + z * hb, hb), hb)
        total = part[c, pl.ds(pl.multiple_of(z * hb, hb), hb), :] + part_rcv[c]
        fin[c] = (gg[at, :].astype(F32) + total).astype(BF16)
        for zi in range(n_model):
            fin_copy(c, zi).start()

    def chain(i, carry):
        compute(i)

        @pl.when((i >= 1) & (p > 0))
        def _():
            finalize(i - 1)
        return carry
    lax.fori_loop(0, nb, chain, 0)

    @pl.when(by_sums & (p < hub))
    def _():
        send_down()

    @pl.when(p > 0)
    def _():
        finalize(nb - 1)

    @pl.when((p >= hub) & (p < last))
    def _():
        send_down()

    @pl.when(by_sums)
    def _():
        def up_oth(j, carry):
            gu_oth[pl.ds(pl.multiple_of(j * 128, 128), 128), :] += up_block(j, oth_ff)
            return carry
        lax.fori_loop(0, width // 128, up_oth, 0)

    @pl.when(by_rows)
    def _():
        send_g.start()
    loads[3].wait()
    loads[4].wait()

    def down_own(j, carry):
        gd_own[pl.ds(pl.multiple_of(j * 128, 128), 128), :] += down_block(j, d)
        return carry
    lax.fori_loop(0, half // 128, down_own, 0)

    @pl.when(by_sums)
    def _():
        sum_gu.start()

    def up_own(j, carry):
        gu_own[pl.ds(pl.multiple_of(j * 128, 128), 128), :] += up_block(j, own_ff)
        return carry
    lax.fori_loop(0, width // 128, up_own, 0)

    @pl.when(by_rows)
    def _():
        send_low.wait_recv()
        pltpu.make_async_copy(aa.at[late_rows], aa.at[late_rows], rrecv.at[2]).wait()

        def oth_pre(i, carry):
            at = pl.ds(pl.multiple_of(i * rb, rb), rb)
            val, slp = gelu_both(mm(aa[pl.ds(pl.multiple_of(rows + i * rb, rb), rb), :], wu_bf[:, own_ff], NN))
            hid_o[at, :] = val.astype(BF16)
            slope_o[at, :] = slp
            return carry
        lax.fori_loop(0, nb, oth_pre, 0)
        send_g.wait_recv()

        def oth_dz(i, carry):
            at = pl.ds(pl.multiple_of(i * rb, rb), rb)
            grad_hid = mm(gg[pl.ds(pl.multiple_of(rows + i * rb, rb), rb), :], wd_bf[own_ff, :], NT)
            dz_o[at, :] = (slope_o[at, :] * grad_hid).astype(BF16)
            return carry
        lax.fori_loop(0, nb, oth_dz, 0)

        def oth_grads(j, carry):
            at = pl.ds(pl.multiple_of(j * 128, 128), 128)
            gd_own[at, :] += mm(hid_o[:, at], gg[theirs, :], TN)
            gu_own[at, :] += mm(aa[theirs, at], dz_o[...], TN)
            return carry
        lax.fori_loop(0, half // 128, oth_grads, 0)

    def combine(own, rcv):
        def body(i, acc):
            at = pl.ds(pl.multiple_of(i * 32, 32), 32)
            mean = (own[at, :] + rcv[at, :]) * 0.5
            own[at, :] = mean
            return acc + jnp.sum((mean * mean).reshape(4, 8, mean.shape[1]), axis=0)
        return body

    def combine_up(acc):
        raw_gu.wait_recv()
        return lax.fori_loop(0, gu_own.shape[0] // 32, combine(gu_own, gu_rcv), acc)

    def combine_down(acc):
        raw_gd.wait_recv()
        return lax.fori_loop(0, gd_own.shape[0] // 32, combine(gd_own, gd_rcv), acc)
    acc = jnp.zeros((8, half), F32)
    acc = combine_down(acc)
    store_d = pltpu.make_async_copy(gd_own, gbd_hbm, st_sem.at[1])
    store_d.start()
    store_early = pltpu.make_async_copy(gd_own.at[pl.ds(0, EARLY_ROWS)], early_hbm, st_sem.at[2])
    store_early.start()
    acc = combine_up(acc)
    store_u = pltpu.make_async_copy(gu_own, gbu_hbm, st_sem.at[0])
    store_u.start()
    store_late = pltpu.make_async_copy(gu_own.at[pl.ds(width - LATE_ROWS, LATE_ROWS)], late_hbm, st_sem.at[3])
    store_late.start()
    tile = acc[:, 0:128]
    for k in range(1, half // 128):
        tile = tile + acc[:, k * 128:(k + 1) * 128]
    n_all = n_model * n_data * n_stage
    my_id = (z * n_data + d) * n_stage + p
    norm_buf[my_id] = tile

    def norm_copy(k):
        peer = lax.rem(my_id + k, n_all)
        device = (peer // (n_data * n_stage), lax.rem(peer // n_stage, n_data), lax.rem(peer, n_stage))
        return remote(norm_buf.at[my_id], norm_buf.at[my_id], nsend.at[k], nrecv.at[my_id], device)
    for k in range(1, n_all):
        norm_copy(k).start()
    for k in range(1, n_all):
        peer = lax.rem(my_id + k, n_all)
        pltpu.make_async_copy(norm_buf.at[peer], norm_buf.at[peer], nrecv.at[peer]).wait()
    total = norm_buf[0]
    for k in range(1, n_all):
        total = total + norm_buf[k]
    norm_out[...] = total

    for k in range(1, n_all):
        norm_copy(k).wait_send()

    @pl.when(by_rows)
    def _():
        for copy in (send_acts, send_low, raw_gu, raw_gd, send_g):
            copy.wait_send()

    @pl.when(p == hub)
    def _():
        relay_over.wait_send()
        relay_back.wait_send()

    @pl.when(by_sums)
    def _():
        sum_gu.wait_send()
        sum_gd.wait_send()

    @pl.when(p > 0)
    def _():
        for c in range(nb):
            part_copy(c).wait_send()
            for zi in range(n_model):
                fin_copy(c, zi).wait_send()
    store_u.wait()
    store_d.wait()
    store_early.wait()
    store_late.wait()


def update_kernel(d_ref, lr_ref, mn_ref, norm_ref, gu, gd, wu, wd, mu, md, vu, vd, *rest):
    owu, owd, omu, omd, ovu, ovd = rest[:6]
    clip = clip_of(norm_ref[...], mn_ref[0])
    rate = lr_ref[0]
    owu[...], omu[...], ovu[...] = adamw_update(wu[...], mu[...], vu[...], clip * gu[...], rate)
    owd[...], omd[...], ovd[...] = adamw_update(wd[...], md[...], vd[...], clip * gd[...], rate)
    if len(rest) == 8:
        rest[6][...] = owu[...].astype(BF16)
        rest[7][...] = owd[...].astype(BF16)


def fill_kernel(d_ref, lr_ref, mn_ref, norm_ref, gu, gd_early, gd_rest, y_in, wu, wd, mu, md, vu, vd, *rest):
    owu, owd, omu, omd, ovu, ovd, y_out = rest[6:]
    clip = clip_of(norm_ref[...], mn_ref[0])
    rate = lr_ref[0]
    step = pl.program_id(0)
    early_at = pl.ds(pl.multiple_of(jnp.minimum(step, EARLY_ROWS // UPD_ROWS - 1) * UPD_ROWS, UPD_ROWS), UPD_ROWS)
    gd = jnp.where(step < EARLY_ROWS // UPD_ROWS, gd_early[early_at, :], gd_rest[...])
    owu[...], omu[...], ovu[...] = adamw_update(wu[...], mu[...], vu[...], clip * gu[...], rate)
    owd[...], omd[...], ovd[...] = adamw_update(wd[...], md[...], vd[...], clip * gd, rate)
    y_out[...] = y_in[...]


def late_kernel(d_ref, lr_ref, mn_ref, norm_ref, gu, wu, mu, vu, *rest):
    owu, omu, ovu = rest[3:]
    clip = clip_of(norm_ref[...], mn_ref[0])
    owu[...], omu[...], ovu[...] = adamw_update(wu[...], mu[...], vu[...], clip * gu[...], lr_ref[0])


def fwd_kernel(dims, bu_hbm, bd_hbm, gbu_hbm, gbd_hbm, x_hbm,
               gu_oth, gd_oth, y_hbm,
               wu_bf, wd_bf, wu_z, wd_z, a_buf, y_buf, part, part_rcv, fin,
               ld_sem, ysend, yrecv, zsend, zrecv, psend, precv, fsend, frecv, agsend, agrecv, outsend, outrecv, turn):
    n_model, n_data, n_stage = dims
    z, d, p = lax.axis_index('model'), lax.axis_index('data'), lax.axis_index('stage')
    zo, do = 1 - z, 1 - d
    ypeer, zpeer = (z, do, p), (zo, d, p)
    last = n_stage - 1
    nc, rb, width = a_buf.shape
    half = wu_bf.shape[1] // 2
    hb = rb // 2
    own_ff = pl.ds(pl.multiple_of(d * half, 128), half)
    oth_ff = pl.ds(pl.multiple_of(do * half, 128), half)
    first = (p == 0) | (p == last)
    partner = (z, d, p + 1 - 2 * lax.rem(p, 2))

    load_u = pltpu.make_async_copy(bu_hbm, wu_bf.at[:, own_ff], ld_sem.at[0])
    load_d = pltpu.make_async_copy(bd_hbm, wd_bf.at[own_ff, :], ld_sem.at[1])
    load_u.start()
    load_d.start()
    x_load = pltpu.make_async_copy(x_hbm, a_buf, ld_sem.at[2])

    @pl.when(p == 0)
    def _():
        x_load.start()
    whole_barrier(n_model, n_data, n_stage)

    send_wu = remote(bu_hbm, wu_bf.at[:, own_ff], ysend.at[0], yrecv.at[0], ypeer)
    send_wd = remote(bd_hbm, wd_bf.at[own_ff, :], ysend.at[1], yrecv.at[1], ypeer)
    send_gu = remote(gbu_hbm.at[pl.ds(0, gu_oth.shape[0])], gu_oth, ysend.at[2], yrecv.at[2], ypeer)
    send_gd = remote(gbd_hbm.at[pl.ds(half - gd_oth.shape[0], gd_oth.shape[0])], gd_oth, ysend.at[3], yrecv.at[3], ypeer)

    shard = [
        remote(bu_hbm, wu_z.at[:, own_ff], zsend.at[0], zrecv.at[0], zpeer),
        remote(bd_hbm, wd_z.at[own_ff, :], zsend.at[1], zrecv.at[1], zpeer),
        remote(wu_bf.at[:, oth_ff], wu_z.at[:, oth_ff], zsend.at[2], zrecv.at[2], zpeer),
        remote(wd_bf.at[oth_ff, :], wd_z.at[oth_ff, :], zsend.at[3], zrecv.at[3], zpeer),
    ]

    @pl.when(p == last)
    def _():
        shard[0].start()
        shard[1].start()

    @pl.when(first)
    def _():
        send_wu.start()
        send_wd.start()
        send_wu.wait_send()
        send_wd.wait_send()
        pl.semaphore_signal(turn, inc=1, device_id=partner, device_id_type=MESH)

    @pl.when(jnp.logical_not(first))
    def _():
        pl.semaphore_wait(turn, 1)
        send_wu.start()
        send_wd.start()
        send_gu.start()
        send_gd.start()
        send_wu.wait_send()
        send_wd.wait_send()
        pl.semaphore_signal(turn, inc=1, device_id=partner, device_id_type=MESH)

    @pl.when(p == 0)
    def _():
        x_load.wait()
    load_u.wait()
    load_d.wait()
    send_wu.wait_recv()

    @pl.when(p == last)
    def _():
        shard[2].start()
    send_wd.wait_recv()

    @pl.when(p == last)
    def _():
        shard[3].start()
        pl.semaphore_wait(turn, 1)
        send_gu.start()
        send_gd.start()
        for copy in shard:
            copy.wait_recv()

    def half_rows(zi):
        return pl.ds(pl.multiple_of(zi * hb, hb), hb)

    def part_copy(c):
        return remote(part.at[c, half_rows(zo)], part_rcv.at[c], psend.at[c], precv.at[c], zpeer)

    def fin_copy(c, zi):
        return remote(fin.at[c], a_buf.at[c, half_rows(z)], fsend.at[c, zi], frecv.at[c, z], (zi, d, lax.min(p + 1, last)))

    def gather_copy(c):
        return remote(fin.at[c], y_buf.at[c, half_rows(z)], agsend.at[c], agrecv.at[c], zpeer)

    def out_copy(c, q):
        return remote(y_buf.at[c], y_hbm.at[c], outsend.at[c, q], outrecv.at[c], (z, d, q))

    def out_local(c):
        return pltpu.make_async_copy(y_buf.at[c], y_hbm.at[c], outsend.at[c, last])

    def arrived(c, zi):
        pltpu.make_async_copy(fin.at[c], a_buf.at[c, half_rows(zi)], frecv.at[c, zi]).wait()

    def branch(rows_in, w_up, w_down):
        hid = gelu_val(mm(rows_in, w_up[...], NN)).astype(BF16)
        return mm(hid, w_down[...], NN)

    def compute(c):
        @pl.when(p < last)
        def _():
            @pl.when(p > 0)
            def _():
                for zi in range(n_model):
                    arrived(c, zi)
            part[c] = branch(a_buf[c], wu_bf, wd_bf)
            part_copy(c).start()

        @pl.when(p == last)
        def _():
            arrived(c, z)
            at = half_rows(z)
            rows_in = a_buf[c, at, :]
            total = branch(rows_in, wu_bf, wd_bf) + branch(rows_in, wu_z, wd_z)
            new = (rows_in.astype(F32) + total).astype(BF16)
            fin[c] = new
            y_buf[c, at, :] = new
            gather_copy(c).start()

    def finalize(c):
        part_copy(c).wait_recv()
        total = part[c, half_rows(z), :] + part_rcv[c]
        fin[c] = (a_buf[c, half_rows(z), :].astype(F32) + total).astype(BF16)
        fin_copy(c, z).start()

        @pl.when(p < last - 1)
        def _():
            fin_copy(c, zo).start()

    def publish(c):
        gather_copy(c).wait_recv()
        out_local(c).start()
        for q in range(last):
            out_copy(c, q).start()

    def chain(i, carry):
        @pl.when(i < nc)
        def _():
            compute(i)

        @pl.when((i >= 1) & (i <= nc) & (p < last))
        def _():
            finalize(i - 1)

        @pl.when((i >= 1) & (i <= nc) & (p == last))
        def _():
            publish(i - 1)

        @pl.when((i == TURN_STEP) & (p == 0))
        def _():
            pl.semaphore_wait(turn, 1)
            send_gu.start()
            send_gd.start()
        return carry
    lax.fori_loop(0, nc + 1, chain, 0)

    def drain(c, carry):
        @pl.when(p < last)
        def _():
            part_copy(c).wait_send()
            fin_copy(c, z).wait_send()

            @pl.when(p < last - 1)
            def _():
                fin_copy(c, zo).wait_send()
            pltpu.make_async_copy(y_buf.at[c], y_hbm.at[c], outrecv.at[c]).wait()

        @pl.when(p == last)
        def _():
            gather_copy(c).wait_send()
            out_local(c).wait()
            for q in range(last):
                out_copy(c, q).wait_send()
        return carry
    lax.fori_loop(0, nc, drain, 0)

    @pl.when(p == last)
    def _():
        for copy in shard:
            copy.wait_send()
    send_gu.wait()
    send_gd.wait()


def solution(mesh):
    n_model, n_data, n_stage = (mesh.shape[k] for k in ('model', 'data', 'stage'))
    dims = (n_model, n_data, n_stage)
    n_all = n_model * n_data * n_stage
    up_spec = P('stage', None, 'model')
    down_spec = P('stage', 'model', None)
    row_spec = P(None, 'data', None)
    in_specs = (up_spec, down_spec, up_spec, down_spec, up_spec, down_spec, P('data', 'stage', None, 'model'), P('data', 'stage', 'model', None), P('stage', 'data', None), P('data', None), row_spec, P(None), P(None))
    out_specs = (up_spec, down_spec, up_spec, down_spec, up_spec, down_spec, row_spec)
    any_spec = pl.BlockSpec(memory_space=pl.ANY)
    vmem_spec = pl.BlockSpec(memory_space=pltpu.VMEM)
    smem_spec = pl.BlockSpec(memory_space=pltpu.SMEM)
    dma = pltpu.SemaphoreType.DMA

    def device_step(w_up, w_down, m_up, m_down, v_up, v_down, g_up, g_down, acts_last, grad_out, x_next, learn_rate, max_norm):
        rows, width = grad_out.shape
        ff = w_up.shape[2]
        half = ff // 2
        nb = rows // BACK_ROWS
        hb = BACK_ROWS // 2
        sds = jax.ShapeDtypeStruct
        gbar_u, gbar_d, early, late, norm_tile = pl.pallas_call(
            functools.partial(bwd_kernel, dims),
            out_shape=(sds((width, half), F32), sds((half, width), F32), sds((EARLY_ROWS, width), F32), sds((LATE_ROWS, half), F32), sds((8, 128), F32)),
            in_specs=[any_spec] * 6,
            out_specs=(any_spec,) * 4 + (vmem_spec,),
            scratch_shapes=[
                pltpu.VMEM((width, ff), F32), pltpu.VMEM((ff, width), F32),
                pltpu.VMEM((width, ff), BF16), pltpu.VMEM((ff, width), BF16),
                pltpu.VMEM((2 * rows, width), BF16), pltpu.VMEM((2 * rows, width), BF16),
                pltpu.VMEM((rows, half), BF16), pltpu.VMEM((rows, half), BF16),
                pltpu.VMEM((rows, ff), F32), pltpu.VMEM((rows, half), F32),
                pltpu.VMEM((rows, ff), BF16), pltpu.VMEM((rows, ff), BF16),
            ] + [pltpu.VMEM((width, half), F32), pltpu.VMEM((half, width), F32)] * 3 + [
                pltpu.VMEM((nb, BACK_ROWS, width), F32), pltpu.VMEM((nb, hb, width), F32),
                pltpu.VMEM((nb, hb, width), BF16), pltpu.VMEM((n_all, 8, 128), F32),
                dma((8,)), dma((4,)), dma((4,)), dma((3,)), dma((3,)), dma((nb,)), dma((nb,)), dma((nb, 2)), dma((nb, 2)),
                dma((n_all,)), dma((n_all,)), dma((4,)),
            ],
            compiler_params=pltpu.CompilerParams(collective_id=0, has_side_effects=True, vmem_limit_bytes=VMEM_LIMIT),
            name='backward',
        )(w_up[0], w_down[0], acts_last[0], grad_out, g_up[0, 0], g_down[0, 0])

        early_oth = lax.ppermute(early, 'data', [(k, 1 - k) for k in range(n_data)])
        blocks = half // UPD_ROWS
        state = (w_up[0], w_down[0], m_up[0], m_down[0], v_up[0], v_down[0])
        state_shapes = tuple(sds(s.shape, F32) for s in state)
        which = lax.axis_index('data').astype(jnp.int32).reshape(1)

        def update_specs(pick):
            up = pl.BlockSpec((UPD_ROWS, half), lambda i, w: (i, pick(w[0])))
            down = pl.BlockSpec((UPD_ROWS, width), lambda i, w: (pick(w[0]) * blocks + i, 0))
            return [up, down]
        plain_up = pl.BlockSpec((UPD_ROWS, half), lambda i, w: (i, 0))
        plain_down = pl.BlockSpec((UPD_ROWS, width), lambda i, w: (i, 0))
        small = [smem_spec, smem_spec, pl.BlockSpec((8, 128), lambda i, w: (0, 0))]
        own = update_specs(lambda w: w)
        *fresh, b_up, b_down = pl.pallas_call(
            update_kernel,
            out_shape=state_shapes + (sds((width, half), BF16), sds((half, width), BF16)),
            grid_spec=pltpu.PrefetchScalarGridSpec(
                num_scalar_prefetch=1, grid=(width // UPD_ROWS,),
                in_specs=small + [plain_up, plain_down] + own * 3,
                out_specs=own * 3 + [plain_up, plain_down]),
            compiler_params=pltpu.CompilerParams(dimension_semantics=('arbitrary',), vmem_limit_bytes=VMEM_LIMIT),
            name='update_own',
        )(which, learn_rate, max_norm, norm_tile, gbar_u, gbar_d, *state)

        n_micro = x_next.shape[0]
        nc = n_micro * rows // FWD_ROWS
        fb = FWD_ROWS // 2
        gu_oth, gd_oth, y_next = pl.pallas_call(
            functools.partial(fwd_kernel, dims),
            out_shape=(sds((width - LATE_ROWS, half), F32), sds((half - EARLY_ROWS, width), F32), sds((nc, FWD_ROWS, width), BF16)),
            in_specs=[any_spec] * 5,
            out_specs=(any_spec, any_spec, any_spec),
            scratch_shapes=[pltpu.VMEM((width, ff), BF16), pltpu.VMEM((ff, width), BF16)] * 2 + [
                pltpu.VMEM((nc, FWD_ROWS, width), BF16), pltpu.VMEM((nc, FWD_ROWS, width), BF16),
                pltpu.VMEM((nc, FWD_ROWS, width), F32), pltpu.VMEM((nc, fb, width), F32),
                pltpu.VMEM((nc, fb, width), BF16),
                dma((3,)), dma((4,)), dma((4,)), dma((4,)), dma((4,)), dma((nc,)), dma((nc,)), dma((nc, 2)), dma((nc, 2)),
                dma((nc,)), dma((nc,)), dma((nc, n_stage)), dma((nc,)), pltpu.SemaphoreType.REGULAR,
            ],
            compiler_params=pltpu.CompilerParams(collective_id=1, has_side_effects=True, vmem_limit_bytes=VMEM_LIMIT),
            name='forward',
        )(b_up, b_down, gbar_u, gbar_d, x_next.reshape(nc, FWD_ROWS, width))

        other = update_specs(lambda w: 1 - w)
        gu_oth, late = lax.optimization_barrier((gu_oth, late))
        late_oth = lax.ppermute(late, 'data', [(k, 1 - k) for k in range(n_data)])
        y_next = y_next.reshape(n_micro * rows, width)
        nearly, nlate = EARLY_ROWS // UPD_ROWS, LATE_ROWS // UPD_ROWS
        steps = width // UPD_ROWS
        lastup = steps - nlate - 1

        def rows_spec(start, count):
            return pl.BlockSpec((UPD_ROWS, width), lambda i, w: (jnp.clip(i - start, 0, count - 1), 0))
        y_spec = pl.BlockSpec((n_micro * rows // steps, width), lambda i, w: (i, 0))
        up_oth = pl.BlockSpec((UPD_ROWS, half), lambda i, w: (jnp.minimum(i, lastup), 1 - w[0]))
        down_oth = pl.BlockSpec((UPD_ROWS, width), lambda i, w: ((1 - w[0]) * blocks + i, 0))
        other = [up_oth, down_oth]
        *filled, y_next = pl.pallas_call(
            fill_kernel,
            out_shape=state_shapes + (sds(y_next.shape, BF16),),
            grid_spec=pltpu.PrefetchScalarGridSpec(
                num_scalar_prefetch=1, grid=(steps,),
                in_specs=small + [rows_spec(0, lastup + 1), vmem_spec, rows_spec(nearly, blocks - nearly), y_spec] + other * 3 + [any_spec] * 6,
                out_specs=other * 3 + [y_spec]),
            input_output_aliases={14 + k: k for k in range(6)},
            compiler_params=pltpu.CompilerParams(dimension_semantics=('arbitrary',), vmem_limit_bytes=VMEM_LIMIT),
            cost_estimate=pl.CostEstimate(flops=10**10, bytes_accessed=40 * 10**6, transcendentals=0),
            name='update_other',
        )(which, learn_rate, max_norm, norm_tile, gu_oth, early_oth, gd_oth, y_next, *state, *fresh)
        up_late = pl.BlockSpec((UPD_ROWS, half), lambda i, w: (steps - nlate + i, 1 - w[0]))
        filled[0], filled[2], filled[4] = pl.pallas_call(
            late_kernel,
            out_shape=(state_shapes[0],) * 3,
            grid_spec=pltpu.PrefetchScalarGridSpec(
                num_scalar_prefetch=1, grid=(nlate,),
                in_specs=small + [plain_up] + [up_late] * 3 + [any_spec] * 3,
                out_specs=[up_late] * 3),
            input_output_aliases={8 + k: k for k in range(3)},
            compiler_params=pltpu.CompilerParams(dimension_semantics=('arbitrary',), vmem_limit_bytes=VMEM_LIMIT),
            name='update_late',
        )(which, learn_rate, max_norm, norm_tile, late_oth, state[0], state[2], state[4], filled[0], filled[2], filled[4])
        return tuple(s[None] for s in filled) + (y_next.reshape(n_micro, rows, width),)

    return jax.shard_map(device_step, mesh=mesh, in_specs=in_specs, out_specs=out_specs, check_vma=False)
```

```python
import functools

import jax
import jax.numpy as jnp
from jax import lax
from jax.experimental import pallas as pl
from jax.experimental.pallas import tpu as pltpu
from jax.sharding import PartitionSpec as P

ADAM_STEP = 10
BETA_ONE = 0.9
BETA_TWO = 0.95
ADAM_EPS = 1e-8
WEIGHT_DECAY = 0.1
NORM_EPS = 1e-6
ONE_CORR = 1.0 - BETA_ONE ** ADAM_STEP
TWO_CORR = 1.0 - BETA_TWO ** ADAM_STEP
GELU_SCALE = (2.0 / 3.141592653589793) ** 0.5
GELU_CUBE = 0.044715
NN = (((1,), (0,)), ((), ()))
NT = (((1,), (1,)), ((), ()))
TN = (((0,), (0,)), ((), ()))
F32 = jnp.float32
BF16 = jnp.bfloat16
MESH = pl.DeviceIdType.MESH
BACK_ROWS = 128
FWD_ROWS = 96
UPD_ROWS = 128
EARLY_ROWS = 256
LATE_ROWS = 128
TURN_STEP = 5
VMEM_LIMIT = 66_000_000


def mm(lhs, rhs, dims):
    return lax.dot_general(lhs, rhs, dims, preferred_element_type=F32)


def gelu_val(pre):
    return pre * (0.5 * (1.0 + jnp.tanh(GELU_SCALE * (pre + GELU_CUBE * (pre * pre * pre)))))


def gelu_both(pre):
    sq = pre * pre
    tan = jnp.tanh(GELU_SCALE * (pre + GELU_CUBE * (sq * pre)))
    cdf = 0.5 * (1.0 + tan)
    slope = cdf + 0.5 * pre * (1.0 - tan * tan) * (GELU_SCALE * (1.0 + (3.0 * GELU_CUBE) * sq))
    return pre * cdf, slope


def adamw_update(weight, moment_one, moment_two, grad_step, step_rate):
    mom_new = BETA_ONE * moment_one + (1.0 - BETA_ONE) * grad_step
    sec_new = BETA_TWO * moment_two + (1.0 - BETA_TWO) * grad_step * grad_step
    direction = (mom_new * (1.0 / ONE_CORR)) / (jnp.sqrt(sec_new * (1.0 / TWO_CORR)) + ADAM_EPS)
    weight_new = weight - step_rate * (direction + WEIGHT_DECAY * weight)
    return weight_new, mom_new, sec_new


def clip_of(norm_tile, max_norm):
    total = jnp.sum(jnp.sum(norm_tile, axis=0, keepdims=True), axis=1, keepdims=True)
    return jnp.minimum(1.0, max_norm / (jnp.sqrt(total) + NORM_EPS))


def whole_barrier(n_model, n_data, n_stage):
    barrier = pltpu.get_barrier_semaphore()
    me = (lax.axis_index('model'), lax.axis_index('data'), lax.axis_index('stage'))
    for dm in range(n_model):
        for dd in range(n_data):
            for ds in range(n_stage):
                if dm or dd or ds:
                    peer = (lax.rem(me[0] + dm, n_model), lax.rem(me[1] + dd, n_data), lax.rem(me[2] + ds, n_stage))
                    pl.semaphore_signal(barrier, inc=1, device_id=peer, device_id_type=MESH)
    pl.semaphore_wait(barrier, n_model * n_data * n_stage - 1)


def replica_barrier(n_model, n_data, n_stage):
    barrier = pltpu.get_barrier_semaphore()
    z, d, p = lax.axis_index('model'), lax.axis_index('data'), lax.axis_index('stage')
    pl.semaphore_signal(barrier, inc=1, device_id=(z, lax.rem(d + 1, n_data), p), device_id_type=MESH)
    for dm in range(n_model):
        for ds in range(n_stage):
            if dm or ds:
                peer = (lax.rem(z + dm, n_model), d, lax.rem(p + ds, n_stage))
                pl.semaphore_signal(barrier, inc=1, device_id=peer, device_id_type=MESH)
    pl.semaphore_wait(barrier, n_model * n_stage)


def remote(src, dst, send_sem, recv_sem, device):
    return pltpu.make_async_remote_copy(src_ref=src, dst_ref=dst, send_sem=send_sem, recv_sem=recv_sem, device_id=device, device_id_type=MESH)


def bwd_kernel(dims, wu_hbm, wd_hbm, acts_hbm, dy_hbm, gu_hbm, gd_hbm,
               gbu_hbm, gbd_hbm, early_hbm, late_hbm, norm_out,
               wu32, wd32, wu_bf, wd_bf, aa, gg, hid_o, dz_o, slope, slope_o, dz_own, h_own,
               gu_own, gd_own, gu_oth, gd_oth, gu_rcv, gd_rcv, part, part_rcv, fin, norm_buf,
               ld_sem, ysend, yrecv, rsend, rrecv, psend, precv, fsend, frecv, nsend, nrecv, st_sem):
    n_model, n_data, n_stage = dims
    z, d, p = lax.axis_index('model'), lax.axis_index('data'), lax.axis_index('stage')
    zo, do = 1 - z, 1 - d
    ypeer, zpeer = (z, do, p), (zo, d, p)
    last = n_stage - 1
    by_rows = p == 0
    by_sums = p > 0
    hub = n_stage // 2
    rows = aa.shape[0] // 2
    width = aa.shape[1]
    half = hid_o.shape[1]
    rb = BACK_ROWS
    hb = rb // 2
    nb = rows // rb
    own_ff = pl.ds(pl.multiple_of(d * half, 128), half)
    oth_ff = pl.ds(pl.multiple_of(do * half, 128), half)
    mine, theirs = pl.ds(0, rows), pl.ds(rows, rows)

    loads = [
        pltpu.make_async_copy(wu_hbm, wu32, ld_sem.at[0]),
        pltpu.make_async_copy(acts_hbm, aa.at[mine], ld_sem.at[2]),
        pltpu.make_async_copy(wd_hbm, wd32, ld_sem.at[1]),
        pltpu.make_async_copy(gu_hbm.at[:, own_ff], gu_own, ld_sem.at[4]),
        pltpu.make_async_copy(gd_hbm.at[own_ff, :], gd_own, ld_sem.at[5]),
    ]
    dy_load = pltpu.make_async_copy(dy_hbm, gg.at[mine], ld_sem.at[3])
    gu_load = pltpu.make_async_copy(gu_hbm.at[:, oth_ff], gu_oth, ld_sem.at[6])
    gd_load = pltpu.make_async_copy(gd_hbm.at[oth_ff, :], gd_oth, ld_sem.at[7])
    for copy in loads[:3]:
        copy.start()

    @pl.when(p == last)
    def _():
        dy_load.start()
    whole_barrier(n_model, n_data, n_stage)
    low, high = pl.ds(0, rows // 2), pl.ds(rows // 2, rows // 2)
    late_rows = pl.ds(rows + rows // 2, rows // 2)
    send_low = remote(acts_hbm.at[low], aa.at[pl.ds(rows, rows // 2)], ysend.at[0], yrecv.at[0], ypeer)
    send_acts = remote(acts_hbm.at[high], hid_o.at[low], rsend.at[2], rrecv.at[0], (z, d, hub))
    relay_over = remote(hid_o.at[low], dz_o.at[low], rsend.at[0], rrecv.at[1], ypeer)
    relay_back = remote(dz_o.at[low], aa.at[late_rows], rsend.at[1], rrecv.at[2], (z, d, 0))
    raw_gu = remote(gu_hbm.at[:, oth_ff], gu_rcv, ysend.at[1], yrecv.at[1], ypeer)
    raw_gd = remote(gd_hbm.at[oth_ff, :], gd_rcv, ysend.at[2], yrecv.at[2], ypeer)
    sum_gu = remote(gu_oth, gu_rcv, ysend.at[1], yrecv.at[1], ypeer)
    sum_gd = remote(gd_oth, gd_rcv, ysend.at[2], yrecv.at[2], ypeer)
    send_g = remote(gg.at[mine], gg.at[theirs], ysend.at[3], yrecv.at[3], ypeer)

    @pl.when(by_rows)
    def _():
        send_acts.start()
        send_low.start()
        raw_gd.start()
        raw_gu.start()

    loads[0].wait()
    loads[1].wait()

    def cast_up(i, carry):
        at = pl.ds(pl.multiple_of(i * 128, 128), 128)
        wu_bf[at, :] = wu32[at, :].astype(BF16)
        return carry
    lax.fori_loop(0, width // 128, cast_up, 0)

    def own_pre(i, carry):
        at = pl.ds(pl.multiple_of(i * rb, rb), rb)
        val, slp = gelu_both(mm(aa[at, :], wu_bf[...], NN))
        h_own[at, :] = val.astype(BF16)
        slope[at, :] = slp
        return carry
    loads[2].wait()

    @pl.when(by_sums)
    def _():
        gd_load.start()
        gu_load.start()
    for copy in loads[3:]:
        copy.start()
    lax.fori_loop(0, nb, own_pre, 0)

    def down_block(j, base):
        at = pl.ds(pl.multiple_of(base * half + j * 128, 128), 128)
        return mm(h_own[:, at], gg[mine, :], TN)

    def up_block(j, ff_at):
        at = pl.ds(pl.multiple_of(j * 128, 128), 128)
        return mm(aa[mine, at], dz_own[:, ff_at], TN)

    def send_down():
        gd_load.wait()

        def down_oth(j, carry):
            gd_oth[pl.ds(pl.multiple_of(j * 128, 128), 128), :] += down_block(j, do)
            return carry
        lax.fori_loop(0, half // 128, down_oth, 0)
        gu_load.wait()
        sum_gd.start()

    @pl.when(p == last)
    def _():
        dy_load.wait()
        send_down()


    def cast_down(i, carry):
        at = pl.ds(pl.multiple_of(i * 128, 128), 128)
        wd_bf[at, :] = wd32[at, :].astype(BF16)
        return carry
    lax.fori_loop(0, 2 * half // 128, cast_down, 0)

    @pl.when(p == hub)
    def _():
        pltpu.make_async_copy(hid_o.at[low], hid_o.at[low], rrecv.at[0]).wait()
        relay_over.start()
        pltpu.make_async_copy(dz_o.at[low], dz_o.at[low], rrecv.at[1]).wait()
        relay_back.start()

    def g_at(c, zi):
        return gg.at[pl.ds(pl.multiple_of(c * rb + zi * hb, hb), hb)]

    def part_copy(c):
        return remote(part.at[c, pl.ds(pl.multiple_of(zo * hb, hb), hb)], part_rcv.at[c], psend.at[c], precv.at[c], zpeer)

    def fin_copy(c, zi):
        return remote(fin.at[c], g_at(c, z), fsend.at[c, zi], frecv.at[c, z], (zi, d, lax.max(p - 1, 0)))

    def compute(c):
        @pl.when(p < last)
        def _():
            for zi in range(n_model):
                pltpu.make_async_copy(fin.at[c], g_at(c, zi), frecv.at[c, zi]).wait()
        at = pl.ds(pl.multiple_of(c * rb, rb), rb)
        grad_hid = mm(gg[at, :], wd_bf[...], NT)
        dz_own[at, :] = (slope[at, :] * grad_hid).astype(BF16)

        @pl.when(p > 0)
        def _():
            part[c] = mm(dz_own[at, :], wu_bf[...], NT)
            part_copy(c).start()

    def finalize(c):
        part_copy(c).wait_recv()
        at = pl.ds(pl.multiple_of(c * rb + z * hb, hb), hb)
        total = part[c, pl.ds(pl.multiple_of(z * hb, hb), hb), :] + part_rcv[c]
        fin[c] = (gg[at, :].astype(F32) + total).astype(BF16)
        for zi in range(n_model):
            fin_copy(c, zi).start()

    def chain(i, carry):
        compute(i)

        @pl.when((i >= 1) & (p > 0))
        def _():
            finalize(i - 1)
        return carry
    lax.fori_loop(0, nb, chain, 0)

    @pl.when(by_sums & (p < hub))
    def _():
        send_down()

    @pl.when(p > 0)
    def _():
        finalize(nb - 1)

    @pl.when((p >= hub) & (p < last))
    def _():
        send_down()

    @pl.when(by_sums)
    def _():
        def up_oth(j, carry):
            gu_oth[pl.ds(pl.multiple_of(j * 128, 128), 128), :] += up_block(j, oth_ff)
            return carry
        lax.fori_loop(0, width // 128, up_oth, 0)

    @pl.when(by_rows)
    def _():
        send_g.start()
    loads[3].wait()
    loads[4].wait()

    def down_own(j, carry):
        gd_own[pl.ds(pl.multiple_of(j * 128, 128), 128), :] += down_block(j, d)
        return carry
    lax.fori_loop(0, half // 128, down_own, 0)

    @pl.when(by_sums)
    def _():
        sum_gu.start()

    def up_own(j, carry):
        gu_own[pl.ds(pl.multiple_of(j * 128, 128), 128), :] += up_block(j, own_ff)
        return carry
    lax.fori_loop(0, width // 128, up_own, 0)

    @pl.when(by_rows)
    def _():
        send_low.wait_recv()
        pltpu.make_async_copy(aa.at[late_rows], aa.at[late_rows], rrecv.at[2]).wait()

        def oth_pre(i, carry):
            at = pl.ds(pl.multiple_of(i * rb, rb), rb)
            val, slp = gelu_both(mm(aa[pl.ds(pl.multiple_of(rows + i * rb, rb), rb), :], wu_bf[:, own_ff], NN))
            hid_o[at, :] = val.astype(BF16)
            slope_o[at, :] = slp
            return carry
        lax.fori_loop(0, nb, oth_pre, 0)
        send_g.wait_recv()

        def oth_dz(i, carry):
            at = pl.ds(pl.multiple_of(i * rb, rb), rb)
            grad_hid = mm(gg[pl.ds(pl.multiple_of(rows + i * rb, rb), rb), :], wd_bf[own_ff, :], NT)
            dz_o[at, :] = (slope_o[at, :] * grad_hid).astype(BF16)
            return carry
        lax.fori_loop(0, nb, oth_dz, 0)

        def oth_grads(j, carry):
            at = pl.ds(pl.multiple_of(j * 128, 128), 128)
            gd_own[at, :] += mm(hid_o[:, at], gg[theirs, :], TN)
            gu_own[at, :] += mm(aa[theirs, at], dz_o[...], TN)
            return carry
        lax.fori_loop(0, half // 128, oth_grads, 0)

    def combine(own, rcv):
        def body(i, acc):
            at = pl.ds(pl.multiple_of(i * 32, 32), 32)
            mean = (own[at, :] + rcv[at, :]) * 0.5
            own[at, :] = mean
            return acc + jnp.sum((mean * mean).reshape(4, 8, mean.shape[1]), axis=0)
        return body

    def combine_up(acc):
        raw_gu.wait_recv()
        return lax.fori_loop(0, gu_own.shape[0] // 32, combine(gu_own, gu_rcv), acc)

    def combine_down(acc):
        raw_gd.wait_recv()
        return lax.fori_loop(0, gd_own.shape[0] // 32, combine(gd_own, gd_rcv), acc)
    acc = jnp.zeros((8, half), F32)
    acc = combine_down(acc)
    store_d = pltpu.make_async_copy(gd_own, gbd_hbm, st_sem.at[1])
    store_d.start()
    store_early = pltpu.make_async_copy(gd_own.at[pl.ds(0, EARLY_ROWS)], early_hbm, st_sem.at[2])
    store_early.start()
    acc = combine_up(acc)
    store_u = pltpu.make_async_copy(gu_own, gbu_hbm, st_sem.at[0])
    store_u.start()
    store_late = pltpu.make_async_copy(gu_own.at[pl.ds(width - LATE_ROWS, LATE_ROWS)], late_hbm, st_sem.at[3])
    store_late.start()
    tile = acc[:, 0:128]
    for k in range(1, half // 128):
        tile = tile + acc[:, k * 128:(k + 1) * 128]
    n_all = n_model * n_data * n_stage
    my_id = (z * n_data + d) * n_stage + p
    norm_buf[my_id] = tile

    def norm_copy(k):
        peer = lax.rem(my_id + k, n_all)
        device = (peer // (n_data * n_stage), lax.rem(peer // n_stage, n_data), lax.rem(peer, n_stage))
        return remote(norm_buf.at[my_id], norm_buf.at[my_id], nsend.at[k], nrecv.at[my_id], device)
    for k in range(1, n_all):
        norm_copy(k).start()
    for k in range(1, n_all):
        peer = lax.rem(my_id + k, n_all)
        pltpu.make_async_copy(norm_buf.at[peer], norm_buf.at[peer], nrecv.at[peer]).wait()
    total = norm_buf[0]
    for k in range(1, n_all):
        total = total + norm_buf[k]
    norm_out[...] = total

    for k in range(1, n_all):
        norm_copy(k).wait_send()

    @pl.when(by_rows)
    def _():
        for copy in (send_acts, send_low, raw_gu, raw_gd, send_g):
            copy.wait_send()

    @pl.when(p == hub)
    def _():
        relay_over.wait_send()
        relay_back.wait_send()

    @pl.when(by_sums)
    def _():
        sum_gu.wait_send()
        sum_gd.wait_send()

    @pl.when(p > 0)
    def _():
        for c in range(nb):
            part_copy(c).wait_send()
            for zi in range(n_model):
                fin_copy(c, zi).wait_send()
    store_u.wait()
    store_d.wait()
    store_early.wait()
    store_late.wait()


def update_kernel(d_ref, lr_ref, mn_ref, norm_ref, gu, gd, wu, wd, mu, md, vu, vd, *rest):
    owu, owd, omu, omd, ovu, ovd = rest[:6]
    clip = clip_of(norm_ref[...], mn_ref[0])
    rate = lr_ref[0]
    owu[...], omu[...], ovu[...] = adamw_update(wu[...], mu[...], vu[...], clip * gu[...], rate)
    owd[...], omd[...], ovd[...] = adamw_update(wd[...], md[...], vd[...], clip * gd[...], rate)
    if len(rest) == 8:
        rest[6][...] = owu[...].astype(BF16)
        rest[7][...] = owd[...].astype(BF16)


def fill_kernel(d_ref, lr_ref, mn_ref, norm_ref, gu, gd_early, gd_rest, y_in, wu, wd, mu, md, vu, vd, *rest):
    owu, owd, omu, omd, ovu, ovd, y_out = rest[6:]
    clip = clip_of(norm_ref[...], mn_ref[0])
    rate = lr_ref[0]
    step = pl.program_id(0)
    early_at = pl.ds(pl.multiple_of(jnp.minimum(step, EARLY_ROWS // UPD_ROWS - 1) * UPD_ROWS, UPD_ROWS), UPD_ROWS)
    gd = jnp.where(step < EARLY_ROWS // UPD_ROWS, gd_early[early_at, :], gd_rest[...])
    owu[...], omu[...], ovu[...] = adamw_update(wu[...], mu[...], vu[...], clip * gu[...], rate)
    owd[...], omd[...], ovd[...] = adamw_update(wd[...], md[...], vd[...], clip * gd, rate)
    y_out[...] = y_in[...]


def late_kernel(d_ref, lr_ref, mn_ref, norm_ref, gu, wu, mu, vu, *rest):
    owu, omu, ovu = rest[3:]
    clip = clip_of(norm_ref[...], mn_ref[0])
    owu[...], omu[...], ovu[...] = adamw_update(wu[...], mu[...], vu[...], clip * gu[...], lr_ref[0])


def fwd_kernel(dims, bu_hbm, bd_hbm, gbu_hbm, gbd_hbm, x_hbm,
               gu_oth, gd_oth, y_hbm,
               wu_bf, wd_bf, wu_z, wd_z, a_buf, y_buf, part, part_rcv, fin,
               ld_sem, ysend, yrecv, zsend, zrecv, psend, precv, fsend, frecv, agsend, agrecv, outsend, outrecv, turn):
    n_model, n_data, n_stage = dims
    z, d, p = lax.axis_index('model'), lax.axis_index('data'), lax.axis_index('stage')
    zo, do = 1 - z, 1 - d
    ypeer, zpeer = (z, do, p), (zo, d, p)
    last = n_stage - 1
    nc, rb, width = a_buf.shape
    half = wu_bf.shape[1] // 2
    hb = rb // 2
    own_ff = pl.ds(pl.multiple_of(d * half, 128), half)
    oth_ff = pl.ds(pl.multiple_of(do * half, 128), half)
    first = (p == 0) | (p == last)
    partner = (z, d, p + 1 - 2 * lax.rem(p, 2))

    load_u = pltpu.make_async_copy(bu_hbm, wu_bf.at[:, own_ff], ld_sem.at[0])
    load_d = pltpu.make_async_copy(bd_hbm, wd_bf.at[own_ff, :], ld_sem.at[1])
    load_u.start()
    load_d.start()
    x_load = pltpu.make_async_copy(x_hbm, a_buf, ld_sem.at[2])

    @pl.when(p == 0)
    def _():
        x_load.start()
    replica_barrier(n_model, n_data, n_stage)

    send_wu = remote(bu_hbm, wu_bf.at[:, own_ff], ysend.at[0], yrecv.at[0], ypeer)
    send_wd = remote(bd_hbm, wd_bf.at[own_ff, :], ysend.at[1], yrecv.at[1], ypeer)
    send_gu = remote(gbu_hbm.at[pl.ds(0, gu_oth.shape[0])], gu_oth, ysend.at[2], yrecv.at[2], ypeer)
    send_gd = remote(gbd_hbm.at[pl.ds(half - gd_oth.shape[0], gd_oth.shape[0])], gd_oth, ysend.at[3], yrecv.at[3], ypeer)

    shard = [
        remote(bu_hbm, wu_z.at[:, own_ff], zsend.at[0], zrecv.at[0], zpeer),
        remote(bd_hbm, wd_z.at[own_ff, :], zsend.at[1], zrecv.at[1], zpeer),
        remote(wu_bf.at[:, oth_ff], wu_z.at[:, oth_ff], zsend.at[2], zrecv.at[2], zpeer),
        remote(wd_bf.at[oth_ff, :], wd_z.at[oth_ff, :], zsend.at[3], zrecv.at[3], zpeer),
    ]

    @pl.when(p == last)
    def _():
        shard[0].start()
        shard[1].start()

    @pl.when(first)
    def _():
        send_wu.start()
        send_wd.start()
        send_wu.wait_send()
        send_wd.wait_send()
        pl.semaphore_signal(turn, inc=1, device_id=partner, device_id_type=MESH)

    @pl.when(jnp.logical_not(first))
    def _():
        pl.semaphore_wait(turn, 1)
        send_wu.start()
        send_wd.start()
        send_gu.start()
        send_gd.start()
        send_wu.wait_send()
        send_wd.wait_send()
        pl.semaphore_signal(turn, inc=1, device_id=partner, device_id_type=MESH)

    @pl.when(p == 0)
    def _():
        x_load.wait()
    load_u.wait()
    load_d.wait()
    send_wu.wait_recv()

    @pl.when(p == last)
    def _():
        shard[2].start()
    send_wd.wait_recv()

    @pl.when(p == last)
    def _():
        shard[3].start()
        for copy in shard:
            copy.wait_recv()

    def half_rows(zi):
        return pl.ds(pl.multiple_of(zi * hb, hb), hb)

    def part_copy(c):
        return remote(part.at[c, half_rows(zo)], part_rcv.at[c], psend.at[c], precv.at[c], zpeer)

    def fin_copy(c, zi):
        return remote(fin.at[c], a_buf.at[c, half_rows(z)], fsend.at[c, zi], frecv.at[c, z], (zi, d, lax.min(p + 1, last)))

    def gather_copy(c):
        return remote(fin.at[c], y_buf.at[c, half_rows(z)], agsend.at[c], agrecv.at[c], zpeer)

    def out_copy(c, q):
        return remote(y_buf.at[c], y_hbm.at[c], outsend.at[c, q], outrecv.at[c], (z, d, q))

    def out_local(c):
        return pltpu.make_async_copy(y_buf.at[c], y_hbm.at[c], outsend.at[c, last])

    def arrived(c, zi):
        pltpu.make_async_copy(fin.at[c], a_buf.at[c, half_rows(zi)], frecv.at[c, zi]).wait()

    def branch(rows_in, w_up, w_down):
        hid = gelu_val(mm(rows_in, w_up[...], NN)).astype(BF16)
        return mm(hid, w_down[...], NN)

    def compute(c):
        @pl.when(p < last)
        def _():
            @pl.when(p > 0)
            def _():
                for zi in range(n_model):
                    arrived(c, zi)
            part[c] = branch(a_buf[c], wu_bf, wd_bf)
            part_copy(c).start()

        @pl.when(p == last)
        def _():
            arrived(c, z)
            at = half_rows(z)
            rows_in = a_buf[c, at, :]
            total = branch(rows_in, wu_bf, wd_bf) + branch(rows_in, wu_z, wd_z)
            new = (rows_in.astype(F32) + total).astype(BF16)
            fin[c] = new
            y_buf[c, at, :] = new
            gather_copy(c).start()

    def finalize(c):
        part_copy(c).wait_recv()
        total = part[c, half_rows(z), :] + part_rcv[c]
        fin[c] = (a_buf[c, half_rows(z), :].astype(F32) + total).astype(BF16)
        fin_copy(c, z).start()

        @pl.when(p < last - 1)
        def _():
            fin_copy(c, zo).start()

    def publish(c):
        gather_copy(c).wait_recv()
        out_local(c).start()
        for q in range(last):
            out_copy(c, q).start()

    def chain(i, carry):
        @pl.when(i < nc)
        def _():
            compute(i)

        @pl.when((i >= 1) & (i <= nc) & (p < last))
        def _():
            finalize(i - 1)

        @pl.when((i >= 1) & (i <= nc) & (p == last))
        def _():
            publish(i - 1)

        @pl.when((i == TURN_STEP) & first)
        def _():
            pl.semaphore_wait(turn, 1)
            send_gu.start()
            send_gd.start()
        return carry
    lax.fori_loop(0, nc + 1, chain, 0)

    def drain(c, carry):
        @pl.when(p < last)
        def _():
            part_copy(c).wait_send()
            fin_copy(c, z).wait_send()

            @pl.when(p < last - 1)
            def _():
                fin_copy(c, zo).wait_send()
            pltpu.make_async_copy(y_buf.at[c], y_hbm.at[c], outrecv.at[c]).wait()

        @pl.when(p == last)
        def _():
            gather_copy(c).wait_send()
            out_local(c).wait()
            for q in range(last):
                out_copy(c, q).wait_send()
        return carry
    lax.fori_loop(0, nc, drain, 0)

    @pl.when(p == last)
    def _():
        for copy in shard:
            copy.wait_send()
    send_gu.wait()
    send_gd.wait()


def solution(mesh):
    n_model, n_data, n_stage = (mesh.shape[k] for k in ('model', 'data', 'stage'))
    dims = (n_model, n_data, n_stage)
    n_all = n_model * n_data * n_stage
    up_spec = P('stage', None, 'model')
    down_spec = P('stage', 'model', None)
    row_spec = P(None, 'data', None)
    in_specs = (up_spec, down_spec, up_spec, down_spec, up_spec, down_spec, P('data', 'stage', None, 'model'), P('data', 'stage', 'model', None), P('stage', 'data', None), P('data', None), row_spec, P(None), P(None))
    out_specs = (up_spec, down_spec, up_spec, down_spec, up_spec, down_spec, row_spec)
    any_spec = pl.BlockSpec(memory_space=pl.ANY)
    vmem_spec = pl.BlockSpec(memory_space=pltpu.VMEM)
    smem_spec = pl.BlockSpec(memory_space=pltpu.SMEM)
    dma = pltpu.SemaphoreType.DMA

    def device_step(w_up, w_down, m_up, m_down, v_up, v_down, g_up, g_down, acts_last, grad_out, x_next, learn_rate, max_norm):
        rows, width = grad_out.shape
        ff = w_up.shape[2]
        half = ff // 2
        nb = rows // BACK_ROWS
        hb = BACK_ROWS // 2
        sds = jax.ShapeDtypeStruct
        gbar_u, gbar_d, early, late, norm_tile = pl.pallas_call(
            functools.partial(bwd_kernel, dims),
            out_shape=(sds((width, half), F32), sds((half, width), F32), sds((EARLY_ROWS, width), F32), sds((LATE_ROWS, half), F32), sds((8, 128), F32)),
            in_specs=[any_spec] * 6,
            out_specs=(any_spec,) * 4 + (vmem_spec,),
            scratch_shapes=[
                pltpu.VMEM((width, ff), F32), pltpu.VMEM((ff, width), F32),
                pltpu.VMEM((width, ff), BF16), pltpu.VMEM((ff, width), BF16),
                pltpu.VMEM((2 * rows, width), BF16), pltpu.VMEM((2 * rows, width), BF16),
                pltpu.VMEM((rows, half), BF16), pltpu.VMEM((rows, half), BF16),
                pltpu.VMEM((rows, ff), F32), pltpu.VMEM((rows, half), F32),
                pltpu.VMEM((rows, ff), BF16), pltpu.VMEM((rows, ff), BF16),
            ] + [pltpu.VMEM((width, half), F32), pltpu.VMEM((half, width), F32)] * 3 + [
                pltpu.VMEM((nb, BACK_ROWS, width), F32), pltpu.VMEM((nb, hb, width), F32),
                pltpu.VMEM((nb, hb, width), BF16), pltpu.VMEM((n_all, 8, 128), F32),
                dma((8,)), dma((4,)), dma((4,)), dma((3,)), dma((3,)), dma((nb,)), dma((nb,)), dma((nb, 2)), dma((nb, 2)),
                dma((n_all,)), dma((n_all,)), dma((4,)),
            ],
            compiler_params=pltpu.CompilerParams(collective_id=0, has_side_effects=True, vmem_limit_bytes=VMEM_LIMIT),
            name='backward',
        )(w_up[0], w_down[0], acts_last[0], grad_out, g_up[0, 0], g_down[0, 0])

        early_oth = lax.ppermute(early, 'data', [(k, 1 - k) for k in range(n_data)])
        blocks = half // UPD_ROWS
        state = (w_up[0], w_down[0], m_up[0], m_down[0], v_up[0], v_down[0])
        state_shapes = tuple(sds(s.shape, F32) for s in state)
        which = lax.axis_index('data').astype(jnp.int32).reshape(1)

        def update_specs(pick):
            up = pl.BlockSpec((UPD_ROWS, half), lambda i, w: (i, pick(w[0])))
            down = pl.BlockSpec((UPD_ROWS, width), lambda i, w: (pick(w[0]) * blocks + i, 0))
            return [up, down]
        plain_up = pl.BlockSpec((UPD_ROWS, half), lambda i, w: (i, 0))
        plain_down = pl.BlockSpec((UPD_ROWS, width), lambda i, w: (i, 0))
        small = [smem_spec, smem_spec, pl.BlockSpec((8, 128), lambda i, w: (0, 0))]
        own = update_specs(lambda w: w)
        *fresh, b_up, b_down = pl.pallas_call(
            update_kernel,
            out_shape=state_shapes + (sds((width, half), BF16), sds((half, width), BF16)),
            grid_spec=pltpu.PrefetchScalarGridSpec(
                num_scalar_prefetch=1, grid=(width // UPD_ROWS,),
                in_specs=small + [plain_up, plain_down] + own * 3,
                out_specs=own * 3 + [plain_up, plain_down]),
            compiler_params=pltpu.CompilerParams(dimension_semantics=('arbitrary',), vmem_limit_bytes=VMEM_LIMIT),
            name='update_own',
        )(which, learn_rate, max_norm, norm_tile, gbar_u, gbar_d, *state)

        n_micro = x_next.shape[0]
        nc = n_micro * rows // FWD_ROWS
        fb = FWD_ROWS // 2
        gu_oth, gd_oth, y_next = pl.pallas_call(
            functools.partial(fwd_kernel, dims),
            out_shape=(sds((width - LATE_ROWS, half), F32), sds((half - EARLY_ROWS, width), F32), sds((nc, FWD_ROWS, width), BF16)),
            in_specs=[any_spec] * 5,
            out_specs=(any_spec, any_spec, any_spec),
            scratch_shapes=[pltpu.VMEM((width, ff), BF16), pltpu.VMEM((ff, width), BF16)] * 2 + [
                pltpu.VMEM((nc, FWD_ROWS, width), BF16), pltpu.VMEM((nc, FWD_ROWS, width), BF16),
                pltpu.VMEM((nc, FWD_ROWS, width), F32), pltpu.VMEM((nc, fb, width), F32),
                pltpu.VMEM((nc, fb, width), BF16),
                dma((3,)), dma((4,)), dma((4,)), dma((4,)), dma((4,)), dma((nc,)), dma((nc,)), dma((nc, 2)), dma((nc, 2)),
                dma((nc,)), dma((nc,)), dma((nc, n_stage)), dma((nc,)), pltpu.SemaphoreType.REGULAR,
            ],
            compiler_params=pltpu.CompilerParams(collective_id=1, has_side_effects=True, vmem_limit_bytes=VMEM_LIMIT),
            name='forward',
        )(b_up, b_down, gbar_u, gbar_d, x_next.reshape(nc, FWD_ROWS, width))

        other = update_specs(lambda w: 1 - w)
        gu_oth, late = lax.optimization_barrier((gu_oth, late))
        late_oth = lax.ppermute(late, 'data', [(k, 1 - k) for k in range(n_data)])
        y_next = y_next.reshape(n_micro * rows, width)
        nearly, nlate = EARLY_ROWS // UPD_ROWS, LATE_ROWS // UPD_ROWS
        steps = width // UPD_ROWS
        lastup = steps - nlate - 1

        def rows_spec(start, count):
            return pl.BlockSpec((UPD_ROWS, width), lambda i, w: (jnp.clip(i - start, 0, count - 1), 0))
        y_spec = pl.BlockSpec((n_micro * rows // steps, width), lambda i, w: (i, 0))
        up_oth = pl.BlockSpec((UPD_ROWS, half), lambda i, w: (jnp.minimum(i, lastup), 1 - w[0]))
        down_oth = pl.BlockSpec((UPD_ROWS, width), lambda i, w: ((1 - w[0]) * blocks + i, 0))
        other = [up_oth, down_oth]
        *filled, y_next = pl.pallas_call(
            fill_kernel,
            out_shape=state_shapes + (sds(y_next.shape, BF16),),
            grid_spec=pltpu.PrefetchScalarGridSpec(
                num_scalar_prefetch=1, grid=(steps,),
                in_specs=small + [rows_spec(0, lastup + 1), vmem_spec, rows_spec(nearly, blocks - nearly), y_spec] + other * 3 + [any_spec] * 6,
                out_specs=other * 3 + [y_spec]),
            input_output_aliases={14 + k: k for k in range(6)},
            compiler_params=pltpu.CompilerParams(dimension_semantics=('arbitrary',), vmem_limit_bytes=VMEM_LIMIT),
            cost_estimate=pl.CostEstimate(flops=10**10, bytes_accessed=40 * 10**6, transcendentals=0),
            name='update_other',
        )(which, learn_rate, max_norm, norm_tile, gu_oth, early_oth, gd_oth, y_next, *state, *fresh)
        up_late = pl.BlockSpec((UPD_ROWS, half), lambda i, w: (steps - nlate + i, 1 - w[0]))
        filled[0], filled[2], filled[4] = pl.pallas_call(
            late_kernel,
            out_shape=(state_shapes[0],) * 3,
            grid_spec=pltpu.PrefetchScalarGridSpec(
                num_scalar_prefetch=1, grid=(nlate,),
                in_specs=small + [plain_up] + [up_late] * 3 + [any_spec] * 3,
                out_specs=[up_late] * 3),
            input_output_aliases={8 + k: k for k in range(3)},
            compiler_params=pltpu.CompilerParams(dimension_semantics=('arbitrary',), vmem_limit_bytes=VMEM_LIMIT),
            name='update_late',
        )(which, learn_rate, max_norm, norm_tile, late_oth, state[0], state[2], state[4], filled[0], filled[2], filled[4])
        return tuple(s[None] for s in filled) + (y_next.reshape(n_micro, rows, width),)

    return jax.shard_map(device_step, mesh=mesh, in_specs=in_specs, out_specs=out_specs, check_vma=False)
```
